32 devices in a mesh: dp: 1 (over z), tp: 4 (over y), ep: 8 (over x, core).
Axes of the slice: x: 4, y: 4, z: 1, core: 2. Of those that a mesh axis runs over, the one named last changes fastest.
The devices are a block of a 4x4x8 slice.
Arguments:
- tokens: bfloat16 [8192, 1536], P(('dp', 'ep', 'tp'))
- expert_ids: int32 [8192, 8], P(('dp', 'ep', 'tp'))
- gate_vals: float32 [8192, 8], P(('dp', 'ep', 'tp'))
- w_one: bfloat16 [40, 1536, 512], P('ep', None, 'tp')
- w_three: bfloat16 [40, 1536, 512], P('ep', None, 'tp')
- w_two: bfloat16 [40, 512, 1536], P('ep', 'tp')
- d_out: bfloat16 [8192, 1536], P(('dp', 'ep', 'tp'))
Outputs:
- output 1: bfloat16 [8192, 1536], P(('dp', 'ep', 'tp'))
- output 2: bfloat16 [8192, 1536], P(('dp', 'ep', 'tp'))
- output 3: bfloat16 [40, 1536, 512], P(('dp', 'ep'), None, 'tp')
- output 4: bfloat16 [40, 1536, 512], P(('dp', 'ep'), None, 'tp')
- output 5: bfloat16 [40, 512, 1536], P(('dp', 'ep'), 'tp')
All inputs are finite; a program needn't handle non-finite values.
Results may differ from the reference program's by a relative error of at most 0.0104073.
Values are sent between devices in bfloat16 or wider.
A program may use at most 768 MiB of HBM per device.

```python
import math
import jax
import jax.numpy as jnp
from jax import lax

D = 1536
FF = 512
EXPERTS = 40
TOP = 8
TOK = 256
CAP = 64
BLOCKS = 32
TOKENS = TOK * BLOCKS


def draw_routes(route_key):
    score_key, hot_key = jax.random.split(route_key)
    score_span = 2 ** 20
    bonus_size = 2 ** 29
    scores = jax.random.randint(score_key, (BLOCKS, TOK, EXPERTS), 0, score_span, dtype=jnp.int32) * EXPERTS + jnp.arange(EXPERTS, dtype=jnp.int32)
    hot_ids = jax.random.randint(hot_key, (BLOCKS, 1, 1), 0, EXPERTS, dtype=jnp.int32)
    hot_rows = CAP + CAP // 16 + 1
    is_hot = jnp.arange(EXPERTS, dtype=jnp.int32)[None, None, :] == hot_ids
    lead_rows = (jnp.arange(TOK, dtype=jnp.int32) < hot_rows)[None, :, None]
    bonus = jnp.where(is_hot, jnp.where(lead_rows, bonus_size, -bonus_size), 0)
    chosen = lax.top_k(scores + bonus, TOP)[1]
    return chosen.astype(jnp.int32).reshape(BLOCKS * TOK, TOP)


def setup_inputs(seed: int = 0, part: int = 0) -> dict:
    base_key = jax.random.key(seed)
    key_one, key_three, key_two = jax.random.split(jax.random.fold_in(base_key, 1), 3)
    part_key = jax.random.fold_in(jax.random.fold_in(base_key, 2), part)
    key_tok, key_route, key_gate, key_grad = jax.random.split(part_key, 4)
    tokens = jax.random.normal(key_tok, (TOKENS, D), jnp.float32).astype(jnp.bfloat16)
    expert_ids = draw_routes(key_route)
    gate_vals = jax.random.uniform(key_gate, (TOKENS, TOP), jnp.float32, 0.5, 1.5) / math.sqrt(TOP)
    in_scale = D ** -0.5
    mid_scale = FF ** -0.5
    w_one = (jax.random.normal(key_one, (EXPERTS, D, FF), jnp.float32) * in_scale).astype(jnp.bfloat16)
    w_three = (jax.random.normal(key_three, (EXPERTS, D, FF), jnp.float32) * in_scale).astype(jnp.bfloat16)
    w_two = (jax.random.normal(key_two, (EXPERTS, FF, D), jnp.float32) * mid_scale).astype(jnp.bfloat16)
    d_out = jax.random.normal(key_grad, (TOKENS, D), jnp.float32).astype(jnp.bfloat16)
    return {"tokens": tokens, "expert_ids": expert_ids, "gate_vals": gate_vals, "w_one": w_one, "w_three": w_three, "w_two": w_two, "d_out": d_out}


def route_tables(block_ids):
    hit_mask = block_ids[:, :, None] == jnp.arange(EXPERTS, dtype=jnp.int32)
    per_row = jnp.sum(hit_mask, axis=1, dtype=jnp.int32)
    before = jnp.cumsum(per_row, axis=0) - per_row
    slot_pos = jnp.sum(jnp.where(hit_mask, before[:, None, :], 0), axis=2)
    copy_slot = jnp.where(slot_pos < CAP, block_ids * CAP + slot_pos, EXPERTS * CAP)
    slot_copy = jnp.full((EXPERTS * CAP,), TOK * TOP, jnp.int32)
    slot_copy = slot_copy.at[copy_slot.reshape(-1)].set(jnp.arange(TOK * TOP, dtype=jnp.int32), mode="drop")
    return slot_copy, copy_slot


def take_rows(source, index_list):
    return jnp.take(source, index_list, axis=0, mode="fill", fill_value=0)


def by_expert(slot_rows):
    return slot_rows.reshape(BLOCKS, EXPERTS, CAP, D).transpose(1, 0, 2, 3).reshape(EXPERTS, BLOCKS * CAP, D)


def by_block(expert_rows):
    return expert_rows.reshape(EXPERTS, BLOCKS, CAP, D).transpose(1, 0, 2, 3).reshape(BLOCKS, EXPERTS * CAP, D)


def expert_pass(operands):
    slot_in, slot_grad, w_a, w_b, w_c = operands
    act_one = jnp.dot(slot_in, w_a, preferred_element_type=jnp.float32)
    act_three = jnp.dot(slot_in, w_b, preferred_element_type=jnp.float32)
    sig_one = jax.nn.sigmoid(act_one)
    silu_one = act_one * sig_one
    hidden = (silu_one * act_three).astype(jnp.bfloat16)
    slot_out = jnp.dot(hidden, w_c, preferred_element_type=jnp.float32).astype(jnp.bfloat16)
    d_hidden = jnp.dot(slot_grad, w_c.T, preferred_element_type=jnp.float32)
    grad_c = jnp.dot(hidden.T, slot_grad, preferred_element_type=jnp.float32).astype(jnp.bfloat16)
    d_one = (d_hidden * act_three * sig_one * (1.0 + act_one * (1.0 - sig_one))).astype(jnp.bfloat16)
    d_three = (d_hidden * silu_one).astype(jnp.bfloat16)
    grad_a = jnp.dot(slot_in.T, d_one, preferred_element_type=jnp.float32).astype(jnp.bfloat16)
    grad_b = jnp.dot(slot_in.T, d_three, preferred_element_type=jnp.float32).astype(jnp.bfloat16)
    slot_dx = (jnp.dot(d_one, w_a.T, preferred_element_type=jnp.float32) + jnp.dot(d_three, w_b.T, preferred_element_type=jnp.float32)).astype(jnp.bfloat16)
    return slot_out, slot_dx, grad_a, grad_b, grad_c


def reference(tokens, expert_ids, gate_vals, w_one, w_three, w_two, d_out):
    slot_copy, copy_slot = jax.vmap(route_tables)(expert_ids.reshape(BLOCKS, TOK, TOP))
    gather_rows = jax.vmap(take_rows)
    slot_in = gather_rows(tokens.reshape(BLOCKS, TOK, D), slot_copy // TOP)
    grad_copies = (gate_vals[:, :, None] * d_out.astype(jnp.float32)[:, None, :]).astype(jnp.bfloat16)
    slot_grad = gather_rows(grad_copies.reshape(BLOCKS, TOK * TOP, D), slot_copy)
    slot_out, slot_dx, grad_one, grad_three, grad_two = lax.map(expert_pass, (by_expert(slot_in), by_expert(slot_grad), w_one, w_three, w_two))
    out_copies = gather_rows(by_block(slot_out), copy_slot)
    block_gates = gate_vals.reshape(BLOCKS, TOK, TOP)
    out_rows = jnp.sum(block_gates[:, :, :, None] * out_copies.astype(jnp.float32), axis=2).astype(jnp.bfloat16)
    dx_copies = gather_rows(by_block(slot_dx), copy_slot)
    dx_rows = jnp.sum(dx_copies.astype(jnp.float32), axis=2).astype(jnp.bfloat16)
    return out_rows.reshape(TOKENS, D), dx_rows.reshape(TOKENS, D), grad_one, grad_three, grad_two
```

```python
import functools

import jax
import jax.numpy as jnp
from jax import lax
from jax.experimental import pallas as pl
from jax.experimental.pallas import tpu as pltpu
from jax.sharding import PartitionSpec as P

BF16 = jnp.bfloat16
F32 = jnp.float32


def slot_count(num_top, tok_dev, experts):
    return 8 * ((5 * num_top * tok_dev + 32 * experts - 1) // (32 * experts))


def dot(a, b):
    return jnp.dot(a, b, preferred_element_type=F32)


def dot_tb(a, b):
    return lax.dot_general(a, b, (((1,), (1,)), ((), ())), preferred_element_type=F32)


def dot_ta(a, b):
    return lax.dot_general(a, b, (((0,), (0,)), ((), ())), preferred_element_type=F32)


def block_tables(expert_ids, gate_vals, experts, groups):
    rows = expert_ids.shape[0]
    hit = expert_ids[:, :, None] == jnp.arange(experts, dtype=jnp.int32)
    gate = jnp.sum(jnp.where(hit, gate_vals[:, :, None], 0.0), axis=1)
    routed = jnp.any(hit, axis=1)
    earlier = jnp.arange(rows)[None, :] < jnp.arange(rows)[:, None]
    before = dot(earlier.astype(BF16), routed.astype(BF16))
    pos = jnp.where(routed, before, -1.0)
    own = experts // groups
    table = jnp.stack([pos.T.reshape(groups, own, rows), gate.T.reshape(groups, own, rows)], axis=1)
    return table.reshape(groups * 2 * own, rows)


def hit_masks(table, own, cap):
    slot = lax.broadcasted_iota(jnp.int32, (cap, table.shape[1]), 0).astype(F32)
    return [table[e : e + 1, :] == slot for e in range(own)]


def one_hot(masks):
    return jnp.concatenate([jnp.where(m, 1.0, 0.0) for m in masks], axis=0).astype(BF16)


def slot_gates(masks, table, own):
    return jnp.concatenate([jnp.where(m, table[own + e : own + e + 1, :], 0.0) for e, m in enumerate(masks)], axis=0)


def three_parts(x):
    hi = x.astype(BF16)
    rest = x - hi.astype(F32)
    mid = rest.astype(BF16)
    return hi, mid, (rest - mid.astype(F32)).astype(BF16)


def wgrad_kernel(own, cap, width, tab, x, dy, w13, w2, g1, g3, g2, xs, us, acc13, acc2):
    step = pl.program_id(0)
    blocks = x.shape[1]

    @pl.when(step == 0)
    def _():
        acc13[...] = jnp.zeros_like(acc13)
        acc2[...] = jnp.zeros_like(acc2)

    def gather(b, carry):
        table = tab[0, b]
        masks = hit_masks(table, own, cap)
        pick = one_hot(masks)
        gates = jnp.sum(slot_gates(masks, table, own), axis=1, keepdims=True)
        rows = pl.ds(pl.multiple_of(b * cap, cap), cap)
        picked = dot(pick, x[0, b]).astype(BF16)
        for e in range(own):
            xs[e, rows, :] = picked[e * cap : (e + 1) * cap]
        scaled = (gates * dot(pick, dy[0, b])).astype(BF16)
        for e in range(own):
            us[e, rows, :] = scaled[e * cap : (e + 1) * cap]
        return carry

    lax.fori_loop(0, blocks, gather, 0)

    def expert(e, carry):
        ab = dot(xs[e], w13[e])
        a, b = ab[:, :width], ab[:, width:]
        dh = dot_tb(us[e], w2[e])
        sig = jax.nn.sigmoid(a)
        silu = a * sig
        h = (silu * b).astype(BF16)
        da = (dh * b * sig * (1.0 + a * (1.0 - sig))).astype(BF16)
        db = (dh * silu).astype(BF16)
        acc13[e] += dot_ta(jnp.concatenate([da, db], axis=1), xs[e])
        acc2[e] += dot_ta(h, us[e])
        return carry

    lax.fori_loop(0, own, expert, 0)

    @pl.when(step == pl.num_programs(0) - 1)
    def _():
        def finish(e, carry):
            g1[e] = acc13[e, :width, :].T.astype(BF16)
            g3[e] = acc13[e, width:, :].T.astype(BF16)
            g2[e] = acc2[e].astype(BF16)
            return carry

        lax.fori_loop(0, own, finish, 0)


def weight_grads(table, x_all, dy_all, w13, w2, cap):
    groups, blocks, tok, model = x_all.shape
    own, width = w2.shape[0], w2.shape[1]
    rows = blocks * cap
    whole = lambda *shape: pl.BlockSpec(shape, lambda s: (0,) * len(shape), pipeline_mode=pl.Buffered(1))
    col = jax.ShapeDtypeStruct((own, model, width), BF16)
    slot_rows = groups * rows * own
    return pl.pallas_call(
        functools.partial(wgrad_kernel, own, cap, width),
        grid=(groups,),
        in_specs=[
            pl.BlockSpec((1, blocks, 2 * own, tok), lambda s: (s, 0, 0, 0)),
            pl.BlockSpec((1, blocks, tok, model), lambda s: (s, 0, 0, 0)),
            pl.BlockSpec((1, blocks, tok, model), lambda s: (s, 0, 0, 0)),
            whole(own, model, 2 * width),
            whole(own, width, model),
        ],
        out_specs=[whole(own, model, width), whole(own, model, width), whole(own, width, model)],
        out_shape=[col, col, jax.ShapeDtypeStruct((own, width, model), BF16)],
        scratch_shapes=[
            pltpu.VMEM((own, rows, model), BF16),
            pltpu.VMEM((own, rows, model), BF16),
            pltpu.VMEM((own, 2 * width, model), F32),
            pltpu.VMEM((own, width, model), F32),
        ],
        compiler_params=pltpu.CompilerParams(vmem_limit_bytes=62 * 2**20),
        cost_estimate=pl.CostEstimate(
            flops=2 * slot_rows * model * (2 * tok + 6 * width),
            bytes_accessed=2 * 2 * groups * blocks * tok * model,
            transcendentals=0,
        ),
        name="weight_grads",
    )(table, x_all, dy_all, w13, w2)


def forward_kernel(own, cap, width, where, tab, x, w13, w2, y_out, ab_out, xs, ys):
    step = pl.program_id(0)
    blocks, shards = ys.shape[0], w13.shape[0]

    @pl.when(step < blocks)
    def _():
        pick = one_hot(hit_masks(tab[step, 0], own, cap))
        picked = dot(pick, x[0, 0]).astype(BF16)
        rows = pl.ds(pl.multiple_of(step * cap, cap), cap)
        for e in range(own):
            xs[e, rows, :] = picked[e * cap : (e + 1) * cap]

    @pl.when((step >= blocks) & (step < blocks + own))
    def _():
        e = step - blocks
        parts = []
        for j in range(shards):
            ab = dot(xs[e], w13[j, 0])
            ab_out[0, :, 2 * width * j : 2 * width * (j + 1)] = ab
            a, b = ab[:, :width], ab[:, width:]
            parts.append((a * jax.nn.sigmoid(a) * b).astype(BF16))
        h = jnp.concatenate(parts, axis=1)
        y = dot(h, w2[:, 0].reshape(shards * width, w2.shape[3])).astype(BF16)
        at = pl.ds(pl.multiple_of(e * cap, cap), cap)
        for k in range(blocks):
            ys[k, at, :] = y[k * cap : (k + 1) * cap]

    @pl.when(step >= blocks + own)
    def _():
        k = step - blocks - own
        table = tab[k, 0]
        hi, mid, low = three_parts(slot_gates(hit_masks(table, own, cap), table, own))
        rows = ys[k]
        y_out[0] = dot_ta(hi, rows) + (dot_ta(mid, rows) + dot_ta(low, rows))


def backward_kernel(own, cap, width, where, tab, dy, ab_in, w13, w2, dx_out, us, vs):
    step = pl.program_id(0)
    blocks, shards = vs.shape[0], w13.shape[0]

    @pl.when(step < blocks)
    def _():
        table = tab[step, 0]
        masks = hit_masks(table, own, cap)
        gates = jnp.sum(slot_gates(masks, table, own), axis=1, keepdims=True)
        scaled = (gates * dot(one_hot(masks), dy[0, 0])).astype(BF16)
        rows = pl.ds(pl.multiple_of(step * cap, cap), cap)
        for e in range(own):
            us[e, rows, :] = scaled[e * cap : (e + 1) * cap]

    @pl.when((step >= blocks) & (step < blocks + own))
    def _():
        e = step - blocks
        v = None
        for j in range(shards):
            dh = dot_tb(us[e], w2[j, 0])
            a = ab_in[0, :, 2 * width * j : 2 * width * j + width]
            b = ab_in[0, :, 2 * width * j + width : 2 * width * (j + 1)]
            sig = jax.nn.sigmoid(a)
            da = (dh * b * sig * (1.0 + a * (1.0 - sig))).astype(BF16)
            db = (dh * (a * sig)).astype(BF16)
            part = dot_tb(jnp.concatenate([da, db], axis=1), w13[j, 0])
            v = part if v is None else v + part
        v = v.astype(BF16)
        at = pl.ds(pl.multiple_of(e * cap, cap), cap)
        for k in range(blocks):
            vs[k, at, :] = v[k * cap : (k + 1) * cap]

    @pl.when(step >= blocks + own)
    def _():
        k = step - blocks - own
        pick = one_hot(hit_masks(tab[k, 0], own, cap))
        dx_out[0] = dot_ta(pick, vs[k])


def token_specs(blocks, own, tok, model, width, shards):
    gather = lambda s, w: (jnp.minimum(s, blocks - 1), w[0], 0, 0)
    expert = lambda s: jnp.clip(s - blocks, 0, own - 1)
    return dict(
        tab=pl.BlockSpec((blocks, 1, 2 * own, tok), lambda s, w: (0, w[0], 0, 0)),
        rows=pl.BlockSpec((1, 1, tok, model), gather),
        w13=pl.BlockSpec((shards, 1, model, 2 * width), lambda s, w: (0, expert(s), 0, 0)),
        w2=pl.BlockSpec((shards, 1, width, model), lambda s, w: (0, expert(s), 0, 0)),
        out=pl.BlockSpec((1, tok, model), lambda s, w: (jnp.clip(s - blocks - own, 0, blocks - 1), 0, 0)),
        act=lambda rows: pl.BlockSpec((1, rows, 2 * width * shards), lambda s, w: (expert(s), 0, 0)),
    )


def forward_rows(where, table, x_all, w13_all, w2_all, cap):
    blocks, _, tok, model = x_all.shape
    shards, own, width, _ = w2_all.shape
    rows = blocks * cap
    specs = token_specs(blocks, own, tok, model, width, shards)
    return pl.pallas_call(
        functools.partial(forward_kernel, own, cap, width),
        grid_spec=pltpu.PrefetchScalarGridSpec(
            num_scalar_prefetch=1,
            grid=(2 * blocks + own,),
            in_specs=[specs["tab"], specs["rows"], specs["w13"], specs["w2"]],
            out_specs=[specs["out"], specs["act"](rows)],
            scratch_shapes=[pltpu.VMEM((own, rows, model), BF16), pltpu.VMEM((blocks, own * cap, model), BF16)],
        ),
        out_shape=[
            jax.ShapeDtypeStruct((blocks, tok, model), F32),
            jax.ShapeDtypeStruct((own, rows, 2 * width * shards), F32),
        ],
        compiler_params=pltpu.CompilerParams(vmem_limit_bytes=62 * 2**20),
        cost_estimate=pl.CostEstimate(
            flops=2 * own * rows * model * (4 * tok + 3 * width * shards),
            bytes_accessed=2 * own * 3 * model * width * shards,
            transcendentals=0,
        ),
        name="forward_rows",
    )(where, table, x_all, w13_all, w2_all)


def backward_rows(where, table, dy_all, ab, w13_all, w2_all, cap):
    blocks, _, tok, model = dy_all.shape
    shards, own, width, _ = w2_all.shape
    rows = blocks * cap
    specs = token_specs(blocks, own, tok, model, width, shards)
    return pl.pallas_call(
        functools.partial(backward_kernel, own, cap, width),
        grid_spec=pltpu.PrefetchScalarGridSpec(
            num_scalar_prefetch=1,
            grid=(2 * blocks + own,),
            in_specs=[specs["tab"], specs["rows"], specs["act"](rows), specs["w13"], specs["w2"]],
            out_specs=specs["out"],
            scratch_shapes=[pltpu.VMEM((own, rows, model), BF16), pltpu.VMEM((blocks, own * cap, model), BF16)],
        ),
        out_shape=jax.ShapeDtypeStruct((blocks, tok, model), F32),
        compiler_params=pltpu.CompilerParams(vmem_limit_bytes=62 * 2**20),
        cost_estimate=pl.CostEstimate(
            flops=2 * own * rows * model * (2 * tok + 3 * width * shards),
            bytes_accessed=2 * own * 3 * model * width * shards,
            transcendentals=0,
        ),
        name="backward_rows",
    )(where, table, dy_all, ab, w13_all, w2_all)


def solution(mesh):
    ep_size, tp_size = mesh.shape["ep"], mesh.shape["tp"]
    row_spec = P(("dp", "ep", "tp"), None)
    col_spec = P("ep", None, "tp")
    down_spec = P("ep", "tp", None)
    grad_col = P(("dp", "ep"), None, "tp")
    grad_down = P(("dp", "ep"), "tp", None)

    def local_step(tokens, expert_ids, gate_vals, w_one, w_three, w_two, d_out):
        tok, model = tokens.shape
        own = w_one.shape[0]
        experts = own * ep_size
        cap = slot_count(expert_ids.shape[1], tok, experts)

        def everyone(rows):
            full = lax.all_gather(rows, ("ep", "tp"), axis=0, tiled=True)
            return full.reshape(ep_size, tp_size, rows.shape[0], rows.shape[1])

        w13 = jnp.concatenate([w_one, w_three], axis=2)
        w2_all = lax.all_gather(w_two, "tp", axis=0)
        w13_all = lax.all_gather(w13, "tp", axis=0)

        table = block_tables(expert_ids, gate_vals, experts, ep_size)
        table, w2_all = lax.optimization_barrier((table, w2_all))
        table = everyone(table)
        ep = lax.axis_index("ep")
        table = lax.dynamic_slice_in_dim(table, ep * 2 * own, 2 * own, axis=2)
        where = lax.axis_index("tp").astype(jnp.int32).reshape(1)
        x_all = everyone(tokens)
        dy_all = everyone(d_out)

        y_part, ab = forward_rows(where, table, x_all, w13_all, w2_all, cap)
        out = lax.psum_scatter(y_part, "ep", scatter_dimension=0, tiled=False).astype(BF16)
        dx_part = backward_rows(where, table, dy_all, ab, w13_all, w2_all, cap)
        dx = lax.psum_scatter(dx_part, "ep", scatter_dimension=0, tiled=False).astype(BF16)
        grad_one, grad_three, grad_two = weight_grads(table, x_all, dy_all, w13, w_two, cap)
        return out, dx, grad_one, grad_three, grad_two

    return jax.shard_map(local_step, mesh=mesh,
                         in_specs=(row_spec, row_spec, row_spec, col_spec, col_spec, down_spec, row_spec),
                         out_specs=(row_spec, row_spec, grad_col, grad_col, grad_down), check_vma=False)
```

```python
import functools

import jax
import jax.numpy as jnp
from jax import lax
from jax.experimental import pallas as pl
from jax.experimental.pallas import tpu as pltpu
from jax.sharding import PartitionSpec as P

BF16 = jnp.bfloat16
F32 = jnp.float32
MESH = pl.DeviceIdType.MESH
VMEM_LIMIT = 62 * 2**20


def slot_count(num_top, tok_dev, experts):
    return 8 * ((5 * num_top * tok_dev + 32 * experts - 1) // (32 * experts))


def dot(a, b):
    return jnp.dot(a, b, preferred_element_type=F32)


def dot_tb(a, b):
    return lax.dot_general(a, b, (((1,), (1,)), ((), ())), preferred_element_type=F32)


def dot_ta(a, b):
    return lax.dot_general(a, b, (((0,), (0,)), ((), ())), preferred_element_type=F32)


def earlier_rows(tok):
    row = lax.broadcasted_iota(jnp.int32, (tok, tok), 0)
    col = lax.broadcasted_iota(jnp.int32, (tok, tok), 1)
    return jnp.where(row < col, 1.0, 0.0).astype(BF16)


def expert_rows(routes, first, own, earlier):
    top = routes.shape[0] // 2
    ids, gates = routes[:top], routes[top:]
    hits = [ids == (first + e).astype(F32) for e in range(own)]
    routed = jnp.concatenate([jnp.sum(jnp.where(m, 1.0, 0.0), axis=0, keepdims=True) for m in hits], axis=0)
    gate = jnp.concatenate([jnp.sum(jnp.where(m, gates, 0.0), axis=0, keepdims=True) for m in hits], axis=0)
    return jnp.where(routed > 0.0, dot(routed.astype(BF16), earlier), -1.0), gate


def hit_masks(pos, cap):
    slot = lax.broadcasted_iota(jnp.int32, (cap, pos.shape[1]), 0).astype(F32)
    return [pos[e : e + 1, :] == slot for e in range(pos.shape[0])]


def one_hot(masks):
    return jnp.concatenate([jnp.where(m, 1.0, 0.0) for m in masks], axis=0).astype(BF16)


def slot_gates(masks, gate):
    return jnp.concatenate([jnp.where(m, gate[e : e + 1, :], 0.0) for e, m in enumerate(masks)], axis=0)


def three_parts(x):
    hi = x.astype(BF16)
    rest = x - hi.astype(F32)
    mid = rest.astype(BF16)
    return hi, mid, (rest - mid.astype(F32)).astype(BF16)


class Links:
    def __init__(self, send_sem, recv_sem):
        self.send_sem, self.recv_sem, self.sent = send_sem, recv_sem, []

    def copy(self, k, src, dst, to):
        return pltpu.make_async_remote_copy(src_ref=src, dst_ref=dst, send_sem=self.send_sem.at[k],
                                            recv_sem=self.recv_sem.at[k], device_id=to, device_id_type=MESH)

    def send(self, src, dst, to):
        k = len(self.sent)
        copy = self.copy(k, src, dst, to)
        copy.start()
        self.sent.append(copy)
        return k

    def arrive(self, k, dst, to):
        self.copy(k, dst, dst, to).wait_recv()

    def drain(self):
        for copy in self.sent:
            copy.wait_send()


def copy_count(own):
    return 9 + 21 * 4 + 7 * own


def gather_kernel(own, cap, width, x_own, dy_own, r_own, w1, w3, w2, x_all, dy_all, r_all, w13_all, w2_all, g1, g3, g2,
                  w13, w2s, xb, dyb, rb, earlier, xs, us, acc13, acc2, send_sem, recv_sem, row_sem, load_sem, w_sem):
    ep, tp = lax.axis_index("ep"), lax.axis_index("tp")
    eps, tps = x_all.shape[0], x_all.shape[1]
    model = x_all.shape[3]
    half = eps // 2
    step = lambda n: lax.rem(ep + (n + eps), eps)
    turn = lambda n: lax.rem(tp + (n + tps), tps)
    right, left, far = step(2), step(-2), step(4)
    mate = ep + 1 - 2 * lax.rem(ep, 2)
    mate_step = lambda n: lax.rem(mate + (n + eps), eps)
    up, down, over = turn(1), turn(-1), turn(2)
    to_right, to_left, to_mate = {"ep": right}, {"ep": left}, {"ep": mate}
    to_up, to_down = {"tp": up}, {"tp": down}
    links = Links(send_sem, recv_sem)

    loads = [pltpu.make_async_copy(w1, w13.at[:, :, pl.ds(0, width)], w_sem.at[0]),
             pltpu.make_async_copy(w3, w13.at[:, :, pl.ds(width, width)], w_sem.at[1]),
             pltpu.make_async_copy(w2, w2s, w_sem.at[2])]
    for copy in loads:
        copy.start()

    barrier = pltpu.get_barrier_semaphore()
    for to in (to_right, to_left, to_mate, to_up, to_down):
        pl.semaphore_signal(barrier, inc=1, device_id=to, device_id_type=MESH)
    pl.semaphore_wait(barrier, 5)

    own_refs, all_refs = (x_own, dy_own, r_own), (x_all, dy_all, r_all)
    upward = (True, False, True)

    def both_ways(kind, src, dst, plus, minus):
        return links.send(src, dst, plus), links.send(src, dst, minus)

    def spread(kinds, t, srcs):
        out = {}
        for kind in kinds:
            dst = all_refs[kind].at[ep, t]
            first, second = (to_right, to_left) if upward[kind] else (to_left, to_right)
            out[kind, upward[kind]] = links.send(srcs[kind], dst, first)
        for kind in kinds:
            dst = all_refs[kind].at[ep, t]
            second = to_left if upward[kind] else to_right
            out[kind, not upward[kind]] = links.send(srcs[kind], dst, second)
        for kind in kinds:
            out[kind, "mate"] = links.send(srcs[kind], all_refs[kind].at[ep, t], to_mate)
        return out

    def pass_on(state, kind, t):
        got, to = (left, to_right) if upward[kind] else (right, to_left)
        block = all_refs[kind].at[got, t]
        links.arrive(state[kind, upward[kind]], block, to)
        state[kind, "far"] = links.send(block, block, to)
        state[kind, "mate1"] = links.send(block, block, to_mate)

    def share(state, kind, t):
        got, to = (right, to_left) if upward[kind] else (left, to_right)
        block = all_refs[kind].at[got, t]
        links.arrive(state[kind, not upward[kind]], block, to)
        state[kind, "mate2"] = links.send(block, block, to_mate)

    def last(state, kind, t):
        block = all_refs[kind].at[far, t]
        links.arrive(state[kind, "far"], block, to_right if upward[kind] else to_left)
        state[kind, "mate3"] = links.send(block, block, to_mate)

    def from_mate(state, t):
        for kind in range(3):
            one, two = (mate_step(-2), mate_step(2)) if upward[kind] else (mate_step(2), mate_step(-2))
            for name, at in (("mate", mate), ("mate1", one), ("mate2", two), ("mate3", mate_step(4))):
                links.arrive(state[kind, name], all_refs[kind].at[at, t], to_mate)

    kinds = (0, 2, 1)

    y_state = {}
    for kind in kinds:
        first = to_up if upward[kind] else to_down
        y_state[kind, upward[kind]] = links.send(own_refs[kind], all_refs[kind].at[ep, tp], first)
    for kind in kinds:
        second = to_down if upward[kind] else to_up
        y_state[kind, not upward[kind]] = links.send(own_refs[kind], all_refs[kind].at[ep, tp], second)
    groups = (tp, down, up, over)
    states = [spread(kinds, tp, own_refs)]
    keep = [pltpu.make_async_copy(own_refs[kind], all_refs[kind].at[ep, tp], row_sem.at[kind]) for kind in range(3)]
    for copy in keep:
        copy.start()
    for copy in loads:
        copy.wait()
    stow = [pltpu.make_async_copy(w13, w13_all.at[tp], w_sem.at[0]), pltpu.make_async_copy(w2s, w2_all.at[tp], w_sem.at[1])]
    for copy in stow:
        copy.start()

    earlier[...] = earlier_rows(earlier.shape[0])
    acc13[...] = jnp.zeros_like(acc13)
    acc2[...] = jnp.zeros_like(acc2)

    cut = 3 * model // 4
    w_state = [None] * own

    def send_weights(e):
        w_state[e] = {(k, s): links.send(ref.at[e], dst.at[tp, e], to)
                      for k, ref, dst in ((0, w13, w13_all), (1, w2s, w2_all)) for s, to in ((True, to_up), (False, to_down))}

    def pass_weights(e):
        state = w_state[e]
        links.arrive(state[0, True], w13_all.at[down, e], to_up)
        head = w13_all.at[down, e, pl.ds(0, cut)]
        state["head"] = links.send(head, head, to_up)
        links.arrive(state[0, False], w13_all.at[up, e], to_down)
        tail = w13_all.at[up, e, pl.ds(cut, model - cut)]
        state["tail"] = links.send(tail, tail, to_down)
        links.arrive(state[1, False], w2_all.at[up, e], to_down)
        state["w2"] = links.send(w2_all.at[up, e], w2_all.at[up, e], to_down)
        links.arrive(state[1, True], w2_all.at[down, e], to_up)

    def have_weights(e):
        state = w_state[e]
        links.arrive(state["head"], w13_all.at[over, e, pl.ds(0, cut)], to_up)
        links.arrive(state["tail"], w13_all.at[over, e, pl.ds(cut, model - cut)], to_down)
        links.arrive(state["w2"], w2_all.at[over, e], to_down)

    def block_loads(t, h):
        at = pl.ds(h * half, half)
        return [pltpu.make_async_copy(src.at[at, t], dst.at[h], load_sem.at[k, h])
                for k, (src, dst) in enumerate(((x_all, xb), (dy_all, dyb), (r_all, rb)))]

    def compute(t):
        for h in range(2):
            for copy in block_loads(t, h):
                copy.start()

        def half_group(h, carry):
            for copy in block_loads(t, h):
                copy.wait()

            def gather(b, carry):
                pos, gate = expert_rows(rb[h, b], ep * own, own, earlier[...])
                masks = hit_masks(pos, cap)
                pick = one_hot(masks)
                gates = jnp.sum(slot_gates(masks, gate), axis=1, keepdims=True)
                rows = pl.ds(pl.multiple_of(b * cap, cap), cap)
                picked = dot(pick, xb[h, b]).astype(BF16)
                for e in range(own):
                    xs[e, rows, :] = picked[e * cap : (e + 1) * cap]
                scaled = (gates * dot(pick, dyb[h, b])).astype(BF16)
                for e in range(own):
                    us[e, rows, :] = scaled[e * cap : (e + 1) * cap]
                return carry

            lax.fori_loop(0, half, gather, 0)

            def expert(e, carry):
                ab = dot(xs[e], w13[e])
                a, b = ab[:, :width], ab[:, width:]
                dh = dot_tb(us[e], w2s[e])
                sig = jax.nn.sigmoid(a)
                silu = a * sig
                h = (silu * b).astype(BF16)
                da = (dh * b * sig * (1.0 + a * (1.0 - sig))).astype(BF16)
                db = (dh * silu).astype(BF16)
                acc13[e] += dot_ta(jnp.concatenate([da, db], axis=1), xs[e])
                acc2[e] += dot_ta(h, us[e])
                return carry

            lax.fori_loop(0, own, expert, 0)
            return carry

        lax.fori_loop(0, 2, half_group, 0)

    def arrivals(g, kinds, what):
        for kind in kinds:
            what(states[g], kind, groups[g])

    def y_arrive(kind, way):
        block = all_refs[kind].at[ep, down if way else up]
        links.arrive(y_state[kind, way], block, to_up if way else to_down)
        return block

    for kind in kinds:
        block = y_arrive(kind, upward[kind])
        y_state[kind, "far"] = links.send(block, block, to_up if upward[kind] else to_down)
    arrivals(0, kinds, pass_on)
    for kind in kinds:
        y_arrive(kind, not upward[kind])
    send_weights(0)
    send_weights(1)
    for g in (1, 2):
        states.append(spread(kinds, groups[g], [ref.at[ep, groups[g]] for ref in all_refs]))
    arrivals(0, kinds, share)
    arrivals(0, kinds, last)
    for kind in kinds:
        links.arrive(y_state[kind, "far"], all_refs[kind].at[ep, over], to_up if upward[kind] else to_down)
    for copy in keep:
        copy.wait()
    from_mate(states[0], groups[0])
    compute(groups[0])

    arrivals(1, kinds, pass_on)
    states.append(spread(kinds, over, [ref.at[ep, over] for ref in all_refs]))
    pass_weights(0)
    send_weights(2)
    arrivals(1, kinds, share)
    arrivals(2, kinds, pass_on)
    pass_weights(1)
    send_weights(3)
    arrivals(2, kinds, share)
    arrivals(1, kinds, last)
    from_mate(states[1], groups[1])
    compute(groups[1])

    arrivals(3, kinds, pass_on)
    pass_weights(2)
    send_weights(4)
    arrivals(3, kinds, share)
    arrivals(2, kinds, last)
    pass_weights(3)
    from_mate(states[2], groups[2])
    compute(groups[2])

    arrivals(3, kinds, last)
    pass_weights(4)
    from_mate(states[3], groups[3])
    compute(groups[3])

    def finish(e, carry):
        g1[e] = acc13[e, :width, :].T.astype(BF16)
        g3[e] = acc13[e, width:, :].T.astype(BF16)
        g2[e] = acc2[e].astype(BF16)
        return carry

    lax.fori_loop(0, own, finish, 0)
    for e in range(own):
        have_weights(e)
    for copy in stow:
        copy.wait()
    links.drain()


def gather_and_wgrad(tokens, d_out, routes, w_one, w_three, w_two, ep_size, tp_size, cap):
    tok, model = tokens.shape
    own, width, _ = w_two.shape
    half = ep_size // 2
    rows = half * cap
    vmem, hbm = pl.BlockSpec(memory_space=pltpu.VMEM), pl.BlockSpec(memory_space=pl.ANY)
    shape = jax.ShapeDtypeStruct
    copies = copy_count(own)
    slot_rows = ep_size * tp_size * cap * own
    return pl.pallas_call(
        functools.partial(gather_kernel, own, cap, width),
        in_specs=[vmem, vmem, vmem, hbm, hbm, hbm],
        out_specs=[hbm] * 5 + [vmem] * 3,
        out_shape=[
            shape((ep_size, tp_size, tok, model), BF16),
            shape((ep_size, tp_size, tok, model), BF16),
            shape((ep_size, tp_size) + routes.shape, F32),
            shape((tp_size, own, model, 2 * width), BF16),
            shape((tp_size, own, width, model), BF16),
            shape((own, model, width), BF16),
            shape((own, model, width), BF16),
            shape((own, width, model), BF16),
        ],
        scratch_shapes=[
            pltpu.VMEM((own, model, 2 * width), BF16),
            pltpu.VMEM((own, width, model), BF16),
            pltpu.VMEM((2, half, tok, model), BF16),
            pltpu.VMEM((2, half, tok, model), BF16),
            pltpu.VMEM((2, half) + routes.shape, F32),
            pltpu.VMEM((tok, tok), BF16),
            pltpu.VMEM((own, rows, model), BF16),
            pltpu.VMEM((own, rows, model), BF16),
            pltpu.VMEM((own, 2 * width, model), F32),
            pltpu.VMEM((own, width, model), F32),
            pltpu.SemaphoreType.DMA((copies,)),
            pltpu.SemaphoreType.DMA((copies,)),
            pltpu.SemaphoreType.DMA((3,)),
            pltpu.SemaphoreType.DMA((3, 2)),
            pltpu.SemaphoreType.DMA((3,)),
        ],
        compiler_params=pltpu.CompilerParams(vmem_limit_bytes=VMEM_LIMIT, collective_id=0, has_side_effects=True),
        cost_estimate=pl.CostEstimate(
            flops=2 * slot_rows * model * (2 * tok + 6 * width),
            bytes_accessed=4 * ep_size * tp_size * tok * model,
            transcendentals=0,
        ),
        name="gather_and_wgrad",
    )(tokens, d_out, routes, w_one, w_three, w_two)


def forward_kernel(own, cap, width, where, routes, x, w13, w2, y_out, ab_out, earlier, xs, ys):
    step = pl.program_id(0)
    blocks, shards = ys.shape[0], w13.shape[0]
    first = where[1] * own

    @pl.when(step == 0)
    def _():
        earlier[...] = earlier_rows(earlier.shape[0])

    @pl.when(step < blocks)
    def _():
        pos, _ = expert_rows(routes[step, 0], first, own, earlier[...])
        picked = dot(one_hot(hit_masks(pos, cap)), x[0, 0]).astype(BF16)
        rows = pl.ds(pl.multiple_of(step * cap, cap), cap)
        for e in range(own):
            xs[e, rows, :] = picked[e * cap : (e + 1) * cap]

    @pl.when((step >= blocks) & (step < blocks + own))
    def _():
        e = step - blocks
        parts = []
        for j in range(shards):
            ab = dot(xs[e], w13[j, 0])
            ab_out[0, :, 2 * width * j : 2 * width * (j + 1)] = ab
            a, b = ab[:, :width], ab[:, width:]
            parts.append((a * jax.nn.sigmoid(a) * b).astype(BF16))
        h = jnp.concatenate(parts, axis=1)
        y = dot(h, w2[:, 0].reshape(shards * width, w2.shape[3])).astype(BF16)
        at = pl.ds(pl.multiple_of(e * cap, cap), cap)
        for k in range(blocks):
            ys[k, at, :] = y[k * cap : (k + 1) * cap]

    @pl.when(step >= blocks + own)
    def _():
        k = step - blocks - own
        pos, gate = expert_rows(routes[k, 0], first, own, earlier[...])
        hi, mid, low = three_parts(slot_gates(hit_masks(pos, cap), gate))
        rows = ys[k]
        y_out[0] = dot_ta(hi, rows) + (dot_ta(mid, rows) + dot_ta(low, rows))


def backward_kernel(own, cap, width, where, routes, dy, ab_in, w13, w2, dx_out, earlier, us, vs):
    step = pl.program_id(0)
    blocks, shards = vs.shape[0], w13.shape[0]
    first = where[1] * own

    @pl.when(step == 0)
    def _():
        earlier[...] = earlier_rows(earlier.shape[0])

    @pl.when(step < blocks)
    def _():
        pos, gate = expert_rows(routes[step, 0], first, own, earlier[...])
        masks = hit_masks(pos, cap)
        gates = jnp.sum(slot_gates(masks, gate), axis=1, keepdims=True)
        scaled = (gates * dot(one_hot(masks), dy[0, 0])).astype(BF16)
        rows = pl.ds(pl.multiple_of(step * cap, cap), cap)
        for e in range(own):
            us[e, rows, :] = scaled[e * cap : (e + 1) * cap]

    @pl.when((step >= blocks) & (step < blocks + own))
    def _():
        e = step - blocks
        v = None
        for j in range(shards):
            dh = dot_tb(us[e], w2[j, 0])
            a = ab_in[0, :, 2 * width * j : 2 * width * j + width]
            b = ab_in[0, :, 2 * width * j + width : 2 * width * (j + 1)]
            sig = jax.nn.sigmoid(a)
            da = (dh * b * sig * (1.0 + a * (1.0 - sig))).astype(BF16)
            db = (dh * (a * sig)).astype(BF16)
            part = dot_tb(jnp.concatenate([da, db], axis=1), w13[j, 0])
            v = part if v is None else v + part
        v = v.astype(BF16)
        at = pl.ds(pl.multiple_of(e * cap, cap), cap)
        for k in range(blocks):
            vs[k, at, :] = v[k * cap : (k + 1) * cap]

    @pl.when(step >= blocks + own)
    def _():
        k = step - blocks - own
        pos, _ = expert_rows(routes[k, 0], first, own, earlier[...])
        dx_out[0] = dot_ta(one_hot(hit_masks(pos, cap)), vs[k])


def token_specs(blocks, own, tok, model, width, shards, routes):
    expert = lambda s: jnp.clip(s - blocks, 0, own - 1)
    return dict(
        routes=pl.BlockSpec((blocks, 1, routes, tok), lambda s, w: (0, w[0], 0, 0)),
        rows=pl.BlockSpec((1, 1, tok, model), lambda s, w: (jnp.minimum(s, blocks - 1), w[0], 0, 0)),
        w13=pl.BlockSpec((shards, 1, model, 2 * width), lambda s, w: (0, expert(s), 0, 0)),
        w2=pl.BlockSpec((shards, 1, width, model), lambda s, w: (0, expert(s), 0, 0)),
        out=pl.BlockSpec((1, tok, model), lambda s, w: (jnp.clip(s - blocks - own, 0, blocks - 1), 0, 0)),
        act=lambda rows: pl.BlockSpec((1, rows, 2 * width * shards), lambda s, w: (expert(s), 0, 0)),
    )


def forward_rows(where, routes, x_all, w13_all, w2_all, cap):
    blocks, _, tok, model = x_all.shape
    shards, own, width, _ = w2_all.shape
    rows = blocks * cap
    specs = token_specs(blocks, own, tok, model, width, shards, routes.shape[2])
    return pl.pallas_call(
        functools.partial(forward_kernel, own, cap, width),
        grid_spec=pltpu.PrefetchScalarGridSpec(
            num_scalar_prefetch=1,
            grid=(2 * blocks + own,),
            in_specs=[specs["routes"], specs["rows"], specs["w13"], specs["w2"]],
            out_specs=[specs["out"], specs["act"](rows)],
            scratch_shapes=[pltpu.VMEM((tok, tok), BF16), pltpu.VMEM((own, rows, model), BF16),
                            pltpu.VMEM((blocks, own * cap, model), BF16)],
        ),
        out_shape=[
            jax.ShapeDtypeStruct((blocks, tok, model), F32),
            jax.ShapeDtypeStruct((own, rows, 2 * width * shards), F32),
        ],
        compiler_params=pltpu.CompilerParams(vmem_limit_bytes=VMEM_LIMIT),
        cost_estimate=pl.CostEstimate(
            flops=2 * own * rows * model * (4 * tok + 3 * width * shards),
            bytes_accessed=2 * own * 3 * model * width * shards,
            transcendentals=0,
        ),
        name="forward_rows",
    )(where, routes, x_all, w13_all, w2_all)


def backward_rows(where, routes, dy_all, ab, w13_all, w2_all, cap):
    blocks, _, tok, model = dy_all.shape
    shards, own, width, _ = w2_all.shape
    rows = blocks * cap
    specs = token_specs(blocks, own, tok, model, width, shards, routes.shape[2])
    return pl.pallas_call(
        functools.partial(backward_kernel, own, cap, width),
        grid_spec=pltpu.PrefetchScalarGridSpec(
            num_scalar_prefetch=1,
            grid=(2 * blocks + own,),
            in_specs=[specs["routes"], specs["rows"], specs["act"](rows), specs["w13"], specs["w2"]],
            out_specs=specs["out"],
            scratch_shapes=[pltpu.VMEM((tok, tok), BF16), pltpu.VMEM((own, rows, model), BF16),
                            pltpu.VMEM((blocks, own * cap, model), BF16)],
        ),
        out_shape=jax.ShapeDtypeStruct((blocks, tok, model), F32),
        compiler_params=pltpu.CompilerParams(vmem_limit_bytes=VMEM_LIMIT),
        cost_estimate=pl.CostEstimate(
            flops=2 * own * rows * model * (2 * tok + 3 * width * shards),
            bytes_accessed=2 * own * 3 * model * width * shards,
            transcendentals=0,
        ),
        name="backward_rows",
    )(where, routes, dy_all, ab, w13_all, w2_all)


def solution(mesh):
    ep_size, tp_size = mesh.shape["ep"], mesh.shape["tp"]
    row_spec = P(("dp", "ep", "tp"), None)
    col_spec = P("ep", None, "tp")
    down_spec = P("ep", "tp", None)
    grad_col = P(("dp", "ep"), None, "tp")
    grad_down = P(("dp", "ep"), "tp", None)

    def local_step(tokens, expert_ids, gate_vals, w_one, w_three, w_two, d_out):
        cap = slot_count(expert_ids.shape[1], tokens.shape[0], w_one.shape[0] * ep_size)
        routes = jnp.concatenate([expert_ids.T.astype(F32), gate_vals.T], axis=0)
        where = jnp.stack([lax.axis_index("tp"), lax.axis_index("ep")]).astype(jnp.int32)

        x_all, dy_all, r_all, w13_all, w2_all, grad_one, grad_three, grad_two = gather_and_wgrad(
            tokens, d_out, routes, w_one, w_three, w_two, ep_size, tp_size, cap)
        y_part, ab = forward_rows(where, r_all, x_all, w13_all, w2_all, cap)
        out = lax.psum_scatter(y_part, "ep", scatter_dimension=0, tiled=False).astype(BF16)
        dx_part = backward_rows(where, r_all, dy_all, ab, w13_all, w2_all, cap)
        dx = lax.psum_scatter(dx_part, "ep", scatter_dimension=0, tiled=False).astype(BF16)
        return out, dx, grad_one, grad_three, grad_two

    return jax.shard_map(local_step, mesh=mesh,
                         in_specs=(row_spec, row_spec, row_spec, col_spec, col_spec, down_spec, row_spec),
                         out_specs=(row_spec, row_spec, grad_col, grad_col, grad_down), check_vma=False)
```

```python
import functools

import jax
import jax.numpy as jnp
from jax import lax
from jax.experimental import pallas as pl
from jax.experimental.pallas import tpu as pltpu
from jax.sharding import PartitionSpec as P

BF16 = jnp.bfloat16
F32 = jnp.float32
MESH = pl.DeviceIdType.MESH
VMEM_LIMIT = 62 * 2**20


def slot_count(num_top, tok_dev, experts):
    return 8 * ((5 * num_top * tok_dev + 32 * experts - 1) // (32 * experts))


def dot(a, b):
    return jnp.dot(a, b, preferred_element_type=F32)


def dot_tb(a, b):
    return lax.dot_general(a, b, (((1,), (1,)), ((), ())), preferred_element_type=F32)


def dot_ta(a, b):
    return lax.dot_general(a, b, (((0,), (0,)), ((), ())), preferred_element_type=F32)


def earlier_rows(tok):
    row = lax.broadcasted_iota(jnp.int32, (tok, tok), 0)
    col = lax.broadcasted_iota(jnp.int32, (tok, tok), 1)
    return jnp.where(row < col, 1.0, 0.0).astype(BF16)


def expert_rows(routes, first, own, earlier):
    top = routes.shape[0] // 2
    ids, gates = routes[:top], routes[top:]
    hits = [ids == (first + e).astype(F32) for e in range(own)]
    routed = jnp.concatenate([jnp.sum(jnp.where(m, 1.0, 0.0), axis=0, keepdims=True) for m in hits], axis=0)
    gate = jnp.concatenate([jnp.sum(jnp.where(m, gates, 0.0), axis=0, keepdims=True) for m in hits], axis=0)
    return jnp.where(routed > 0.0, dot(routed.astype(BF16), earlier), -1.0), gate


def hit_masks(pos, cap):
    slot = lax.broadcasted_iota(jnp.int32, (cap, pos.shape[1]), 0).astype(F32)
    return [pos[e : e + 1, :] == slot for e in range(pos.shape[0])]


def one_hot(masks):
    return jnp.concatenate([jnp.where(m, 1.0, 0.0) for m in masks], axis=0).astype(BF16)


def slot_gates(masks, gate):
    return jnp.concatenate([jnp.where(m, gate[e : e + 1, :], 0.0) for e, m in enumerate(masks)], axis=0)


def three_parts(x):
    hi = x.astype(BF16)
    rest = x - hi.astype(F32)
    mid = rest.astype(BF16)
    return hi, mid, (rest - mid.astype(F32)).astype(BF16)


class Links:
    def __init__(self, send_sem, recv_sem):
        self.send_sem, self.recv_sem, self.sent, self.finished = send_sem, recv_sem, [], set()

    def copy(self, k, src, dst, to):
        return pltpu.make_async_remote_copy(src_ref=src, dst_ref=dst, send_sem=self.send_sem.at[k],
                                            recv_sem=self.recv_sem.at[k], device_id=to, device_id_type=MESH)

    def send(self, src, dst, to):
        k = len(self.sent)
        copy = self.copy(k, src, dst, to)
        copy.start()
        self.sent.append(copy)
        return k

    def arrive(self, k, dst, to):
        self.copy(k, dst, dst, to).wait_recv()

    def finish(self, k):
        self.finished.add(k)
        self.sent[k].wait_send()

    def drain(self):
        for k in range(len(self.sent)):
            if k not in self.finished:
                self.finish(k)


def copy_count(own):
    return 9 + 21 * 4 + 7 * own + 2 * 10


def layer_kernel(own, cap, width, x_own, dy_own, r_own, w1, w3, w2, x_all, dy_all, r_all, w13_all, w2_all, xs_all, us_all,
                 ys_all, sums, mate_land, half_land, last_land, g1, g3, g2, w13, w2s, xb, dyb, rb, routes, earlier, xs, us,
                 acc13, acc2, g_buf, w13e, w2e, ab_buf, h_buf, d_buf, y_buf, v_buf, c_buf, gates_buf, give, keep_sum, mate_sum,
                 turn_sum, send_sem, recv_sem, row_sem, load_sem, w_sem, slot_sem, in_sem, out_sem, c_sem, sum_sem, g_sem):
    ep, tp = lax.axis_index("ep"), lax.axis_index("tp")
    eps, tps = x_all.shape[0], x_all.shape[1]
    model = x_all.shape[3]
    side = model // 2
    half = eps // 2
    step = lambda n: lax.rem(ep + (n + eps), eps)
    turn = lambda n: lax.rem(tp + (n + tps), tps)
    right, left, far = step(2), step(-2), step(4)
    mate = ep + 1 - 2 * lax.rem(ep, 2)
    mate_step = lambda n: lax.rem(mate + (n + eps), eps)
    up, down, over = turn(1), turn(-1), turn(2)
    to_right, to_left, to_mate = {"ep": right}, {"ep": left}, {"ep": mate}
    to_up, to_down = {"tp": up}, {"tp": down}
    links = Links(send_sem, recv_sem)
    wide = 512 if model % 512 == 0 else model

    loads = [pltpu.make_async_copy(w1, w13.at[:, :, pl.ds(0, width)], w_sem.at[0]),
             pltpu.make_async_copy(w3, w13.at[:, :, pl.ds(width, width)], w_sem.at[1]),
             pltpu.make_async_copy(w2, w2s, w_sem.at[2])]
    for copy in loads:
        copy.start()

    barrier = pltpu.get_barrier_semaphore()
    for to in (to_right, to_left, to_mate, to_up, to_down):
        pl.semaphore_signal(barrier, inc=1, device_id=to, device_id_type=MESH)
    pl.semaphore_wait(barrier, 5)

    own_refs, all_refs = (x_own, dy_own, r_own), (x_all, dy_all, r_all)
    upward = (True, False, True)
    kinds = (0, 2, 1)

    def spread(t, srcs):
        out = {}
        for kind in kinds:
            to = to_right if upward[kind] else to_left
            out[kind, upward[kind]] = links.send(srcs[kind], all_refs[kind].at[ep, t], to)
        for kind in kinds:
            to = to_left if upward[kind] else to_right
            out[kind, not upward[kind]] = links.send(srcs[kind], all_refs[kind].at[ep, t], to)
        for kind in kinds:
            out[kind, "mate"] = links.send(srcs[kind], all_refs[kind].at[ep, t], to_mate)
        return out

    def pass_on(g):
        state, t = states[g], groups[g]
        for kind in kinds:
            got, to = (left, to_right) if upward[kind] else (right, to_left)
            block = all_refs[kind].at[got, t]
            links.arrive(state[kind, upward[kind]], block, to)
            state[kind, "far"] = links.send(block, block, to)
            state[kind, "mate1"] = links.send(block, block, to_mate)

    def share(g):
        state, t = states[g], groups[g]
        for kind in kinds:
            got, to = (right, to_left) if upward[kind] else (left, to_right)
            block = all_refs[kind].at[got, t]
            links.arrive(state[kind, not upward[kind]], block, to)
            state[kind, "mate2"] = links.send(block, block, to_mate)

    def last(g):
        state, t = states[g], groups[g]
        for kind in kinds:
            block = all_refs[kind].at[far, t]
            links.arrive(state[kind, "far"], block, to_right if upward[kind] else to_left)
            state[kind, "mate3"] = links.send(block, block, to_mate)

    def from_mate(g):
        state, t = states[g], groups[g]
        for kind in kinds:
            one, two = (mate_step(-2), mate_step(2)) if upward[kind] else (mate_step(2), mate_step(-2))
            for name, at in (("mate", mate), ("mate1", one), ("mate2", two), ("mate3", mate_step(4))):
                links.arrive(state[kind, name], all_refs[kind].at[at, t], to_mate)

    cut = 3 * model // 4
    w_state = [None] * own

    def send_weights(e):
        w_state[e] = {(k, s): links.send(ref.at[e], dst.at[tp, e], to)
                      for k, ref, dst in ((0, w13, w13_all), (1, w2s, w2_all)) for s, to in ((True, to_up), (False, to_down))}

    def pass_weights(e):
        state = w_state[e]
        links.arrive(state[0, True], w13_all.at[down, e], to_up)
        head = w13_all.at[down, e, pl.ds(0, cut)]
        state["head"] = links.send(head, head, to_up)
        links.arrive(state[0, False], w13_all.at[up, e], to_down)
        tail = w13_all.at[up, e, pl.ds(cut, model - cut)]
        state["tail"] = links.send(tail, tail, to_down)
        links.arrive(state[1, False], w2_all.at[up, e], to_down)
        state["w2"] = links.send(w2_all.at[up, e], w2_all.at[up, e], to_down)
        links.arrive(state[1, True], w2_all.at[down, e], to_up)

    def have_weights(e):
        state = w_state[e]
        links.arrive(state["head"], w13_all.at[over, e, pl.ds(0, cut)], to_up)
        links.arrive(state["tail"], w13_all.at[over, e, pl.ds(cut, model - cut)], to_down)
        links.arrive(state["w2"], w2_all.at[over, e], to_down)

    def pair_loads(t, h, p):
        at = pl.ds(h * half + p * (half // 2), half // 2)
        return [pltpu.make_async_copy(src.at[at, t], dst.at[p], load_sem.at[k, p])
                for k, (src, dst) in enumerate(((x_all, xb), (dy_all, dyb), (r_all, rb)))]

    def compute(t, keep):
        for p in range(2):
            for copy in pair_loads(t, 0, p):
                copy.start()

        def half_group(h, carry):
            for p in range(2):
                for copy in pair_loads(t, h, p):
                    copy.wait()

                def gather(b, carry):
                    pos, gate = expert_rows(rb[p, b], ep * own, own, earlier[...])
                    masks = hit_masks(pos, cap)
                    pick = one_hot(masks)
                    gates = jnp.sum(slot_gates(masks, gate), axis=1, keepdims=True)
                    rows = pl.ds(pl.multiple_of((p * (half // 2) + b) * cap, cap), cap)
                    picked = dot(pick, xb[p, b]).astype(BF16)
                    for e in range(own):
                        xs[e, rows, :] = picked[e * cap : (e + 1) * cap]
                    scaled = (gates * dot(pick, dyb[p, b])).astype(BF16)
                    for e in range(own):
                        us[e, rows, :] = scaled[e * cap : (e + 1) * cap]
                    return carry

                lax.fori_loop(0, half // 2, gather, 0)

                @pl.when(h == 0)
                def _():
                    for copy in pair_loads(t, 1, p):
                        copy.start()

            stores = []
            if keep:
                stores = [pltpu.make_async_copy(xs, xs_all.at[:, h], slot_sem.at[0]),
                          pltpu.make_async_copy(us, us_all.at[:, h], slot_sem.at[1])]
            for copy in stores:
                copy.start()

            def expert(e, carry):
                ab = dot(xs[e], w13[e])
                a, b = ab[:, :width], ab[:, width:]
                dh = dot_tb(us[e], w2s[e])
                sig = jax.nn.sigmoid(a)
                silu = a * sig
                hid = (silu * b).astype(BF16)
                da = (dh * b * sig * (1.0 + a * (1.0 - sig))).astype(BF16)
                db = (dh * silu).astype(BF16)
                acc13[e] += dot_ta(jnp.concatenate([da, db], axis=1), xs[e])
                acc2[e] += dot_ta(hid, us[e])
                return carry

            lax.fori_loop(0, own, expert, 0)
            for copy in stores:
                copy.wait()
            return carry

        lax.fori_loop(0, 2, half_group, 0)

    def fetch(e):
        copies = [pltpu.make_async_copy(xs_all.at[e], xs.at[pl.ds(0, 2)], in_sem.at[0]),
                  pltpu.make_async_copy(us_all.at[e], us.at[pl.ds(0, 2)], in_sem.at[1]),
                  pltpu.make_async_copy(w2_all.at[:, e], w2e, in_sem.at[2])]
        copies += [pltpu.make_async_copy(w13_all.at[j, e], w13e.at[j], in_sem.at[3 + j]) for j in range(tps)]
        for k in (0, 3, 4, 5, 6, 2, 1):
            copies[k].start()
        return copies

    slots = eps * cap
    pending = {}

    def put(name, buf, e, value, at):
        for k in range(eps):
            buf[k, :, at] = value[k * cap : (k + 1) * cap]

    def store_rows(kind, buf, e):
        copy = pltpu.make_async_copy(buf, ys_all.at[kind, :, e], out_sem.at[kind])
        copy.start()
        pending[kind] = copy

    def settle_rows(kind):
        if kind in pending:
            pending.pop(kind).wait()

    def forward(e, copies):
        copies[0].wait()

        def shard(j, carry):
            pltpu.make_async_copy(w13_all.at[j, e], w13e.at[j], in_sem.at[3 + j]).wait()
            ab = dot(xs[0:2].reshape(slots, model), w13e[j])
            ab_buf[j] = ab
            a, b = ab[:, :width], ab[:, width:]
            h_buf[:, pl.ds(pl.multiple_of(j * width, width), width)] = (a * jax.nn.sigmoid(a) * b).astype(BF16)
            return carry

        lax.fori_loop(0, tps, shard, 0)
        copies[2].wait()
        settle_rows(0)

        def columns(n, carry):
            at = pl.ds(pl.multiple_of(n * wide, wide), wide)
            put("y", y_buf, e, dot(h_buf[...], w2e[:, :, at].reshape(tps * width, wide)).astype(BF16), at)
            return carry

        lax.fori_loop(0, model // wide, columns, 0)
        store_rows(0, y_buf, e)

    def backward(e, copies):
        copies[1].wait()

        def shard(j, carry):
            dh = dot_tb(us[0:2].reshape(slots, model), w2e[j])
            a, b = ab_buf[j, :, :width], ab_buf[j, :, width:]
            sig = jax.nn.sigmoid(a)
            d_buf[j, :, :width] = (dh * b * sig * (1.0 + a * (1.0 - sig))).astype(BF16)
            d_buf[j, :, width:] = (dh * (a * sig)).astype(BF16)
            return carry

        lax.fori_loop(0, tps, shard, 0)
        settle_rows(1)

        def columns(n, carry):
            at = pl.ds(pl.multiple_of(n * wide, wide), wide)
            v = dot_tb(d_buf[0], w13e[0, at, :])
            for j in range(1, tps):
                v = v + dot_tb(d_buf[j], w13e[j, at, :])
            put("v", v_buf, e, v.astype(BF16), at)
            return carry

        lax.fori_loop(0, model // wide, columns, 0)
        store_rows(1, v_buf, e)

    def expert(e):
        have_weights(e)
        copies = fetch(e)
        forward(e, copies)
        backward(e, copies)

    offsets = (4, 2, -2, 0)

    def row_load(kind, block, slot):
        return pltpu.make_async_copy(ys_all.at[kind, block], c_buf.at[slot], c_sem.at[slot])

    def combine(kind, block, slot, tile):
        pos, gate = expert_rows(routes[block], ep * own, own, earlier[...])
        masks = hit_masks(pos, cap)
        parts = three_parts(slot_gates(masks, gate)) if kind == 0 else (one_hot(masks),)
        for k, part in enumerate(parts):
            gates_buf[k] = part
        row_load(kind, block, slot).wait()
        for s in range(2):
            total = None
            rows = c_buf[slot, :, :, s * side : (s + 1) * side].reshape(own * cap, side)
            for k in reversed(range(len(parts))):
                term = dot_ta(gates_buf[k], rows)
                total = term if total is None else total + term
            tile[s] = total

    def sum_up(kind):
        settle_rows(kind)
        state = {}
        blocks = [(mate_step(o), step(o)) for o in offsets]
        order = [b for pair in blocks for b in pair]
        row_load(kind, order[0], 0).start()

        def one(n, tile):
            if n + 1 < len(order):
                row_load(kind, order[n + 1], (n + 1) % 2).start()
            combine(kind, order[n], n % 2, tile)

        gifts, writes = [], []

        def give_block(i):
            if i >= 2:
                links.finish(gifts[i - 2])
            one(2 * i, give.at[i % 2])
            gifts.append(links.send(give.at[i % 2], mate_land.at[kind, i], to_mate))

        def own_block(i):
            one(2 * i + 1, keep_sum.at[i % 2])

        def add_mate(i):
            links.arrive(gifts[i], mate_land.at[kind, i], to_mate)
            copy = pltpu.make_async_copy(mate_land.at[kind, i], mate_sum, sum_sem.at[0])
            copy.start()
            copy.wait()
            keep_sum[i % 2] += mate_sum[...]
            writes.append(pltpu.make_async_copy(keep_sum.at[i % 2], sums.at[kind, i], sum_sem.at[1 + i % 2]))
            writes[i].start()

        def send_sum(i):
            writes[i].wait()
            if i == 0:
                state["far right"] = links.send(sums.at[kind, 0, 0], half_land.at[kind, 0], to_right)
                state["far left"] = links.send(sums.at[kind, 0, 1], half_land.at[kind, 1], to_left)
            elif i == 1:
                state["right"] = links.send(sums.at[kind, 1, 1], last_land.at[kind, 0, 1], to_right)
            elif i == 2:
                state["left"] = links.send(sums.at[kind, 2, 0], last_land.at[kind, 1, 0], to_left)

        give_block(0)
        own_block(0)
        give_block(1)
        add_mate(0)
        send_sum(0)
        own_block(1)
        give_block(2)
        add_mate(1)
        own_block(2)
        send_sum(1)
        give_block(3)
        add_mate(2)
        own_block(3)
        send_sum(2)
        add_mate(3)
        send_sum(3)
        links.finish(gifts[2])
        links.finish(gifts[3])
        return state

    def turn_sums(kind, state):
        for s, key, to, back in ((0, "far right", to_right, to_right), (1, "far left", to_left, to_left)):
            links.arrive(state[key], half_land.at[kind, s], back)
            tile = turn_sum.at[kind, s]
            a = pltpu.make_async_copy(sums.at[kind, 1 + s, s], tile, sum_sem.at[0])
            b = pltpu.make_async_copy(half_land.at[kind, s], mate_sum.at[s], sum_sem.at[1])
            a.start()
            b.start()
            a.wait()
            b.wait()
            turn_sum[kind, s] += mate_sum[s]
            state["turn", s] = links.send(tile, last_land.at[kind, s, s], to)

    def sums_here(kind, state):
        links.arrive(state["right"], last_land.at[kind, 0, 1], to_right)
        links.arrive(state["left"], last_land.at[kind, 1, 0], to_left)
        links.arrive(state["turn", 0], last_land.at[kind, 0, 0], to_right)
        links.arrive(state["turn", 1], last_land.at[kind, 1, 1], to_left)

    y_state = {}
    for way in (True, False):
        for kind in kinds:
            go_up = upward[kind] == way
            y_state[kind, go_up] = links.send(own_refs[kind], all_refs[kind].at[ep, tp], to_up if go_up else to_down)
    groups = (tp, down, up, over)
    states = [spread(tp, own_refs)]
    hold = [pltpu.make_async_copy(own_refs[kind], all_refs[kind].at[ep, tp], row_sem.at[kind]) for kind in range(3)]
    for copy in hold:
        copy.start()
    for copy in loads:
        copy.wait()
    stow = [pltpu.make_async_copy(w13, w13_all.at[tp], w_sem.at[0]), pltpu.make_async_copy(w2s, w2_all.at[tp], w_sem.at[1])]
    for copy in stow:
        copy.start()
    earlier[...] = earlier_rows(earlier.shape[0])
    acc13[...] = jnp.zeros_like(acc13)
    acc2[...] = jnp.zeros_like(acc2)

    def y_arrive(kind, way):
        block = all_refs[kind].at[ep, down if way else up]
        links.arrive(y_state[kind, way], block, to_up if way else to_down)
        return block

    for kind in kinds:
        block = y_arrive(kind, upward[kind])
        y_state[kind, "far"] = links.send(block, block, to_up if upward[kind] else to_down)
    pass_on(0)
    for kind in kinds:
        y_arrive(kind, not upward[kind])
    send_weights(0)
    send_weights(1)
    for g in (1, 2):
        states.append(spread(groups[g], [ref.at[ep, groups[g]] for ref in all_refs]))
    share(0)
    last(0)
    for kind in kinds:
        links.arrive(y_state[kind, "far"], all_refs[kind].at[ep, over], to_up if upward[kind] else to_down)
    for copy in hold + stow:
        copy.wait()
    from_mate(0)
    route_copy = pltpu.make_async_copy(r_all.at[:, tp], routes, row_sem.at[0])
    route_copy.start()
    route_copy.wait()
    compute(tp, True)

    pass_on(1)
    states.append(spread(over, [ref.at[ep, over] for ref in all_refs]))
    pass_weights(0)
    send_weights(2)
    share(1)
    pass_on(2)
    pass_weights(1)
    send_weights(3)
    expert(0)
    share(2)
    last(1)
    from_mate(1)
    compute(groups[1], False)
    pass_weights(2)
    send_weights(4)
    pass_on(3)
    expert(1)
    share(3)
    pass_weights(3)
    last(2)
    from_mate(2)
    expert(2)
    last(3)
    compute(groups[2], False)
    pass_weights(4)
    expert(3)
    have_weights(4)
    copies = fetch(4)
    forward(4, copies)
    y_sum = sum_up(0)
    backward(4, copies)
    dx_sum = sum_up(1)
    turn_sums(0, y_sum)
    from_mate(3)
    compute(groups[3], False)
    turn_sums(1, dx_sum)

    def finish(e, carry):
        g_buf[0] = acc13[e, :width, :].T.astype(BF16)
        g_buf[1] = acc13[e, width:, :].T.astype(BF16)
        copies = [pltpu.make_async_copy(g_buf.at[0], g1.at[e], g_sem.at[0]), pltpu.make_async_copy(g_buf.at[1], g3.at[e], g_sem.at[1])]
        xs[0, pl.ds(0, width), :] = acc2[e].astype(BF16)
        copies.append(pltpu.make_async_copy(xs.at[0, pl.ds(0, width)], g2.at[e], g_sem.at[2]))
        for copy in copies:
            copy.start()
        for copy in copies:
            copy.wait()
        return carry

    lax.fori_loop(0, own, finish, 0)
    sums_here(0, y_sum)
    sums_here(1, dx_sum)
    links.drain()


def layer(tokens, d_out, routes, w_one, w_three, w_two, ep_size, tp_size, cap):
    tok, model = tokens.shape
    own, width, _ = w_two.shape
    half = ep_size // 2
    rows = half * cap
    side = model // 2
    vmem, hbm = pl.BlockSpec(memory_space=pltpu.VMEM), pl.BlockSpec(memory_space=pl.ANY)
    shape = jax.ShapeDtypeStruct
    copies = copy_count(own)
    slot_rows = ep_size * tp_size * cap * own
    vector = pltpu.VMEM
    dma = pltpu.SemaphoreType.DMA
    outs = pl.pallas_call(
        functools.partial(layer_kernel, own, cap, width),
        in_specs=[vmem, vmem, vmem, hbm, hbm, hbm],
        out_specs=[hbm] * 15,
        out_shape=[
            shape((ep_size, tp_size, tok, model), BF16),
            shape((ep_size, tp_size, tok, model), BF16),
            shape((ep_size, tp_size) + routes.shape, F32),
            shape((tp_size, own, model, 2 * width), BF16),
            shape((tp_size, own, width, model), BF16),
            shape((own, 2, rows, model), BF16),
            shape((own, 2, rows, model), BF16),
            shape((2, ep_size, own, cap, model), BF16),
            shape((2, 4, 2, tok, side), F32),
            shape((2, 4, 2, tok, side), F32),
            shape((2, 2, tok, side), F32),
            shape((2, 2, 2, tok, side), F32),
            shape((own, model, width), BF16),
            shape((own, model, width), BF16),
            shape((own, width, model), BF16),
        ],
        scratch_shapes=[
            vector((own, model, 2 * width), BF16),
            vector((own, width, model), BF16),
            vector((2, half // 2, tok, model), BF16),
            vector((2, half // 2, tok, model), BF16),
            vector((2, half // 2) + routes.shape, F32),
            vector((ep_size,) + routes.shape, F32),
            vector((tok, tok), BF16),
            vector((own, rows, model), BF16),
            vector((own, rows, model), BF16),
            vector((own, 2 * width, model), F32),
            vector((own, width, model), F32),
            vector((2, model, width), BF16),
            vector((tp_size, model, 2 * width), BF16),
            vector((tp_size, width, model), BF16),
            vector((tp_size, 2 * rows, 2 * width), F32),
            vector((2 * rows, tp_size * width), BF16),
            vector((tp_size, 2 * rows, 2 * width), BF16),
            vector((ep_size, cap, model), BF16),
            vector((ep_size, cap, model), BF16),
            vector((2, own, cap, model), BF16),
            vector((3, own * cap, tok), BF16),
            vector((2, 2, tok, side), F32),
            vector((2, 2, tok, side), F32),
            vector((2, tok, side), F32),
            vector((2, 2, tok, side), F32),
            dma((copies,)),
            dma((copies,)),
            dma((3,)),
            dma((3, 2)),
            dma((3,)),
            dma((2,)),
            dma((3 + tp_size,)),
            dma((2,)),
            dma((2,)),
            dma((3,)),
            dma((3,)),
        ],
        compiler_params=pltpu.CompilerParams(vmem_limit_bytes=VMEM_LIMIT, collective_id=0, has_side_effects=True),
        cost_estimate=pl.CostEstimate(
            flops=2 * slot_rows * model * (2 * tok + 12 * width),
            bytes_accessed=4 * ep_size * tp_size * tok * model,
            transcendentals=0,
        ),
        name="layer",
    )(tokens, d_out, routes, w_one, w_three, w_two)
    return outs[8], outs[11], outs[12:]


def result_kernel(sums, last_land, g1, g3, g2, out, dx, o1, o3, o2, parts, rows, b1, b3, b2, in_sem, out_sem):
    grads = ((g1, b1, o1), (g3, b3, o3), (g2, b2, o2))
    takes = [pltpu.make_async_copy(src, buf, in_sem.at[k]) for k, (src, buf, _) in enumerate(grads)]
    terms = [[pltpu.make_async_copy(sums.at[kind, 3], parts.at[kind, 2], in_sem.at[3 + kind]),
              pltpu.make_async_copy(last_land.at[kind], parts.at[kind, pl.ds(0, 2)], in_sem.at[5 + kind])] for kind in range(2)]
    for copy in terms[0] + terms[1] + takes:
        copy.start()
    puts = []
    side = parts.shape[4]
    for kind, to in ((0, out), (1, dx)):
        for copy in terms[kind]:
            copy.wait()
        for s in range(2):
            total = parts[kind, 2, s] + (parts[kind, 0, s] + parts[kind, 1, s])
            rows[kind, :, s * side : (s + 1) * side] = total.astype(BF16)
        puts.append(pltpu.make_async_copy(rows.at[kind], to, out_sem.at[3 + kind]))
        puts[-1].start()
    for k, (take, (_, buf, to)) in enumerate(zip(takes, grads)):
        take.wait()
        puts.append(pltpu.make_async_copy(buf, to, out_sem.at[k]))
        puts[-1].start()
    for copy in puts:
        copy.wait()


def results(sums, last_land, grads):
    _, _, _, tok, side = sums.shape
    hbm = pl.BlockSpec(memory_space=pl.ANY)
    row = jax.ShapeDtypeStruct((tok, 2 * side), BF16)
    return pl.pallas_call(
        result_kernel,
        in_specs=[hbm] * 5,
        out_specs=[hbm] * 5,
        out_shape=[row, row] + [jax.ShapeDtypeStruct(g.shape, g.dtype) for g in grads],
        scratch_shapes=[pltpu.VMEM((2, 3, 2, tok, side), F32), pltpu.VMEM((2, tok, 2 * side), BF16)]
        + [pltpu.VMEM(g.shape, g.dtype) for g in grads]
        + [pltpu.SemaphoreType.DMA((7,)), pltpu.SemaphoreType.DMA((5,))],
        compiler_params=pltpu.CompilerParams(vmem_limit_bytes=VMEM_LIMIT),
        name="results",
    )(sums, last_land, *grads)


def solution(mesh):
    ep_size, tp_size = mesh.shape["ep"], mesh.shape["tp"]
    row_spec = P(("dp", "ep", "tp"), None)
    col_spec = P("ep", None, "tp")
    down_spec = P("ep", "tp", None)
    grad_col = P(("dp", "ep"), None, "tp")
    grad_down = P(("dp", "ep"), "tp", None)

    def local_step(tokens, expert_ids, gate_vals, w_one, w_three, w_two, d_out):
        cap = slot_count(expert_ids.shape[1], tokens.shape[0], w_one.shape[0] * ep_size)
        routes = jnp.concatenate([expert_ids.T.astype(F32), gate_vals.T], axis=0)
        sums, last_land, grads = layer(tokens, d_out, routes, w_one, w_three, w_two, ep_size, tp_size, cap)
        return tuple(results(sums, last_land, grads))

    return jax.shard_map(local_step, mesh=mesh,
                         in_specs=(row_spec, row_spec, row_spec, col_spec, col_spec, down_spec, row_spec),
                         out_specs=(row_spec, row_spec, grad_col, grad_col, grad_down), check_vma=False)
```

```python
import functools

import jax
import jax.numpy as jnp
from jax import lax
from jax.experimental import pallas as pl
from jax.experimental.pallas import tpu as pltpu
from jax.sharding import PartitionSpec as P

BF16 = jnp.bfloat16
F32 = jnp.float32
MESH = pl.DeviceIdType.MESH
VMEM_LIMIT = 62 * 2**20


def slot_count(num_top, tok_dev, experts):
    return 8 * ((5 * num_top * tok_dev + 32 * experts - 1) // (32 * experts))


def dot(a, b):
    return jnp.dot(a, b, preferred_element_type=F32)


def dot_tb(a, b):
    return lax.dot_general(a, b, (((1,), (1,)), ((), ())), preferred_element_type=F32)


def dot_ta(a, b):
    return lax.dot_general(a, b, (((0,), (0,)), ((), ())), preferred_element_type=F32)


def earlier_rows(tok):
    row = lax.broadcasted_iota(jnp.int32, (tok, tok), 0)
    col = lax.broadcasted_iota(jnp.int32, (tok, tok), 1)
    return jnp.where(row < col, 1.0, 0.0).astype(BF16)


def expert_rows(routes, first, own, earlier):
    top = routes.shape[0] // 2
    ids, gates = routes[:top], routes[top:]
    hits = [ids == (first + e).astype(F32) for e in range(own)]
    routed = jnp.concatenate([jnp.sum(jnp.where(m, 1.0, 0.0), axis=0, keepdims=True) for m in hits], axis=0)
    gate = jnp.concatenate([jnp.sum(jnp.where(m, gates, 0.0), axis=0, keepdims=True) for m in hits], axis=0)
    return jnp.where(routed > 0.0, dot(routed.astype(BF16), earlier), -1.0), gate


def hit_masks(pos, cap):
    slot = lax.broadcasted_iota(jnp.int32, (cap, pos.shape[1]), 0).astype(F32)
    return [pos[e : e + 1, :] == slot for e in range(pos.shape[0])]


def one_hot(masks):
    return jnp.concatenate([jnp.where(m, 1.0, 0.0) for m in masks], axis=0).astype(BF16)


def slot_gates(masks, gate):
    return jnp.concatenate([jnp.where(m, gate[e : e + 1, :], 0.0) for e, m in enumerate(masks)], axis=0)


def three_parts(x):
    hi = x.astype(BF16)
    rest = x - hi.astype(F32)
    mid = rest.astype(BF16)
    return hi, mid, (rest - mid.astype(F32)).astype(BF16)


class Links:
    def __init__(self, send_sem, recv_sem):
        self.send_sem, self.recv_sem, self.sent, self.finished = send_sem, recv_sem, [], set()

    def copy(self, k, src, dst, to):
        return pltpu.make_async_remote_copy(src_ref=src, dst_ref=dst, send_sem=self.send_sem.at[k],
                                            recv_sem=self.recv_sem.at[k], device_id=to, device_id_type=MESH)

    def send(self, src, dst, to):
        k = len(self.sent)
        copy = self.copy(k, src, dst, to)
        copy.start()
        self.sent.append(copy)
        return k

    def arrive(self, k, dst, to):
        self.copy(k, dst, dst, to).wait_recv()

    def finish(self, k):
        self.finished.add(k)
        self.sent[k].wait_send()

    def drain(self):
        for k in range(len(self.sent)):
            if k not in self.finished:
                self.finish(k)


def copy_count(own):
    return 6 + 21 * 3 + 24 + 7 * own + 2 * 10


def layer_kernel(own, cap, width, x_own, dy_own, r_own, w1, w3, w2, x_all, dy_all, r_all, w13_all, w2_all, xs_all, us_all,
                 ys_all, sums, mate_land, half_land, last_land, g1, g3, g2, w13, w2s, xb, dyb, rb, routes, earlier, xs, us,
                 acc13, acc2, g_buf, w13e, w2e, ab_buf, h_buf, d_buf, y_buf, v_buf, c_buf, gates_buf, give, keep_sum, mate_sum,
                 turn_sum, send_sem, recv_sem, row_sem, load_sem, w_sem, slot_sem, in_sem, out_sem, c_sem, sum_sem, g_sem):
    ep, tp = lax.axis_index("ep"), lax.axis_index("tp")
    eps, tps = x_all.shape[0], x_all.shape[1]
    model = x_all.shape[3]
    side = model // 2
    half = eps // 2
    step = lambda n: lax.rem(ep + (n + eps), eps)
    turn = lambda n: lax.rem(tp + (n + tps), tps)
    right, left, far = step(2), step(-2), step(4)
    mate = ep + 1 - 2 * lax.rem(ep, 2)
    mate_step = lambda n: lax.rem(mate + (n + eps), eps)
    up, down, over = turn(1), turn(-1), turn(2)
    to_right, to_left, to_mate = {"ep": right}, {"ep": left}, {"ep": mate}
    to_up, to_down = {"tp": up}, {"tp": down}
    links = Links(send_sem, recv_sem)
    wide = 512 if model % 512 == 0 else model

    loads = [pltpu.make_async_copy(w1, w13.at[:, :, pl.ds(0, width)], w_sem.at[0]),
             pltpu.make_async_copy(w3, w13.at[:, :, pl.ds(width, width)], w_sem.at[1]),
             pltpu.make_async_copy(w2, w2s, w_sem.at[2])]
    for copy in loads:
        copy.start()

    barrier = pltpu.get_barrier_semaphore()
    for to in (to_right, to_left, to_mate, to_up, to_down):
        pl.semaphore_signal(barrier, inc=1, device_id=to, device_id_type=MESH)
    pl.semaphore_wait(barrier, 5)

    own_refs, all_refs = (x_own, dy_own, r_own), (x_all, dy_all, r_all)
    upward = (True, False, True)
    kinds = (0, 2, 1)

    def spread(t, srcs):
        out = {}
        for kind in kinds:
            to = to_right if upward[kind] else to_left
            out[kind, upward[kind]] = links.send(srcs[kind], all_refs[kind].at[ep, t], to)
        for kind in kinds:
            to = to_left if upward[kind] else to_right
            out[kind, not upward[kind]] = links.send(srcs[kind], all_refs[kind].at[ep, t], to)
        for kind in kinds:
            out[kind, "mate"] = links.send(srcs[kind], all_refs[kind].at[ep, t], to_mate)
        return out

    def pass_on(g):
        state, t = states[g], groups[g]
        for kind in kinds:
            got, to = (left, to_right) if upward[kind] else (right, to_left)
            block = all_refs[kind].at[got, t]
            links.arrive(state[kind, upward[kind]], block, to)
            state[kind, "far"] = links.send(block, block, to)
            state[kind, "mate1"] = links.send(block, block, to_mate)

    def share(g):
        state, t = states[g], groups[g]
        for kind in kinds:
            got, to = (right, to_left) if upward[kind] else (left, to_right)
            block = all_refs[kind].at[got, t]
            links.arrive(state[kind, not upward[kind]], block, to)
            state[kind, "mate2"] = links.send(block, block, to_mate)

    def last(g):
        state, t = states[g], groups[g]
        for kind in kinds:
            block = all_refs[kind].at[far, t]
            links.arrive(state[kind, "far"], block, to_right if upward[kind] else to_left)
            state[kind, "mate3"] = links.send(block, block, to_mate)

    def from_mate(g):
        state, t = states[g], groups[g]
        for kind in kinds:
            one, two = (mate_step(-2), mate_step(2)) if upward[kind] else (mate_step(2), mate_step(-2))
            for name, at in (("mate", mate), ("mate1", one), ("mate2", two), ("mate3", mate_step(4))):
                links.arrive(state[kind, name], all_refs[kind].at[at, t], to_mate)

    core = lax.rem(ep, 2)

    def send_over():
        return [{kind: links.send(all_refs[kind].at[core + 2 * m, down if upward[kind] else up],
                                  all_refs[kind].at[core + 2 * m, down if upward[kind] else up],
                                  to_up if upward[kind] else to_down) for kind in kinds} for m in range(half)]

    def share_over(m):
        for kind in kinds:
            block = all_refs[kind].at[core + 2 * m, over]
            links.arrive(over_state[m][kind], block, to_up if upward[kind] else to_down)
            over_state[m][kind, "mate"] = links.send(block, block, to_mate)

    def have_over(m):
        for kind in kinds:
            links.arrive(over_state[m][kind, "mate"], all_refs[kind].at[1 - core + 2 * m, over], to_mate)

    cut = 3 * model // 4
    w_state = [None] * own

    def send_weights(e):
        w_state[e] = {(k, s): links.send(ref.at[e], dst.at[tp, e], to)
                      for k, ref, dst in ((0, w13, w13_all), (1, w2s, w2_all)) for s, to in ((True, to_up), (False, to_down))}

    def pass_weights(e):
        state = w_state[e]
        links.arrive(state[0, True], w13_all.at[down, e], to_up)
        head = w13_all.at[down, e, pl.ds(0, cut)]
        state["head"] = links.send(head, head, to_up)
        links.arrive(state[0, False], w13_all.at[up, e], to_down)
        tail = w13_all.at[up, e, pl.ds(cut, model - cut)]
        state["tail"] = links.send(tail, tail, to_down)
        links.arrive(state[1, False], w2_all.at[up, e], to_down)
        state["w2"] = links.send(w2_all.at[up, e], w2_all.at[up, e], to_down)
        links.arrive(state[1, True], w2_all.at[down, e], to_up)

    def have_weights(e):
        state = w_state[e]
        links.arrive(state["head"], w13_all.at[over, e, pl.ds(0, cut)], to_up)
        links.arrive(state["tail"], w13_all.at[over, e, pl.ds(cut, model - cut)], to_down)
        links.arrive(state["w2"], w2_all.at[over, e], to_down)

    def pair_loads(t, h, p):
        at = pl.ds(h * half + p * (half // 2), half // 2)
        return [pltpu.make_async_copy(src.at[at, t], dst.at[p], load_sem.at[k, p])
                for k, (src, dst) in enumerate(((x_all, xb), (dy_all, dyb), (r_all, rb)))]

    def half_group(t, h, keep, ahead):
        for p in range(2):
            for copy in pair_loads(t, h, p):
                copy.wait()

            def gather(b, carry):
                pos, gate = expert_rows(rb[p, b], ep * own, own, earlier[...])
                masks = hit_masks(pos, cap)
                pick = one_hot(masks)
                gates = jnp.sum(slot_gates(masks, gate), axis=1, keepdims=True)
                rows = pl.ds(pl.multiple_of((p * (half // 2) + b) * cap, cap), cap)
                picked = dot(pick, xb[p, b]).astype(BF16)
                for e in range(own):
                    xs[e, rows, :] = picked[e * cap : (e + 1) * cap]
                scaled = (gates * dot(pick, dyb[p, b])).astype(BF16)
                for e in range(own):
                    us[e, rows, :] = scaled[e * cap : (e + 1) * cap]
                return carry

            lax.fori_loop(0, half // 2, gather, 0)

            @pl.when(ahead)
            def _():
                for copy in pair_loads(t, 1, p):
                    copy.start()

        stores = []
        if keep:
            stores = [pltpu.make_async_copy(xs, xs_all.at[:, h], slot_sem.at[0]),
                      pltpu.make_async_copy(us, us_all.at[:, h], slot_sem.at[1])]
        for copy in stores:
            copy.start()

        def expert(e, carry):
            ab = dot(xs[e], w13[e])
            a, b = ab[:, :width], ab[:, width:]
            dh = dot_tb(us[e], w2s[e])
            sig = jax.nn.sigmoid(a)
            silu = a * sig
            hid = (silu * b).astype(BF16)
            da = (dh * b * sig * (1.0 + a * (1.0 - sig))).astype(BF16)
            db = (dh * silu).astype(BF16)
            acc13[e] += dot_ta(jnp.concatenate([da, db], axis=1), xs[e])
            acc2[e] += dot_ta(hid, us[e])
            return carry

        lax.fori_loop(0, own, expert, 0)
        for copy in stores:
            copy.wait()

    def start_loads(t, h):
        for p in range(2):
            for copy in pair_loads(t, h, p):
                copy.start()

    def compute(t, keep):
        start_loads(t, 0)

        def one_half(h, carry):
            half_group(t, h, keep, h == 0)
            return carry

        lax.fori_loop(0, 2, one_half, 0)

    def fetch(e):
        copies = [pltpu.make_async_copy(xs_all.at[e], xs.at[pl.ds(0, 2)], in_sem.at[0]),
                  pltpu.make_async_copy(us_all.at[e], us.at[pl.ds(0, 2)], in_sem.at[1]),
                  pltpu.make_async_copy(w2_all.at[:, e], w2e, in_sem.at[2])]
        copies += [pltpu.make_async_copy(w13_all.at[j, e], w13e.at[j], in_sem.at[3 + j]) for j in range(tps)]
        for k in (0, 3, 4, 5, 6, 2, 1):
            copies[k].start()
        return copies

    slots = eps * cap
    pending = {}

    def put(name, buf, e, value, at):
        for k in range(eps):
            buf[k, :, at] = value[k * cap : (k + 1) * cap]

    def store_rows(kind, buf, e):
        copy = pltpu.make_async_copy(buf, ys_all.at[kind, :, e], out_sem.at[kind])
        copy.start()
        pending[kind] = copy

    def settle_rows(kind):
        if kind in pending:
            pending.pop(kind).wait()

    def forward(e, copies):
        copies[0].wait()

        def shard(j, carry):
            pltpu.make_async_copy(w13_all.at[j, e], w13e.at[j], in_sem.at[3 + j]).wait()
            ab = dot(xs[0:2].reshape(slots, model), w13e[j])
            ab_buf[j] = ab
            a, b = ab[:, :width], ab[:, width:]
            h_buf[:, pl.ds(pl.multiple_of(j * width, width), width)] = (a * jax.nn.sigmoid(a) * b).astype(BF16)
            return carry

        lax.fori_loop(0, tps, shard, 0)
        copies[2].wait()
        settle_rows(0)

        def columns(n, carry):
            at = pl.ds(pl.multiple_of(n * wide, wide), wide)
            put("y", y_buf, e, dot(h_buf[...], w2e[:, :, at].reshape(tps * width, wide)).astype(BF16), at)
            return carry

        lax.fori_loop(0, model // wide, columns, 0)
        store_rows(0, y_buf, e)

    def backward(e, copies):
        copies[1].wait()

        def shard(j, carry):
            dh = dot_tb(us[0:2].reshape(slots, model), w2e[j])
            a, b = ab_buf[j, :, :width], ab_buf[j, :, width:]
            sig = jax.nn.sigmoid(a)
            d_buf[j, :, :width] = (dh * b * sig * (1.0 + a * (1.0 - sig))).astype(BF16)
            d_buf[j, :, width:] = (dh * (a * sig)).astype(BF16)
            return carry

        lax.fori_loop(0, tps, shard, 0)
        settle_rows(1)

        def columns(n, carry):
            at = pl.ds(pl.multiple_of(n * wide, wide), wide)
            v = dot_tb(d_buf[0], w13e[0, at, :])
            for j in range(1, tps):
                v = v + dot_tb(d_buf[j], w13e[j, at, :])
            put("v", v_buf, e, v.astype(BF16), at)
            return carry

        lax.fori_loop(0, model // wide, columns, 0)
        store_rows(1, v_buf, e)

    def expert(e):
        have_weights(e)
        copies = fetch(e)
        forward(e, copies)
        backward(e, copies)

    offsets = (4, 2, -2, 0)

    def row_load(kind, block, slot):
        return pltpu.make_async_copy(ys_all.at[kind, block], c_buf.at[slot], c_sem.at[slot])

    def combine(kind, block, slot, tile):
        pos, gate = expert_rows(routes[block], ep * own, own, earlier[...])
        masks = hit_masks(pos, cap)
        parts = three_parts(slot_gates(masks, gate)) if kind == 0 else (one_hot(masks),)
        for k, part in enumerate(parts):
            gates_buf[k] = part
        row_load(kind, block, slot).wait()

        def one_side(s, carry):
            rows = c_buf[slot, :, :, pl.ds(pl.multiple_of(s * side, side), side)].reshape(own * cap, side)
            total = None
            for k in reversed(range(len(parts))):
                term = dot_ta(gates_buf[k], rows)
                total = term if total is None else total + term
            tile[s] = total
            return carry

        lax.fori_loop(0, 2, one_side, 0)

    def sum_up(kind):
        settle_rows(kind)
        state = {}
        blocks = [(mate_step(o), step(o)) for o in offsets]
        order = [b for pair in blocks for b in pair]
        row_load(kind, order[0], 0).start()

        def one(n, tile):
            if n + 1 < len(order):
                row_load(kind, order[n + 1], (n + 1) % 2).start()
            combine(kind, order[n], n % 2, tile)

        gifts, writes = [], []

        def give_block(i):
            if i >= 2:
                links.finish(gifts[i - 2])
            one(2 * i, give.at[i % 2])
            gifts.append(links.send(give.at[i % 2], mate_land.at[kind, i], to_mate))

        def own_block(i):
            one(2 * i + 1, keep_sum.at[i % 2])

        def add_mate(i):
            links.arrive(gifts[i], mate_land.at[kind, i], to_mate)
            copy = pltpu.make_async_copy(mate_land.at[kind, i], mate_sum, sum_sem.at[0])
            copy.start()
            copy.wait()
            keep_sum[i % 2] += mate_sum[...]
            writes.append(pltpu.make_async_copy(keep_sum.at[i % 2], sums.at[kind, i], sum_sem.at[1 + i % 2]))
            writes[i].start()

        def send_sum(i):
            writes[i].wait()
            if i == 0:
                state["far right"] = links.send(sums.at[kind, 0, 0], half_land.at[kind, 0], to_right)
                state["far left"] = links.send(sums.at[kind, 0, 1], half_land.at[kind, 1], to_left)
            elif i == 1:
                state["right"] = links.send(sums.at[kind, 1, 1], last_land.at[kind, 0, 1], to_right)
            elif i == 2:
                state["left"] = links.send(sums.at[kind, 2, 0], last_land.at[kind, 1, 0], to_left)

        give_block(0)
        own_block(0)
        give_block(1)
        add_mate(0)
        send_sum(0)
        own_block(1)
        give_block(2)
        add_mate(1)
        own_block(2)
        send_sum(1)
        give_block(3)
        add_mate(2)
        own_block(3)
        send_sum(2)
        add_mate(3)
        send_sum(3)
        links.finish(gifts[2])
        links.finish(gifts[3])
        return state

    def turn_sums(kind, state):
        for s, key, to, back in ((0, "far right", to_right, to_right), (1, "far left", to_left, to_left)):
            links.arrive(state[key], half_land.at[kind, s], back)
            tile = turn_sum.at[kind, s]
            a = pltpu.make_async_copy(sums.at[kind, 1 + s, s], tile, sum_sem.at[0])
            b = pltpu.make_async_copy(half_land.at[kind, s], mate_sum.at[s], sum_sem.at[1])
            a.start()
            b.start()
            a.wait()
            b.wait()
            turn_sum[kind, s] += mate_sum[s]
            state["turn", s] = links.send(tile, last_land.at[kind, s, s], to)

    def sums_here(kind, state):
        links.arrive(state["right"], last_land.at[kind, 0, 1], to_right)
        links.arrive(state["left"], last_land.at[kind, 1, 0], to_left)
        links.arrive(state["turn", 0], last_land.at[kind, 0, 0], to_right)
        links.arrive(state["turn", 1], last_land.at[kind, 1, 1], to_left)

    y_state = {}
    for way in (True, False):
        for kind in kinds:
            go_up = upward[kind] == way
            y_state[kind, go_up] = links.send(own_refs[kind], all_refs[kind].at[ep, tp], to_up if go_up else to_down)
    groups = (tp, down, up)
    states = [spread(tp, own_refs)]
    hold = [pltpu.make_async_copy(own_refs[kind], all_refs[kind].at[ep, tp], row_sem.at[kind]) for kind in range(3)]
    for copy in hold:
        copy.start()
    for copy in loads:
        copy.wait()
    stow = [pltpu.make_async_copy(w13, w13_all.at[tp], w_sem.at[0]), pltpu.make_async_copy(w2s, w2_all.at[tp], w_sem.at[1])]
    for copy in stow:
        copy.start()
    earlier[...] = earlier_rows(earlier.shape[0])
    acc13[...] = jnp.zeros_like(acc13)
    acc2[...] = jnp.zeros_like(acc2)

    def y_arrive(kind, way):
        block = all_refs[kind].at[ep, down if way else up]
        links.arrive(y_state[kind, way], block, to_up if way else to_down)
        return block

    pass_on(0)
    for way in (True, False):
        for kind in kinds:
            y_arrive(kind, way)
    send_weights(0)
    send_weights(1)
    for g in (1, 2):
        states.append(spread(groups[g], [ref.at[ep, groups[g]] for ref in all_refs]))
    share(0)
    last(0)
    for copy in hold + stow:
        copy.wait()
    from_mate(0)
    route_copy = pltpu.make_async_copy(r_all.at[:, tp], routes, row_sem.at[0])
    route_copy.start()
    route_copy.wait()
    compute(tp, True)

    pass_weights(0)
    send_weights(2)
    pass_on(1)
    share(1)
    pass_weights(1)
    send_weights(3)
    expert(0)
    pass_on(2)
    share(2)
    pass_weights(2)
    send_weights(4)
    last(1)
    from_mate(1)
    expert(1)
    last(2)
    compute(groups[1], False)
    pass_weights(3)
    expert(2)
    from_mate(2)
    compute(groups[2], False)
    pass_weights(4)
    over_state = send_over()
    expert(3)
    have_weights(own - 1)
    copies = fetch(own - 1)
    forward(own - 1, copies)
    y_sum = sum_up(0)
    share_over(0)
    backward(own - 1, copies)
    dx_sum = sum_up(1)
    turn_sums(0, y_sum)
    share_over(1)
    have_over(0)
    have_over(1)
    start_loads(over, 0)
    half_group(over, 0, False, False)
    share_over(2)
    turn_sums(1, dx_sum)
    share_over(3)
    have_over(2)
    have_over(3)
    start_loads(over, 1)
    half_group(over, 1, False, False)

    def finish(e, carry):
        g_buf[0] = acc13[e, :width, :].T.astype(BF16)
        g_buf[1] = acc13[e, width:, :].T.astype(BF16)
        copies = [pltpu.make_async_copy(g_buf.at[0], g1.at[e], g_sem.at[0]), pltpu.make_async_copy(g_buf.at[1], g3.at[e], g_sem.at[1])]
        xs[0, pl.ds(0, width), :] = acc2[e].astype(BF16)
        copies.append(pltpu.make_async_copy(xs.at[0, pl.ds(0, width)], g2.at[e], g_sem.at[2]))
        for copy in copies:
            copy.start()
        for copy in copies:
            copy.wait()
        return carry

    lax.fori_loop(0, own, finish, 0)
    sums_here(0, y_sum)
    sums_here(1, dx_sum)
    links.drain()


def layer(tokens, d_out, routes, w_one, w_three, w_two, ep_size, tp_size, cap):
    tok, model = tokens.shape
    own, width, _ = w_two.shape
    half = ep_size // 2
    rows = half * cap
    side = model // 2
    vmem, hbm = pl.BlockSpec(memory_space=pltpu.VMEM), pl.BlockSpec(memory_space=pl.ANY)
    shape = jax.ShapeDtypeStruct
    copies = copy_count(own)
    slot_rows = ep_size * tp_size * cap * own
    vector = pltpu.VMEM
    dma = pltpu.SemaphoreType.DMA
    outs = pl.pallas_call(
        functools.partial(layer_kernel, own, cap, width),
        in_specs=[vmem, vmem, vmem, hbm, hbm, hbm],
        out_specs=[hbm] * 15,
        out_shape=[
            shape((ep_size, tp_size, tok, model), BF16),
            shape((ep_size, tp_size, tok, model), BF16),
            shape((ep_size, tp_size) + routes.shape, F32),
            shape((tp_size, own, model, 2 * width), BF16),
            shape((tp_size, own, width, model), BF16),
            shape((own, 2, rows, model), BF16),
            shape((own, 2, rows, model), BF16),
            shape((2, ep_size, own, cap, model), BF16),
            shape((2, 4, 2, tok, side), F32),
            shape((2, 4, 2, tok, side), F32),
            shape((2, 2, tok, side), F32),
            shape((2, 2, 2, tok, side), F32),
            shape((own, model, width), BF16),
            shape((own, model, width), BF16),
            shape((own, width, model), BF16),
        ],
        scratch_shapes=[
            vector((own, model, 2 * width), BF16),
            vector((own, width, model), BF16),
            vector((2, half // 2, tok, model), BF16),
            vector((2, half // 2, tok, model), BF16),
            vector((2, half // 2) + routes.shape, F32),
            vector((ep_size,) + routes.shape, F32),
            vector((tok, tok), BF16),
            vector((own, rows, model), BF16),
            vector((own, rows, model), BF16),
            vector((own, 2 * width, model), F32),
            vector((own, width, model), F32),
            vector((2, model, width), BF16),
            vector((tp_size, model, 2 * width), BF16),
            vector((tp_size, width, model), BF16),
            vector((tp_size, 2 * rows, 2 * width), F32),
            vector((2 * rows, tp_size * width), BF16),
            vector((tp_size, 2 * rows, 2 * width), BF16),
            vector((ep_size, cap, model), BF16),
            vector((ep_size, cap, model), BF16),
            vector((2, own, cap, model), BF16),
            vector((3, own * cap, tok), BF16),
            vector((2, 2, tok, side), F32),
            vector((2, 2, tok, side), F32),
            vector((2, tok, side), F32),
            vector((2, 2, tok, side), F32),
            dma((copies,)),
            dma((copies,)),
            dma((3,)),
            dma((3, 2)),
            dma((3,)),
            dma((2,)),
            dma((3 + tp_size,)),
            dma((2,)),
            dma((2,)),
            dma((3,)),
            dma((3,)),
        ],
        compiler_params=pltpu.CompilerParams(vmem_limit_bytes=VMEM_LIMIT, collective_id=0, has_side_effects=True),
        cost_estimate=pl.CostEstimate(
            flops=2 * slot_rows * model * (2 * tok + 12 * width),
            bytes_accessed=4 * ep_size * tp_size * tok * model,
            transcendentals=0,
        ),
        name="layer",
    )(tokens, d_out, routes, w_one, w_three, w_two)
    return outs[8], outs[11], outs[12:]


def result_kernel(sums, last_land, g1, g3, g2, out, dx, o1, o3, o2, parts, rows, b1, b3, b2, in_sem, out_sem):
    grads = ((g1, b1, o1), (g3, b3, o3), (g2, b2, o2))
    takes = [pltpu.make_async_copy(src, buf, in_sem.at[k]) for k, (src, buf, _) in enumerate(grads)]
    terms = [[pltpu.make_async_copy(sums.at[kind, 3], parts.at[kind, 2], in_sem.at[3 + kind]),
              pltpu.make_async_copy(last_land.at[kind], parts.at[kind, pl.ds(0, 2)], in_sem.at[5 + kind])] for kind in range(2)]
    for copy in terms[0] + terms[1] + takes:
        copy.start()
    puts = []
    side = parts.shape[4]
    for kind, to in ((0, out), (1, dx)):
        for copy in terms[kind]:
            copy.wait()
        for s in range(2):
            total = parts[kind, 2, s] + (parts[kind, 0, s] + parts[kind, 1, s])
            rows[kind, :, s * side : (s + 1) * side] = total.astype(BF16)
        puts.append(pltpu.make_async_copy(rows.at[kind], to, out_sem.at[3 + kind]))
        puts[-1].start()
    for k, (take, (_, buf, to)) in enumerate(zip(takes, grads)):
        take.wait()
        puts.append(pltpu.make_async_copy(buf, to, out_sem.at[k]))
        puts[-1].start()
    for copy in puts:
        copy.wait()


def results(sums, last_land, grads):
    _, _, _, tok, side = sums.shape
    hbm = pl.BlockSpec(memory_space=pl.ANY)
    row = jax.ShapeDtypeStruct((tok, 2 * side), BF16)
    return pl.pallas_call(
        result_kernel,
        in_specs=[hbm] * 5,
        out_specs=[hbm] * 5,
        out_shape=[row, row] + [jax.ShapeDtypeStruct(g.shape, g.dtype) for g in grads],
        scratch_shapes=[pltpu.VMEM((2, 3, 2, tok, side), F32), pltpu.VMEM((2, tok, 2 * side), BF16)]
        + [pltpu.VMEM(g.shape, g.dtype) for g in grads]
        + [pltpu.SemaphoreType.DMA((7,)), pltpu.SemaphoreType.DMA((5,))],
        compiler_params=pltpu.CompilerParams(vmem_limit_bytes=VMEM_LIMIT),
        name="results",
    )(sums, last_land, *grads)


def solution(mesh):
    ep_size, tp_size = mesh.shape["ep"], mesh.shape["tp"]
    row_spec = P(("dp", "ep", "tp"), None)
    col_spec = P("ep", None, "tp")
    down_spec = P("ep", "tp", None)
    grad_col = P(("dp", "ep"), None, "tp")
    grad_down = P(("dp", "ep"), "tp", None)

    def local_step(tokens, expert_ids, gate_vals, w_one, w_three, w_two, d_out):
        cap = slot_count(expert_ids.shape[1], tokens.shape[0], w_one.shape[0] * ep_size)
        routes = jnp.concatenate([expert_ids.T.astype(F32), gate_vals.T], axis=0)
        sums, last_land, grads = layer(tokens, d_out, routes, w_one, w_three, w_two, ep_size, tp_size, cap)
        return tuple(results(sums, last_land, grads))

    return jax.shard_map(local_step, mesh=mesh,
                         in_specs=(row_spec, row_spec, row_spec, col_spec, col_spec, down_spec, row_spec),
                         out_specs=(row_spec, row_spec, grad_col, grad_col, grad_down), check_vma=False)
```

```python
import functools

import jax
import jax.numpy as jnp
from jax import lax
from jax.experimental import pallas as pl
from jax.experimental.pallas import tpu as pltpu
from jax.sharding import PartitionSpec as P

BF16 = jnp.bfloat16
F32 = jnp.float32
MESH = pl.DeviceIdType.MESH
VMEM_LIMIT = 62 * 2**20


def slot_count(num_top, tok_dev, experts):
    return 8 * ((5 * num_top * tok_dev + 32 * experts - 1) // (32 * experts))


def dot(a, b):
    return jnp.dot(a, b, preferred_element_type=F32)


def dot_tb(a, b):
    return lax.dot_general(a, b, (((1,), (1,)), ((), ())), preferred_element_type=F32)


def dot_ta(a, b):
    return lax.dot_general(a, b, (((0,), (0,)), ((), ())), preferred_element_type=F32)


def earlier_rows(tok):
    row = lax.broadcasted_iota(jnp.int32, (tok, tok), 0)
    col = lax.broadcasted_iota(jnp.int32, (tok, tok), 1)
    return jnp.where(row < col, 1.0, 0.0).astype(BF16)


def expert_rows(routes, first, own, earlier):
    top = routes.shape[0] // 2
    ids, gates = routes[:top], routes[top:]
    hits = [ids == (first + e).astype(F32) for e in range(own)]
    routed = jnp.concatenate([jnp.sum(jnp.where(m, 1.0, 0.0), axis=0, keepdims=True) for m in hits], axis=0)
    gate = jnp.concatenate([jnp.sum(jnp.where(m, gates, 0.0), axis=0, keepdims=True) for m in hits], axis=0)
    return jnp.where(routed > 0.0, dot(routed.astype(BF16), earlier), -1.0), gate


def hit_masks(pos, cap):
    slot = lax.broadcasted_iota(jnp.int32, (cap, pos.shape[1]), 0).astype(F32)
    return [pos[e : e + 1, :] == slot for e in range(pos.shape[0])]


def one_hot(masks):
    return jnp.concatenate([jnp.where(m, 1.0, 0.0) for m in masks], axis=0).astype(BF16)


def slot_gates(masks, gate):
    return jnp.concatenate([jnp.where(m, gate[e : e + 1, :], 0.0) for e, m in enumerate(masks)], axis=0)


def three_parts(x):
    hi = x.astype(BF16)
    rest = x - hi.astype(F32)
    mid = rest.astype(BF16)
    return hi, mid, (rest - mid.astype(F32)).astype(BF16)


class Links:
    def __init__(self, send_sem, recv_sem):
        self.send_sem, self.recv_sem, self.sent, self.finished = send_sem, recv_sem, [], set()

    def copy(self, k, src, dst, to):
        return pltpu.make_async_remote_copy(src_ref=src, dst_ref=dst, send_sem=self.send_sem.at[k],
                                            recv_sem=self.recv_sem.at[k], device_id=to, device_id_type=MESH)

    def send(self, src, dst, to):
        k = len(self.sent)
        copy = self.copy(k, src, dst, to)
        copy.start()
        self.sent.append(copy)
        return k

    def arrive(self, k, dst, to):
        self.copy(k, dst, dst, to).wait_recv()

    def finish(self, k):
        self.finished.add(k)
        self.sent[k].wait_send()

    def drain(self):
        for k in range(len(self.sent)):
            if k not in self.finished:
                self.finish(k)


def copy_count(own):
    return 6 + 21 * 3 + 24 + 7 * own + 2 * 10 + 1


def layer_kernel(own, cap, width, tokens, d_out, ids, gate_vals, w1, w3, w2, x_all, dy_all, r_all, w13_all, w2_all, xs_all, us_all,
                 ys_all, sums, mate_land, half_land, last_land, out, g1, g3, g2, x_own, dy_own, r_own, i_own, far_gates, w13, w2s, xb, dyb, rb, routes, earlier, xs, us,
                 acc13, acc2, g_buf, w13e, w2e, ab_buf, h_buf, d_buf, y_buf, v_buf, c_buf, gates_buf, give, keep_sum, far_sum, mate_sum,
                 turn_sum, send_sem, recv_sem, row_sem, load_sem, w_sem, slot_sem, in_sem, out_sem, c_sem, sum_sem, g_sem):
    ep, tp = lax.axis_index("ep"), lax.axis_index("tp")
    eps, tps = x_all.shape[0], x_all.shape[1]
    model = x_all.shape[3]
    side = model // 2
    half = eps // 2
    step = lambda n: lax.rem(ep + (n + eps), eps)
    turn = lambda n: lax.rem(tp + (n + tps), tps)
    right, left, far = step(2), step(-2), step(4)
    mate = ep + 1 - 2 * lax.rem(ep, 2)
    mate_step = lambda n: lax.rem(mate + (n + eps), eps)
    up, down, over = turn(1), turn(-1), turn(2)
    to_right, to_left, to_mate = {"ep": right}, {"ep": left}, {"ep": mate}
    to_up, to_down = {"tp": up}, {"tp": down}
    links = Links(send_sem, recv_sem)
    wide = 512 if model % 512 == 0 else model

    barrier = pltpu.get_barrier_semaphore()
    for to in (to_right, to_left, to_mate, to_up, to_down):
        pl.semaphore_signal(barrier, inc=1, device_id=to, device_id_type=MESH)
    top = ids.shape[0]
    firsts = [pltpu.make_async_copy(ids, i_own, row_sem.at[0]), pltpu.make_async_copy(gate_vals, r_own.at[pl.ds(top, top)], row_sem.at[1]),
              pltpu.make_async_copy(tokens, x_own, row_sem.at[2]), pltpu.make_async_copy(d_out, dy_own, row_sem.at[3])]
    loads = [pltpu.make_async_copy(w1, w13.at[:, :, pl.ds(0, width)], w_sem.at[0]),
             pltpu.make_async_copy(w3, w13.at[:, :, pl.ds(width, width)], w_sem.at[1]),
             pltpu.make_async_copy(w2, w2s, w_sem.at[2])]
    for copy in firsts + loads:
        copy.start()
    firsts[0].wait()
    r_own[0:top] = i_own[...].astype(F32)
    for copy in firsts[1:]:
        copy.wait()
    with jax.named_scope("barrier"):
        pl.semaphore_wait(barrier, 5)

    own_refs, all_refs = (x_own, dy_own, r_own), (x_all, dy_all, r_all)
    upward = (True, False, True)
    kinds = (0, 1, 2)

    def spread(t, srcs):
        out = {}
        for kind in kinds:
            to = to_right if upward[kind] else to_left
            out[kind, upward[kind]] = links.send(srcs[kind], all_refs[kind].at[ep, t], to)
        for kind in kinds:
            to = to_left if upward[kind] else to_right
            out[kind, not upward[kind]] = links.send(srcs[kind], all_refs[kind].at[ep, t], to)
        for kind in kinds:
            out[kind, "mate"] = links.send(srcs[kind], all_refs[kind].at[ep, t], to_mate)
        return out

    def pass_on(g):
        state, t = states[g], groups[g]
        for kind in kinds:
            got, to = (left, to_right) if upward[kind] else (right, to_left)
            block = all_refs[kind].at[got, t]
            links.arrive(state[kind, upward[kind]], block, to)
            state[kind, "far"] = links.send(block, block, to)
            state[kind, "mate1"] = links.send(block, block, to_mate)

    def share(g):
        state, t = states[g], groups[g]
        for kind in kinds:
            got, to = (right, to_left) if upward[kind] else (left, to_right)
            block = all_refs[kind].at[got, t]
            links.arrive(state[kind, not upward[kind]], block, to)
            state[kind, "mate2"] = links.send(block, block, to_mate)

    def last(g):
        state, t = states[g], groups[g]
        for kind in kinds:
            block = all_refs[kind].at[far, t]
            links.arrive(state[kind, "far"], block, to_right if upward[kind] else to_left)
            state[kind, "mate3"] = links.send(block, block, to_mate)

    def from_mate(g):
        state, t = states[g], groups[g]
        for kind in kinds:
            one, two = (mate_step(-2), mate_step(2)) if upward[kind] else (mate_step(2), mate_step(-2))
            for name, at in (("mate", mate), ("mate1", one), ("mate2", two), ("mate3", mate_step(4))):
                links.arrive(state[kind, name], all_refs[kind].at[at, t], to_mate)

    core = lax.rem(ep, 2)

    def send_over():
        return [{kind: links.send(all_refs[kind].at[core + 2 * m, down if upward[kind] else up],
                                  all_refs[kind].at[core + 2 * m, down if upward[kind] else up],
                                  to_up if upward[kind] else to_down) for kind in kinds} for m in range(half)]

    def share_over(m):
        for kind in kinds:
            block = all_refs[kind].at[core + 2 * m, over]
            links.arrive(over_state[m][kind], block, to_up if upward[kind] else to_down)
            over_state[m][kind, "mate"] = links.send(block, block, to_mate)

    def have_over(m):
        for kind in kinds:
            links.arrive(over_state[m][kind, "mate"], all_refs[kind].at[1 - core + 2 * m, over], to_mate)

    cut = 3 * model // 4
    w_state = [None] * own

    def send_weights(e):
        w_state[e] = {(k, s): links.send(ref.at[e], dst.at[tp, e], to)
                      for k, ref, dst in ((0, w13, w13_all), (1, w2s, w2_all)) for s, to in ((True, to_up), (False, to_down))}

    def pass_weights(e):
        state = w_state[e]
        links.arrive(state[0, True], w13_all.at[down, e], to_up)
        head = w13_all.at[down, e, pl.ds(0, cut)]
        state["head"] = links.send(head, head, to_up)
        links.arrive(state[0, False], w13_all.at[up, e], to_down)
        tail = w13_all.at[up, e, pl.ds(cut, model - cut)]
        state["tail"] = links.send(tail, tail, to_down)
        links.arrive(state[1, False], w2_all.at[up, e], to_down)
        state["w2"] = links.send(w2_all.at[up, e], w2_all.at[up, e], to_down)
        links.arrive(state[1, True], w2_all.at[down, e], to_up)

    def have_weights(e):
        state = w_state[e]
        links.arrive(state["head"], w13_all.at[over, e, pl.ds(0, cut)], to_up)
        links.arrive(state["tail"], w13_all.at[over, e, pl.ds(cut, model - cut)], to_down)
        links.arrive(state["w2"], w2_all.at[over, e], to_down)

    def pair_loads(t, h, p):
        at = pl.ds(h * half + p * (half // 2), half // 2)
        return [pltpu.make_async_copy(src.at[at, t], dst.at[p], load_sem.at[k, p])
                for k, (src, dst) in enumerate(((x_all, xb), (dy_all, dyb), (r_all, rb)))]

    def half_group(t, h, keep, ahead):
        for p in range(2):
            for copy in pair_loads(t, h, p):
                copy.wait()

            def gather(b, carry):
                pos, gate = expert_rows(rb[p, b], ep * own, own, earlier[...])
                masks = hit_masks(pos, cap)
                pick = one_hot(masks)
                gates = jnp.sum(slot_gates(masks, gate), axis=1, keepdims=True)
                rows = pl.ds(pl.multiple_of((p * (half // 2) + b) * cap, cap), cap)
                picked = dot(pick, xb[p, b]).astype(BF16)
                for e in range(own):
                    xs[e, rows, :] = picked[e * cap : (e + 1) * cap]
                scaled = (gates * dot(pick, dyb[p, b])).astype(BF16)
                for e in range(own):
                    us[e, rows, :] = scaled[e * cap : (e + 1) * cap]
                return carry

            lax.fori_loop(0, half // 2, gather, 0)

            @pl.when(ahead)
            def _():
                for copy in pair_loads(t, 1, p):
                    copy.start()

        stores = []
        if keep:
            stores = [pltpu.make_async_copy(xs, xs_all.at[:, h], slot_sem.at[0]),
                      pltpu.make_async_copy(us, us_all.at[:, h], slot_sem.at[1])]
        for copy in stores:
            copy.start()

        def expert(e, carry):
            ab = dot(xs[e], w13[e])
            a, b = ab[:, :width], ab[:, width:]
            dh = dot_tb(us[e], w2s[e])
            sig = jax.nn.sigmoid(a)
            silu = a * sig
            hid = (silu * b).astype(BF16)
            da = (dh * b * sig * (1.0 + a * (1.0 - sig))).astype(BF16)
            db = (dh * silu).astype(BF16)
            acc13[e] += dot_ta(jnp.concatenate([da, db], axis=1), xs[e])
            acc2[e] += dot_ta(hid, us[e])
            return carry

        lax.fori_loop(0, own, expert, 0)
        for copy in stores:
            copy.wait()

    def start_loads(t, h):
        for p in range(2):
            for copy in pair_loads(t, h, p):
                copy.start()

    def compute(t, keep):
        start_loads(t, 0)

        def one_half(h, carry):
            half_group(t, h, keep, h == 0)
            return carry

        lax.fori_loop(0, 2, one_half, 0)

    def fetch_rows(e):
        copies = [pltpu.make_async_copy(xs_all.at[e], xs.at[pl.ds(0, 2)], in_sem.at[0]),
                  pltpu.make_async_copy(us_all.at[e], us.at[pl.ds(0, 2)], in_sem.at[1])]
        for copy in copies:
            copy.start()
        return copies

    def fetch(e):
        copies = fetch_rows(e)
        weights = [pltpu.make_async_copy(w13_all.at[j, e], w13e.at[j], in_sem.at[3 + j]) for j in range(tps)]
        weights.append(pltpu.make_async_copy(w2_all.at[:, e], w2e, in_sem.at[2]))
        for copy in weights:
            copy.start()
        return copies + weights[-1:]

    slots = eps * cap
    pending = {}

    def put(name, buf, e, value, at):
        for k in range(eps):
            buf[k, :, at] = value[k * cap : (k + 1) * cap]

    def store_rows(kind, buf, e):
        copy = pltpu.make_async_copy(buf, ys_all.at[kind, :, e], out_sem.at[kind])
        copy.start()
        pending[kind] = copy

    def settle_rows(kind):
        if kind in pending:
            pending.pop(kind).wait()

    def hidden(e, j):
        pltpu.make_async_copy(w13_all.at[j, e], w13e.at[j], in_sem.at[3 + j]).wait()
        ab = dot(xs[0:2].reshape(slots, model), w13e[j])
        ab_buf[j] = ab
        a, b = ab[:, :width], ab[:, width:]
        h_buf[:, pl.ds(pl.multiple_of(j * width, width), width)] = (a * jax.nn.sigmoid(a) * b).astype(BF16)

    def rows_out(e):
        settle_rows(0)

        def columns(n, carry):
            at = pl.ds(pl.multiple_of(n * wide, wide), wide)
            put("y", y_buf, e, dot(h_buf[...], w2e[:, :, at].reshape(tps * width, wide)).astype(BF16), at)
            return carry

        lax.fori_loop(0, model // wide, columns, 0)
        store_rows(0, y_buf, e)

    def forward(e, copies):
        copies[0].wait()

        def shard(j, carry):
            hidden(e, j)
            return carry

        lax.fori_loop(0, tps, shard, 0)
        copies[2].wait()
        rows_out(e)

    def forward_early(e):
        copies = fetch_rows(e)
        for j in (tp, up, down):
            pltpu.make_async_copy(w13_all.at[j, e], w13e.at[j], in_sem.at[3 + j]).start()
        copies[0].wait()

        def shard(i, carry):
            hidden(e, lax.rem(tp + i + i // 2, tps))
            return carry

        lax.fori_loop(0, tps - 1, shard, 0)
        return copies

    def forward_late(e):
        pltpu.make_async_copy(w13_all.at[over, e], w13e.at[over], in_sem.at[3 + over]).start()
        w2_copy = pltpu.make_async_copy(w2_all.at[:, e], w2e, in_sem.at[2])
        w2_copy.start()
        hidden(e, over)
        w2_copy.wait()
        rows_out(e)

    def backward(e, copies):
        copies[1].wait()

        def shard(j, carry):
            dh = dot_tb(us[0:2].reshape(slots, model), w2e[j])
            a, b = ab_buf[j, :, :width], ab_buf[j, :, width:]
            sig = jax.nn.sigmoid(a)
            d_buf[j, :, :width] = (dh * b * sig * (1.0 + a * (1.0 - sig))).astype(BF16)
            d_buf[j, :, width:] = (dh * (a * sig)).astype(BF16)
            return carry

        lax.fori_loop(0, tps, shard, 0)
        settle_rows(1)

        def columns(n, carry):
            at = pl.ds(pl.multiple_of(n * wide, wide), wide)
            v = dot_tb(d_buf[0], w13e[0, at, :])
            for j in range(1, tps):
                v = v + dot_tb(d_buf[j], w13e[j, at, :])
            put("v", v_buf, e, v.astype(BF16), at)
            return carry

        lax.fori_loop(0, model // wide, columns, 0)
        store_rows(1, v_buf, e)

    def expert(e):
        have_weights(e)
        copies = fetch(e)
        forward(e, copies)
        backward(e, copies)

    offsets = (4, 2, -2, 0)

    def row_load(kind, block, slot, first=0, count=None):
        part = pl.ds(first, own if count is None else count)
        return pltpu.make_async_copy(ys_all.at[kind, block, part], c_buf.at[slot, part], c_sem.at[slot])

    def block_parts(kind, block, parts):
        pos, gate = expert_rows(routes[block], ep * own, own, earlier[...])
        masks = hit_masks(pos, cap)
        for k, part in enumerate(three_parts(slot_gates(masks, gate)) if kind == 0 else (one_hot(masks),)):
            parts[k] = part

    def gated(parts, count, first, rows):
        total = None
        for k in reversed(range(count)):
            term = dot_ta(parts[k, first : first + rows.shape[0]], rows)
            total = term if total is None else total + term
        return total

    def columns_of(s):
        return pl.ds(pl.multiple_of(s * side, side), side)

    def combine(kind, block, slot, tile):
        block_parts(kind, block, gates_buf)
        row_load(kind, block, slot).wait()

        def one_side(s, carry):
            tile[s] = gated(gates_buf, 3 if kind == 0 else 1, 0, c_buf[slot, :, :, columns_of(s)].reshape(own * cap, side))
            return carry

        lax.fori_loop(0, 2, one_side, 0)

    early = own - 2
    far_blocks = (mate_step(4), far)
    far_tiles = (give.at[0], far_sum)

    def combine_early():
        for slot, block in enumerate(far_blocks):
            row_load(0, block, slot, 0, early).start()
        for slot, block in enumerate(far_blocks):
            block_parts(0, block, far_gates.at[slot])
            row_load(0, block, slot, 0, early).wait()

            def one_side(s, carry):
                rows = c_buf[slot, 0:early, :, columns_of(s)].reshape(early * cap, side)
                far_tiles[slot][s] = gated(far_gates.at[slot], 3, 0, rows)
                return carry

            lax.fori_loop(0, 2, one_side, 0)

    def load_next():
        settle_rows(0)
        for slot, block in enumerate(far_blocks):
            row_load(0, block, slot, early, 1).start()

    def combine_late(slot, s):
        block = far_blocks[slot]
        rows = jnp.concatenate([c_buf[slot, early, :, columns_of(s)], y_buf[block, :, columns_of(s)]], axis=0)
        far_tiles[slot][s] += gated(far_gates.at[slot], 3, early * cap, rows)

    def sum_up(kind):
        state = {}
        order = [b for o in offsets for b in (mate_step(o), step(o))]

        def one(n, tile):
            if n + 1 < len(order):
                row_load(kind, order[n + 1], (n + 1) % 2).start()
            combine(kind, order[n], n % 2, tile)

        gifts, writes = [], [None]

        def give_block(i):
            if i >= 2:
                if i > 2 or kind == 1:
                    links.finish(gifts[i - 2])
                else:
                    for k in gifts[0]:
                        links.finish(k)
            one(2 * i, give.at[i % 2])
            gifts.append(links.send(give.at[i % 2], mate_land.at[kind, i], to_mate))

        def own_block(i):
            one(2 * i + 1, keep_sum.at[i % 2])

        def send_far(s, to):
            state["far", s] = links.send(far_sum.at[s], half_land.at[kind, s], to)

        def first_blocks():
            if kind == 0:
                for slot in range(2):
                    row_load(0, far_blocks[slot], slot, early, 1).wait()
                pair = []
                for s in range(2):
                    combine_late(0, s)
                    pair.append(links.send(give.at[0, s], mate_sum.at[s], to_mate))
                gifts.append(pair)
                for s in range(2):
                    combine_late(1, s)
                settle_rows(0)
                row_load(kind, order[2], 0).start()
                for s, to in ((0, to_right), (1, to_left)):
                    links.arrive(pair[s], mate_sum.at[s], to_mate)
                    far_sum[s] += mate_sum[s]
                    send_far(s, to)
            else:
                settle_rows(1)
                row_load(kind, order[0], 0).start()
                give_block(0)
                for s in range(2):
                    links.finish(y_sum["far", s])
                one(1, far_sum)

        def first_sum():
            links.arrive(gifts[0], mate_land.at[kind, 0], to_mate)
            copy = pltpu.make_async_copy(mate_land.at[kind, 0], mate_sum, sum_sem.at[0])
            copy.start()
            copy.wait()
            for s, to in ((0, to_right), (1, to_left)):
                far_sum[s] += mate_sum[s]
                send_far(s, to)

        def add_mate(i):
            links.arrive(gifts[i], mate_land.at[kind, i], to_mate)
            copy = pltpu.make_async_copy(mate_land.at[kind, i], mate_sum, sum_sem.at[0])
            copy.start()
            copy.wait()
            keep_sum[i % 2] += mate_sum[...]
            writes.append(pltpu.make_async_copy(keep_sum.at[i % 2], sums.at[kind, i], sum_sem.at[1 + i % 2]))
            writes[i].start()

        def send_sum(i):
            writes[i].wait()
            if i == 1:
                state["right"] = links.send(sums.at[kind, 1, 1], last_land.at[kind, 0, 1], to_right)
            elif i == 2:
                state["left"] = links.send(sums.at[kind, 2, 0], last_land.at[kind, 1, 0], to_left)

        with jax.named_scope("first_blocks"):
            first_blocks()
        with jax.named_scope("give_block_1"):
            give_block(1)
        if kind == 1:
            with jax.named_scope("first_sum"):
                first_sum()
        with jax.named_scope("own_block_1"):
            own_block(1)
        with jax.named_scope("give_block_2"):
            give_block(2)
        with jax.named_scope("add_mate_1"):
            add_mate(1)
        with jax.named_scope("own_block_2"):
            own_block(2)
        with jax.named_scope("send_sum_1"):
            send_sum(1)
        with jax.named_scope("give_block_3"):
            give_block(3)
        with jax.named_scope("add_mate_2"):
            add_mate(2)
        with jax.named_scope("own_block_3"):
            own_block(3)
        with jax.named_scope("send_sum_2"):
            send_sum(2)
        with jax.named_scope("add_mate_3"):
            add_mate(3)
        with jax.named_scope("send_sum_3"):
            send_sum(3)
        links.finish(gifts[2])
        links.finish(gifts[3])
        return state

    def turn_sums(kind, state):
        for s, to in ((0, to_right), (1, to_left)):
            links.arrive(state["far", s], half_land.at[kind, s], to)
            tile = turn_sum.at[kind, s]
            a = pltpu.make_async_copy(sums.at[kind, 1 + s, s], tile, sum_sem.at[0])
            b = pltpu.make_async_copy(half_land.at[kind, s], mate_sum.at[s], sum_sem.at[1])
            a.start()
            b.start()
            a.wait()
            b.wait()
            turn_sum[kind, s] += mate_sum[s]
            state["turn", s] = links.send(tile, last_land.at[kind, s, s], to)

    def direct_here(kind, state):
        links.arrive(state["right"], last_land.at[kind, 0, 1], to_right)
        links.arrive(state["left"], last_land.at[kind, 1, 0], to_left)

    def turned_here(kind, state):
        links.arrive(state["turn", 0], last_land.at[kind, 0, 0], to_right)
        links.arrive(state["turn", 1], last_land.at[kind, 1, 1], to_left)

    def add_direct(kind):
        copies = [pltpu.make_async_copy(sums.at[kind, 3], keep_sum.at[0], sum_sem.at[0]),
                  pltpu.make_async_copy(last_land.at[kind, 1, 0], mate_sum.at[0], sum_sem.at[1]),
                  pltpu.make_async_copy(last_land.at[kind, 0, 1], mate_sum.at[1], sum_sem.at[2])]
        for copy in copies:
            copy.start()
        for copy in copies:
            copy.wait()
        keep_sum[0] += mate_sum[...]

    def finish_out():
        add_direct(0)
        copies = [pltpu.make_async_copy(last_land.at[0, s, s], mate_sum.at[s], sum_sem.at[s]) for s in range(2)]
        for copy in copies:
            copy.start()
        for s in range(2):
            copies[s].wait()
            xb[0, 0, :, s * side : (s + 1) * side] = (keep_sum[0, s] + mate_sum[s]).astype(BF16)
        copy = pltpu.make_async_copy(xb.at[0, 0], out, sum_sem.at[0])
        copy.start()
        copy.wait()

    def fold_dx():
        add_direct(1)
        copy = pltpu.make_async_copy(keep_sum.at[0], sums.at[1, 3], sum_sem.at[0])
        copy.start()
        copy.wait()

    y_state = {}
    for way in (True, False):
        for kind in kinds:
            go_up = upward[kind] == way
            y_state[kind, go_up] = links.send(own_refs[kind], all_refs[kind].at[ep, tp], to_up if go_up else to_down)
    groups = (tp, down, up)
    states = [spread(tp, own_refs)]
    hold = [pltpu.make_async_copy(own_refs[kind], all_refs[kind].at[ep, tp], row_sem.at[kind]) for kind in range(3)]
    for copy in hold:
        copy.start()
    for copy in loads:
        copy.wait()
    stow = [pltpu.make_async_copy(w13, w13_all.at[tp], w_sem.at[0]), pltpu.make_async_copy(w2s, w2_all.at[tp], w_sem.at[1])]
    for copy in stow:
        copy.start()
    earlier[...] = earlier_rows(earlier.shape[0])
    with jax.named_scope("zeros"):
        acc13[...] = jnp.zeros_like(acc13)
        acc2[...] = jnp.zeros_like(acc2)

    def y_arrive(kind, way):
        block = all_refs[kind].at[ep, down if way else up]
        links.arrive(y_state[kind, way], block, to_up if way else to_down)
        return block

    with jax.named_scope("pass_on_0"):
        pass_on(0)
    with jax.named_scope("y_arrive"):
        for way in (True, False):
            for kind in kinds:
                y_arrive(kind, way)
    with jax.named_scope("send_weights_0"):
        send_weights(0)
    with jax.named_scope("send_weights_1"):
        send_weights(1)
    for g in (1, 2):
        states.append(spread(groups[g], [ref.at[ep, groups[g]] for ref in all_refs]))
    with jax.named_scope("share_0"):
        share(0)
    with jax.named_scope("last_0"):
        last(0)
    for copy in hold + stow:
        copy.wait()
    with jax.named_scope("from_mate_0"):
        from_mate(0)
    route_copy = pltpu.make_async_copy(r_all.at[:, tp], routes, row_sem.at[0])
    route_copy.start()
    route_copy.wait()
    with jax.named_scope("compute_tp_True"):
        compute(tp, True)

    with jax.named_scope("pass_weights_0"):
        pass_weights(0)
    with jax.named_scope("send_weights_2"):
        send_weights(2)
    with jax.named_scope("pass_on_1"):
        pass_on(1)
    with jax.named_scope("share_1"):
        share(1)
    with jax.named_scope("pass_weights_1"):
        pass_weights(1)
    with jax.named_scope("send_weights_3"):
        send_weights(3)
    with jax.named_scope("expert_0"):
        expert(0)
    with jax.named_scope("pass_on_2"):
        pass_on(2)
    with jax.named_scope("share_2"):
        share(2)
    with jax.named_scope("pass_weights_2"):
        pass_weights(2)
    with jax.named_scope("send_weights_4"):
        send_weights(4)
    with jax.named_scope("last_1"):
        last(1)
    with jax.named_scope("from_mate_1"):
        from_mate(1)
    with jax.named_scope("expert_1"):
        expert(1)
    with jax.named_scope("last_2"):
        last(2)
    with jax.named_scope("compute_groups_1_False"):
        compute(groups[1], False)
    with jax.named_scope("pass_weights_3"):
        pass_weights(3)
    with jax.named_scope("expert_2"):
        expert(2)
    with jax.named_scope("from_mate_2"):
        from_mate(2)
    with jax.named_scope("compute_groups_2_False"):
        compute(groups[2], False)
    with jax.named_scope("pass_weights_4"):
        pass_weights(4)
    with jax.named_scope("send_over_"):
        over_state = send_over()
    with jax.named_scope("combine_early"):
        settle_rows(0)
        combine_early()
    with jax.named_scope("expert_3"):
        expert(3)
    with jax.named_scope("forward_early"):
        load_next()
        copies = forward_early(own - 1)
    with jax.named_scope("have_weights_own_1"):
        have_weights(own - 1)
    with jax.named_scope("forward_late"):
        forward_late(own - 1)
    with jax.named_scope("sum_up_0"):
        y_sum = sum_up(0)
    with jax.named_scope("share_over_0"):
        share_over(0)
    with jax.named_scope("backward_own_1_copies"):
        backward(own - 1, copies)
    with jax.named_scope("sum_up_1"):
        dx_sum = sum_up(1)
    with jax.named_scope("turn_sums_0_y_sum"):
        turn_sums(0, y_sum)
    with jax.named_scope("share_over_1"):
        share_over(1)
    with jax.named_scope("have_over_1"):
        have_over(0)
        have_over(1)
    with jax.named_scope("half_group_over_0"):
        start_loads(over, 0)
        half_group(over, 0, False, False)
    with jax.named_scope("share_over_2"):
        share_over(2)
    with jax.named_scope("turn_sums_1_dx_sum"):
        turn_sums(1, dx_sum)
    with jax.named_scope("share_over_3"):
        share_over(3)
    with jax.named_scope("have_over_3"):
        have_over(2)
        have_over(3)
    with jax.named_scope("half_group_over_1"):
        start_loads(over, 1)
        half_group(over, 1, False, False)

    def finish(e, carry):
        g_buf[0] = acc13[e, :width, :].T.astype(BF16)
        g_buf[1] = acc13[e, width:, :].T.astype(BF16)
        copies = [pltpu.make_async_copy(g_buf.at[0], g1.at[e], g_sem.at[0]), pltpu.make_async_copy(g_buf.at[1], g3.at[e], g_sem.at[1])]
        xs[0, pl.ds(0, width), :] = acc2[e].astype(BF16)
        copies.append(pltpu.make_async_copy(xs.at[0, pl.ds(0, width)], g2.at[e], g_sem.at[2]))
        for copy in copies:
            copy.start()
        for copy in copies:
            copy.wait()
        return carry

    with jax.named_scope("finish"):
        lax.fori_loop(0, own, finish, 0)
    with jax.named_scope("direct_here"):
        direct_here(0, y_sum)
        direct_here(1, dx_sum)
    with jax.named_scope("fold_dx"):
        fold_dx()
    with jax.named_scope("turned_here_0"):
        turned_here(0, y_sum)
    with jax.named_scope("finish_out"):
        finish_out()
    with jax.named_scope("turned_here_1"):
        turned_here(1, dx_sum)
    with jax.named_scope("drain"):
        links.drain()


def layer(tokens, d_out, ids, gate_vals, w_one, w_three, w_two, ep_size, tp_size, cap):
    tok, model = tokens.shape
    own, width, _ = w_two.shape
    half = ep_size // 2
    rows = half * cap
    side = model // 2
    hbm = pl.BlockSpec(memory_space=pl.ANY)
    shape = jax.ShapeDtypeStruct
    routes = (2 * ids.shape[0], tok)
    copies = copy_count(own)
    slot_rows = ep_size * tp_size * cap * own
    vector = pltpu.VMEM
    dma = pltpu.SemaphoreType.DMA
    outs = pl.pallas_call(
        functools.partial(layer_kernel, own, cap, width),
        in_specs=[hbm] * 7,
        out_specs=[hbm] * 16,
        out_shape=[
            shape((ep_size, tp_size, tok, model), BF16),
            shape((ep_size, tp_size, tok, model), BF16),
            shape((ep_size, tp_size) + routes, F32),
            shape((tp_size, own, model, 2 * width), BF16),
            shape((tp_size, own, width, model), BF16),
            shape((own, 2, rows, model), BF16),
            shape((own, 2, rows, model), BF16),
            shape((2, ep_size, own, cap, model), BF16),
            shape((2, 4, 2, tok, side), F32),
            shape((2, 4, 2, tok, side), F32),
            shape((2, 2, tok, side), F32),
            shape((2, 2, 2, tok, side), F32),
            shape((tok, model), BF16),
            shape((own, model, width), BF16),
            shape((own, model, width), BF16),
            shape((own, width, model), BF16),
        ],
        scratch_shapes=[
            vector((tok, model), BF16),
            vector((tok, model), BF16),
            vector(routes, F32),
            vector(ids.shape, jnp.int32),
            vector((2, 3, own * cap, tok), BF16),
            vector((own, model, 2 * width), BF16),
            vector((own, width, model), BF16),
            vector((2, half // 2, tok, model), BF16),
            vector((2, half // 2, tok, model), BF16),
            vector((2, half // 2) + routes, F32),
            vector((ep_size,) + routes, F32),
            vector((tok, tok), BF16),
            vector((own, rows, model), BF16),
            vector((own, rows, model), BF16),
            vector((own, 2 * width, model), F32),
            vector((own, width, model), F32),
            vector((2, model, width), BF16),
            vector((tp_size, model, 2 * width), BF16),
            vector((tp_size, width, model), BF16),
            vector((tp_size, 2 * rows, 2 * width), F32),
            vector((2 * rows, tp_size * width), BF16),
            vector((tp_size, 2 * rows, 2 * width), BF16),
            vector((ep_size, cap, model), BF16),
            vector((ep_size, cap, model), BF16),
            vector((2, own, cap, model), BF16),
            vector((3, own * cap, tok), BF16),
            vector((2, 2, tok, side), F32),
            vector((2, 2, tok, side), F32),
            vector((2, tok, side), F32),
            vector((2, tok, side), F32),
            vector((2, 2, tok, side), F32),
            dma((copies,)),
            dma((copies,)),
            dma((4,)),
            dma((3, 2)),
            dma((3,)),
            dma((2,)),
            dma((3 + tp_size,)),
            dma((2,)),
            dma((2,)),
            dma((3,)),
            dma((3,)),
        ],
        compiler_params=pltpu.CompilerParams(vmem_limit_bytes=VMEM_LIMIT, collective_id=0, has_side_effects=True),
        cost_estimate=pl.CostEstimate(
            flops=2 * slot_rows * model * (2 * tok + 12 * width),
            bytes_accessed=4 * ep_size * tp_size * tok * model,
            transcendentals=0,
        ),
        name="layer",
    )(tokens, d_out, ids, gate_vals, w_one, w_three, w_two)
    return outs[8], outs[11], outs[12], outs[13:]


def result_kernel(sums, last_land, rows_in, g1, g3, g2, out, dx, o1, o3, o2, parts, rows, row_buf, b1, b3, b2, in_sem, out_sem):
    moves = ((g1, b1, o1), (g3, b3, o3), (g2, b2, o2), (rows_in, row_buf, out))
    takes = [pltpu.make_async_copy(src, buf, in_sem.at[k]) for k, (src, buf, _) in enumerate(moves)]
    terms = [pltpu.make_async_copy(sums.at[1, 3], parts.at[0], in_sem.at[4])]
    terms += [pltpu.make_async_copy(last_land.at[1, s, s], parts.at[1, s], in_sem.at[5 + s]) for s in range(2)]
    for copy in terms + takes:
        copy.start()
    for copy in terms:
        copy.wait()
    side = parts.shape[3]
    for s in range(2):
        rows[:, s * side : (s + 1) * side] = (parts[0, s] + parts[1, s]).astype(BF16)
    puts = [pltpu.make_async_copy(rows, dx, out_sem.at[4])]
    puts[0].start()
    for k, (take, (_, buf, to)) in enumerate(zip(takes, moves)):
        take.wait()
        puts.append(pltpu.make_async_copy(buf, to, out_sem.at[k]))
        puts[-1].start()
    for copy in puts:
        copy.wait()


def results(sums, last_land, out, grads):
    _, _, _, tok, side = sums.shape
    hbm = pl.BlockSpec(memory_space=pl.ANY)
    row = jax.ShapeDtypeStruct((tok, 2 * side), BF16)
    rows = pltpu.VMEM((tok, 2 * side), BF16)
    return pl.pallas_call(
        result_kernel,
        in_specs=[hbm] * 6,
        out_specs=[hbm] * 5,
        out_shape=[row, row] + [jax.ShapeDtypeStruct(g.shape, g.dtype) for g in grads],
        scratch_shapes=[pltpu.VMEM((2, 2, tok, side), F32), rows, rows]
        + [pltpu.VMEM(g.shape, g.dtype) for g in grads]
        + [pltpu.SemaphoreType.DMA((7,)), pltpu.SemaphoreType.DMA((5,))],
        compiler_params=pltpu.CompilerParams(vmem_limit_bytes=VMEM_LIMIT),
        name="results",
    )(sums, last_land, out, *grads)


def solution(mesh):
    ep_size, tp_size = mesh.shape["ep"], mesh.shape["tp"]
    row_spec = P(("dp", "ep", "tp"), None)
    col_spec = P("ep", None, "tp")
    down_spec = P("ep", "tp", None)
    grad_col = P(("dp", "ep"), None, "tp")
    grad_down = P(("dp", "ep"), "tp", None)

    def local_step(tokens, expert_ids, gate_vals, w_one, w_three, w_two, d_out):
        cap = slot_count(expert_ids.shape[1], tokens.shape[0], w_one.shape[0] * ep_size)
        sums, last_land, out, grads = layer(tokens, d_out, expert_ids.T, gate_vals.T, w_one, w_three, w_two, ep_size, tp_size, cap)
        return tuple(results(sums, last_land, out, grads))

    return jax.shard_map(local_step, mesh=mesh,
                         in_specs=(row_spec, row_spec, row_spec, col_spec, col_spec, down_spec, row_spec),
                         out_specs=(row_spec, row_spec, grad_col, grad_col, grad_down), check_vma=False)
```

```python
import functools

import jax
import jax.numpy as jnp
from jax import lax
from jax.experimental import pallas as pl
from jax.experimental.pallas import tpu as pltpu
from jax.sharding import PartitionSpec as P

BF16 = jnp.bfloat16
F32 = jnp.float32
MESH = pl.DeviceIdType.MESH
VMEM_LIMIT = 62 * 2**20


def slot_count(num_top, tok_dev, experts):
    return 8 * ((5 * num_top * tok_dev + 32 * experts - 1) // (32 * experts))


def dot(a, b):
    return jnp.dot(a, b, preferred_element_type=F32)


def dot_tb(a, b):
    return lax.dot_general(a, b, (((1,), (1,)), ((), ())), preferred_element_type=F32)


def dot_ta(a, b):
    return lax.dot_general(a, b, (((0,), (0,)), ((), ())), preferred_element_type=F32)


def earlier_rows(tok):
    row = lax.broadcasted_iota(jnp.int32, (tok, tok), 0)
    col = lax.broadcasted_iota(jnp.int32, (tok, tok), 1)
    return jnp.where(row < col, 1.0, 0.0).astype(BF16)


def expert_rows(routes, first, own, earlier):
    top = routes.shape[0] // 2
    ids, gates = routes[:top], routes[top:]
    hits = [ids == (first + e).astype(F32) for e in range(own)]
    routed = jnp.concatenate([jnp.sum(jnp.where(m, 1.0, 0.0), axis=0, keepdims=True) for m in hits], axis=0)
    gate = jnp.concatenate([jnp.sum(jnp.where(m, gates, 0.0), axis=0, keepdims=True) for m in hits], axis=0)
    return jnp.where(routed > 0.0, dot(routed.astype(BF16), earlier), -1.0), gate


def hit_masks(pos, cap):
    slot = lax.broadcasted_iota(jnp.int32, (cap, pos.shape[1]), 0).astype(F32)
    return [pos[e : e + 1, :] == slot for e in range(pos.shape[0])]


def one_hot(masks):
    return jnp.concatenate([jnp.where(m, 1.0, 0.0) for m in masks], axis=0).astype(BF16)


def slot_gates(masks, gate):
    return jnp.concatenate([jnp.where(m, gate[e : e + 1, :], 0.0) for e, m in enumerate(masks)], axis=0)


def three_parts(x):
    hi = x.astype(BF16)
    rest = x - hi.astype(F32)
    mid = rest.astype(BF16)
    return hi, mid, (rest - mid.astype(F32)).astype(BF16)


class Links:
    def __init__(self, send_sem, recv_sem):
        self.send_sem, self.recv_sem, self.sent, self.finished = send_sem, recv_sem, [], set()

    def copy(self, k, src, dst, to):
        return pltpu.make_async_remote_copy(src_ref=src, dst_ref=dst, send_sem=self.send_sem.at[k],
                                            recv_sem=self.recv_sem.at[k], device_id=to, device_id_type=MESH)

    def send(self, src, dst, to):
        k = len(self.sent)
        copy = self.copy(k, src, dst, to)
        copy.start()
        self.sent.append(copy)
        return k

    def arrive(self, k, dst, to):
        self.copy(k, dst, dst, to).wait_recv()

    def finish(self, k):
        self.finished.add(k)
        self.sent[k].wait_send()

    def drain(self):
        for k in range(len(self.sent)):
            if k not in self.finished:
                self.finish(k)


def copy_count(own):
    return 6 + 21 * 3 + 24 + 7 * own + 2 * 10 + 1


def layer_kernel(own, cap, width, tokens, d_out, ids, gate_vals, w1, w3, w2, x_all, dy_all, r_all, w13_all, w2_all, xs_all, us_all,
                 ys_all, sums, mate_land, half_land, last_land, out, g1, g3, g2, x_own, dy_own, r_own, i_own, far_gates, w13, w2s, xb, dyb, rb, routes, earlier, xs, us,
                 acc13, acc2, g_buf, w13e, w2e, ab_buf, h_buf, d_buf, y_buf, v_buf, c_buf, gates_buf, give, keep_sum, far_sum, mate_sum,
                 turn_sum, send_sem, recv_sem, row_sem, load_sem, w_sem, slot_sem, in_sem, out_sem, c_sem, sum_sem, g_sem):
    ep, tp = lax.axis_index("ep"), lax.axis_index("tp")
    eps, tps = x_all.shape[0], x_all.shape[1]
    model = x_all.shape[3]
    side = model // 2
    half = eps // 2
    step = lambda n: lax.rem(ep + (n + eps), eps)
    turn = lambda n: lax.rem(tp + (n + tps), tps)
    right, left, far = step(2), step(-2), step(4)
    mate = ep + 1 - 2 * lax.rem(ep, 2)
    mate_step = lambda n: lax.rem(mate + (n + eps), eps)
    up, down, over = turn(1), turn(-1), turn(2)
    to_right, to_left, to_mate = {"ep": right}, {"ep": left}, {"ep": mate}
    to_up, to_down = {"tp": up}, {"tp": down}
    links = Links(send_sem, recv_sem)
    wide = 512 if model % 512 == 0 else model

    barrier = pltpu.get_barrier_semaphore()
    for to in (to_right, to_left, to_mate, to_up, to_down):
        pl.semaphore_signal(barrier, inc=1, device_id=to, device_id_type=MESH)
    top = ids.shape[0]
    firsts = [pltpu.make_async_copy(ids, i_own, row_sem.at[0]), pltpu.make_async_copy(gate_vals, r_own.at[pl.ds(top, top)], row_sem.at[1]),
              pltpu.make_async_copy(tokens, x_own, row_sem.at[2]), pltpu.make_async_copy(d_out, dy_own, row_sem.at[3])]
    loads = [pltpu.make_async_copy(w1, w13.at[:, :, pl.ds(0, width)], w_sem.at[0]),
             pltpu.make_async_copy(w3, w13.at[:, :, pl.ds(width, width)], w_sem.at[1]),
             pltpu.make_async_copy(w2, w2s, w_sem.at[2])]
    for copy in firsts + loads:
        copy.start()
    firsts[0].wait()
    r_own[0:top] = i_own[...].astype(F32)
    for copy in firsts[1:]:
        copy.wait()
    with jax.named_scope("barrier"):
        pl.semaphore_wait(barrier, 5)

    own_refs, all_refs = (x_own, dy_own, r_own), (x_all, dy_all, r_all)
    upward = (True, False, True)
    kinds = (0, 1, 2)

    def spread(t, srcs):
        out = {}
        for kind in kinds:
            to = to_right if upward[kind] else to_left
            out[kind, upward[kind]] = links.send(srcs[kind], all_refs[kind].at[ep, t], to)
        for kind in kinds:
            to = to_left if upward[kind] else to_right
            out[kind, not upward[kind]] = links.send(srcs[kind], all_refs[kind].at[ep, t], to)
        for kind in kinds:
            out[kind, "mate"] = links.send(srcs[kind], all_refs[kind].at[ep, t], to_mate)
        return out

    def pass_on(g):
        state, t = states[g], groups[g]
        for kind in kinds:
            got, to = (left, to_right) if upward[kind] else (right, to_left)
            block = all_refs[kind].at[got, t]
            links.arrive(state[kind, upward[kind]], block, to)
            state[kind, "far"] = links.send(block, block, to)
            state[kind, "mate1"] = links.send(block, block, to_mate)

    def share(g):
        state, t = states[g], groups[g]
        for kind in kinds:
            got, to = (right, to_left) if upward[kind] else (left, to_right)
            block = all_refs[kind].at[got, t]
            links.arrive(state[kind, not upward[kind]], block, to)
            state[kind, "mate2"] = links.send(block, block, to_mate)

    def last(g):
        state, t = states[g], groups[g]
        for kind in kinds:
            block = all_refs[kind].at[far, t]
            links.arrive(state[kind, "far"], block, to_right if upward[kind] else to_left)
            state[kind, "mate3"] = links.send(block, block, to_mate)

    def from_mate(g):
        state, t = states[g], groups[g]
        for kind in kinds:
            one, two = (mate_step(-2), mate_step(2)) if upward[kind] else (mate_step(2), mate_step(-2))
            for name, at in (("mate", mate), ("mate1", one), ("mate2", two), ("mate3", mate_step(4))):
                links.arrive(state[kind, name], all_refs[kind].at[at, t], to_mate)

    core = lax.rem(ep, 2)

    def send_over():
        return [{kind: links.send(all_refs[kind].at[core + 2 * m, down if upward[kind] else up],
                                  all_refs[kind].at[core + 2 * m, down if upward[kind] else up],
                                  to_up if upward[kind] else to_down) for kind in kinds} for m in range(half)]

    def share_over(m):
        for kind in kinds:
            block = all_refs[kind].at[core + 2 * m, over]
            links.arrive(over_state[m][kind], block, to_up if upward[kind] else to_down)
            over_state[m][kind, "mate"] = links.send(block, block, to_mate)

    def have_over(m):
        for kind in kinds:
            links.arrive(over_state[m][kind, "mate"], all_refs[kind].at[1 - core + 2 * m, over], to_mate)

    cut = 3 * model // 4
    w_state = [None] * own

    def send_weights(e):
        w_state[e] = {(k, s): links.send(ref.at[e], dst.at[tp, e], to)
                      for k, ref, dst in ((0, w13, w13_all), (1, w2s, w2_all)) for s, to in ((True, to_up), (False, to_down))}

    def pass_weights(e):
        state = w_state[e]
        links.arrive(state[0, True], w13_all.at[down, e], to_up)
        head = w13_all.at[down, e, pl.ds(0, cut)]
        state["head"] = links.send(head, head, to_up)
        links.arrive(state[0, False], w13_all.at[up, e], to_down)
        tail = w13_all.at[up, e, pl.ds(cut, model - cut)]
        state["tail"] = links.send(tail, tail, to_down)
        links.arrive(state[1, False], w2_all.at[up, e], to_down)
        state["w2"] = links.send(w2_all.at[up, e], w2_all.at[up, e], to_down)
        links.arrive(state[1, True], w2_all.at[down, e], to_up)

    def have_weights(e):
        state = w_state[e]
        links.arrive(state["head"], w13_all.at[over, e, pl.ds(0, cut)], to_up)
        links.arrive(state["tail"], w13_all.at[over, e, pl.ds(cut, model - cut)], to_down)
        links.arrive(state["w2"], w2_all.at[over, e], to_down)

    def pair_loads(t, h, p):
        at = pl.ds(h * half + p * (half // 2), half // 2)
        return [pltpu.make_async_copy(src.at[at, t], dst.at[p], load_sem.at[k, p])
                for k, (src, dst) in enumerate(((x_all, xb), (dy_all, dyb), (r_all, rb)))]

    def half_group(t, h, keep, ahead):
        for p in range(2):
            for copy in pair_loads(t, h, p):
                copy.wait()

            def gather(b, carry):
                pos, gate = expert_rows(rb[p, b], ep * own, own, earlier[...])
                masks = hit_masks(pos, cap)
                pick = one_hot(masks)
                gates = jnp.sum(slot_gates(masks, gate), axis=1, keepdims=True)
                rows = pl.ds(pl.multiple_of((p * (half // 2) + b) * cap, cap), cap)
                picked = dot(pick, xb[p, b]).astype(BF16)
                for e in range(own):
                    xs[e, rows, :] = picked[e * cap : (e + 1) * cap]
                scaled = (gates * dot(pick, dyb[p, b])).astype(BF16)
                for e in range(own):
                    us[e, rows, :] = scaled[e * cap : (e + 1) * cap]
                return carry

            lax.fori_loop(0, half // 2, gather, 0)

            @pl.when(ahead)
            def _():
                for copy in pair_loads(t, 1, p):
                    copy.start()

        stores = []
        if keep:
            stores = [pltpu.make_async_copy(xs, xs_all.at[:, h], slot_sem.at[0]),
                      pltpu.make_async_copy(us, us_all.at[:, h], slot_sem.at[1])]
        for copy in stores:
            copy.start()

        def expert(e, carry):
            ab = dot(xs[e], w13[e])
            a, b = ab[:, :width], ab[:, width:]
            dh = dot_tb(us[e], w2s[e])
            sig = jax.nn.sigmoid(a)
            silu = a * sig
            hid = (silu * b).astype(BF16)
            da = (dh * b * sig * (1.0 + a * (1.0 - sig))).astype(BF16)
            db = (dh * silu).astype(BF16)
            acc13[e] += dot_ta(jnp.concatenate([da, db], axis=1), xs[e])
            acc2[e] += dot_ta(hid, us[e])
            return carry

        lax.fori_loop(0, own, expert, 0)
        for copy in stores:
            copy.wait()

    def start_loads(t, h):
        for p in range(2):
            for copy in pair_loads(t, h, p):
                copy.start()

    def compute(t, keep):
        start_loads(t, 0)

        def one_half(h, carry):
            half_group(t, h, keep, h == 0)
            return carry

        lax.fori_loop(0, 2, one_half, 0)

    def fetch_rows(e):
        copies = [pltpu.make_async_copy(xs_all.at[e], xs.at[pl.ds(0, 2)], in_sem.at[0]),
                  pltpu.make_async_copy(us_all.at[e], us.at[pl.ds(0, 2)], in_sem.at[1])]
        for copy in copies:
            copy.start()
        return copies

    def fetch(e):
        copies = fetch_rows(e)
        weights = [pltpu.make_async_copy(w13_all.at[j, e], w13e.at[j], in_sem.at[3 + j]) for j in range(tps)]
        weights.append(pltpu.make_async_copy(w2_all.at[:, e], w2e, in_sem.at[2]))
        for copy in weights:
            copy.start()
        return copies + weights[-1:]

    slots = eps * cap
    pending = {}

    def put(name, buf, e, value, at):
        for k in range(eps):
            buf[k, :, at] = value[k * cap : (k + 1) * cap]

    def store_rows(kind, buf, e):
        copy = pltpu.make_async_copy(buf, ys_all.at[kind, :, e], out_sem.at[kind])
        copy.start()
        pending[kind] = copy

    def settle_rows(kind):
        if kind in pending:
            pending.pop(kind).wait()

    def hidden(e, j):
        pltpu.make_async_copy(w13_all.at[j, e], w13e.at[j], in_sem.at[3 + j]).wait()
        ab = dot(xs[0:2].reshape(slots, model), w13e[j])
        ab_buf[j] = ab
        a, b = ab[:, :width], ab[:, width:]
        h_buf[:, pl.ds(pl.multiple_of(j * width, width), width)] = (a * jax.nn.sigmoid(a) * b).astype(BF16)

    def rows_out(e):
        settle_rows(0)

        def columns(n, carry):
            at = pl.ds(pl.multiple_of(n * wide, wide), wide)
            put("y", y_buf, e, dot(h_buf[...], w2e[:, :, at].reshape(tps * width, wide)).astype(BF16), at)
            return carry

        lax.fori_loop(0, model // wide, columns, 0)
        store_rows(0, y_buf, e)

    def forward(e, copies):
        copies[0].wait()

        def shard(j, carry):
            hidden(e, j)
            return carry

        lax.fori_loop(0, tps, shard, 0)
        copies[2].wait()
        rows_out(e)

    def forward_early(e):
        copies = fetch_rows(e)
        for j in (tp, up, down):
            pltpu.make_async_copy(w13_all.at[j, e], w13e.at[j], in_sem.at[3 + j]).start()
        downs = [pltpu.make_async_copy(w2_all.at[j, e], w2e.at[j], in_sem.at[2]) for j in (tp, up, down)]
        copies[0].wait()

        def shard(i, carry):
            hidden(e, lax.rem(tp + i + i // 2, tps))
            return carry

        lax.fori_loop(0, tps - 1, shard, 0)
        for copy in downs:
            copy.start()
            copy.wait()
        return copies

    def forward_late(e):
        pltpu.make_async_copy(w13_all.at[over, e], w13e.at[over], in_sem.at[3 + over]).start()
        w2_copy = pltpu.make_async_copy(w2_all.at[over, e], w2e.at[over], in_sem.at[2])
        w2_copy.start()
        hidden(e, over)
        w2_copy.wait()
        rows_out(e)

    def backward(e, copies):
        copies[1].wait()

        def shard(j, carry):
            dh = dot_tb(us[0:2].reshape(slots, model), w2e[j])
            a, b = ab_buf[j, :, :width], ab_buf[j, :, width:]
            sig = jax.nn.sigmoid(a)
            d_buf[j, :, :width] = (dh * b * sig * (1.0 + a * (1.0 - sig))).astype(BF16)
            d_buf[j, :, width:] = (dh * (a * sig)).astype(BF16)
            return carry

        lax.fori_loop(0, tps, shard, 0)
        settle_rows(1)

        def columns(n, carry):
            at = pl.ds(pl.multiple_of(n * wide, wide), wide)
            v = dot_tb(d_buf[0], w13e[0, at, :])
            for j in range(1, tps):
                v = v + dot_tb(d_buf[j], w13e[j, at, :])
            put("v", v_buf, e, v.astype(BF16), at)
            return carry

        lax.fori_loop(0, model // wide, columns, 0)
        store_rows(1, v_buf, e)

    def expert(e):
        have_weights(e)
        copies = fetch(e)
        forward(e, copies)
        backward(e, copies)

    offsets = (4, 2, -2, 0)

    def row_load(kind, block, slot, first=0, count=None):
        part = pl.ds(first, own if count is None else count)
        return pltpu.make_async_copy(ys_all.at[kind, block, part], c_buf.at[slot, part], c_sem.at[slot])

    def block_parts(kind, block, parts):
        pos, gate = expert_rows(routes[block], ep * own, own, earlier[...])
        masks = hit_masks(pos, cap)
        for k, part in enumerate(three_parts(slot_gates(masks, gate)) if kind == 0 else (one_hot(masks),)):
            parts[k] = part

    def gated(parts, count, first, rows):
        total = None
        for k in reversed(range(count)):
            term = dot_ta(parts[k, first : first + rows.shape[0]], rows)
            total = term if total is None else total + term
        return total

    def columns_of(s):
        return pl.ds(pl.multiple_of(s * side, side), side)

    def combine(kind, block, slot, tile):
        block_parts(kind, block, gates_buf)
        row_load(kind, block, slot).wait()

        def one_side(s, carry):
            tile[s] = gated(gates_buf, 3 if kind == 0 else 1, 0, c_buf[slot, :, :, columns_of(s)].reshape(own * cap, side))
            return carry

        lax.fori_loop(0, 2, one_side, 0)

    early = own - 2
    far_blocks = (mate_step(4), far)
    far_tiles = (give.at[0], far_sum)

    def combine_early():
        for slot, block in enumerate(far_blocks):
            row_load(0, block, slot, 0, early).start()
        for slot, block in enumerate(far_blocks):
            block_parts(0, block, far_gates.at[slot])
            row_load(0, block, slot, 0, early).wait()

            def one_side(s, carry):
                rows = c_buf[slot, 0:early, :, columns_of(s)].reshape(early * cap, side)
                far_tiles[slot][s] = gated(far_gates.at[slot], 3, 0, rows)
                return carry

            lax.fori_loop(0, 2, one_side, 0)

    def load_next():
        settle_rows(0)
        for slot, block in enumerate(far_blocks):
            row_load(0, block, slot, early, 1).start()

    def combine_late(slot, s):
        block = far_blocks[slot]
        rows = jnp.concatenate([c_buf[slot, early, :, columns_of(s)], y_buf[block, :, columns_of(s)]], axis=0)
        far_tiles[slot][s] += gated(far_gates.at[slot], 3, early * cap, rows)

    def sum_up(kind):
        state = {}
        order = [b for o in offsets for b in (mate_step(o), step(o))]

        def one(n, tile):
            if n + 1 < len(order):
                row_load(kind, order[n + 1], (n + 1) % 2).start()
            combine(kind, order[n], n % 2, tile)

        gifts, writes = [], [None]

        def give_block(i):
            if i >= 2:
                if i > 2 or kind == 1:
                    links.finish(gifts[i - 2])
                else:
                    for k in gifts[0]:
                        links.finish(k)
            one(2 * i, give.at[i % 2])
            gifts.append(links.send(give.at[i % 2], mate_land.at[kind, i], to_mate))

        def own_block(i):
            one(2 * i + 1, keep_sum.at[i % 2])

        def send_far(s, to):
            state["far", s] = links.send(far_sum.at[s], half_land.at[kind, s], to)

        def first_blocks():
            if kind == 0:
                for slot in range(2):
                    row_load(0, far_blocks[slot], slot, early, 1).wait()
                pair = []
                for s in range(2):
                    combine_late(0, s)
                    pair.append(links.send(give.at[0, s], mate_sum.at[s], to_mate))
                gifts.append(pair)
                for s in range(2):
                    combine_late(1, s)
                settle_rows(0)
                row_load(kind, order[2], 0).start()
                for s, to in ((0, to_right), (1, to_left)):
                    links.arrive(pair[s], mate_sum.at[s], to_mate)
                    far_sum[s] += mate_sum[s]
                    send_far(s, to)
            else:
                settle_rows(1)
                row_load(kind, order[0], 0).start()
                give_block(0)
                for s in range(2):
                    links.finish(y_sum["far", s])
                one(1, far_sum)

        def first_sum():
            links.arrive(gifts[0], mate_land.at[kind, 0], to_mate)
            copy = pltpu.make_async_copy(mate_land.at[kind, 0], mate_sum, sum_sem.at[0])
            copy.start()
            copy.wait()
            for s, to in ((0, to_right), (1, to_left)):
                far_sum[s] += mate_sum[s]
                send_far(s, to)

        def add_mate(i):
            links.arrive(gifts[i], mate_land.at[kind, i], to_mate)
            copy = pltpu.make_async_copy(mate_land.at[kind, i], mate_sum, sum_sem.at[0])
            copy.start()
            copy.wait()
            keep_sum[i % 2] += mate_sum[...]
            writes.append(pltpu.make_async_copy(keep_sum.at[i % 2], sums.at[kind, i], sum_sem.at[1 + i % 2]))
            writes[i].start()

        def send_sum(i):
            writes[i].wait()
            if i == 1:
                state["right"] = links.send(sums.at[kind, 1, 1], last_land.at[kind, 0, 1], to_right)
            elif i == 2:
                state["left"] = links.send(sums.at[kind, 2, 0], last_land.at[kind, 1, 0], to_left)

        with jax.named_scope("first_blocks"):
            first_blocks()
        with jax.named_scope("give_block_1"):
            give_block(1)
        if kind == 1:
            with jax.named_scope("first_sum"):
                first_sum()
        with jax.named_scope("own_block_1"):
            own_block(1)
        with jax.named_scope("give_block_2"):
            give_block(2)
        with jax.named_scope("add_mate_1"):
            add_mate(1)
        with jax.named_scope("own_block_2"):
            own_block(2)
        with jax.named_scope("send_sum_1"):
            send_sum(1)
        with jax.named_scope("give_block_3"):
            give_block(3)
        with jax.named_scope("add_mate_2"):
            add_mate(2)
        with jax.named_scope("own_block_3"):
            own_block(3)
        with jax.named_scope("send_sum_2"):
            send_sum(2)
        with jax.named_scope("add_mate_3"):
            add_mate(3)
        with jax.named_scope("send_sum_3"):
            send_sum(3)
        links.finish(gifts[2])
        links.finish(gifts[3])
        return state

    def turn_sums(kind, state):
        for s, to in ((0, to_right), (1, to_left)):
            links.arrive(state["far", s], half_land.at[kind, s], to)
            tile = turn_sum.at[kind, s]
            a = pltpu.make_async_copy(sums.at[kind, 1 + s, s], tile, sum_sem.at[0])
            b = pltpu.make_async_copy(half_land.at[kind, s], mate_sum.at[s], sum_sem.at[1])
            a.start()
            b.start()
            a.wait()
            b.wait()
            turn_sum[kind, s] += mate_sum[s]
            state["turn", s] = links.send(tile, last_land.at[kind, s, s], to)

    def direct_here(kind, state):
        links.arrive(state["right"], last_land.at[kind, 0, 1], to_right)
        links.arrive(state["left"], last_land.at[kind, 1, 0], to_left)

    def turned_here(kind, state):
        links.arrive(state["turn", 0], last_land.at[kind, 0, 0], to_right)
        links.arrive(state["turn", 1], last_land.at[kind, 1, 1], to_left)

    def add_direct(kind):
        copies = [pltpu.make_async_copy(sums.at[kind, 3], keep_sum.at[0], sum_sem.at[0]),
                  pltpu.make_async_copy(last_land.at[kind, 1, 0], mate_sum.at[0], sum_sem.at[1]),
                  pltpu.make_async_copy(last_land.at[kind, 0, 1], mate_sum.at[1], sum_sem.at[2])]
        for copy in copies:
            copy.start()
        for copy in copies:
            copy.wait()
        keep_sum[0] += mate_sum[...]

    def finish_out():
        add_direct(0)
        copies = [pltpu.make_async_copy(last_land.at[0, s, s], mate_sum.at[s], sum_sem.at[s]) for s in range(2)]
        for copy in copies:
            copy.start()
        for s in range(2):
            copies[s].wait()
            xb[0, 0, :, s * side : (s + 1) * side] = (keep_sum[0, s] + mate_sum[s]).astype(BF16)
        copy = pltpu.make_async_copy(xb.at[0, 0], out, sum_sem.at[0])
        copy.start()
        copy.wait()

    def fold_dx():
        add_direct(1)
        copy = pltpu.make_async_copy(keep_sum.at[0], sums.at[1, 3], sum_sem.at[0])
        copy.start()
        copy.wait()

    y_state = {}
    for way in (True, False):
        for kind in kinds:
            go_up = upward[kind] == way
            y_state[kind, go_up] = links.send(own_refs[kind], all_refs[kind].at[ep, tp], to_up if go_up else to_down)
    groups = (tp, down, up)
    states = [spread(tp, own_refs)]
    hold = [pltpu.make_async_copy(own_refs[kind], all_refs[kind].at[ep, tp], row_sem.at[kind]) for kind in range(3)]
    for copy in hold:
        copy.start()
    for copy in loads:
        copy.wait()
    stow = [pltpu.make_async_copy(w13, w13_all.at[tp], w_sem.at[0]), pltpu.make_async_copy(w2s, w2_all.at[tp], w_sem.at[1])]
    for copy in stow:
        copy.start()
    earlier[...] = earlier_rows(earlier.shape[0])
    with jax.named_scope("zeros"):
        acc13[...] = jnp.zeros_like(acc13)
        acc2[...] = jnp.zeros_like(acc2)

    def y_arrive(kind, way):
        block = all_refs[kind].at[ep, down if way else up]
        links.arrive(y_state[kind, way], block, to_up if way else to_down)
        return block

    with jax.named_scope("pass_on_0"):
        pass_on(0)
    with jax.named_scope("y_arrive"):
        for way in (True, False):
            for kind in kinds:
                y_arrive(kind, way)
    with jax.named_scope("send_weights_0"):
        send_weights(0)
    with jax.named_scope("send_weights_1"):
        send_weights(1)
    for g in (1, 2):
        states.append(spread(groups[g], [ref.at[ep, groups[g]] for ref in all_refs]))
    with jax.named_scope("share_0"):
        share(0)
    with jax.named_scope("last_0"):
        last(0)
    for copy in hold + stow:
        copy.wait()
    with jax.named_scope("from_mate_0"):
        from_mate(0)
    route_copy = pltpu.make_async_copy(r_all.at[:, tp], routes, row_sem.at[0])
    route_copy.start()
    route_copy.wait()
    with jax.named_scope("compute_tp_True"):
        compute(tp, True)

    with jax.named_scope("pass_weights_0"):
        pass_weights(0)
    with jax.named_scope("send_weights_2"):
        send_weights(2)
    with jax.named_scope("pass_on_1"):
        pass_on(1)
    with jax.named_scope("share_1"):
        share(1)
    with jax.named_scope("pass_weights_1"):
        pass_weights(1)
    with jax.named_scope("send_weights_3"):
        send_weights(3)
    with jax.named_scope("expert_0"):
        expert(0)
    with jax.named_scope("pass_on_2"):
        pass_on(2)
    with jax.named_scope("share_2"):
        share(2)
    with jax.named_scope("pass_weights_2"):
        pass_weights(2)
    with jax.named_scope("send_weights_4"):
        send_weights(4)
    with jax.named_scope("last_1"):
        last(1)
    with jax.named_scope("from_mate_1"):
        from_mate(1)
    with jax.named_scope("expert_1"):
        expert(1)
    with jax.named_scope("last_2"):
        last(2)
    with jax.named_scope("compute_groups_1_False"):
        compute(groups[1], False)
    with jax.named_scope("pass_weights_3"):
        pass_weights(3)
    with jax.named_scope("expert_2"):
        expert(2)
    with jax.named_scope("from_mate_2"):
        from_mate(2)
    with jax.named_scope("compute_groups_2_False"):
        compute(groups[2], False)
    with jax.named_scope("pass_weights_4"):
        pass_weights(4)
    with jax.named_scope("send_over_"):
        over_state = send_over()
    with jax.named_scope("combine_early"):
        settle_rows(0)
        combine_early()
    with jax.named_scope("expert_3"):
        expert(3)
    with jax.named_scope("forward_early"):
        load_next()
        copies = forward_early(own - 1)
    with jax.named_scope("have_weights_own_1"):
        have_weights(own - 1)
    with jax.named_scope("forward_late"):
        forward_late(own - 1)
    with jax.named_scope("sum_up_0"):
        y_sum = sum_up(0)
    with jax.named_scope("share_over_0"):
        share_over(0)
    with jax.named_scope("backward_own_1_copies"):
        backward(own - 1, copies)
    with jax.named_scope("sum_up_1"):
        dx_sum = sum_up(1)
    with jax.named_scope("turn_sums_0_y_sum"):
        turn_sums(0, y_sum)
    with jax.named_scope("share_over_1"):
        share_over(1)
    with jax.named_scope("have_over_1"):
        have_over(0)
        have_over(1)
    with jax.named_scope("half_group_over_0"):
        start_loads(over, 0)
        half_group(over, 0, False, False)
    with jax.named_scope("share_over_2"):
        share_over(2)
    with jax.named_scope("turn_sums_1_dx_sum"):
        turn_sums(1, dx_sum)
    with jax.named_scope("share_over_3"):
        share_over(3)
    with jax.named_scope("have_over_3"):
        have_over(2)
        have_over(3)
    with jax.named_scope("half_group_over_1"):
        start_loads(over, 1)
        half_group(over, 1, False, False)

    def finish(e, carry):
        g_buf[0] = acc13[e, :width, :].T.astype(BF16)
        g_buf[1] = acc13[e, width:, :].T.astype(BF16)
        copies = [pltpu.make_async_copy(g_buf.at[0], g1.at[e], g_sem.at[0]), pltpu.make_async_copy(g_buf.at[1], g3.at[e], g_sem.at[1])]
        xs[0, pl.ds(0, width), :] = acc2[e].astype(BF16)
        copies.append(pltpu.make_async_copy(xs.at[0, pl.ds(0, width)], g2.at[e], g_sem.at[2]))
        for copy in copies:
            copy.start()
        for copy in copies:
            copy.wait()
        return carry

    with jax.named_scope("finish"):
        lax.fori_loop(0, own, finish, 0)
    with jax.named_scope("direct_here"):
        direct_here(0, y_sum)
        direct_here(1, dx_sum)
    with jax.named_scope("fold_dx"):
        fold_dx()
    with jax.named_scope("turned_here_0"):
        turned_here(0, y_sum)
    with jax.named_scope("finish_out"):
        finish_out()
    with jax.named_scope("turned_here_1"):
        turned_here(1, dx_sum)
    with jax.named_scope("drain"):
        links.drain()


def layer(tokens, d_out, ids, gate_vals, w_one, w_three, w_two, ep_size, tp_size, cap):
    tok, model = tokens.shape
    own, width, _ = w_two.shape
    half = ep_size // 2
    rows = half * cap
    side = model // 2
    hbm = pl.BlockSpec(memory_space=pl.ANY)
    shape = jax.ShapeDtypeStruct
    routes = (2 * ids.shape[0], tok)
    copies = copy_count(own)
    slot_rows = ep_size * tp_size * cap * own
    vector = pltpu.VMEM
    dma = pltpu.SemaphoreType.DMA
    outs = pl.pallas_call(
        functools.partial(layer_kernel, own, cap, width),
        in_specs=[hbm] * 7,
        out_specs=[hbm] * 16,
        out_shape=[
            shape((ep_size, tp_size, tok, model), BF16),
            shape((ep_size, tp_size, tok, model), BF16),
            shape((ep_size, tp_size) + routes, F32),
            shape((tp_size, own, model, 2 * width), BF16),
            shape((tp_size, own, width, model), BF16),
            shape((own, 2, rows, model), BF16),
            shape((own, 2, rows, model), BF16),
            shape((2, ep_size, own, cap, model), BF16),
            shape((2, 4, 2, tok, side), F32),
            shape((2, 4, 2, tok, side), F32),
            shape((2, 2, tok, side), F32),
            shape((2, 2, 2, tok, side), F32),
            shape((tok, model), BF16),
            shape((own, model, width), BF16),
            shape((own, model, width), BF16),
            shape((own, width, model), BF16),
        ],
        scratch_shapes=[
            vector((tok, model), BF16),
            vector((tok, model), BF16),
            vector(routes, F32),
            vector(ids.shape, jnp.int32),
            vector((2, 3, own * cap, tok), BF16),
            vector((own, model, 2 * width), BF16),
            vector((own, width, model), BF16),
            vector((2, half // 2, tok, model), BF16),
            vector((2, half // 2, tok, model), BF16),
            vector((2, half // 2) + routes, F32),
            vector((ep_size,) + routes, F32),
            vector((tok, tok), BF16),
            vector((own, rows, model), BF16),
            vector((own, rows, model), BF16),
            vector((own, 2 * width, model), F32),
            vector((own, width, model), F32),
            vector((2, model, width), BF16),
            vector((tp_size, model, 2 * width), BF16),
            vector((tp_size, width, model), BF16),
            vector((tp_size, 2 * rows, 2 * width), F32),
            vector((2 * rows, tp_size * width), BF16),
            vector((tp_size, 2 * rows, 2 * width), BF16),
            vector((ep_size, cap, model), BF16),
            vector((ep_size, cap, model), BF16),
            vector((2, own, cap, model), BF16),
            vector((3, own * cap, tok), BF16),
            vector((2, 2, tok, side), F32),
            vector((2, 2, tok, side), F32),
            vector((2, tok, side), F32),
            vector((2, tok, side), F32),
            vector((2, 2, tok, side), F32),
            dma((copies,)),
            dma((copies,)),
            dma((4,)),
            dma((3, 2)),
            dma((3,)),
            dma((2,)),
            dma((3 + tp_size,)),
            dma((2,)),
            dma((2,)),
            dma((3,)),
            dma((3,)),
        ],
        compiler_params=pltpu.CompilerParams(vmem_limit_bytes=VMEM_LIMIT, collective_id=0, has_side_effects=True),
        cost_estimate=pl.CostEstimate(
            flops=2 * slot_rows * model * (2 * tok + 12 * width),
            bytes_accessed=4 * ep_size * tp_size * tok * model,
            transcendentals=0,
        ),
        name="layer",
    )(tokens, d_out, ids, gate_vals, w_one, w_three, w_two)
    return outs[8], outs[11], outs[12], outs[13:]


def result_kernel(sums, last_land, rows_in, g1, g3, g2, out, dx, o1, o3, o2, parts, rows, row_buf, b1, b3, b2, in_sem, out_sem):
    moves = ((g1, b1, o1), (g3, b3, o3), (g2, b2, o2), (rows_in, row_buf, out))
    takes = [pltpu.make_async_copy(src, buf, in_sem.at[k]) for k, (src, buf, _) in enumerate(moves)]
    terms = [pltpu.make_async_copy(sums.at[1, 3], parts.at[0], in_sem.at[4])]
    terms += [pltpu.make_async_copy(last_land.at[1, s, s], parts.at[1, s], in_sem.at[5 + s]) for s in range(2)]
    for copy in terms + takes:
        copy.start()
    for copy in terms:
        copy.wait()
    side = parts.shape[3]
    for s in range(2):
        rows[:, s * side : (s + 1) * side] = (parts[0, s] + parts[1, s]).astype(BF16)
    puts = [pltpu.make_async_copy(rows, dx, out_sem.at[4])]
    puts[0].start()
    for k, (take, (_, buf, to)) in enumerate(zip(takes, moves)):
        take.wait()
        puts.append(pltpu.make_async_copy(buf, to, out_sem.at[k]))
        puts[-1].start()
    for copy in puts:
        copy.wait()


def results(sums, last_land, out, grads):
    _, _, _, tok, side = sums.shape
    hbm = pl.BlockSpec(memory_space=pl.ANY)
    row = jax.ShapeDtypeStruct((tok, 2 * side), BF16)
    rows = pltpu.VMEM((tok, 2 * side), BF16)
    return pl.pallas_call(
        result_kernel,
        in_specs=[hbm] * 6,
        out_specs=[hbm] * 5,
        out_shape=[row, row] + [jax.ShapeDtypeStruct(g.shape, g.dtype) for g in grads],
        scratch_shapes=[pltpu.VMEM((2, 2, tok, side), F32), rows, rows]
        + [pltpu.VMEM(g.shape, g.dtype) for g in grads]
        + [pltpu.SemaphoreType.DMA((7,)), pltpu.SemaphoreType.DMA((5,))],
        compiler_params=pltpu.CompilerParams(vmem_limit_bytes=VMEM_LIMIT),
        name="results",
    )(sums, last_land, out, *grads)


def solution(mesh):
    ep_size, tp_size = mesh.shape["ep"], mesh.shape["tp"]
    row_spec = P(("dp", "ep", "tp"), None)
    col_spec = P("ep", None, "tp")
    down_spec = P("ep", "tp", None)
    grad_col = P(("dp", "ep"), None, "tp")
    grad_down = P(("dp", "ep"), "tp", None)

    def local_step(tokens, expert_ids, gate_vals, w_one, w_three, w_two, d_out):
        cap = slot_count(expert_ids.shape[1], tokens.shape[0], w_one.shape[0] * ep_size)
        sums, last_land, out, grads = layer(tokens, d_out, expert_ids.T, gate_vals.T, w_one, w_three, w_two, ep_size, tp_size, cap)
        return tuple(results(sums, last_land, out, grads))

    return jax.shard_map(local_step, mesh=mesh,
                         in_specs=(row_spec, row_spec, row_spec, col_spec, col_spec, down_spec, row_spec),
                         out_specs=(row_spec, row_spec, grad_col, grad_col, grad_down), check_vma=False)
```

```python
import functools

import jax
import jax.numpy as jnp
from jax import lax
from jax.experimental import pallas as pl
from jax.experimental.pallas import tpu as pltpu
from jax.sharding import PartitionSpec as P

BF16 = jnp.bfloat16
F32 = jnp.float32
MESH = pl.DeviceIdType.MESH
VMEM_LIMIT = 62 * 2**20


def slot_count(num_top, tok_dev, experts):
    return 8 * ((5 * num_top * tok_dev + 32 * experts - 1) // (32 * experts))


def dot(a, b):
    return jnp.dot(a, b, preferred_element_type=F32)


def dot_tb(a, b):
    return lax.dot_general(a, b, (((1,), (1,)), ((), ())), preferred_element_type=F32)


def dot_ta(a, b):
    return lax.dot_general(a, b, (((0,), (0,)), ((), ())), preferred_element_type=F32)


def earlier_rows(tok):
    row = lax.broadcasted_iota(jnp.int32, (tok, tok), 0)
    col = lax.broadcasted_iota(jnp.int32, (tok, tok), 1)
    return jnp.where(row < col, 1.0, 0.0).astype(BF16)


def expert_rows(routes, first, own, earlier):
    top = routes.shape[0] // 2
    ids, gates = routes[:top], routes[top:]
    hits = [ids == (first + e).astype(F32) for e in range(own)]
    routed = jnp.concatenate([jnp.sum(jnp.where(m, 1.0, 0.0), axis=0, keepdims=True) for m in hits], axis=0)
    gate = jnp.concatenate([jnp.sum(jnp.where(m, gates, 0.0), axis=0, keepdims=True) for m in hits], axis=0)
    return jnp.where(routed > 0.0, dot(routed.astype(BF16), earlier), -1.0), gate


def hit_masks(pos, cap):
    slot = lax.broadcasted_iota(jnp.int32, (cap, pos.shape[1]), 0).astype(F32)
    return [pos[e : e + 1, :] == slot for e in range(pos.shape[0])]


def one_hot(masks):
    return jnp.concatenate([jnp.where(m, 1.0, 0.0) for m in masks], axis=0).astype(BF16)


def slot_gates(masks, gate):
    return jnp.concatenate([jnp.where(m, gate[e : e + 1, :], 0.0) for e, m in enumerate(masks)], axis=0)


def three_parts(x):
    hi = x.astype(BF16)
    rest = x - hi.astype(F32)
    mid = rest.astype(BF16)
    return hi, mid, (rest - mid.astype(F32)).astype(BF16)


class Links:
    def __init__(self, send_sem, recv_sem):
        self.send_sem, self.recv_sem, self.sent, self.finished = send_sem, recv_sem, [], set()

    def copy(self, k, src, dst, to):
        return pltpu.make_async_remote_copy(src_ref=src, dst_ref=dst, send_sem=self.send_sem.at[k],
                                            recv_sem=self.recv_sem.at[k], device_id=to, device_id_type=MESH)

    def send(self, src, dst, to):
        k = len(self.sent)
        copy = self.copy(k, src, dst, to)
        copy.start()
        self.sent.append(copy)
        return k

    def arrive(self, k, dst, to):
        self.copy(k, dst, dst, to).wait_recv()

    def finish(self, k):
        self.finished.add(k)
        self.sent[k].wait_send()

    def drain(self):
        for k in range(len(self.sent)):
            if k not in self.finished:
                self.finish(k)


def copy_count(own):
    return 6 + 21 * 3 + 24 + 4 * own + 4 * 4 + 8 * 4


def layer_kernel(own, cap, width, tokens, d_out, ids, gate_vals, w1, w3, w2, x_all, dy_all, r_all, w13_all, w2_all, xs_all,
                 us_all, ab_all, sums, mate_land, far_land, last_land, out, g1, g3, g2, x_own, dy_own, r_own, i_own, w13, w2s, xb,
                 dyb, rb, routes, earlier, xs, us, acc13, acc2, g_buf, wide_buf, w2v, ab_buf, d_all, y_buf, give, keep_sum, mate_sum,
                 turn_sum, send_sem, recv_sem, row_sem, load_sem, w_sem, slot_sem, in_sem, ab_sem, sum_sem, g_sem):
    ep, tp = lax.axis_index("ep"), lax.axis_index("tp")
    eps, tps = x_all.shape[0], x_all.shape[1]
    model = x_all.shape[3]
    part = model // 4
    half = eps // 2
    step = lambda n: lax.rem(ep + (n + eps), eps)
    turn = lambda n: lax.rem(tp + (n + tps), tps)
    right, left, far = step(2), step(-2), step(4)
    mate = ep + 1 - 2 * lax.rem(ep, 2)
    mate_step = lambda n: lax.rem(mate + (n + eps), eps)
    up, down, over = turn(1), turn(-1), turn(2)
    to_right, to_left, to_mate = {"ep": right}, {"ep": left}, {"ep": mate}
    to_up, to_down = {"tp": up}, {"tp": down}
    links = Links(send_sem, recv_sem)

    barrier = pltpu.get_barrier_semaphore()
    for to in (to_right, to_left, to_mate, to_up, to_down):
        pl.semaphore_signal(barrier, inc=1, device_id=to, device_id_type=MESH)
    top = ids.shape[0]
    firsts = [pltpu.make_async_copy(ids, i_own, row_sem.at[0]), pltpu.make_async_copy(gate_vals, r_own.at[pl.ds(top, top)], row_sem.at[1]),
              pltpu.make_async_copy(tokens, x_own, row_sem.at[2]), pltpu.make_async_copy(d_out, dy_own, row_sem.at[3])]
    loads = [pltpu.make_async_copy(src.at[:, pl.ds(m * part, part)], w13.at[:, m, :, pl.ds(k * width, width)], w_sem.at[4 * k + m])
             for k, src in ((0, w1), (1, w3)) for m in range(4)]
    loads.append(pltpu.make_async_copy(w2, w2s, w_sem.at[8]))
    for copy in firsts + loads:
        copy.start()
    firsts[0].wait()
    r_own[0:top] = i_own[...].astype(F32)
    for copy in firsts[1:]:
        copy.wait()
    with jax.named_scope("barrier"):
        pl.semaphore_wait(barrier, 5)

    own_refs, all_refs = (x_own, dy_own, r_own), (x_all, dy_all, r_all)
    upward = (True, False, True)
    kinds = (0, 1, 2)

    def spread(t, srcs):
        out = {}
        for kind in kinds:
            to = to_right if upward[kind] else to_left
            out[kind, upward[kind]] = links.send(srcs[kind], all_refs[kind].at[ep, t], to)
        for kind in kinds:
            to = to_left if upward[kind] else to_right
            out[kind, not upward[kind]] = links.send(srcs[kind], all_refs[kind].at[ep, t], to)
        for kind in kinds:
            out[kind, "mate"] = links.send(srcs[kind], all_refs[kind].at[ep, t], to_mate)
        return out

    def pass_on(g):
        state, t = states[g], groups[g]
        for kind in kinds:
            got, to = (left, to_right) if upward[kind] else (right, to_left)
            block = all_refs[kind].at[got, t]
            links.arrive(state[kind, upward[kind]], block, to)
            state[kind, "far"] = links.send(block, block, to)
            state[kind, "mate1"] = links.send(block, block, to_mate)

    def share(g):
        state, t = states[g], groups[g]
        for kind in kinds:
            got, to = (right, to_left) if upward[kind] else (left, to_right)
            block = all_refs[kind].at[got, t]
            links.arrive(state[kind, not upward[kind]], block, to)
            state[kind, "mate2"] = links.send(block, block, to_mate)

    def last(g):
        state, t = states[g], groups[g]
        for kind in kinds:
            block = all_refs[kind].at[far, t]
            links.arrive(state[kind, "far"], block, to_right if upward[kind] else to_left)
            state[kind, "mate3"] = links.send(block, block, to_mate)

    def from_mate(g):
        state, t = states[g], groups[g]
        for kind in kinds:
            one, two = (mate_step(-2), mate_step(2)) if upward[kind] else (mate_step(2), mate_step(-2))
            for name, at in (("mate", mate), ("mate1", one), ("mate2", two), ("mate3", mate_step(4))):
                links.arrive(state[kind, name], all_refs[kind].at[at, t], to_mate)

    core = lax.rem(ep, 2)

    def send_over():
        return [{kind: links.send(all_refs[kind].at[core + 2 * m, down if upward[kind] else up],
                                  all_refs[kind].at[core + 2 * m, down if upward[kind] else up],
                                  to_up if upward[kind] else to_down) for kind in kinds} for m in range(half)]

    def share_over(m):
        for kind in kinds:
            block = all_refs[kind].at[core + 2 * m, over]
            links.arrive(over_state[m][kind], block, to_up if upward[kind] else to_down)
            over_state[m][kind, "mate"] = links.send(block, block, to_mate)

    def have_over(m):
        for kind in kinds:
            links.arrive(over_state[m][kind, "mate"], all_refs[kind].at[1 - core + 2 * m, over], to_mate)

    def both_ways(src, dst):
        return {True: links.send(src, dst, to_up), False: links.send(src, dst, to_down)}

    def pass_halves(state, below, above, split):
        links.arrive(state[True], below, to_up)
        state["first"] = links.send(split(below, 0), split(below, 0), to_up)
        links.arrive(state[False], above, to_down)
        state["second"] = links.send(split(above, 1), split(above, 1), to_down)

    def have_halves(state, block, split):
        links.arrive(state["first"], split(block, 0), to_up)
        links.arrive(state["second"], split(block, 1), to_down)

    w13_state, w2_state = [None] * own, [None] * 4
    split13 = lambda ref, k: ref.at[pl.ds(2 * k, 2)]
    split2 = lambda ref, k: ref.at[:, pl.ds(k * (width // 2), width // 2)]

    def send13(e):
        w13_state[e] = both_ways(w13.at[e], w13_all.at[tp, e])

    def pass13(e):
        pass_halves(w13_state[e], w13_all.at[down, e], w13_all.at[up, e], split13)

    def have13(e):
        have_halves(w13_state[e], w13_all.at[over, e], split13)

    def send2(q):
        w2_state[q] = both_ways(w2s.at[:, :, pl.ds(q * part, part)], w2_all.at[tp, q])

    def pass2(q):
        pass_halves(w2_state[q], w2_all.at[down, q], w2_all.at[up, q], split2)

    def have2(q):
        have_halves(w2_state[q], w2_all.at[over, q], split2)

    def pair_loads(t, h, p):
        at = pl.ds(h * half + p * (half // 2), half // 2)
        return [pltpu.make_async_copy(src.at[at, t], dst.at[p], load_sem.at[k, p])
                for k, (src, dst) in enumerate(((x_all, xb), (dy_all, dyb), (r_all, rb)))]

    def half_group(t, h, keep, ahead):
        for p in range(2):
            for copy in pair_loads(t, h, p):
                copy.wait()

            def gather(b, carry):
                pos, gate = expert_rows(rb[p, b], ep * own, own, earlier[...])
                masks = hit_masks(pos, cap)
                pick = one_hot(masks)
                gates = jnp.sum(slot_gates(masks, gate), axis=1, keepdims=True)
                rows = pl.ds(pl.multiple_of((p * (half // 2) + b) * cap, cap), cap)
                picked = dot(pick, xb[p, b]).astype(BF16)
                for e in range(own):
                    xs[e, rows, :] = picked[e * cap : (e + 1) * cap]
                scaled = (gates * dot(pick, dyb[p, b])).astype(BF16)
                for e in range(own):
                    us[e, rows, :] = scaled[e * cap : (e + 1) * cap]
                return carry

            lax.fori_loop(0, half // 2, gather, 0)

            @pl.when(ahead)
            def _():
                for copy in pair_loads(t, 1, p):
                    copy.start()

        stores = []
        if keep:
            stores = [pltpu.make_async_copy(xs, xs_all.at[:, h], slot_sem.at[0]),
                      pltpu.make_async_copy(us, us_all.at[:, h], slot_sem.at[1])]
        for copy in stores:
            copy.start()

        def expert(e, carry):
            ab = dot(xs[e], w13[e].reshape(model, 2 * width))
            a, b = ab[:, :width], ab[:, width:]
            dh = dot_tb(us[e], w2s[e])
            sig = jax.nn.sigmoid(a)
            silu = a * sig
            hid = (silu * b).astype(BF16)
            da = (dh * b * sig * (1.0 + a * (1.0 - sig))).astype(BF16)
            db = (dh * silu).astype(BF16)
            acc13[e] += dot_ta(jnp.concatenate([da, db], axis=1), xs[e])
            acc2[e] += dot_ta(hid, us[e])
            return carry

        lax.fori_loop(0, own, expert, 0)
        for copy in stores:
            copy.wait()

    def start_loads(t, h):
        for p in range(2):
            for copy in pair_loads(t, h, p):
                copy.start()

    def compute(t, keep):
        start_loads(t, 0)

        def one_half(h, carry):
            half_group(t, h, keep, h == 0)
            return carry

        lax.fori_loop(0, 2, one_half, 0)

    slots = eps * cap
    pending = []

    def settle():
        while pending:
            pending.pop().wait()

    def hidden(e):
        rows = pltpu.make_async_copy(xs_all.at[e], xs.at[pl.ds(0, 2)], in_sem.at[tps])
        rows.start()
        for j in range(tps):
            pltpu.make_async_copy(w13_all.at[j, e], wide_buf.at[pl.ds(0, 4), j], in_sem.at[j]).start()
        settle()
        rows.wait()

        def shard(j, carry):
            pltpu.make_async_copy(w13_all.at[j, e], wide_buf.at[pl.ds(0, 4), j], in_sem.at[j]).wait()
            ab = dot(xs[0:2].reshape(slots, model), wide_buf[0:4, j].reshape(model, 2 * width))
            ab_buf[j] = ab
            a, b = ab[:, :width], ab[:, width:]
            at = pl.ds(pl.multiple_of(lax.rem(j, 2) * width, width), width)
            d_all[e, j // 2, :, at] = (a * jax.nn.sigmoid(a) * b).astype(BF16)
            return carry

        lax.fori_loop(0, tps, shard, 0)
        pending.append(pltpu.make_async_copy(ab_buf, ab_all.at[e], ab_sem.at[0]))
        pending[-1].start()

    def put_rows(e, value):
        for k in range(eps):
            y_buf[k, e] = value[k * cap : (k + 1) * cap]

    def y_part(q):
        load = pltpu.make_async_copy(w2_all.at[:, q], w2v.at[q], in_sem.at[0])
        load.start()
        load.wait()

        def one(e, carry):
            y = dot(d_all[e, 0], w2v[q, 0:2, e].reshape(2 * width, part)) + dot(d_all[e, 1], w2v[q, 2:4, e].reshape(2 * width, part))
            put_rows(e, y.astype(BF16))
            return carry

        lax.fori_loop(0, own, one, 0)

    def ab_load(e, j):
        return pltpu.make_async_copy(ab_all.at[e, j], ab_buf.at[j], ab_sem.at[j])

    def u_load(e, slot):
        return pltpu.make_async_copy(us_all.at[e], us.at[pl.ds(2 * slot, 2)], in_sem.at[1 + slot])

    def hidden_grads():
        settle()
        u_load(0, 0).start()
        for j in range(tps):
            ab_load(0, j).start()

        def one(e, carry):
            slot = lax.rem(e, 2)
            u_load(e, slot).wait()

            @pl.when(e + 1 < own)
            def _():
                u_load(e + 1, 1 - slot).start()

            def two(k, carry):
                dh = None
                for q in range(4):
                    at = pl.ds(q * part, part)
                    u = us[pl.ds(2 * slot, 2), :, at].reshape(slots, part)
                    term = dot_tb(u, w2v[q, pl.ds(2 * k, 2), e].reshape(2 * width, part))
                    dh = term if dh is None else dh + term
                for i in range(2):
                    j = 2 * k + i
                    ab_load(e, j).wait()
                    a, b, d = ab_buf[j, :, :width], ab_buf[j, :, width:], dh[:, i * width : (i + 1) * width]
                    sig = jax.nn.sigmoid(a)
                    d_all[e, j, :, :width] = (d * b * sig * (1.0 + a * (1.0 - sig))).astype(BF16)
                    d_all[e, j, :, width:] = (d * (a * sig)).astype(BF16)

                    @pl.when(e + 1 < own)
                    def _():
                        ab_load(e + 1, j).start()
                return carry

            lax.fori_loop(0, tps // 2, two, 0)
            return carry

        lax.fori_loop(0, own, one, 0)

    def v_load(q):
        return pltpu.make_async_copy(w13_all.at[:, :, q], wide_buf, in_sem.at[0])

    def v_part(q):
        v_load(q).wait()

        def one(e, carry):
            v = dot_tb(d_all[e, 0], wide_buf[0, e])
            for j in range(1, tps):
                v = v + dot_tb(d_all[e, j], wide_buf[j, e])
            put_rows(e, v.astype(BF16))
            return carry

        lax.fori_loop(0, own, one, 0)
        if q < 3:
            v_load(q + 1).start()

    gifts, writes, stages = {}, {}, {}

    def combine(kind, block):
        pos, gate = expert_rows(routes[block], ep * own, own, earlier[...])
        masks = hit_masks(pos, cap)
        rows = y_buf[block].reshape(own * cap, part)
        if kind == 1:
            return dot_ta(one_hot(masks), rows)
        hi, mid, low = three_parts(slot_gates(masks, gate))
        return dot_ta(hi, rows) + (dot_ta(mid, rows) + dot_ta(low, rows))

    def sum_begin(kind, q):
        before = (kind, q - 1) if q else (kind - 1, 3)
        if before in gifts:
            links.finish(gifts[before])

        def to_other(i, carry):
            give[i] = combine(kind, lax.rem(mate + 4 - 2 * i + eps, eps))
            return carry

        def to_own(i, carry):
            keep_sum[i] = combine(kind, lax.rem(ep + 4 - 2 * i + eps, eps))
            return carry

        lax.fori_loop(0, 4, to_other, 0)
        gifts[kind, q] = links.send(give, mate_land.at[kind, q], to_mate)
        lax.fori_loop(0, 4, to_own, 0)

    def sum_end(kind, q):
        links.arrive(gifts[kind, q], mate_land.at[kind, q], to_mate)
        load = pltpu.make_async_copy(mate_land.at[kind, q], mate_sum, sum_sem.at[0])
        load.start()
        load.wait()
        keep_sum[...] += mate_sum[...]
        write = pltpu.make_async_copy(keep_sum, sums.at[kind, q], sum_sem.at[1])
        write.start()
        write.wait()
        far_way, near_way, near, side = (to_right, to_left, 3, 1) if q % 2 == 0 else (to_left, to_right, 1, 0)
        stages[kind, q, "far"] = links.send(sums.at[kind, q, 0], far_land.at[kind, q], far_way)
        stages[kind, q, "near"] = links.send(sums.at[kind, q, near], last_land.at[kind, side, q], near_way)

    turned = []

    def sum_turn(kind, q):
        way, at, side = (to_right, 1, 0) if q % 2 == 0 else (to_left, 3, 1)
        slot = len(turned) % 4
        if len(turned) >= 4:
            links.finish(turned[-4])
        links.arrive(stages[kind, q, "far"], far_land.at[kind, q], way)
        a = pltpu.make_async_copy(sums.at[kind, q, at], turn_sum.at[slot], sum_sem.at[0])
        b = pltpu.make_async_copy(far_land.at[kind, q], mate_sum.at[0], sum_sem.at[1])
        a.start()
        b.start()
        a.wait()
        b.wait()
        turn_sum[slot] += mate_sum[0]
        turned.append(links.send(turn_sum.at[slot], last_land.at[kind, side, q], way))
        stages[kind, q, "turn"] = turned[-1]

    def sums_here(kind):
        for q in range(4):
            (way, back), sides = ((to_right, to_left), (0, 1)) if q % 2 == 0 else ((to_left, to_right), (1, 0))
            links.arrive(stages[kind, q, "near"], last_land.at[kind, sides[1], q], back)
            links.arrive(stages[kind, q, "turn"], last_land.at[kind, sides[0], q], way)

    def finish_out():
        links.finish(gifts[1, 3])
        copies = [pltpu.make_async_copy(sums.at[0, :, 2], give, sum_sem.at[0]),
                  pltpu.make_async_copy(last_land.at[0, 0], keep_sum, sum_sem.at[1]),
                  pltpu.make_async_copy(last_land.at[0, 1], mate_sum, sum_sem.at[2])]
        for copy in copies:
            copy.start()
        for copy in copies:
            copy.wait()
        for q in range(4):
            xb[0, 0, :, q * part : (q + 1) * part] = (give[q] + (keep_sum[q] + mate_sum[q])).astype(BF16)
        copy = pltpu.make_async_copy(xb.at[0, 0], out, sum_sem.at[0])
        copy.start()
        copy.wait()

    y_state = {}
    for way in (True, False):
        for kind in kinds:
            go_up = upward[kind] == way
            y_state[kind, go_up] = links.send(own_refs[kind], all_refs[kind].at[ep, tp], to_up if go_up else to_down)
    groups = (tp, down, up)
    states = [spread(tp, own_refs)]
    hold = [pltpu.make_async_copy(own_refs[kind], all_refs[kind].at[ep, tp], row_sem.at[kind]) for kind in range(3)]
    for copy in hold:
        copy.start()
    for copy in loads:
        copy.wait()
    stow = [pltpu.make_async_copy(w13, w13_all.at[tp], w_sem.at[0])]
    stow += [pltpu.make_async_copy(w2s.at[:, :, pl.ds(q * part, part)], w2_all.at[tp, q], w_sem.at[1 + q]) for q in range(4)]
    for copy in stow:
        copy.start()
    earlier[...] = earlier_rows(earlier.shape[0])
    with jax.named_scope("zeros"):
        acc13[...] = jnp.zeros_like(acc13)
        acc2[...] = jnp.zeros_like(acc2)

    def y_arrive(kind, way):
        block = all_refs[kind].at[ep, down if way else up]
        links.arrive(y_state[kind, way], block, to_up if way else to_down)
        return block

    with jax.named_scope("pass_on_0"):
        pass_on(0)
    with jax.named_scope("y_arrive"):
        for way in (True, False):
            for kind in kinds:
                y_arrive(kind, way)
    with jax.named_scope("send13_0"):
        send13(0)
    with jax.named_scope("send13_1"):
        send13(1)
    with jax.named_scope("send13_2"):
        send13(2)
    states.append(spread(down, [ref.at[ep, down] for ref in all_refs]))
    with jax.named_scope("share_0"):
        share(0)
    with jax.named_scope("last_0"):
        last(0)
    for copy in hold + stow:
        copy.wait()
    with jax.named_scope("from_mate_0"):
        from_mate(0)
    route_copy = pltpu.make_async_copy(r_all.at[:, tp], routes, row_sem.at[0])
    route_copy.start()
    route_copy.wait()
    with jax.named_scope("compute_tp_True"):
        compute(tp, True)
    with jax.named_scope("pass13_0"):
        pass13(0)
    with jax.named_scope("send13_3"):
        send13(3)
    with jax.named_scope("pass_on_1"):
        pass_on(1)
    states.append(spread(up, [ref.at[ep, up] for ref in all_refs]))
    with jax.named_scope("share_1"):
        share(1)
    with jax.named_scope("pass13_1"):
        pass13(1)
    with jax.named_scope("send13_4"):
        send13(4)
    with jax.named_scope("have13_0"):
        have13(0)
    with jax.named_scope("hidden_0"):
        hidden(0)
    with jax.named_scope("pass13_2"):
        pass13(2)
    with jax.named_scope("last_1"):
        last(1)
    with jax.named_scope("from_mate_1"):
        from_mate(1)
    with jax.named_scope("compute_down_False"):
        compute(down, False)
    with jax.named_scope("pass13_3"):
        pass13(3)
    with jax.named_scope("send2_0"):
        send2(0)
    with jax.named_scope("pass_on_2"):
        pass_on(2)
    with jax.named_scope("have13_1"):
        have13(1)
    with jax.named_scope("hidden_1"):
        hidden(1)
    with jax.named_scope("share_2"):
        share(2)
    with jax.named_scope("pass13_4"):
        pass13(4)
    with jax.named_scope("send2_1"):
        send2(1)
    with jax.named_scope("have13_2"):
        have13(2)
    with jax.named_scope("hidden_2"):
        hidden(2)
    with jax.named_scope("last_2"):
        last(2)
    with jax.named_scope("from_mate_2"):
        from_mate(2)
    with jax.named_scope("start_loads_up_0"):
        start_loads(up, 0)
    with jax.named_scope("half_group_up_0_False_True"):
        half_group(up, 0, False, True)
    with jax.named_scope("pass2_0"):
        pass2(0)
    with jax.named_scope("send2_2"):
        send2(2)
    with jax.named_scope("half_group_up_1_False_False"):
        half_group(up, 1, False, False)
    with jax.named_scope("have13_3"):
        have13(3)
    with jax.named_scope("hidden_3"):
        hidden(3)
    with jax.named_scope("pass2_1"):
        pass2(1)
    with jax.named_scope("send2_3"):
        send2(3)
    with jax.named_scope("have13_4"):
        have13(4)
    with jax.named_scope("hidden_4"):
        hidden(4)
    with jax.named_scope("have2_0"):
        have2(0)
    with jax.named_scope("y_part_0"):
        y_part(0)
    with jax.named_scope("sum_begin_0_0"):
        sum_begin(0, 0)
    with jax.named_scope("sum_end_0_0"):
        sum_end(0, 0)
    with jax.named_scope("pass2_2"):
        pass2(2)
    with jax.named_scope("have2_1"):
        have2(1)
    with jax.named_scope("y_part_1"):
        y_part(1)
    with jax.named_scope("sum_begin_0_1"):
        sum_begin(0, 1)
    with jax.named_scope("sum_end_0_1"):
        sum_end(0, 1)
    with jax.named_scope("sum_turn_0_0"):
        sum_turn(0, 0)
    with jax.named_scope("pass2_3"):
        pass2(3)
    over_state = send_over()
    with jax.named_scope("have2_2"):
        have2(2)
    with jax.named_scope("y_part_2"):
        y_part(2)
    with jax.named_scope("sum_begin_0_2"):
        sum_begin(0, 2)
    with jax.named_scope("sum_end_0_2"):
        sum_end(0, 2)
    with jax.named_scope("sum_turn_0_1"):
        sum_turn(0, 1)
    with jax.named_scope("have2_3"):
        have2(3)
    with jax.named_scope("y_part_3"):
        y_part(3)
    with jax.named_scope("sum_begin_0_3"):
        sum_begin(0, 3)
    with jax.named_scope("sum_end_0_3"):
        sum_end(0, 3)
    v_load(0).start()
    with jax.named_scope("hidden_grads"):
        hidden_grads()
    with jax.named_scope("sum_turn_0_2"):
        sum_turn(0, 2)
    with jax.named_scope("v_part_0"):
        v_part(0)
    with jax.named_scope("sum_begin_1_0"):
        sum_begin(1, 0)
    with jax.named_scope("sum_end_1_0"):
        sum_end(1, 0)
    with jax.named_scope("sum_turn_0_3"):
        sum_turn(0, 3)
    with jax.named_scope("share_over_0"):
        share_over(0)
    with jax.named_scope("v_part_1"):
        v_part(1)
    with jax.named_scope("sum_begin_1_1"):
        sum_begin(1, 1)
    with jax.named_scope("sum_end_1_1"):
        sum_end(1, 1)
    with jax.named_scope("sum_turn_1_0"):
        sum_turn(1, 0)
    with jax.named_scope("share_over_1"):
        share_over(1)
    with jax.named_scope("v_part_2"):
        v_part(2)
    with jax.named_scope("sum_begin_1_2"):
        sum_begin(1, 2)
    with jax.named_scope("sum_end_1_2"):
        sum_end(1, 2)
    with jax.named_scope("sum_turn_1_1"):
        sum_turn(1, 1)
    with jax.named_scope("v_part_3"):
        v_part(3)
    with jax.named_scope("sum_begin_1_3"):
        sum_begin(1, 3)
    with jax.named_scope("sum_end_1_3"):
        sum_end(1, 3)
    with jax.named_scope("have_over_0"):
        have_over(0)
    with jax.named_scope("have_over_1"):
        have_over(1)
    with jax.named_scope("start_loads_over_0"):
        start_loads(over, 0)
    with jax.named_scope("sum_turn_1_2"):
        sum_turn(1, 2)
    with jax.named_scope("half_group_over_0_False_False"):
        half_group(over, 0, False, False)
    with jax.named_scope("sum_turn_1_3"):
        sum_turn(1, 3)
    with jax.named_scope("share_over_2"):
        share_over(2)
    with jax.named_scope("share_over_3"):
        share_over(3)
    with jax.named_scope("have_over_2"):
        have_over(2)
    with jax.named_scope("have_over_3"):
        have_over(3)
    with jax.named_scope("start_loads_over_1"):
        start_loads(over, 1)
    with jax.named_scope("half_group_over_1_False_False"):
        half_group(over, 1, False, False)

    def grad_stores(e, slot):
        return [pltpu.make_async_copy(g_buf.at[slot, 0], g1.at[e], g_sem.at[slot, 0]),
                pltpu.make_async_copy(g_buf.at[slot, 1], g3.at[e], g_sem.at[slot, 1]),
                pltpu.make_async_copy(xs.at[slot, pl.ds(0, width)], g2.at[e], g_sem.at[slot, 2])]

    def finish(e, carry):
        slot = lax.rem(e, 2)

        @pl.when(e >= 2)
        def _():
            for copy in grad_stores(e - 2, slot):
                copy.wait()

        g_buf[slot, 0] = acc13[e, :width, :].T.astype(BF16)
        g_buf[slot, 1] = acc13[e, width:, :].T.astype(BF16)
        xs[slot, pl.ds(0, width), :] = acc2[e].astype(BF16)
        for copy in grad_stores(e, slot):
            copy.start()
        return carry

    with jax.named_scope("finish"):
        lax.fori_loop(0, own, finish, 0)
        for e in range(max(own - 2, 0), own):
            for copy in grad_stores(e, e % 2):
                copy.wait()
    with jax.named_scope("sums_here_0"):
        sums_here(0)
    with jax.named_scope("finish_out"):
        finish_out()
    with jax.named_scope("sums_here_1"):
        sums_here(1)
    with jax.named_scope("drain"):
        links.drain()


def layer(tokens, d_out, ids, gate_vals, w_one, w_three, w_two, ep_size, tp_size, cap):
    tok, model = tokens.shape
    own, width, _ = w_two.shape
    half = ep_size // 2
    rows = half * cap
    part = model // 4
    hbm = pl.BlockSpec(memory_space=pl.ANY)
    shape = jax.ShapeDtypeStruct
    routes = (2 * ids.shape[0], tok)
    copies = copy_count(own)
    slot_rows = ep_size * tp_size * cap * own
    vector = pltpu.VMEM
    dma = pltpu.SemaphoreType.DMA
    outs = pl.pallas_call(
        functools.partial(layer_kernel, own, cap, width),
        in_specs=[hbm] * 7,
        out_specs=[hbm] * 16,
        out_shape=[
            shape((ep_size, tp_size, tok, model), BF16),
            shape((ep_size, tp_size, tok, model), BF16),
            shape((ep_size, tp_size) + routes, F32),
            shape((tp_size, own, 4, part, 2 * width), BF16),
            shape((tp_size, 4, own, width, part), BF16),
            shape((own, 2, rows, model), BF16),
            shape((own, 2, rows, model), BF16),
            shape((own, tp_size, 2 * rows, 2 * width), F32),
            shape((2, 4, 4, tok, part), F32),
            shape((2, 4, 4, tok, part), F32),
            shape((2, 4, tok, part), F32),
            shape((2, 2, 4, tok, part), F32),
            shape((tok, model), BF16),
            shape((own, model, width), BF16),
            shape((own, model, width), BF16),
            shape((own, width, model), BF16),
        ],
        scratch_shapes=[
            vector((tok, model), BF16),
            vector((tok, model), BF16),
            vector(routes, F32),
            vector(ids.shape, jnp.int32),
            vector((own, 4, part, 2 * width), BF16),
            vector((own, width, model), BF16),
            vector((2, half // 2, tok, model), BF16),
            vector((2, half // 2, tok, model), BF16),
            vector((2, half // 2) + routes, F32),
            vector((ep_size,) + routes, F32),
            vector((tok, tok), BF16),
            vector((own, rows, model), BF16),
            vector((own, rows, model), BF16),
            vector((own, 2 * width, model), F32),
            vector((own, width, model), F32),
            vector((2, 2, model, width), BF16),
            vector((tp_size, own, part, 2 * width), BF16),
            vector((4, tp_size, own, width, part), BF16),
            vector((tp_size, 2 * rows, 2 * width), F32),
            vector((own, tp_size, 2 * rows, 2 * width), BF16),
            vector((ep_size, own, cap, part), BF16),
            vector((4, tok, part), F32),
            vector((4, tok, part), F32),
            vector((4, tok, part), F32),
            vector((4, tok, part), F32),
            dma((copies,)),
            dma((copies,)),
            dma((4,)),
            dma((3, 2)),
            dma((9,)),
            dma((2,)),
            dma((1 + tp_size,)),
            dma((tp_size,)),
            dma((3,)),
            dma((2, 3)),
        ],
        compiler_params=pltpu.CompilerParams(vmem_limit_bytes=VMEM_LIMIT, collective_id=0, has_side_effects=True),
        cost_estimate=pl.CostEstimate(
            flops=2 * slot_rows * model * (2 * tok + 12 * width),
            bytes_accessed=4 * ep_size * tp_size * tok * model,
            transcendentals=0,
        ),
        name="layer",
    )(tokens, d_out, ids, gate_vals, w_one, w_three, w_two)
    return outs[8], outs[11], outs[12], outs[13:]


def result_kernel(sums, last_land, rows_in, g1, g3, g2, out, dx, o1, o3, o2, parts, rows, row_buf, b1, b3, b2, in_sem, out_sem):
    moves = ((g1, b1, o1), (g3, b3, o3), (g2, b2, o2), (rows_in, row_buf, out))
    takes = [pltpu.make_async_copy(src, buf, in_sem.at[k]) for k, (src, buf, _) in enumerate(moves)]
    terms = [pltpu.make_async_copy(src, parts.at[k], in_sem.at[4 + k])
             for k, src in enumerate((sums.at[1, :, 2], last_land.at[1, 0], last_land.at[1, 1]))]
    for copy in terms + takes:
        copy.start()
    for copy in terms:
        copy.wait()
    part = parts.shape[3]
    for q in range(parts.shape[1]):
        rows[:, q * part : (q + 1) * part] = (parts[0, q] + (parts[1, q] + parts[2, q])).astype(BF16)
    puts = [pltpu.make_async_copy(rows, dx, out_sem.at[4])]
    puts[0].start()
    for k, (take, (_, buf, to)) in enumerate(zip(takes, moves)):
        take.wait()
        puts.append(pltpu.make_async_copy(buf, to, out_sem.at[k]))
        puts[-1].start()
    for copy in puts:
        copy.wait()


def results(sums, last_land, out, grads):
    _, quarters, _, tok, part = sums.shape
    hbm = pl.BlockSpec(memory_space=pl.ANY)
    row = jax.ShapeDtypeStruct((tok, quarters * part), BF16)
    rows = pltpu.VMEM((tok, quarters * part), BF16)
    return pl.pallas_call(
        result_kernel,
        in_specs=[hbm] * 6,
        out_specs=[hbm] * 5,
        out_shape=[row, row] + [jax.ShapeDtypeStruct(g.shape, g.dtype) for g in grads],
        scratch_shapes=[pltpu.VMEM((3, quarters, tok, part), F32), rows, rows]
        + [pltpu.VMEM(g.shape, g.dtype) for g in grads]
        + [pltpu.SemaphoreType.DMA((7,)), pltpu.SemaphoreType.DMA((5,))],
        compiler_params=pltpu.CompilerParams(vmem_limit_bytes=VMEM_LIMIT),
        name="results",
    )(sums, last_land, out, *grads)


def solution(mesh):
    ep_size, tp_size = mesh.shape["ep"], mesh.shape["tp"]
    row_spec = P(("dp", "ep", "tp"), None)
    col_spec = P("ep", None, "tp")
    down_spec = P("ep", "tp", None)
    grad_col = P(("dp", "ep"), None, "tp")
    grad_down = P(("dp", "ep"), "tp", None)

    def local_step(tokens, expert_ids, gate_vals, w_one, w_three, w_two, d_out):
        cap = slot_count(expert_ids.shape[1], tokens.shape[0], w_one.shape[0] * ep_size)
        sums, last_land, out, grads = layer(tokens, d_out, expert_ids.T, gate_vals.T, w_one, w_three, w_two, ep_size, tp_size, cap)
        return tuple(results(sums, last_land, out, grads))

    return jax.shard_map(local_step, mesh=mesh,
                         in_specs=(row_spec, row_spec, row_spec, col_spec, col_spec, down_spec, row_spec),
                         out_specs=(row_spec, row_spec, grad_col, grad_col, grad_down), check_vma=False)
```

```python
import functools

import jax
import jax.numpy as jnp
from jax import lax
from jax.experimental import pallas as pl
from jax.experimental.pallas import tpu as pltpu
from jax.sharding import PartitionSpec as P

BF16 = jnp.bfloat16
F32 = jnp.float32
MESH = pl.DeviceIdType.MESH
VMEM_LIMIT = 67_043_328
PARTS = 3


def slot_count(num_top, tok_dev, experts):
    return 8 * ((5 * num_top * tok_dev + 32 * experts - 1) // (32 * experts))


def dot(a, b):
    return jnp.dot(a, b, preferred_element_type=F32)


def dot_tb(a, b):
    return lax.dot_general(a, b, (((1,), (1,)), ((), ())), preferred_element_type=F32)


def dot_ta(a, b):
    return lax.dot_general(a, b, (((0,), (0,)), ((), ())), preferred_element_type=F32)


def earlier_rows(tok):
    row = lax.broadcasted_iota(jnp.int32, (tok, tok), 0)
    col = lax.broadcasted_iota(jnp.int32, (tok, tok), 1)
    return jnp.where(row < col, 1.0, 0.0).astype(BF16)


def expert_rows(routes, first, own, earlier):
    top = routes.shape[0] // 2
    ids, gates = routes[:top], routes[top:]
    hits = [ids == (first + e).astype(F32) for e in range(own)]
    routed = jnp.concatenate([jnp.sum(jnp.where(m, 1.0, 0.0), axis=0, keepdims=True) for m in hits], axis=0)
    gate = jnp.concatenate([jnp.sum(jnp.where(m, gates, 0.0), axis=0, keepdims=True) for m in hits], axis=0)
    return jnp.where(routed > 0.0, dot(routed.astype(BF16), earlier), -1.0), gate


def hit_masks(pos, cap):
    slot = lax.broadcasted_iota(jnp.int32, (cap, pos.shape[1]), 0).astype(F32)
    return [pos[e : e + 1, :] == slot for e in range(pos.shape[0])]


def one_hot(masks):
    return jnp.concatenate([jnp.where(m, 1.0, 0.0) for m in masks], axis=0).astype(BF16)


def slot_gates(masks, gate):
    return jnp.concatenate([jnp.where(m, gate[e : e + 1, :], 0.0) for e, m in enumerate(masks)], axis=0)


def three_parts(x):
    hi = x.astype(BF16)
    rest = x - hi.astype(F32)
    mid = rest.astype(BF16)
    return hi, mid, (rest - mid.astype(F32)).astype(BF16)


class Links:
    def __init__(self, send_sem, recv_sem):
        self.send_sem, self.recv_sem, self.sent, self.finished = send_sem, recv_sem, [], set()

    def copy(self, k, src, dst, to):
        return pltpu.make_async_remote_copy(src_ref=src, dst_ref=dst, send_sem=self.send_sem.at[k],
                                            recv_sem=self.recv_sem.at[k], device_id=to, device_id_type=MESH)

    def send(self, src, dst, to):
        k = len(self.sent)
        copy = self.copy(k, src, dst, to)
        copy.start()
        self.sent.append(copy)
        return k

    def arrive(self, k, dst, to):
        self.copy(k, dst, dst, to).wait_recv()

    def finish(self, k):
        self.finished.add(k)
        self.sent[k].wait_send()

    def drain(self):
        for k in range(len(self.sent)):
            if k not in self.finished:
                self.finish(k)


def copy_count(own):
    return 6 + 21 * 3 + 24 + 4 * own + 4 * (PARTS + 1) + 2 * PARTS * 4


def layer_kernel(own, cap, width, tokens, d_out, ids, gate_vals, w1, w3, w2, x_all, dy_all, r_all, w13_all, w2_all, xs_all,
                 us_all, ab_all, sums, far_land, last_land, out, g1, g3, g2, r_own, i_own, w13, w2s, xb,
                 dyb, rb, routes, earlier, xs, us, acc13, acc2, wide_buf, w2v, ab_buf, d_all, y_buf, give, keep_sum, mate_sum,
                 far_sum, send_sem, recv_sem, row_sem, load_sem, w_sem, slot_sem, in_sem, ab_sem, sum_sem, own_sem, g_sem, free_sem):
    ep, tp = lax.axis_index("ep"), lax.axis_index("tp")
    eps, tps = x_all.shape[0], x_all.shape[1]
    model = x_all.shape[3]
    part = model // PARTS
    half = eps // 2
    x_own, dy_own = xs.at[0], xs.at[1]
    step = lambda n: lax.rem(ep + (n + eps), eps)
    turn = lambda n: lax.rem(tp + (n + tps), tps)
    right, left, far = step(2), step(-2), step(4)
    mate = ep + 1 - 2 * lax.rem(ep, 2)
    mate_step = lambda n: lax.rem(mate + (n + eps), eps)
    up, down, over = turn(1), turn(-1), turn(2)
    to_right, to_left, to_mate = {"ep": right}, {"ep": left}, {"ep": mate}
    to_up, to_down = {"tp": up}, {"tp": down}
    links = Links(send_sem, recv_sem)

    barrier = pltpu.get_barrier_semaphore()
    for to in (to_right, to_left, to_mate, to_up, to_down):
        pl.semaphore_signal(barrier, inc=1, device_id=to, device_id_type=MESH)
    top = ids.shape[0]
    firsts = [pltpu.make_async_copy(ids, i_own, row_sem.at[0]), pltpu.make_async_copy(gate_vals, r_own.at[pl.ds(top, top)], row_sem.at[1]),
              pltpu.make_async_copy(tokens, x_own, row_sem.at[2]), pltpu.make_async_copy(d_out, dy_own, row_sem.at[3])]
    loads = [pltpu.make_async_copy(src.at[:, pl.ds(m * part, part)], w13.at[:, m, :, pl.ds(k * width, width)], w_sem.at[PARTS * k + m])
             for k, src in ((0, w1), (1, w3)) for m in range(PARTS)]
    loads.append(pltpu.make_async_copy(w2, w2s, w_sem.at[2 * PARTS]))
    for copy in firsts + loads:
        copy.start()
    firsts[0].wait()
    r_own[0:top] = i_own[...].astype(F32)
    for copy in firsts[1:]:
        copy.wait()
    with jax.named_scope("barrier"):
        pl.semaphore_wait(barrier, 5)

    own_refs, all_refs = (x_own, dy_own, r_own), (x_all, dy_all, r_all)
    upward = (True, False, True)
    kinds = (0, 1, 2)

    def spread(t, srcs):
        out = {}
        for kind in kinds:
            to = to_right if upward[kind] else to_left
            out[kind, upward[kind]] = links.send(srcs[kind], all_refs[kind].at[ep, t], to)
        for kind in kinds:
            to = to_left if upward[kind] else to_right
            out[kind, not upward[kind]] = links.send(srcs[kind], all_refs[kind].at[ep, t], to)
        for kind in kinds:
            out[kind, "mate"] = links.send(srcs[kind], all_refs[kind].at[ep, t], to_mate)
        return out

    def pass_on(g):
        state, t = states[g], groups[g]
        for kind in kinds:
            got, to = (left, to_right) if upward[kind] else (right, to_left)
            block = all_refs[kind].at[got, t]
            links.arrive(state[kind, upward[kind]], block, to)
            state[kind, "far"] = links.send(block, block, to)
            state[kind, "mate1"] = links.send(block, block, to_mate)

    def share(g):
        state, t = states[g], groups[g]
        for kind in kinds:
            got, to = (right, to_left) if upward[kind] else (left, to_right)
            block = all_refs[kind].at[got, t]
            links.arrive(state[kind, not upward[kind]], block, to)
            state[kind, "mate2"] = links.send(block, block, to_mate)

    def last(g):
        state, t = states[g], groups[g]
        for kind in kinds:
            block = all_refs[kind].at[far, t]
            links.arrive(state[kind, "far"], block, to_right if upward[kind] else to_left)
            state[kind, "mate3"] = links.send(block, block, to_mate)

    def from_mate(g):
        state, t = states[g], groups[g]
        for kind in kinds:
            one, two = (mate_step(-2), mate_step(2)) if upward[kind] else (mate_step(2), mate_step(-2))
            for name, at in (("mate", mate), ("mate1", one), ("mate2", two), ("mate3", mate_step(4))):
                links.arrive(state[kind, name], all_refs[kind].at[at, t], to_mate)

    core = lax.rem(ep, 2)

    def send_over():
        return [{kind: links.send(all_refs[kind].at[core + 2 * m, down if upward[kind] else up],
                                  all_refs[kind].at[core + 2 * m, down if upward[kind] else up],
                                  to_up if upward[kind] else to_down) for kind in kinds} for m in range(half)]

    def share_over(m):
        for kind in kinds:
            block = all_refs[kind].at[core + 2 * m, over]
            links.arrive(over_state[m][kind], block, to_up if upward[kind] else to_down)
            over_state[m][kind, "mate"] = links.send(block, block, to_mate)

    def have_over(m):
        for kind in kinds:
            links.arrive(over_state[m][kind, "mate"], all_refs[kind].at[1 - core + 2 * m, over], to_mate)

    def both_ways(src, dst):
        return {True: links.send(src, dst, to_up), False: links.send(src, dst, to_down)}

    def pass_halves(state, below, above, split):
        links.arrive(state[True], below, to_up)
        state["first"] = links.send(split(below, 0), split(below, 0), to_up)
        links.arrive(state[False], above, to_down)
        state["second"] = links.send(split(above, 1), split(above, 1), to_down)

    def have_halves(state, block, split):
        links.arrive(state["first"], split(block, 0), to_up)
        links.arrive(state["second"], split(block, 1), to_down)

    w13_state, w2_state = [None] * own, [None] * (PARTS + 1)
    split13 = lambda ref, k: ref.at[:, pl.ds(k * (part // 2), part // 2)]
    split2 = lambda ref, k: ref.at[:, pl.ds(k * (width // 2), width // 2)]

    def send13(e):
        w13_state[e] = both_ways(w13.at[e], w13_all.at[tp, e])

    def pass13(e):
        pass_halves(w13_state[e], w13_all.at[down, e], w13_all.at[up, e], split13)

    def have13(e):
        have_halves(w13_state[e], w13_all.at[over, e], split13)

    pieces = [(q, pl.ds(0, own)) for q in range(PARTS - 1)] + [(PARTS - 1, pl.ds(0, 2)), (PARTS - 1, pl.ds(2, own - 2))]

    def piece(j, p):
        q, experts = pieces[p]
        return w2_all.at[j, q, experts]

    def send2(p):
        q, experts = pieces[p]
        w2_state[p] = both_ways(w2s.at[experts, :, pl.ds(q * part, part)], piece(tp, p))

    def pass2(p):
        pass_halves(w2_state[p], piece(down, p), piece(up, p), split2)

    def have2(p):
        have_halves(w2_state[p], piece(over, p), split2)

    def pair_loads(t, h, p):
        at = pl.ds(h * half + p * (half // 2), half // 2)
        return [pltpu.make_async_copy(src.at[at, t], dst.at[p], load_sem.at[k, p])
                for k, (src, dst) in enumerate(((x_all, xb), (dy_all, dyb), (r_all, rb)))]

    def half_group(t, h, keep, ahead):
        for p in range(2):
            for copy in pair_loads(t, h, p):
                copy.wait()

            def gather(b, carry):
                pos, gate = expert_rows(rb[p, b], ep * own, own, earlier[...])
                masks = hit_masks(pos, cap)
                pick = one_hot(masks)
                gates = jnp.sum(slot_gates(masks, gate), axis=1, keepdims=True)
                rows = pl.ds(pl.multiple_of((p * (half // 2) + b) * cap, cap), cap)
                picked = dot(pick, xb[p, b]).astype(BF16)
                for e in range(own):
                    xs[e, rows, :] = picked[e * cap : (e + 1) * cap]
                scaled = (gates * dot(pick, dyb[p, b])).astype(BF16)
                for e in range(own):
                    us[e, rows, :] = scaled[e * cap : (e + 1) * cap]
                return carry

            lax.fori_loop(0, half // 2, gather, 0)

            @pl.when(ahead)
            def _():
                for copy in pair_loads(t, 1, p):
                    copy.start()

        stores = []
        if keep:
            stores = [pltpu.make_async_copy(xs, xs_all.at[:, h], slot_sem.at[0]),
                      pltpu.make_async_copy(us, us_all.at[:, h], slot_sem.at[1])]
        for copy in stores:
            copy.start()

        def expert(e, carry):
            ab = dot(xs[e], w13[e].reshape(model, 2 * width))
            a, b = ab[:, :width], ab[:, width:]
            dh = dot_tb(us[e], w2s[e])
            sig = jax.nn.sigmoid(a)
            silu = a * sig
            hid = (silu * b).astype(BF16)
            da = (dh * b * sig * (1.0 + a * (1.0 - sig))).astype(BF16)
            db = (dh * silu).astype(BF16)
            acc13[e] += dot_ta(jnp.concatenate([da, db], axis=1), xs[e])
            acc2[e] += dot_ta(hid, us[e])
            return carry

        lax.fori_loop(0, own, expert, 0)
        for copy in stores:
            copy.wait()

    def start_loads(t, h):
        for p in range(2):
            for copy in pair_loads(t, h, p):
                copy.start()

    def compute(t, keep):
        start_loads(t, 0)

        def one_half(h, carry):
            half_group(t, h, keep, h == 0)
            return carry

        lax.fori_loop(0, 2, one_half, 0)

    slots = eps * cap
    pending = []

    def settle():
        while pending:
            pending.pop().wait()

    def hidden(e):
        rows = pltpu.make_async_copy(xs_all.at[e], xs.at[pl.ds(0, 2)], in_sem.at[tps])
        rows.start()
        for j in range(tps):
            pltpu.make_async_copy(w13_all.at[j, e], wide_buf.at[pl.ds(0, PARTS), j], in_sem.at[j]).start()
        settle()
        rows.wait()

        def shard(j, carry):
            pltpu.make_async_copy(w13_all.at[j, e], wide_buf.at[pl.ds(0, PARTS), j], in_sem.at[j]).wait()
            ab = dot(xs[0:2].reshape(slots, model), wide_buf[0:PARTS, j].reshape(model, 2 * width))
            ab_buf[j] = ab
            a, b = ab[:, :width], ab[:, width:]
            at = pl.ds(pl.multiple_of(lax.rem(j, 2) * width, width), width)
            d_all[e, j // 2, :, at] = (a * jax.nn.sigmoid(a) * b).astype(BF16)
            return carry

        lax.fori_loop(0, tps, shard, 0)
        pending.append(pltpu.make_async_copy(ab_buf, ab_all.at[e], ab_sem.at[0]))
        pending[-1].start()

    def put_rows(e, value):
        for k in range(eps):
            y_buf[k, e] = value[k * cap : (k + 1) * cap]

    def y_part(q):
        load = pltpu.make_async_copy(w2_all.at[:, q], w2v.at[q], in_sem.at[0])
        load.start()
        load.wait()

        def one(e, carry):
            y = dot(d_all[e, 0], w2v[q, 0:2, e].reshape(2 * width, part)) + dot(d_all[e, 1], w2v[q, 2:4, e].reshape(2 * width, part))
            put_rows(e, y.astype(BF16))
            return carry

        lax.fori_loop(0, own, one, 0)

    def ab_load(e, j):
        return pltpu.make_async_copy(ab_all.at[e, j], ab_buf.at[j], ab_sem.at[j])

    def u_load(e, slot):
        return pltpu.make_async_copy(us_all.at[e], us.at[pl.ds(2 * slot, 2)], in_sem.at[1 + slot])

    def hidden_grads():
        settle()
        u_load(0, 0).start()
        for j in range(tps):
            ab_load(0, j).start()

        def one(e, carry):
            slot = lax.rem(e, 2)
            u_load(e, slot).wait()

            @pl.when(e + 1 < own)
            def _():
                u_load(e + 1, 1 - slot).start()

            def two(k, carry):
                dh = None
                for q in range(PARTS):
                    at = pl.ds(q * part, part)
                    u = us[pl.ds(2 * slot, 2), :, at].reshape(slots, part)
                    term = dot_tb(u, w2v[q, pl.ds(2 * k, 2), e].reshape(2 * width, part))
                    dh = term if dh is None else dh + term
                for i in range(2):
                    j = 2 * k + i
                    ab_load(e, j).wait()
                    a, b, d = ab_buf[j, :, :width], ab_buf[j, :, width:], dh[:, i * width : (i + 1) * width]
                    sig = jax.nn.sigmoid(a)
                    d_all[e, j, :, :width] = (d * b * sig * (1.0 + a * (1.0 - sig))).astype(BF16)
                    d_all[e, j, :, width:] = (d * (a * sig)).astype(BF16)

                    @pl.when(e + 1 < own)
                    def _():
                        ab_load(e + 1, j).start()
                return carry

            lax.fori_loop(0, tps // 2, two, 0)
            return carry

        lax.fori_loop(0, own, one, 0)

    def v_load(q):
        return pltpu.make_async_copy(w13_all.at[:, :, q], wide_buf, in_sem.at[0])

    def v_part(q):
        v_load(q).wait()

        def one(e, carry):
            v = dot_tb(d_all[e, 0], wide_buf[0, e])
            for j in range(1, tps):
                v = v + dot_tb(d_all[e, j], wide_buf[j, e])
            put_rows(e, v.astype(BF16))
            return carry

        lax.fori_loop(0, own, one, 0)
        if q + 1 < PARTS:
            v_load(q + 1).start()

    gifts, writes, stages = {}, {}, {}

    def combine(kind, block):
        pos, gate = expert_rows(routes[block], ep * own, own, earlier[...])
        masks = hit_masks(pos, cap)
        rows = y_buf[block].reshape(own * cap, part)
        if kind == 1:
            return dot_ta(one_hot(masks), rows)
        hi, mid, low = three_parts(slot_gates(masks, gate))
        return dot_ta(hi, rows) + (dot_ta(mid, rows) + dot_ta(low, rows))

    numbers = {}

    def rightward(kind, q):
        return (kind + q) % 2 == 0

    def sum_begin(kind, q):
        n = numbers[kind, q] = len(numbers)
        slot = n % 2
        if n:
            links.finish(gifts[n - 1])
        for k in ready.pop(n - 2, ()):
            links.finish(k)
        if n - 2 in writes:
            writes.pop(n - 2).wait()

        def to_other(i, carry):
            give[i] = combine(kind, lax.rem(mate + 4 - 2 * i + eps, eps))
            return carry

        def to_own(i, carry):
            keep_sum[slot, i] = combine(kind, lax.rem(ep + 4 - 2 * i + eps, eps))
            return carry

        lax.fori_loop(0, 4, to_other, 0)
        if n:
            pl.semaphore_wait(free_sem, 1)
        gifts[n] = links.send(give, mate_sum, to_mate)
        lax.fori_loop(0, 4, to_own, 0)

    def sum_end(kind, q):
        n = numbers[kind, q]
        slot = n % 2
        links.arrive(gifts[n], mate_sum, to_mate)
        keep_sum[slot] += mate_sum[...]
        if n + 1 < 2 * PARTS:
            pl.semaphore_signal(free_sem, inc=1, device_id=to_mate, device_id_type=MESH)
        far_way, near_way, near, side = (to_right, to_left, 3, 1) if rightward(kind, q) else (to_left, to_right, 1, 0)
        stages[kind, q, "far"] = links.send(keep_sum.at[slot, 0], far_land.at[kind, q], far_way)
        stages[kind, q, "near"] = links.send(keep_sum.at[slot, near], last_land.at[kind, side, q], near_way)
        writes[n] = pltpu.make_async_copy(keep_sum.at[slot, 2], sums.at[kind, q], own_sem.at[slot])
        writes[n].start()

    def sum_turn(kind, q):
        n = numbers[kind, q]
        slot = n % 2
        way, at, side = (to_right, 1, 0) if rightward(kind, q) else (to_left, 3, 1)
        links.arrive(stages[kind, q, "far"], far_land.at[kind, q], way)
        load = pltpu.make_async_copy(far_land.at[kind, q], far_sum, sum_sem.at[0])
        load.start()
        load.wait()
        keep_sum[slot, at] += far_sum[...]
        stages[kind, q, "turn"] = links.send(keep_sum.at[slot, at], last_land.at[kind, side, q], way)
        ready[n] = tuple(stages[kind, q, name] for name in ("far", "near", "turn"))

    ready = {}

    def sums_here(kind):
        for q in range(PARTS):
            (way, back), sides = ((to_right, to_left), (0, 1)) if rightward(kind, q) else ((to_left, to_right), (1, 0))
            links.arrive(stages[kind, q, "near"], last_land.at[kind, sides[1], q], back)
            links.arrive(stages[kind, q, "turn"], last_land.at[kind, sides[0], q], way)

    def finish_out():
        links.finish(gifts[2 * PARTS - 1])
        three = pl.ds(0, PARTS)
        copies = [pltpu.make_async_copy(sums.at[0], give.at[three], sum_sem.at[0]),
                  pltpu.make_async_copy(last_land.at[0, 0], mate_sum.at[three], sum_sem.at[1])]
        for copy in copies:
            copy.start()
        for copy in copies:
            copy.wait()
        give[three] += mate_sum[three]
        copy = pltpu.make_async_copy(last_land.at[0, 1], mate_sum.at[three], sum_sem.at[0])
        copy.start()
        copy.wait()
        for q in range(PARTS):
            xb[0, 0, :, q * part : (q + 1) * part] = (give[q] + mate_sum[q]).astype(BF16)
        copy = pltpu.make_async_copy(xb.at[0, 0], out, sum_sem.at[0])
        copy.start()
        copy.wait()

    y_state = {}
    for way in (True, False):
        for kind in kinds:
            go_up = upward[kind] == way
            y_state[kind, go_up] = links.send(own_refs[kind], all_refs[kind].at[ep, tp], to_up if go_up else to_down)
    groups = (tp, down, up)
    states = [spread(tp, own_refs)]
    first_sends = range(len(links.sent))
    hold = [pltpu.make_async_copy(own_refs[kind], all_refs[kind].at[ep, tp], row_sem.at[kind]) for kind in range(3)]
    for copy in hold:
        copy.start()
    for copy in loads:
        copy.wait()
    stow = [pltpu.make_async_copy(w13, w13_all.at[tp], w_sem.at[0])]
    stow += [pltpu.make_async_copy(w2s.at[:, :, pl.ds(q * part, part)], w2_all.at[tp, q], w_sem.at[1 + q]) for q in range(PARTS)]
    for copy in stow:
        copy.start()
    earlier[...] = earlier_rows(earlier.shape[0])
    with jax.named_scope("zeros"):
        acc13[...] = jnp.zeros_like(acc13)
        acc2[...] = jnp.zeros_like(acc2)

    def y_arrive(kind, way):
        block = all_refs[kind].at[ep, down if way else up]
        links.arrive(y_state[kind, way], block, to_up if way else to_down)
        return block

    with jax.named_scope("pass_on_0"):
        pass_on(0)
    with jax.named_scope("y_arrive"):
        for way in (True, False):
            for kind in kinds:
                y_arrive(kind, way)
    with jax.named_scope("send13_0"):
        send13(0)
    with jax.named_scope("send13_1"):
        send13(1)
    with jax.named_scope("send13_2"):
        send13(2)
    states.append(spread(down, [ref.at[ep, down] for ref in all_refs]))
    with jax.named_scope("share_0"):
        share(0)
    with jax.named_scope("last_0"):
        last(0)
    for copy in hold + stow:
        copy.wait()
    with jax.named_scope("from_mate_0"):
        from_mate(0)
    route_copy = pltpu.make_async_copy(r_all.at[:, tp], routes, row_sem.at[0])
    route_copy.start()
    route_copy.wait()
    for k in first_sends:
        links.finish(k)
    with jax.named_scope("compute_tp_True"):
        compute(tp, True)
    with jax.named_scope("pass13_0"):
        pass13(0)
    with jax.named_scope("send13_3"):
        send13(3)
    with jax.named_scope("pass_on_1"):
        pass_on(1)
    states.append(spread(up, [ref.at[ep, up] for ref in all_refs]))
    with jax.named_scope("share_1"):
        share(1)
    with jax.named_scope("pass13_1"):
        pass13(1)
    with jax.named_scope("send13_4"):
        send13(4)
    with jax.named_scope("have13_0"):
        have13(0)
    with jax.named_scope("hidden_0"):
        hidden(0)
    with jax.named_scope("pass13_2"):
        pass13(2)
    with jax.named_scope("last_1"):
        last(1)
    with jax.named_scope("from_mate_1"):
        from_mate(1)
    with jax.named_scope("compute_down_False"):
        compute(down, False)
    with jax.named_scope("pass13_3"):
        pass13(3)
    with jax.named_scope("send2_0"):
        send2(0)
    with jax.named_scope("pass_on_2"):
        pass_on(2)
    with jax.named_scope("have13_1"):
        have13(1)
    with jax.named_scope("hidden_1"):
        hidden(1)
    with jax.named_scope("share_2"):
        share(2)
    with jax.named_scope("pass13_4"):
        pass13(4)
    with jax.named_scope("have13_2"):
        have13(2)
    with jax.named_scope("hidden_2"):
        hidden(2)
    with jax.named_scope("last_2"):
        last(2)
    with jax.named_scope("from_mate_2"):
        from_mate(2)
    with jax.named_scope("have13_3"):
        have13(3)
    with jax.named_scope("hidden_3"):
        hidden(3)
    with jax.named_scope("start_loads_up_0"):
        start_loads(up, 0)
    with jax.named_scope("half_group_up_0_False_True"):
        half_group(up, 0, False, True)
    with jax.named_scope("pass2_0"):
        pass2(0)
    with jax.named_scope("send2_1"):
        send2(1)
        send2(2)
    with jax.named_scope("half_group_up_1_False_False"):
        half_group(up, 1, False, False)
    with jax.named_scope("have13_4"):
        have13(4)
    with jax.named_scope("hidden_4"):
        hidden(4)

    with jax.named_scope("have2_0"):
        have2(0)
    with jax.named_scope("y_part_0"):
        y_part(0)
    with jax.named_scope("sum_begin_0_0"):
        sum_begin(0, 0)
    with jax.named_scope("sum_end_0_0"):
        sum_end(0, 0)
    with jax.named_scope("pass2_1"):
        pass2(1)
    with jax.named_scope("send2_3"):
        send2(3)
    with jax.named_scope("pass2_2"):
        pass2(2)
    with jax.named_scope("sum_turn_0_0"):
        sum_turn(0, 0)
    with jax.named_scope("have2_1"):
        have2(1)
    with jax.named_scope("y_part_1"):
        y_part(1)
    with jax.named_scope("sum_begin_0_1"):
        sum_begin(0, 1)
    with jax.named_scope("pass2_3"):
        pass2(3)
    over_state = send_over()
    with jax.named_scope("sum_end_0_1"):
        sum_end(0, 1)
    with jax.named_scope("have2_2"):
        have2(2)
        have2(3)
    with jax.named_scope("y_part_2"):
        y_part(2)
    with jax.named_scope("sum_begin_0_2"):
        sum_begin(0, 2)
    with jax.named_scope("sum_end_0_2"):
        sum_end(0, 2)
    v_load(0).start()
    with jax.named_scope("sum_turn_0_1"):
        sum_turn(0, 1)
    with jax.named_scope("hidden_grads"):
        hidden_grads()
    with jax.named_scope("sum_turn_0_2"):
        sum_turn(0, 2)
    with jax.named_scope("v_part_0"):
        v_part(0)
    with jax.named_scope("sum_begin_1_0"):
        sum_begin(1, 0)
    with jax.named_scope("sum_end_1_0"):
        sum_end(1, 0)
    with jax.named_scope("share_over_0"):
        share_over(0)
    with jax.named_scope("v_part_1"):
        v_part(1)
    with jax.named_scope("sum_begin_1_1"):
        sum_begin(1, 1)
    with jax.named_scope("sum_end_1_1"):
        sum_end(1, 1)
    with jax.named_scope("sum_turn_1_0"):
        sum_turn(1, 0)
    with jax.named_scope("share_over_1"):
        share_over(1)
    with jax.named_scope("v_part_2"):
        v_part(2)
    with jax.named_scope("sum_begin_1_2"):
        sum_begin(1, 2)
    with jax.named_scope("sum_end_1_2"):
        sum_end(1, 2)
    with jax.named_scope("have_over_0"):
        have_over(0)
    with jax.named_scope("have_over_1"):
        have_over(1)
    with jax.named_scope("start_loads_over_0"):
        start_loads(over, 0)
    with jax.named_scope("sum_turn_1_1"):
        sum_turn(1, 1)
    with jax.named_scope("half_group_over_0_False_False"):
        half_group(over, 0, False, False)
    with jax.named_scope("sum_turn_1_2"):
        sum_turn(1, 2)
    with jax.named_scope("share_over_2"):
        share_over(2)
    with jax.named_scope("share_over_3"):
        share_over(3)
    with jax.named_scope("have_over_2"):
        have_over(2)
    with jax.named_scope("have_over_3"):
        have_over(3)
    with jax.named_scope("start_loads_over_1"):
        start_loads(over, 1)
    with jax.named_scope("half_group_over_1_False_False"):
        half_group(over, 1, False, False)

    def grad_stores(e, slot):
        rows = pl.ds(0, PARTS)
        return [pltpu.make_async_copy(wide_buf.at[slot, rows, :, pl.ds(0, width)], g1.at[e], g_sem.at[slot, 0]),
                pltpu.make_async_copy(wide_buf.at[slot, rows, :, pl.ds(width, width)], g3.at[e], g_sem.at[slot, 1]),
                pltpu.make_async_copy(xs.at[slot, pl.ds(0, width)], g2.at[e], g_sem.at[slot, 2])]

    def finish(e, carry):
        slot = lax.rem(e, 2)

        @pl.when(e >= 2)
        def _():
            for copy in grad_stores(e - 2, slot):
                copy.wait()

        for m in range(PARTS):
            wide_buf[slot, m] = acc13[e, :, m * part : (m + 1) * part].T.astype(BF16)
        xs[slot, pl.ds(0, width), :] = acc2[e].astype(BF16)
        for copy in grad_stores(e, slot):
            copy.start()
        return carry

    with jax.named_scope("finish"):
        lax.fori_loop(0, own, finish, 0)
        for e in range(max(own - 2, 0), own):
            for copy in grad_stores(e, e % 2):
                copy.wait()
    with jax.named_scope("sums_here_0"):
        sums_here(0)
    with jax.named_scope("finish_out"):
        finish_out()
    with jax.named_scope("sums_here_1"):
        sums_here(1)
    for n in sorted(writes):
        writes[n].wait()
    with jax.named_scope("drain"):
        links.drain()


def layer(tokens, d_out, ids, gate_vals, w_one, w_three, w_two, ep_size, tp_size, cap):
    tok, model = tokens.shape
    own, width, _ = w_two.shape
    half = ep_size // 2
    rows = half * cap
    part = model // PARTS
    hbm = pl.BlockSpec(memory_space=pl.ANY)
    shape = jax.ShapeDtypeStruct
    routes = (2 * ids.shape[0], tok)
    copies = copy_count(own)
    slot_rows = ep_size * tp_size * cap * own
    vector = pltpu.VMEM
    dma = pltpu.SemaphoreType.DMA
    outs = pl.pallas_call(
        functools.partial(layer_kernel, own, cap, width),
        in_specs=[hbm] * 7,
        out_specs=[hbm] * 15,
        out_shape=[
            shape((ep_size, tp_size, tok, model), BF16),
            shape((ep_size, tp_size, tok, model), BF16),
            shape((ep_size, tp_size) + routes, F32),
            shape((tp_size, own, PARTS, part, 2 * width), BF16),
            shape((tp_size, PARTS, own, width, part), BF16),
            shape((own, 2, rows, model), BF16),
            shape((own, 2, rows, model), BF16),
            shape((own, tp_size, 2 * rows, 2 * width), F32),
            shape((2, PARTS, tok, part), F32),
            shape((2, PARTS, tok, part), F32),
            shape((2, 2, PARTS, tok, part), F32),
            shape((tok, model), BF16),
            shape((own, PARTS, part, width), BF16),
            shape((own, PARTS, part, width), BF16),
            shape((own, width, model), BF16),
        ],
        scratch_shapes=[
            vector(routes, F32),
            vector(ids.shape, jnp.int32),
            vector((own, PARTS, part, 2 * width), BF16),
            vector((own, width, model), BF16),
            vector((2, half // 2, tok, model), BF16),
            vector((2, half // 2, tok, model), BF16),
            vector((2, half // 2) + routes, F32),
            vector((ep_size,) + routes, F32),
            vector((tok, tok), BF16),
            vector((own, rows, model), BF16),
            vector((own, rows, model), BF16),
            vector((own, 2 * width, model), F32),
            vector((own, width, model), F32),
            vector((tp_size, own, part, 2 * width), BF16),
            vector((PARTS, tp_size, own, width, part), BF16),
            vector((tp_size, 2 * rows, 2 * width), F32),
            vector((own, tp_size, 2 * rows, 2 * width), BF16),
            vector((ep_size, own, cap, part), BF16),
            vector((4, tok, part), F32),
            vector((2, 4, tok, part), F32),
            vector((4, tok, part), F32),
            vector((tok, part), F32),
            dma((copies,)),
            dma((copies,)),
            dma((4,)),
            dma((3, 2)),
            dma((2 * PARTS + 1,)),
            dma((2,)),
            dma((1 + tp_size,)),
            dma((tp_size,)),
            dma((2,)),
            dma((2,)),
            dma((2, 3)),
            pltpu.SemaphoreType.REGULAR,
        ],
        compiler_params=pltpu.CompilerParams(vmem_limit_bytes=VMEM_LIMIT, collective_id=0, has_side_effects=True),
        cost_estimate=pl.CostEstimate(
            flops=2 * slot_rows * model * (2 * tok + 12 * width),
            bytes_accessed=4 * ep_size * tp_size * tok * model,
            transcendentals=0,
        ),
        name="layer",
    )(tokens, d_out, ids, gate_vals, w_one, w_three, w_two)
    g1, g3, g2 = outs[12:]
    return outs[8], outs[10], outs[11], (g1.reshape(own, model, width), g3.reshape(own, model, width), g2)


def result_kernel(sums, last_land, rows_in, g1, g3, g2, out, dx, o1, o3, o2, parts, rows, row_buf, b1, b3, b2, in_sem, out_sem):
    moves = ((g1, b1, o1), (g3, b3, o3), (g2, b2, o2), (rows_in, row_buf, out))
    takes = [pltpu.make_async_copy(src, buf, in_sem.at[k]) for k, (src, buf, _) in enumerate(moves)]
    terms = [pltpu.make_async_copy(src, parts.at[k], in_sem.at[4 + k])
             for k, src in enumerate((sums.at[1], last_land.at[1, 0], last_land.at[1, 1]))]
    for copy in terms + takes:
        copy.start()
    for copy in terms:
        copy.wait()
    part = parts.shape[3]
    for q in range(parts.shape[1]):
        rows[:, q * part : (q + 1) * part] = (parts[0, q] + (parts[1, q] + parts[2, q])).astype(BF16)
    puts = [pltpu.make_async_copy(rows, dx, out_sem.at[4])]
    puts[0].start()
    for k, (take, (_, buf, to)) in enumerate(zip(takes, moves)):
        take.wait()
        puts.append(pltpu.make_async_copy(buf, to, out_sem.at[k]))
        puts[-1].start()
    for copy in puts:
        copy.wait()


def results(sums, last_land, out, grads):
    _, count, tok, part = sums.shape
    hbm = pl.BlockSpec(memory_space=pl.ANY)
    row = jax.ShapeDtypeStruct((tok, count * part), BF16)
    rows = pltpu.VMEM((tok, count * part), BF16)
    return pl.pallas_call(
        result_kernel,
        in_specs=[hbm] * 6,
        out_specs=[hbm] * 5,
        out_shape=[row, row] + [jax.ShapeDtypeStruct(g.shape, g.dtype) for g in grads],
        scratch_shapes=[pltpu.VMEM((3, count, tok, part), F32), rows, rows]
        + [pltpu.VMEM(g.shape, g.dtype) for g in grads]
        + [pltpu.SemaphoreType.DMA((7,)), pltpu.SemaphoreType.DMA((5,))],
        compiler_params=pltpu.CompilerParams(vmem_limit_bytes=VMEM_LIMIT),
        name="results",
    )(sums, last_land, out, *grads)


def solution(mesh):
    ep_size, tp_size = mesh.shape["ep"], mesh.shape["tp"]
    row_spec = P(("dp", "ep", "tp"), None)
    col_spec = P("ep", None, "tp")
    down_spec = P("ep", "tp", None)
    grad_col = P(("dp", "ep"), None, "tp")
    grad_down = P(("dp", "ep"), "tp", None)

    def local_step(tokens, expert_ids, gate_vals, w_one, w_three, w_two, d_out):
        cap = slot_count(expert_ids.shape[1], tokens.shape[0], w_one.shape[0] * ep_size)
        sums, last_land, out, grads = layer(tokens, d_out, expert_ids.T, gate_vals.T, w_one, w_three, w_two, ep_size, tp_size, cap)
        return tuple(results(sums, last_land, out, grads))

    return jax.shard_map(local_step, mesh=mesh,
                         in_specs=(row_spec, row_spec, row_spec, col_spec, col_spec, down_spec, row_spec),
                         out_specs=(row_spec, row_spec, grad_col, grad_col, grad_down), check_vma=False)
```

```python
import functools

import jax
import jax.numpy as jnp
from jax import lax
from jax.experimental import pallas as pl
from jax.experimental.pallas import tpu as pltpu
from jax.sharding import PartitionSpec as P

BF16 = jnp.bfloat16
F32 = jnp.float32
MESH = pl.DeviceIdType.MESH
VMEM_LIMIT = 67_043_328
PARTS = 3


def slot_count(num_top, tok_dev, experts):
    return 8 * ((5 * num_top * tok_dev + 32 * experts - 1) // (32 * experts))


def dot(a, b):
    return jnp.dot(a, b, preferred_element_type=F32)


def dot_tb(a, b):
    return lax.dot_general(a, b, (((1,), (1,)), ((), ())), preferred_element_type=F32)


def dot_ta(a, b):
    return lax.dot_general(a, b, (((0,), (0,)), ((), ())), preferred_element_type=F32)


def earlier_rows(tok):
    row = lax.broadcasted_iota(jnp.int32, (tok, tok), 0)
    col = lax.broadcasted_iota(jnp.int32, (tok, tok), 1)
    return jnp.where(row < col, 1.0, 0.0).astype(BF16)


def expert_rows(routes, first, own, earlier):
    top = routes.shape[0] // 2
    ids, gates = routes[:top], routes[top:]
    hits = [ids == (first + e).astype(F32) for e in range(own)]
    routed = jnp.concatenate([jnp.sum(jnp.where(m, 1.0, 0.0), axis=0, keepdims=True) for m in hits], axis=0)
    gate = jnp.concatenate([jnp.sum(jnp.where(m, gates, 0.0), axis=0, keepdims=True) for m in hits], axis=0)
    return jnp.where(routed > 0.0, dot(routed.astype(BF16), earlier), -1.0), gate


def hit_masks(pos, cap):
    slot = lax.broadcasted_iota(jnp.int32, (cap, pos.shape[1]), 0).astype(F32)
    return [pos[e : e + 1, :] == slot for e in range(pos.shape[0])]


def one_hot(masks):
    return jnp.concatenate([jnp.where(m, 1.0, 0.0) for m in masks], axis=0).astype(BF16)


def slot_gates(masks, gate):
    return jnp.concatenate([jnp.where(m, gate[e : e + 1, :], 0.0) for e, m in enumerate(masks)], axis=0)


def three_parts(x):
    hi = x.astype(BF16)
    rest = x - hi.astype(F32)
    mid = rest.astype(BF16)
    return hi, mid, (rest - mid.astype(F32)).astype(BF16)


class Links:
    def __init__(self, send_sem, recv_sem):
        self.send_sem, self.recv_sem, self.sent, self.finished = send_sem, recv_sem, [], set()

    def copy(self, k, src, dst, to):
        return pltpu.make_async_remote_copy(src_ref=src, dst_ref=dst, send_sem=self.send_sem.at[k],
                                            recv_sem=self.recv_sem.at[k], device_id=to, device_id_type=MESH)

    def send(self, src, dst, to):
        k = len(self.sent)
        copy = self.copy(k, src, dst, to)
        copy.start()
        self.sent.append(copy)
        return k

    def arrive(self, k, dst, to):
        self.copy(k, dst, dst, to).wait_recv()

    def finish(self, k):
        self.finished.add(k)
        self.sent[k].wait_send()

    def drain(self):
        for k in range(len(self.sent)):
            if k not in self.finished:
                self.finish(k)


def copy_count(own):
    return 6 + 21 * 3 + 24 + 4 * own + 4 * (PARTS + 1) + 2 * PARTS * 7


def layer_kernel(own, cap, width, tokens, d_out, ids, gate_vals, w1, w3, w2, x_all, dy_all, r_all, w13_all, w2_all, xs_all,
                 us_all, ab_all, sums, far_land, last_land, out, g1, g3, g2, r_own, i_own, w13, w2s, xb,
                 dyb, rb, routes, earlier, xs, us, acc13, acc2, wide_buf, w2v, ab_buf, d_all, y_buf, give, keep_sum, mate_sum,
                 far_sum, send_sem, recv_sem, row_sem, load_sem, w_sem, slot_sem, in_sem, ab_sem, sum_sem, own_sem, g_sem, free_sem):
    ep, tp = lax.axis_index("ep"), lax.axis_index("tp")
    eps, tps = x_all.shape[0], x_all.shape[1]
    model = x_all.shape[3]
    part = model // PARTS
    half = eps // 2
    x_own, dy_own = xs.at[0], xs.at[1]
    step = lambda n: lax.rem(ep + (n + eps), eps)
    turn = lambda n: lax.rem(tp + (n + tps), tps)
    right, left, far = step(2), step(-2), step(4)
    mate = ep + 1 - 2 * lax.rem(ep, 2)
    mate_step = lambda n: lax.rem(mate + (n + eps), eps)
    up, down, over = turn(1), turn(-1), turn(2)
    to_right, to_left, to_mate = {"ep": right}, {"ep": left}, {"ep": mate}
    to_up, to_down = {"tp": up}, {"tp": down}
    links = Links(send_sem, recv_sem)

    barrier = pltpu.get_barrier_semaphore()
    for to in (to_right, to_left, to_mate, to_up, to_down):
        pl.semaphore_signal(barrier, inc=1, device_id=to, device_id_type=MESH)
    top = ids.shape[0]
    firsts = [pltpu.make_async_copy(ids, i_own, row_sem.at[0]), pltpu.make_async_copy(gate_vals, r_own.at[pl.ds(top, top)], row_sem.at[1]),
              pltpu.make_async_copy(tokens, x_own, row_sem.at[2]), pltpu.make_async_copy(d_out, dy_own, row_sem.at[3])]
    loads = [pltpu.make_async_copy(src.at[:, pl.ds(m * part, part)], w13.at[:, m, :, pl.ds(k * width, width)], w_sem.at[PARTS * k + m])
             for k, src in ((0, w1), (1, w3)) for m in range(PARTS)]
    loads.append(pltpu.make_async_copy(w2, w2s, w_sem.at[2 * PARTS]))
    for copy in firsts + loads:
        copy.start()
    firsts[0].wait()
    r_own[0:top] = i_own[...].astype(F32)
    for copy in firsts[1:]:
        copy.wait()
    with jax.named_scope("barrier"):
        pl.semaphore_wait(barrier, 5)

    own_refs, all_refs = (x_own, dy_own, r_own), (x_all, dy_all, r_all)
    upward = (True, False, True)
    kinds = (0, 1, 2)

    def spread(t, srcs):
        out = {}
        for kind in kinds:
            to = to_right if upward[kind] else to_left
            out[kind, upward[kind]] = links.send(srcs[kind], all_refs[kind].at[ep, t], to)
        for kind in kinds:
            to = to_left if upward[kind] else to_right
            out[kind, not upward[kind]] = links.send(srcs[kind], all_refs[kind].at[ep, t], to)
        for kind in kinds:
            out[kind, "mate"] = links.send(srcs[kind], all_refs[kind].at[ep, t], to_mate)
        return out

    def pass_on(g):
        state, t = states[g], groups[g]
        for kind in kinds:
            got, to = (left, to_right) if upward[kind] else (right, to_left)
            block = all_refs[kind].at[got, t]
            links.arrive(state[kind, upward[kind]], block, to)
            state[kind, "far"] = links.send(block, block, to)
            state[kind, "mate1"] = links.send(block, block, to_mate)

    def share(g):
        state, t = states[g], groups[g]
        for kind in kinds:
            got, to = (right, to_left) if upward[kind] else (left, to_right)
            block = all_refs[kind].at[got, t]
            links.arrive(state[kind, not upward[kind]], block, to)
            state[kind, "mate2"] = links.send(block, block, to_mate)

    def last(g):
        state, t = states[g], groups[g]
        for kind in kinds:
            block = all_refs[kind].at[far, t]
            links.arrive(state[kind, "far"], block, to_right if upward[kind] else to_left)
            state[kind, "mate3"] = links.send(block, block, to_mate)

    def from_mate(g):
        state, t = states[g], groups[g]
        for kind in kinds:
            one, two = (mate_step(-2), mate_step(2)) if upward[kind] else (mate_step(2), mate_step(-2))
            for name, at in (("mate", mate), ("mate1", one), ("mate2", two), ("mate3", mate_step(4))):
                links.arrive(state[kind, name], all_refs[kind].at[at, t], to_mate)

    core = lax.rem(ep, 2)

    def send_over():
        return [{kind: links.send(all_refs[kind].at[core + 2 * m, down if upward[kind] else up],
                                  all_refs[kind].at[core + 2 * m, down if upward[kind] else up],
                                  to_up if upward[kind] else to_down) for kind in kinds} for m in range(half)]

    def share_over(m):
        for kind in kinds:
            block = all_refs[kind].at[core + 2 * m, over]
            links.arrive(over_state[m][kind], block, to_up if upward[kind] else to_down)
            over_state[m][kind, "mate"] = links.send(block, block, to_mate)

    def have_over(m):
        for kind in kinds:
            links.arrive(over_state[m][kind, "mate"], all_refs[kind].at[1 - core + 2 * m, over], to_mate)

    def both_ways(src, dst):
        return {True: links.send(src, dst, to_up), False: links.send(src, dst, to_down)}

    def pass_halves(state, below, above, split):
        links.arrive(state[True], below, to_up)
        state["first"] = links.send(split(below, 0), split(below, 0), to_up)
        links.arrive(state[False], above, to_down)
        state["second"] = links.send(split(above, 1), split(above, 1), to_down)

    def have_halves(state, block, split):
        links.arrive(state["first"], split(block, 0), to_up)
        links.arrive(state["second"], split(block, 1), to_down)

    w13_state, w2_state = [None] * own, [None] * (PARTS + 1)
    split13 = lambda ref, k: ref.at[:, pl.ds(k * (part // 2), part // 2)]
    split2 = lambda ref, k: ref.at[:, pl.ds(k * (width // 2), width // 2)]

    def send13(e):
        w13_state[e] = both_ways(w13.at[e], w13_all.at[tp, e])

    def pass13(e):
        pass_halves(w13_state[e], w13_all.at[down, e], w13_all.at[up, e], split13)

    def have13(e):
        have_halves(w13_state[e], w13_all.at[over, e], split13)

    pieces = [(q, pl.ds(0, own)) for q in range(PARTS - 1)] + [(PARTS - 1, pl.ds(0, 2)), (PARTS - 1, pl.ds(2, own - 2))]

    def piece(j, p):
        q, experts = pieces[p]
        return w2_all.at[j, q, experts]

    def send2(p):
        q, experts = pieces[p]
        w2_state[p] = both_ways(w2s.at[experts, :, pl.ds(q * part, part)], piece(tp, p))

    def pass2(p):
        pass_halves(w2_state[p], piece(down, p), piece(up, p), split2)

    def have2(p):
        have_halves(w2_state[p], piece(over, p), split2)

    def pair_loads(t, h, p):
        at = pl.ds(h * half + p * (half // 2), half // 2)
        return [pltpu.make_async_copy(src.at[at, t], dst.at[p], load_sem.at[k, p])
                for k, (src, dst) in enumerate(((x_all, xb), (dy_all, dyb), (r_all, rb)))]

    def half_group(t, h, keep, ahead):
        for p in range(2):
            for copy in pair_loads(t, h, p):
                copy.wait()

            def gather(b, carry):
                pos, gate = expert_rows(rb[p, b], ep * own, own, earlier[...])
                masks = hit_masks(pos, cap)
                pick = one_hot(masks)
                gates = jnp.sum(slot_gates(masks, gate), axis=1, keepdims=True)
                rows = pl.ds(pl.multiple_of((p * (half // 2) + b) * cap, cap), cap)
                picked = dot(pick, xb[p, b]).astype(BF16)
                for e in range(own):
                    xs[e, rows, :] = picked[e * cap : (e + 1) * cap]
                scaled = (gates * dot(pick, dyb[p, b])).astype(BF16)
                for e in range(own):
                    us[e, rows, :] = scaled[e * cap : (e + 1) * cap]
                return carry

            lax.fori_loop(0, half // 2, gather, 0)

            @pl.when(ahead)
            def _():
                for copy in pair_loads(t, 1, p):
                    copy.start()

        stores = []
        if keep:
            stores = [pltpu.make_async_copy(xs, xs_all.at[:, h], slot_sem.at[0]),
                      pltpu.make_async_copy(us, us_all.at[:, h], slot_sem.at[1])]
        for copy in stores:
            copy.start()

        def expert(e, carry):
            ab = dot(xs[e], w13[e].reshape(model, 2 * width))
            a, b = ab[:, :width], ab[:, width:]
            dh = dot_tb(us[e], w2s[e])
            sig = jax.nn.sigmoid(a)
            silu = a * sig
            hid = (silu * b).astype(BF16)
            da = (dh * b * sig * (1.0 + a * (1.0 - sig))).astype(BF16)
            db = (dh * silu).astype(BF16)
            acc13[e] += dot_ta(jnp.concatenate([da, db], axis=1), xs[e])
            acc2[e] += dot_ta(hid, us[e])
            return carry

        lax.fori_loop(0, own, expert, 0)
        for copy in stores:
            copy.wait()

    def start_loads(t, h):
        for p in range(2):
            for copy in pair_loads(t, h, p):
                copy.start()

    def compute(t, keep):
        start_loads(t, 0)

        def one_half(h, carry):
            half_group(t, h, keep, h == 0)
            return carry

        lax.fori_loop(0, 2, one_half, 0)

    slots = eps * cap
    pending = []

    def settle():
        while pending:
            pending.pop().wait()

    def hidden(e):
        rows = pltpu.make_async_copy(xs_all.at[e], xs.at[pl.ds(0, 2)], in_sem.at[tps])
        rows.start()
        for j in range(tps):
            pltpu.make_async_copy(w13_all.at[j, e], wide_buf.at[pl.ds(0, PARTS), j], in_sem.at[j]).start()
        settle()
        rows.wait()

        def shard(j, carry):
            pltpu.make_async_copy(w13_all.at[j, e], wide_buf.at[pl.ds(0, PARTS), j], in_sem.at[j]).wait()
            ab = dot(xs[0:2].reshape(slots, model), wide_buf[0:PARTS, j].reshape(model, 2 * width))
            ab_buf[j] = ab
            a, b = ab[:, :width], ab[:, width:]
            at = pl.ds(pl.multiple_of(lax.rem(j, 2) * width, width), width)
            d_all[e, j // 2, :, at] = (a * jax.nn.sigmoid(a) * b).astype(BF16)
            return carry

        lax.fori_loop(0, tps, shard, 0)
        pending.append(pltpu.make_async_copy(ab_buf, ab_all.at[e], ab_sem.at[0]))
        pending[-1].start()

    def put_rows(e, value):
        for k in range(eps):
            y_buf[k, e] = value[k * cap : (k + 1) * cap]

    def y_part(q):
        load = pltpu.make_async_copy(w2_all.at[:, q], w2v.at[q], in_sem.at[0])
        load.start()
        load.wait()

        def one(e, carry):
            y = dot(d_all[e, 0], w2v[q, 0:2, e].reshape(2 * width, part)) + dot(d_all[e, 1], w2v[q, 2:4, e].reshape(2 * width, part))
            put_rows(e, y.astype(BF16))
            return carry

        lax.fori_loop(0, own, one, 0)

    def ab_load(e, j):
        return pltpu.make_async_copy(ab_all.at[e, j], ab_buf.at[j], ab_sem.at[j])

    def u_load(e, slot):
        return pltpu.make_async_copy(us_all.at[e], us.at[pl.ds(2 * slot, 2)], in_sem.at[1 + slot])

    def hidden_grads():
        settle()
        u_load(0, 0).start()
        for j in range(tps):
            ab_load(0, j).start()

        def one(e, carry):
            slot = lax.rem(e, 2)
            u_load(e, slot).wait()

            @pl.when(e + 1 < own)
            def _():
                u_load(e + 1, 1 - slot).start()

            def two(k, carry):
                dh = None
                for q in range(PARTS):
                    at = pl.ds(q * part, part)
                    u = us[pl.ds(2 * slot, 2), :, at].reshape(slots, part)
                    term = dot_tb(u, w2v[q, pl.ds(2 * k, 2), e].reshape(2 * width, part))
                    dh = term if dh is None else dh + term
                for i in range(2):
                    j = 2 * k + i
                    ab_load(e, j).wait()
                    a, b, d = ab_buf[j, :, :width], ab_buf[j, :, width:], dh[:, i * width : (i + 1) * width]
                    sig = jax.nn.sigmoid(a)
                    d_all[e, j, :, :width] = (d * b * sig * (1.0 + a * (1.0 - sig))).astype(BF16)
                    d_all[e, j, :, width:] = (d * (a * sig)).astype(BF16)

                    @pl.when(e + 1 < own)
                    def _():
                        ab_load(e + 1, j).start()
                return carry

            lax.fori_loop(0, tps // 2, two, 0)
            return carry

        lax.fori_loop(0, own, one, 0)

    def v_load(q):
        return pltpu.make_async_copy(w13_all.at[:, :, q], wide_buf, in_sem.at[0])

    def v_part(q):
        v_load(q).wait()

        def one(e, carry):
            v = dot_tb(d_all[e, 0], wide_buf[0, e])
            for j in range(1, tps):
                v = v + dot_tb(d_all[e, j], wide_buf[j, e])
            put_rows(e, v.astype(BF16))
            return carry

        lax.fori_loop(0, own, one, 0)
        if q + 1 < PARTS:
            v_load(q + 1).start()

    gifts, writes, stages = {}, {}, {}

    def combine(kind, block):
        pos, gate = expert_rows(routes[block], ep * own, own, earlier[...])
        masks = hit_masks(pos, cap)
        rows = y_buf[block].reshape(own * cap, part)
        if kind == 1:
            return dot_ta(one_hot(masks), rows)
        hi, mid, low = three_parts(slot_gates(masks, gate))
        return dot_ta(hi, rows) + (dot_ta(mid, rows) + dot_ta(low, rows))

    numbers, ready = {}, {}
    tok = far_sum.shape[0] // 2
    fold = part // 2
    buffers = [keep_sum.at[0], keep_sum.at[1], keep_sum.at[0], ab_buf, keep_sum.at[1], keep_sum.at[0]]
    earlier_user = {2: 0, 4: 1, 5: 2}
    assert ab_buf.shape == give.shape and len(buffers) == 2 * PARTS
    halves = (pl.ds(0, tok), pl.ds(tok, tok))

    def put_tile(ref, i, value):
        ref[i, 0:tok] = value[:, :fold]
        ref[i, tok : 2 * tok] = value[:, fold:]

    def sum_begin(kind, q):
        n = numbers[kind, q] = len(numbers)
        tiles = buffers[n]
        if n:
            links.finish(gifts[n - 1])
        if n in earlier_user:
            for k in ready[earlier_user[n]]:
                links.finish(k)
            writes.pop(earlier_user[n]).wait()

        def to_other(i, carry):
            put_tile(give, i, combine(kind, lax.rem(mate + 4 - 2 * i + eps, eps)))
            return carry

        def to_own(i, carry):
            put_tile(tiles, i, combine(kind, lax.rem(ep + 4 - 2 * i + eps, eps)))
            return carry

        lax.fori_loop(0, 4, to_other, 0)
        if n:
            pl.semaphore_wait(free_sem, 1)
        gifts[n] = links.send(give, mate_sum, to_mate)
        lax.fori_loop(0, 4, to_own, 0)

    def sum_end(kind, q):
        n = numbers[kind, q]
        tiles = buffers[n]
        links.arrive(gifts[n], mate_sum, to_mate)
        tiles[...] += mate_sum[...]
        if n + 1 < 2 * PARTS:
            pl.semaphore_signal(free_sem, inc=1, device_id=to_mate, device_id_type=MESH)
        stages[n] = [links.send(tiles.at[0, halves[h]], far_land.at[kind, q, halves[h]], to) for h, to in ((0, to_right), (1, to_left))]
        stages[n] += [links.send(tiles.at[i, halves[h]], last_land.at[kind, side, q, halves[h]], to)
                      for i, h, side, to in ((1, 1, 0, to_right), (3, 0, 1, to_left))]
        writes[n] = pltpu.make_async_copy(tiles.at[2], sums.at[kind, q], own_sem.at[n])
        writes[n].start()

    def sum_turn(kind, q):
        n = numbers[kind, q]
        tiles = buffers[n]
        for h, to in ((0, to_right), (1, to_left)):
            links.arrive(stages[n][h], far_land.at[kind, q, halves[h]], to)
        load = pltpu.make_async_copy(far_land.at[kind, q], far_sum, sum_sem.at[0])
        load.start()
        load.wait()
        for i, h, side, to in ((1, 0, 0, to_right), (3, 1, 1, to_left)):
            tiles[i, halves[h]] += far_sum[halves[h]]
            stages[n].append(links.send(tiles.at[i, halves[h]], last_land.at[kind, side, q, halves[h]], to))
        ready[n] = tuple(stages[n])

    def sums_here(kind):
        for q in range(PARTS):
            sent = stages[numbers[kind, q]]
            for k, h, side, to in ((2, 1, 0, to_right), (3, 0, 1, to_left), (4, 0, 0, to_right), (5, 1, 1, to_left)):
                links.arrive(sent[k], last_land.at[kind, side, q, halves[h]], to)

    def finish_out():
        links.finish(gifts[2 * PARTS - 1])
        three = pl.ds(0, PARTS)
        copies = [pltpu.make_async_copy(sums.at[0], give.at[three], sum_sem.at[0]),
                  pltpu.make_async_copy(last_land.at[0, 0], mate_sum.at[three], sum_sem.at[1])]
        for copy in copies:
            copy.start()
        for copy in copies:
            copy.wait()
        give[three] += mate_sum[three]
        copy = pltpu.make_async_copy(last_land.at[0, 1], mate_sum.at[three], sum_sem.at[0])
        copy.start()
        copy.wait()
        for q in range(PARTS):
            for h in range(2):
                at = q * part + h * fold
                xb[0, 0, :, at : at + fold] = (give[q, halves[h]] + mate_sum[q, halves[h]]).astype(BF16)
        copy = pltpu.make_async_copy(xb.at[0, 0], out, sum_sem.at[0])
        copy.start()
        copy.wait()

    y_state = {}
    for way in (True, False):
        for kind in kinds:
            go_up = upward[kind] == way
            y_state[kind, go_up] = links.send(own_refs[kind], all_refs[kind].at[ep, tp], to_up if go_up else to_down)
    groups = (tp, down, up)
    states = [spread(tp, own_refs)]
    first_sends = range(len(links.sent))
    hold = [pltpu.make_async_copy(own_refs[kind], all_refs[kind].at[ep, tp], row_sem.at[kind]) for kind in range(3)]
    for copy in hold:
        copy.start()
    for copy in loads:
        copy.wait()
    stow = [pltpu.make_async_copy(w13, w13_all.at[tp], w_sem.at[0])]
    stow += [pltpu.make_async_copy(w2s.at[:, :, pl.ds(q * part, part)], w2_all.at[tp, q], w_sem.at[1 + q]) for q in range(PARTS)]
    for copy in stow:
        copy.start()
    earlier[...] = earlier_rows(earlier.shape[0])
    with jax.named_scope("zeros"):
        acc13[...] = jnp.zeros_like(acc13)
        acc2[...] = jnp.zeros_like(acc2)

    def y_arrive(kind, way):
        block = all_refs[kind].at[ep, down if way else up]
        links.arrive(y_state[kind, way], block, to_up if way else to_down)
        return block

    with jax.named_scope("pass_on_0"):
        pass_on(0)
    with jax.named_scope("y_arrive"):
        for way in (True, False):
            for kind in kinds:
                y_arrive(kind, way)
    with jax.named_scope("send13_0"):
        send13(0)
    with jax.named_scope("send13_1"):
        send13(1)
    with jax.named_scope("send13_2"):
        send13(2)
    states.append(spread(down, [ref.at[ep, down] for ref in all_refs]))
    with jax.named_scope("share_0"):
        share(0)
    with jax.named_scope("last_0"):
        last(0)
    for copy in hold + stow:
        copy.wait()
    with jax.named_scope("from_mate_0"):
        from_mate(0)
    route_copy = pltpu.make_async_copy(r_all.at[:, tp], routes, row_sem.at[0])
    route_copy.start()
    route_copy.wait()
    for k in first_sends:
        links.finish(k)
    with jax.named_scope("compute_tp_True"):
        compute(tp, True)
    with jax.named_scope("pass13_0"):
        pass13(0)
    with jax.named_scope("send13_3"):
        send13(3)
    with jax.named_scope("pass_on_1"):
        pass_on(1)
    states.append(spread(up, [ref.at[ep, up] for ref in all_refs]))
    with jax.named_scope("share_1"):
        share(1)
    with jax.named_scope("pass13_1"):
        pass13(1)
    with jax.named_scope("send13_4"):
        send13(4)
    with jax.named_scope("have13_0"):
        have13(0)
    with jax.named_scope("hidden_0"):
        hidden(0)
    with jax.named_scope("pass13_2"):
        pass13(2)
    with jax.named_scope("last_1"):
        last(1)
    with jax.named_scope("from_mate_1"):
        from_mate(1)
    with jax.named_scope("compute_down_False"):
        compute(down, False)
    with jax.named_scope("pass13_3"):
        pass13(3)
    with jax.named_scope("send2_0"):
        send2(0)
    with jax.named_scope("pass_on_2"):
        pass_on(2)
    with jax.named_scope("have13_1"):
        have13(1)
    with jax.named_scope("hidden_1"):
        hidden(1)
    with jax.named_scope("share_2"):
        share(2)
    with jax.named_scope("pass13_4"):
        pass13(4)
    with jax.named_scope("have13_2"):
        have13(2)
    with jax.named_scope("hidden_2"):
        hidden(2)
    with jax.named_scope("last_2"):
        last(2)
    with jax.named_scope("from_mate_2"):
        from_mate(2)
    with jax.named_scope("have13_3"):
        have13(3)
    with jax.named_scope("hidden_3"):
        hidden(3)
    with jax.named_scope("start_loads_up_0"):
        start_loads(up, 0)
    with jax.named_scope("half_group_up_0_False_True"):
        half_group(up, 0, False, True)
    with jax.named_scope("pass2_0"):
        pass2(0)
    with jax.named_scope("send2_1"):
        send2(1)
        send2(2)
    with jax.named_scope("half_group_up_1_False_False"):
        half_group(up, 1, False, False)
    with jax.named_scope("have13_4"):
        have13(4)
    with jax.named_scope("hidden_4"):
        hidden(4)

    with jax.named_scope("have2_0"):
        have2(0)
    with jax.named_scope("y_part_0"):
        y_part(0)
    with jax.named_scope("sum_begin_0_0"):
        sum_begin(0, 0)
    with jax.named_scope("sum_end_0_0"):
        sum_end(0, 0)
    with jax.named_scope("pass2_1"):
        pass2(1)
    with jax.named_scope("send2_3"):
        send2(3)
    with jax.named_scope("pass2_2"):
        pass2(2)
    with jax.named_scope("sum_turn_0_0"):
        sum_turn(0, 0)
    with jax.named_scope("have2_1"):
        have2(1)
    with jax.named_scope("y_part_1"):
        y_part(1)
    with jax.named_scope("sum_begin_0_1"):
        sum_begin(0, 1)
    with jax.named_scope("pass2_3"):
        pass2(3)
    over_state = send_over()
    with jax.named_scope("sum_end_0_1"):
        sum_end(0, 1)
    with jax.named_scope("have2_2"):
        have2(2)
        have2(3)
    with jax.named_scope("y_part_2"):
        y_part(2)
    with jax.named_scope("sum_begin_0_2"):
        sum_begin(0, 2)
    with jax.named_scope("sum_end_0_2"):
        sum_end(0, 2)
    v_load(0).start()
    with jax.named_scope("sum_turn_0_1"):
        sum_turn(0, 1)
    with jax.named_scope("hidden_grads"):
        hidden_grads()
    with jax.named_scope("sum_turn_0_2"):
        sum_turn(0, 2)
    with jax.named_scope("v_part_0"):
        v_part(0)
    with jax.named_scope("sum_begin_1_0"):
        sum_begin(1, 0)
    with jax.named_scope("sum_end_1_0"):
        sum_end(1, 0)
    with jax.named_scope("share_over_0"):
        share_over(0)
    with jax.named_scope("v_part_1"):
        v_part(1)
    with jax.named_scope("sum_begin_1_1"):
        sum_begin(1, 1)
    with jax.named_scope("sum_end_1_1"):
        sum_end(1, 1)
    with jax.named_scope("share_over_1"):
        share_over(1)
    with jax.named_scope("sum_turn_1_0"):
        sum_turn(1, 0)
    with jax.named_scope("v_part_2"):
        v_part(2)
    with jax.named_scope("sum_begin_1_2"):
        sum_begin(1, 2)
    with jax.named_scope("sum_end_1_2"):
        sum_end(1, 2)
    with jax.named_scope("have_over_0"):
        have_over(0)
    with jax.named_scope("have_over_1"):
        have_over(1)
    with jax.named_scope("start_loads_over_0"):
        start_loads(over, 0)
    with jax.named_scope("sum_turn_1_1"):
        sum_turn(1, 1)
    with jax.named_scope("half_group_over_0_False_False"):
        half_group(over, 0, False, False)
    with jax.named_scope("share_over_2"):
        share_over(2)
    with jax.named_scope("share_over_3"):
        share_over(3)
    with jax.named_scope("have_over_2"):
        have_over(2)
    with jax.named_scope("have_over_3"):
        have_over(3)
    with jax.named_scope("start_loads_over_1"):
        start_loads(over, 1)
    with jax.named_scope("half_group_over_1_False_False"):
        half_group(over, 1, False, False)
    with jax.named_scope("sum_turn_1_2"):
        sum_turn(1, 2)

    def grad_stores(e, slot):
        rows = pl.ds(0, PARTS)
        return [pltpu.make_async_copy(wide_buf.at[slot, rows, :, pl.ds(0, width)], g1.at[e], g_sem.at[slot, 0]),
                pltpu.make_async_copy(wide_buf.at[slot, rows, :, pl.ds(width, width)], g3.at[e], g_sem.at[slot, 1]),
                pltpu.make_async_copy(xs.at[slot, pl.ds(0, width)], g2.at[e], g_sem.at[slot, 2])]

    def finish(e, carry):
        slot = lax.rem(e, 2)

        @pl.when(e >= 2)
        def _():
            for copy in grad_stores(e - 2, slot):
                copy.wait()

        for m in range(PARTS):
            wide_buf[slot, m] = acc13[e, :, m * part : (m + 1) * part].T.astype(BF16)
        xs[slot, pl.ds(0, width), :] = acc2[e].astype(BF16)
        for copy in grad_stores(e, slot):
            copy.start()
        return carry

    with jax.named_scope("finish"):
        lax.fori_loop(0, own, finish, 0)
        for e in range(max(own - 2, 0), own):
            for copy in grad_stores(e, e % 2):
                copy.wait()
    with jax.named_scope("sums_here_0"):
        sums_here(0)
    with jax.named_scope("finish_out"):
        finish_out()
    with jax.named_scope("sums_here_1"):
        sums_here(1)
    for n in sorted(writes):
        writes[n].wait()
    with jax.named_scope("drain"):
        links.drain()


def layer(tokens, d_out, ids, gate_vals, w_one, w_three, w_two, ep_size, tp_size, cap):
    tok, model = tokens.shape
    own, width, _ = w_two.shape
    half = ep_size // 2
    rows = half * cap
    part = model // PARTS
    hbm = pl.BlockSpec(memory_space=pl.ANY)
    shape = jax.ShapeDtypeStruct
    routes = (2 * ids.shape[0], tok)
    copies = copy_count(own)
    slot_rows = ep_size * tp_size * cap * own
    vector = pltpu.VMEM
    dma = pltpu.SemaphoreType.DMA
    outs = pl.pallas_call(
        functools.partial(layer_kernel, own, cap, width),
        in_specs=[hbm] * 7,
        out_specs=[hbm] * 15,
        out_shape=[
            shape((ep_size, tp_size, tok, model), BF16),
            shape((ep_size, tp_size, tok, model), BF16),
            shape((ep_size, tp_size) + routes, F32),
            shape((tp_size, own, PARTS, part, 2 * width), BF16),
            shape((tp_size, PARTS, own, width, part), BF16),
            shape((own, 2, rows, model), BF16),
            shape((own, 2, rows, model), BF16),
            shape((own, tp_size, 2 * rows, 2 * width), F32),
            shape((2, PARTS, 2 * tok, part // 2), F32),
            shape((2, PARTS, 2 * tok, part // 2), F32),
            shape((2, 2, PARTS, 2 * tok, part // 2), F32),
            shape((tok, model), BF16),
            shape((own, PARTS, part, width), BF16),
            shape((own, PARTS, part, width), BF16),
            shape((own, width, model), BF16),
        ],
        scratch_shapes=[
            vector(routes, F32),
            vector(ids.shape, jnp.int32),
            vector((own, PARTS, part, 2 * width), BF16),
            vector((own, width, model), BF16),
            vector((2, half // 2, tok, model), BF16),
            vector((2, half // 2, tok, model), BF16),
            vector((2, half // 2) + routes, F32),
            vector((ep_size,) + routes, F32),
            vector((tok, tok), BF16),
            vector((own, rows, model), BF16),
            vector((own, rows, model), BF16),
            vector((own, 2 * width, model), F32),
            vector((own, width, model), F32),
            vector((tp_size, own, part, 2 * width), BF16),
            vector((PARTS, tp_size, own, width, part), BF16),
            vector((tp_size, 2 * rows, 2 * width), F32),
            vector((own, tp_size, 2 * rows, 2 * width), BF16),
            vector((ep_size, own, cap, part), BF16),
            vector((4, 2 * tok, part // 2), F32),
            vector((2, 4, 2 * tok, part // 2), F32),
            vector((4, 2 * tok, part // 2), F32),
            vector((2 * tok, part // 2), F32),
            dma((copies,)),
            dma((copies,)),
            dma((4,)),
            dma((3, 2)),
            dma((2 * PARTS + 1,)),
            dma((2,)),
            dma((1 + tp_size,)),
            dma((tp_size,)),
            dma((2,)),
            dma((2 * PARTS,)),
            dma((2, 3)),
            pltpu.SemaphoreType.REGULAR,
        ],
        compiler_params=pltpu.CompilerParams(vmem_limit_bytes=VMEM_LIMIT, collective_id=0, has_side_effects=True),
        cost_estimate=pl.CostEstimate(
            flops=2 * slot_rows * model * (2 * tok + 12 * width),
            bytes_accessed=4 * ep_size * tp_size * tok * model,
            transcendentals=0,
        ),
        name="layer",
    )(tokens, d_out, ids, gate_vals, w_one, w_three, w_two)
    g1, g3, g2 = outs[12:]
    return outs[8], outs[10], outs[11], (g1.reshape(own, model, width), g3.reshape(own, model, width), g2)


def result_kernel(sums, last_land, rows_in, g1, g3, g2, out, dx, o1, o3, o2, parts, rows, row_buf, b1, b3, b2, in_sem, out_sem):
    moves = ((g1, b1, o1), (g3, b3, o3), (g2, b2, o2), (rows_in, row_buf, out))
    takes = [pltpu.make_async_copy(src, buf, in_sem.at[k]) for k, (src, buf, _) in enumerate(moves)]
    terms = [pltpu.make_async_copy(src, parts.at[k], in_sem.at[4 + k])
             for k, src in enumerate((sums.at[1], last_land.at[1, 0], last_land.at[1, 1]))]
    for copy in terms + takes:
        copy.start()
    for copy in terms:
        copy.wait()
    tok, fold = rows.shape[0], parts.shape[3]
    for q in range(parts.shape[1]):
        for h in range(2):
            at, half = (2 * q + h) * fold, pl.ds(h * tok, tok)
            rows[:, at : at + fold] = (parts[0, q, half] + (parts[1, q, half] + parts[2, q, half])).astype(BF16)
    puts = [pltpu.make_async_copy(rows, dx, out_sem.at[4])]
    puts[0].start()
    for k, (take, (_, buf, to)) in enumerate(zip(takes, moves)):
        take.wait()
        puts.append(pltpu.make_async_copy(buf, to, out_sem.at[k]))
        puts[-1].start()
    for copy in puts:
        copy.wait()


def results(sums, last_land, out, grads):
    _, count, tall, fold = sums.shape
    tok, model = out.shape
    hbm = pl.BlockSpec(memory_space=pl.ANY)
    row = jax.ShapeDtypeStruct((tok, model), BF16)
    rows = pltpu.VMEM((tok, model), BF16)
    return pl.pallas_call(
        result_kernel,
        in_specs=[hbm] * 6,
        out_specs=[hbm] * 5,
        out_shape=[row, row] + [jax.ShapeDtypeStruct(g.shape, g.dtype) for g in grads],
        scratch_shapes=[pltpu.VMEM((3, count, tall, fold), F32), rows, rows]
        + [pltpu.VMEM(g.shape, g.dtype) for g in grads]
        + [pltpu.SemaphoreType.DMA((7,)), pltpu.SemaphoreType.DMA((5,))],
        compiler_params=pltpu.CompilerParams(vmem_limit_bytes=VMEM_LIMIT),
        name="results",
    )(sums, last_land, out, *grads)


def solution(mesh):
    ep_size, tp_size = mesh.shape["ep"], mesh.shape["tp"]
    row_spec = P(("dp", "ep", "tp"), None)
    col_spec = P("ep", None, "tp")
    down_spec = P("ep", "tp", None)
    grad_col = P(("dp", "ep"), None, "tp")
    grad_down = P(("dp", "ep"), "tp", None)

    def local_step(tokens, expert_ids, gate_vals, w_one, w_three, w_two, d_out):
        cap = slot_count(expert_ids.shape[1], tokens.shape[0], w_one.shape[0] * ep_size)
        sums, last_land, out, grads = layer(tokens, d_out, expert_ids.T, gate_vals.T, w_one, w_three, w_two, ep_size, tp_size, cap)
        return tuple(results(sums, last_land, out, grads))

    return jax.shard_map(local_step, mesh=mesh,
                         in_specs=(row_spec, row_spec, row_spec, col_spec, col_spec, down_spec, row_spec),
                         out_specs=(row_spec, row_spec, grad_col, grad_col, grad_down), check_vma=False)
```

```python
import functools

import jax
import jax.numpy as jnp
from jax import lax
from jax.experimental import pallas as pl
from jax.experimental.pallas import tpu as pltpu
from jax.sharding import PartitionSpec as P

BF16 = jnp.bfloat16
F32 = jnp.float32
MESH = pl.DeviceIdType.MESH
VMEM_LIMIT = 67_043_328
PARTS = 3


def slot_count(num_top, tok_dev, experts):
    return 8 * ((5 * num_top * tok_dev + 32 * experts - 1) // (32 * experts))


def dot(a, b):
    return jnp.dot(a, b, preferred_element_type=F32)


def dot_tb(a, b):
    return lax.dot_general(a, b, (((1,), (1,)), ((), ())), preferred_element_type=F32)


def dot_ta(a, b):
    return lax.dot_general(a, b, (((0,), (0,)), ((), ())), preferred_element_type=F32)


def earlier_rows(tok):
    row = lax.broadcasted_iota(jnp.int32, (tok, tok), 0)
    col = lax.broadcasted_iota(jnp.int32, (tok, tok), 1)
    return jnp.where(row < col, 1.0, 0.0).astype(BF16)


def expert_rows(routes, first, own, earlier):
    top = routes.shape[0] // 2
    ids, gates = routes[:top], routes[top:]
    hits = [ids == (first + e).astype(F32) for e in range(own)]
    routed = jnp.concatenate([jnp.sum(jnp.where(m, 1.0, 0.0), axis=0, keepdims=True) for m in hits], axis=0)
    gate = jnp.concatenate([jnp.sum(jnp.where(m, gates, 0.0), axis=0, keepdims=True) for m in hits], axis=0)
    return jnp.where(routed > 0.0, dot(routed.astype(BF16), earlier), -1.0), gate


def hit_masks(pos, cap):
    slot = lax.broadcasted_iota(jnp.int32, (cap, pos.shape[1]), 0).astype(F32)
    return [pos[e : e + 1, :] == slot for e in range(pos.shape[0])]


def one_hot(masks):
    return jnp.concatenate([jnp.where(m, 1.0, 0.0) for m in masks], axis=0).astype(BF16)


def slot_gates(masks, gate):
    return jnp.concatenate([jnp.where(m, gate[e : e + 1, :], 0.0) for e, m in enumerate(masks)], axis=0)


def three_parts(x):
    hi = x.astype(BF16)
    rest = x - hi.astype(F32)
    mid = rest.astype(BF16)
    return hi, mid, (rest - mid.astype(F32)).astype(BF16)


class Links:
    def __init__(self, send_sem, recv_sem):
        self.send_sem, self.recv_sem, self.sent, self.finished = send_sem, recv_sem, [], set()

    def copy(self, k, src, dst, to):
        return pltpu.make_async_remote_copy(src_ref=src, dst_ref=dst, send_sem=self.send_sem.at[k],
                                            recv_sem=self.recv_sem.at[k], device_id=to, device_id_type=MESH)

    def send(self, src, dst, to):
        k = len(self.sent)
        copy = self.copy(k, src, dst, to)
        copy.start()
        self.sent.append(copy)
        return k

    def arrive(self, k, dst, to):
        self.copy(k, dst, dst, to).wait_recv()

    def finish(self, k):
        self.finished.add(k)
        self.sent[k].wait_send()

    def drain(self):
        for k in range(len(self.sent)):
            if k not in self.finished:
                self.finish(k)


def copy_count(own):
    return 6 + 21 * 3 + 24 + 4 * own + 4 * (PARTS + 1) + 2 * PARTS * 7


def layer_kernel(own, cap, width, tokens, d_out, ids, gate_vals, w1, w3, w2, x_all, dy_all, r_all, w13_all, w2_all, xs_all,
                 us_all, ab_all, sums, far_land, last_land, out, g1, g3, g2, r_own, i_own, w13, w2s, xb,
                 dyb, rb, routes, earlier, xs, us, acc13, acc2, wide_buf, w2v, ab_buf, d_all, y_buf, give, keep_sum, mate_sum,
                 far_sum, send_sem, recv_sem, row_sem, load_sem, w_sem, slot_sem, in_sem, ab_sem, sum_sem, own_sem, g_sem, free_sem):
    ep, tp = lax.axis_index("ep"), lax.axis_index("tp")
    eps, tps = x_all.shape[0], x_all.shape[1]
    model = x_all.shape[3]
    part = model // PARTS
    half = eps // 2
    x_own, dy_own = xs.at[0], xs.at[1]
    step = lambda n: lax.rem(ep + (n + eps), eps)
    turn = lambda n: lax.rem(tp + (n + tps), tps)
    right, left, far = step(2), step(-2), step(4)
    mate = ep + 1 - 2 * lax.rem(ep, 2)
    mate_step = lambda n: lax.rem(mate + (n + eps), eps)
    up, down, over = turn(1), turn(-1), turn(2)
    to_right, to_left, to_mate = {"ep": right}, {"ep": left}, {"ep": mate}
    to_up, to_down = {"tp": up}, {"tp": down}
    links = Links(send_sem, recv_sem)

    barrier = pltpu.get_barrier_semaphore()
    for to in (to_right, to_left, to_mate, to_up, to_down):
        pl.semaphore_signal(barrier, inc=1, device_id=to, device_id_type=MESH)
    top = ids.shape[0]
    firsts = [pltpu.make_async_copy(ids, i_own, row_sem.at[0]), pltpu.make_async_copy(gate_vals, r_own.at[pl.ds(top, top)], row_sem.at[1]),
              pltpu.make_async_copy(tokens, x_own, row_sem.at[2]), pltpu.make_async_copy(d_out, dy_own, row_sem.at[3])]
    loads = [pltpu.make_async_copy(src.at[:, pl.ds(m * part, part)], w13.at[:, m, :, pl.ds(k * width, width)], w_sem.at[PARTS * k + m])
             for k, src in ((0, w1), (1, w3)) for m in range(PARTS)]
    loads.append(pltpu.make_async_copy(w2, w2s, w_sem.at[2 * PARTS]))
    for copy in firsts + loads:
        copy.start()
    firsts[0].wait()
    r_own[0:top] = i_own[...].astype(F32)
    for copy in firsts[1:]:
        copy.wait()
    with jax.named_scope("barrier"):
        pl.semaphore_wait(barrier, 5)

    own_refs, all_refs = (x_own, dy_own, r_own), (x_all, dy_all, r_all)
    upward = (True, False, True)
    kinds = (0, 1, 2)

    def spread(t, srcs):
        out = {}
        for kind in kinds:
            to = to_right if upward[kind] else to_left
            out[kind, upward[kind]] = links.send(srcs[kind], all_refs[kind].at[ep, t], to)
        for kind in kinds:
            to = to_left if upward[kind] else to_right
            out[kind, not upward[kind]] = links.send(srcs[kind], all_refs[kind].at[ep, t], to)
        for kind in kinds:
            out[kind, "mate"] = links.send(srcs[kind], all_refs[kind].at[ep, t], to_mate)
        return out

    def pass_on(g):
        state, t = states[g], groups[g]
        for kind in kinds:
            got, to = (left, to_right) if upward[kind] else (right, to_left)
            block = all_refs[kind].at[got, t]
            links.arrive(state[kind, upward[kind]], block, to)
            state[kind, "far"] = links.send(block, block, to)
            state[kind, "mate1"] = links.send(block, block, to_mate)

    def share(g):
        state, t = states[g], groups[g]
        for kind in kinds:
            got, to = (right, to_left) if upward[kind] else (left, to_right)
            block = all_refs[kind].at[got, t]
            links.arrive(state[kind, not upward[kind]], block, to)
            state[kind, "mate2"] = links.send(block, block, to_mate)

    def last(g):
        state, t = states[g], groups[g]
        for kind in kinds:
            block = all_refs[kind].at[far, t]
            links.arrive(state[kind, "far"], block, to_right if upward[kind] else to_left)
            state[kind, "mate3"] = links.send(block, block, to_mate)

    def from_mate(g):
        state, t = states[g], groups[g]
        for kind in kinds:
            one, two = (mate_step(-2), mate_step(2)) if upward[kind] else (mate_step(2), mate_step(-2))
            for name, at in (("mate", mate), ("mate1", one), ("mate2", two), ("mate3", mate_step(4))):
                links.arrive(state[kind, name], all_refs[kind].at[at, t], to_mate)

    core = lax.rem(ep, 2)

    def send_over():
        return [{kind: links.send(all_refs[kind].at[core + 2 * m, down if upward[kind] else up],
                                  all_refs[kind].at[core + 2 * m, down if upward[kind] else up],
                                  to_up if upward[kind] else to_down) for kind in kinds} for m in range(half)]

    def share_over(m):
        for kind in kinds:
            block = all_refs[kind].at[core + 2 * m, over]
            links.arrive(over_state[m][kind], block, to_up if upward[kind] else to_down)
            over_state[m][kind, "mate"] = links.send(block, block, to_mate)

    def have_over(m):
        for kind in kinds:
            links.arrive(over_state[m][kind, "mate"], all_refs[kind].at[1 - core + 2 * m, over], to_mate)

    def both_ways(src, dst):
        return {True: links.send(src, dst, to_up), False: links.send(src, dst, to_down)}

    def pass_halves(state, below, above, split):
        links.arrive(state[True], below, to_up)
        state["first"] = links.send(split(below, 0), split(below, 0), to_up)
        links.arrive(state[False], above, to_down)
        state["second"] = links.send(split(above, 1), split(above, 1), to_down)

    def have_halves(state, block, split):
        links.arrive(state["first"], split(block, 0), to_up)
        links.arrive(state["second"], split(block, 1), to_down)

    w13_state, w2_state = [None] * own, [None] * (PARTS + 1)
    split13 = lambda ref, k: ref.at[:, pl.ds(k * (part // 2), part // 2)]
    split2 = lambda ref, k: ref.at[:, pl.ds(k * (width // 2), width // 2)]

    def send13(e):
        w13_state[e] = both_ways(w13.at[e], w13_all.at[tp, e])

    def pass13(e):
        pass_halves(w13_state[e], w13_all.at[down, e], w13_all.at[up, e], split13)

    def have13(e):
        have_halves(w13_state[e], w13_all.at[over, e], split13)

    pieces = [(q, pl.ds(0, own)) for q in range(PARTS - 1)] + [(PARTS - 1, pl.ds(0, 2)), (PARTS - 1, pl.ds(2, own - 2))]

    def piece(j, p):
        q, experts = pieces[p]
        return w2_all.at[j, q, experts]

    def send2(p):
        q, experts = pieces[p]
        w2_state[p] = both_ways(w2s.at[experts, :, pl.ds(q * part, part)], piece(tp, p))

    def pass2(p):
        pass_halves(w2_state[p], piece(down, p), piece(up, p), split2)

    def have2(p):
        have_halves(w2_state[p], piece(over, p), split2)

    def pair_loads(t, h, p):
        at = pl.ds(h * half + p * (half // 2), half // 2)
        return [pltpu.make_async_copy(src.at[at, t], dst.at[p], load_sem.at[k, p])
                for k, (src, dst) in enumerate(((x_all, xb), (dy_all, dyb), (r_all, rb)))]

    def half_group(t, h, keep, ahead):
        def gather(p, b):
            pos, gate = expert_rows(rb[p, b], ep * own, own, earlier[...])
            masks = hit_masks(pos, cap)
            pick = one_hot(masks)
            gates = jnp.sum(slot_gates(masks, gate), axis=1, keepdims=True)
            rows = pl.ds(pl.multiple_of((p * (half // 2) + b) * cap, cap), cap)
            picked = dot(pick, xb[p, b]).astype(BF16)
            for e in range(own):
                xs[e, rows, :] = picked[e * cap : (e + 1) * cap]
            scaled = (gates * dot(pick, dyb[p, b])).astype(BF16)
            for e in range(own):
                us[e, rows, :] = scaled[e * cap : (e + 1) * cap]

        def pair(p, carry):
            for copy in pair_loads(t, h, p):
                copy.wait()
            for b in range(half // 2):
                gather(p, b)

            @pl.when(ahead)
            def _():
                for copy in pair_loads(t, 1, p):
                    copy.start()

            return carry

        lax.fori_loop(0, 2, pair, 0)

        stores = []
        if keep:
            stores = [pltpu.make_async_copy(xs, xs_all.at[:, h], slot_sem.at[0]),
                      pltpu.make_async_copy(us, us_all.at[:, h], slot_sem.at[1])]
        for copy in stores:
            copy.start()

        def expert(e, carry):
            ab = dot(xs[e], w13[e].reshape(model, 2 * width))
            a, b = ab[:, :width], ab[:, width:]
            dh = dot_tb(us[e], w2s[e])
            sig = jax.nn.sigmoid(a)
            silu = a * sig
            hid = (silu * b).astype(BF16)
            da = (dh * b * sig * (1.0 + a * (1.0 - sig))).astype(BF16)
            db = (dh * silu).astype(BF16)
            acc13[e] += dot_ta(jnp.concatenate([da, db], axis=1), xs[e])
            acc2[e] += dot_ta(hid, us[e])
            return carry

        lax.fori_loop(0, own, expert, 0)
        for copy in stores:
            copy.wait()

    def start_loads(t, h, pairs=(0, 1)):
        for p in pairs:
            for copy in pair_loads(t, h, p):
                copy.start()

    def compute(t, keep):
        start_loads(t, 0)

        def one_half(h, carry):
            half_group(t, h, keep, h == 0)
            return carry

        lax.fori_loop(0, 2, one_half, 0)

    slots = eps * cap
    pending = []

    def settle():
        while pending:
            pending.pop().wait()

    def hidden(e):
        rows = pltpu.make_async_copy(xs_all.at[e], xs.at[pl.ds(0, 2)], in_sem.at[tps])
        rows.start()
        for j in range(tps):
            pltpu.make_async_copy(w13_all.at[j, e], wide_buf.at[pl.ds(0, PARTS), j], in_sem.at[j]).start()
        settle()
        rows.wait()

        def shard(j, carry):
            pltpu.make_async_copy(w13_all.at[j, e], wide_buf.at[pl.ds(0, PARTS), j], in_sem.at[j]).wait()
            ab = dot(xs[0:2].reshape(slots, model), wide_buf[0:PARTS, j].reshape(model, 2 * width))
            ab_buf[j] = ab
            a, b = ab[:, :width], ab[:, width:]
            at = pl.ds(pl.multiple_of(lax.rem(j, 2) * width, width), width)
            d_all[e, j // 2, :, at] = (a * jax.nn.sigmoid(a) * b).astype(BF16)
            return carry

        lax.fori_loop(0, tps, shard, 0)
        pending.append(pltpu.make_async_copy(ab_buf, ab_all.at[e], ab_sem.at[0]))
        pending[-1].start()

    def put_rows(e, value):
        for k in range(eps):
            y_buf[k, e] = value[k * cap : (k + 1) * cap]

    def y_part(q):
        load = pltpu.make_async_copy(w2_all.at[:, q], w2v.at[q], in_sem.at[0])
        load.start()
        load.wait()

        def one(e, carry):
            y = dot(d_all[e, 0], w2v[q, 0:2, e].reshape(2 * width, part)) + dot(d_all[e, 1], w2v[q, 2:4, e].reshape(2 * width, part))
            put_rows(e, y.astype(BF16))
            return carry

        lax.fori_loop(0, own, one, 0)

    def ab_load(e, j):
        return pltpu.make_async_copy(ab_all.at[e, j], ab_buf.at[j], ab_sem.at[j])

    def u_load(e, slot):
        return pltpu.make_async_copy(us_all.at[e], us.at[pl.ds(2 * slot, 2)], in_sem.at[1 + slot])

    def hidden_grads():
        settle()
        u_load(0, 0).start()
        for j in range(tps):
            ab_load(0, j).start()

        def one(e, carry):
            slot = lax.rem(e, 2)
            u_load(e, slot).wait()

            @pl.when(e + 1 < own)
            def _():
                u_load(e + 1, 1 - slot).start()

            def two(k, carry):
                dh = None
                for q in range(PARTS):
                    at = pl.ds(q * part, part)
                    u = us[pl.ds(2 * slot, 2), :, at].reshape(slots, part)
                    term = dot_tb(u, w2v[q, pl.ds(2 * k, 2), e].reshape(2 * width, part))
                    dh = term if dh is None else dh + term
                for i in range(2):
                    j = 2 * k + i
                    ab_load(e, j).wait()
                    a, b, d = ab_buf[j, :, :width], ab_buf[j, :, width:], dh[:, i * width : (i + 1) * width]
                    sig = jax.nn.sigmoid(a)
                    d_all[e, j, :, :width] = (d * b * sig * (1.0 + a * (1.0 - sig))).astype(BF16)
                    d_all[e, j, :, width:] = (d * (a * sig)).astype(BF16)

                    @pl.when(e + 1 < own)
                    def _():
                        ab_load(e + 1, j).start()
                return carry

            for k in range(tps // 2):
                two(k, carry)
            return carry

        lax.fori_loop(0, own, one, 0)

    def v_load(q):
        return pltpu.make_async_copy(w13_all.at[:, :, q], wide_buf, in_sem.at[0])

    def v_part(q):
        v_load(q).wait()

        def one(e, carry):
            v = dot_tb(d_all[e, 0], wide_buf[0, e])
            for j in range(1, tps):
                v = v + dot_tb(d_all[e, j], wide_buf[j, e])
            put_rows(e, v.astype(BF16))
            return carry

        lax.fori_loop(0, own, one, 0)
        if q + 1 < PARTS:
            v_load(q + 1).start()

    gifts, writes, stages = {}, {}, {}

    def combine(kind, block):
        masks = hit_masks(routes[block, 0:own], cap)
        rows = y_buf[block].reshape(own * cap, part)
        if kind == 1:
            return dot_ta(one_hot(masks), rows)
        hi, mid, low = three_parts(slot_gates(masks, routes[block, top : top + own]))
        return dot_ta(hi, rows) + (dot_ta(mid, rows) + dot_ta(low, rows))

    numbers, ready = {}, {}
    tok = far_sum.shape[0] // 2
    fold = part // 2
    buffers = [keep_sum.at[0], keep_sum.at[1], keep_sum.at[0], ab_buf, keep_sum.at[1], keep_sum.at[0]]
    earlier_user = {2: 0, 4: 1, 5: 2}
    assert ab_buf.shape == give.shape and len(buffers) == 2 * PARTS
    halves = (pl.ds(0, tok), pl.ds(tok, tok))

    def put_tile(ref, i, value):
        ref[i, 0:tok] = value[:, :fold]
        ref[i, tok : 2 * tok] = value[:, fold:]

    def sum_begin(kind, q):
        n = numbers[kind, q] = len(numbers)
        tiles = buffers[n]
        if n:
            links.finish(gifts[n - 1])
        if n in earlier_user:
            for k in ready[earlier_user[n]]:
                links.finish(k)
            writes.pop(earlier_user[n]).wait()

        def to_other(i, carry):
            for k in range(2):
                put_tile(give, 2 * i + k, combine(kind, lax.rem(mate + 4 - 2 * (2 * i + k) + eps, eps)))
            return carry

        def to_own(i, carry):
            for k in range(2):
                put_tile(tiles, 2 * i + k, combine(kind, lax.rem(ep + 4 - 2 * (2 * i + k) + eps, eps)))
            return carry

        lax.fori_loop(0, 2, to_other, 0)
        if n:
            pl.semaphore_wait(free_sem, 1)
        gifts[n] = links.send(give, mate_sum, to_mate)
        lax.fori_loop(0, 2, to_own, 0)

    def sum_end(kind, q):
        n = numbers[kind, q]
        tiles = buffers[n]
        links.arrive(gifts[n], mate_sum, to_mate)
        tiles[...] += mate_sum[...]
        if n + 1 < 2 * PARTS:
            pl.semaphore_signal(free_sem, inc=1, device_id=to_mate, device_id_type=MESH)
        stages[n] = [links.send(tiles.at[0, halves[h]], far_land.at[kind, q, halves[h]], to) for h, to in ((0, to_right), (1, to_left))]
        stages[n] += [links.send(tiles.at[i, halves[h]], last_land.at[kind, side, q, halves[h]], to)
                      for i, h, side, to in ((1, 1, 0, to_right), (3, 0, 1, to_left))]
        writes[n] = pltpu.make_async_copy(tiles.at[2], sums.at[kind, q], own_sem.at[n])
        writes[n].start()

    def sum_turn(kind, q):
        n = numbers[kind, q]
        tiles = buffers[n]
        for h, to in ((0, to_right), (1, to_left)):
            links.arrive(stages[n][h], far_land.at[kind, q, halves[h]], to)
        load = pltpu.make_async_copy(far_land.at[kind, q], far_sum, sum_sem.at[2])
        load.start()
        load.wait()
        for i, h, side, to in ((1, 0, 0, to_right), (3, 1, 1, to_left)):
            tiles[i, halves[h]] += far_sum[halves[h]]
            stages[n].append(links.send(tiles.at[i, halves[h]], last_land.at[kind, side, q, halves[h]], to))
        ready[n] = tuple(stages[n])

    def sums_here(kind):
        for q in range(PARTS):
            sent = stages[numbers[kind, q]]
            for k, h, side, to in ((2, 1, 0, to_right), (3, 0, 1, to_left), (4, 0, 0, to_right), (5, 1, 1, to_left)):
                links.arrive(sent[k], last_land.at[kind, side, q, halves[h]], to)

    three = pl.ds(0, PARTS)
    out_loads = [pltpu.make_async_copy(sums.at[0], give.at[three], sum_sem.at[0]),
                 pltpu.make_async_copy(last_land.at[0, 0], mate_sum.at[three], sum_sem.at[1]),
                 pltpu.make_async_copy(last_land.at[0, 1], mate_sum.at[three], sum_sem.at[1])]
    out_store = pltpu.make_async_copy(xb.at[0, 0], out, sum_sem.at[0])

    def out_start():
        sums_here(0)
        links.finish(gifts[2 * PARTS - 1])
        out_loads[0].start()
        out_loads[1].start()

    def out_middle():
        out_loads[0].wait()
        out_loads[1].wait()
        give[three] += mate_sum[three]
        out_loads[2].start()

    def out_finish():
        out_loads[2].wait()
        for q in range(PARTS):
            for h in range(2):
                at = q * part + h * fold
                xb[0, 0, :, at : at + fold] = (give[q, halves[h]] + mate_sum[q, halves[h]]).astype(BF16)
        out_store.start()

    y_state = {}
    for way in (True, False):
        for kind in kinds:
            go_up = upward[kind] == way
            y_state[kind, go_up] = links.send(own_refs[kind], all_refs[kind].at[ep, tp], to_up if go_up else to_down)
    groups = (tp, down, up)
    states = [spread(tp, own_refs)]
    first_sends = range(len(links.sent))
    hold = [pltpu.make_async_copy(own_refs[kind], all_refs[kind].at[ep, tp], row_sem.at[kind]) for kind in range(3)]
    for copy in hold:
        copy.start()
    for copy in loads:
        copy.wait()
    stow = [pltpu.make_async_copy(w13, w13_all.at[tp], w_sem.at[0])]
    stow += [pltpu.make_async_copy(w2s.at[:, :, pl.ds(q * part, part)], w2_all.at[tp, q], w_sem.at[1 + q]) for q in range(PARTS)]
    for copy in stow:
        copy.start()
    earlier[...] = earlier_rows(earlier.shape[0])
    with jax.named_scope("zeros"):
        acc13[...] = jnp.zeros_like(acc13)
        acc2[...] = jnp.zeros_like(acc2)

    def y_arrive(kind, way):
        block = all_refs[kind].at[ep, down if way else up]
        links.arrive(y_state[kind, way], block, to_up if way else to_down)
        return block

    with jax.named_scope("pass_on_0"):
        pass_on(0)
    with jax.named_scope("y_arrive"):
        for way in (True, False):
            for kind in kinds:
                y_arrive(kind, way)
    with jax.named_scope("send13_0"):
        send13(0)
    with jax.named_scope("send13_1"):
        send13(1)
    with jax.named_scope("send13_2"):
        send13(2)
    states.append(spread(down, [ref.at[ep, down] for ref in all_refs]))
    with jax.named_scope("share_0"):
        share(0)
    with jax.named_scope("last_0"):
        last(0)
    for copy in hold + stow:
        copy.wait()
    with jax.named_scope("from_mate_0"):
        from_mate(0)
    route_copy = pltpu.make_async_copy(r_all.at[:, tp], routes, row_sem.at[0])
    route_copy.start()
    route_copy.wait()

    def tabulate(b, carry):
        pos, gate = expert_rows(routes[b], ep * own, own, earlier[...])
        routes[b, 0:own] = pos
        routes[b, top : top + own] = gate
        return carry

    lax.fori_loop(0, eps, tabulate, 0)
    for k in first_sends:
        links.finish(k)
    with jax.named_scope("compute_tp_True"):
        compute(tp, True)
    with jax.named_scope("pass13_0"):
        pass13(0)
    with jax.named_scope("send13_3"):
        send13(3)
    with jax.named_scope("pass_on_1"):
        pass_on(1)
    states.append(spread(up, [ref.at[ep, up] for ref in all_refs]))
    with jax.named_scope("share_1"):
        share(1)
    with jax.named_scope("pass13_1"):
        pass13(1)
    with jax.named_scope("send13_4"):
        send13(4)
    with jax.named_scope("have13_0"):
        have13(0)
    with jax.named_scope("hidden_0"):
        hidden(0)
    with jax.named_scope("pass13_2"):
        pass13(2)
    with jax.named_scope("last_1"):
        last(1)
    with jax.named_scope("from_mate_1"):
        from_mate(1)
    with jax.named_scope("compute_down_False"):
        compute(down, False)
    with jax.named_scope("pass13_3"):
        pass13(3)
    with jax.named_scope("send2_0"):
        send2(0)
    with jax.named_scope("pass_on_2"):
        pass_on(2)
    with jax.named_scope("have13_1"):
        have13(1)
    with jax.named_scope("hidden_1"):
        hidden(1)
    with jax.named_scope("share_2"):
        share(2)
    with jax.named_scope("pass13_4"):
        pass13(4)
    with jax.named_scope("have13_2"):
        have13(2)
    with jax.named_scope("hidden_2"):
        hidden(2)
    with jax.named_scope("last_2"):
        last(2)
    with jax.named_scope("from_mate_2"):
        from_mate(2)
    with jax.named_scope("have13_3"):
        have13(3)
    with jax.named_scope("hidden_3"):
        hidden(3)
    with jax.named_scope("start_loads_up_0"):
        start_loads(up, 0)
    with jax.named_scope("half_group_up_0_False_True"):
        half_group(up, 0, False, True)
    with jax.named_scope("pass2_0"):
        pass2(0)
    with jax.named_scope("send2_1"):
        send2(1)
        send2(2)
    with jax.named_scope("half_group_up_1_False_False"):
        half_group(up, 1, False, False)
    with jax.named_scope("have13_4"):
        have13(4)
    with jax.named_scope("hidden_4"):
        hidden(4)

    with jax.named_scope("have2_0"):
        have2(0)
    with jax.named_scope("y_part_0"):
        y_part(0)
    with jax.named_scope("sum_begin_0_0"):
        sum_begin(0, 0)
    with jax.named_scope("sum_end_0_0"):
        sum_end(0, 0)
    with jax.named_scope("pass2_1"):
        pass2(1)
    with jax.named_scope("send2_3"):
        send2(3)
    with jax.named_scope("pass2_2"):
        pass2(2)
    with jax.named_scope("sum_turn_0_0"):
        sum_turn(0, 0)
    with jax.named_scope("have2_1"):
        have2(1)
    with jax.named_scope("y_part_1"):
        y_part(1)
    with jax.named_scope("sum_begin_0_1"):
        sum_begin(0, 1)
    with jax.named_scope("pass2_3"):
        pass2(3)
    over_state = send_over()
    with jax.named_scope("sum_end_0_1"):
        sum_end(0, 1)
    with jax.named_scope("have2_2"):
        have2(2)
        have2(3)
    with jax.named_scope("y_part_2"):
        y_part(2)
    with jax.named_scope("sum_begin_0_2"):
        sum_begin(0, 2)
    with jax.named_scope("sum_end_0_2"):
        sum_end(0, 2)
    v_load(0).start()
    with jax.named_scope("sum_turn_0_1"):
        sum_turn(0, 1)
    with jax.named_scope("hidden_grads"):
        hidden_grads()
    with jax.named_scope("share_over_0"):
        share_over(0)
    with jax.named_scope("v_part_0"):
        v_part(0)
    with jax.named_scope("sum_begin_1_0"):
        sum_begin(1, 0)
    with jax.named_scope("sum_turn_0_2"):
        sum_turn(0, 2)
    with jax.named_scope("sum_end_1_0"):
        sum_end(1, 0)
    with jax.named_scope("share_over_1"):
        share_over(1)
    with jax.named_scope("v_part_1"):
        v_part(1)
    with jax.named_scope("sum_begin_1_1"):
        sum_begin(1, 1)
    with jax.named_scope("have_over_0"):
        have_over(0)
    with jax.named_scope("have_over_1"):
        have_over(1)
    with jax.named_scope("start_loads_over_0"):
        start_loads(over, 0)
    with jax.named_scope("sum_end_1_1"):
        sum_end(1, 1)
    with jax.named_scope("v_part_2"):
        v_part(2)
    with jax.named_scope("sum_begin_1_2"):
        sum_begin(1, 2)
    with jax.named_scope("sum_turn_1_0"):
        sum_turn(1, 0)
    with jax.named_scope("sum_end_1_2"):
        sum_end(1, 2)
    with jax.named_scope("share_over_2"):
        share_over(2)
    with jax.named_scope("out_start"):
        out_start()
    with jax.named_scope("half_group_over_0_False_False"):
        half_group(over, 0, False, False)
    with jax.named_scope("out_middle"):
        out_middle()
    with jax.named_scope("sum_turn_1_1"):
        sum_turn(1, 1)
    with jax.named_scope("have_over_2"):
        have_over(2)
    with jax.named_scope("start_loads_over_1_0"):
        start_loads(over, 1, (0,))
    with jax.named_scope("share_over_3"):
        share_over(3)
    with jax.named_scope("sum_turn_1_2"):
        sum_turn(1, 2)
    with jax.named_scope("have_over_3"):
        have_over(3)
    with jax.named_scope("start_loads_over_1_1"):
        start_loads(over, 1, (1,))
    with jax.named_scope("half_group_over_1_False_False"):
        half_group(over, 1, False, False)

    def grad_stores(e, slot):
        rows = pl.ds(0, PARTS)
        return [pltpu.make_async_copy(wide_buf.at[slot, rows, :, pl.ds(0, width)], g1.at[e], g_sem.at[slot, 0]),
                pltpu.make_async_copy(wide_buf.at[slot, rows, :, pl.ds(width, width)], g3.at[e], g_sem.at[slot, 1]),
                pltpu.make_async_copy(xs.at[slot, pl.ds(0, width)], g2.at[e], g_sem.at[slot, 2])]

    def finish(e, carry):
        slot = lax.rem(e, 2)

        @pl.when(e >= 2)
        def _():
            for copy in grad_stores(e - 2, slot):
                copy.wait()

        for m in range(PARTS):
            wide_buf[slot, m] = acc13[e, :, m * part : (m + 1) * part].T.astype(BF16)
        xs[slot, pl.ds(0, width), :] = acc2[e].astype(BF16)
        for copy in grad_stores(e, slot):
            copy.start()
        return carry

    with jax.named_scope("finish"):
        lax.fori_loop(0, own, finish, 0)
        for e in range(max(own - 2, 0), own):
            for copy in grad_stores(e, e % 2):
                copy.wait()
    with jax.named_scope("out_finish"):
        out_finish()
    with jax.named_scope("sums_here_1"):
        sums_here(1)
    out_store.wait()
    for n in sorted(writes):
        writes[n].wait()
    with jax.named_scope("drain"):
        links.drain()


def layer(tokens, d_out, ids, gate_vals, w_one, w_three, w_two, ep_size, tp_size, cap):
    tok, model = tokens.shape
    own, width, _ = w_two.shape
    half = ep_size // 2
    rows = half * cap
    part = model // PARTS
    hbm = pl.BlockSpec(memory_space=pl.ANY)
    shape = jax.ShapeDtypeStruct
    routes = (2 * ids.shape[0], tok)
    copies = copy_count(own)
    slot_rows = ep_size * tp_size * cap * own
    vector = pltpu.VMEM
    dma = pltpu.SemaphoreType.DMA
    outs = pl.pallas_call(
        functools.partial(layer_kernel, own, cap, width),
        in_specs=[hbm] * 7,
        out_specs=[hbm] * 15,
        out_shape=[
            shape((ep_size, tp_size, tok, model), BF16),
            shape((ep_size, tp_size, tok, model), BF16),
            shape((ep_size, tp_size) + routes, F32),
            shape((tp_size, own, PARTS, part, 2 * width), BF16),
            shape((tp_size, PARTS, own, width, part), BF16),
            shape((own, 2, rows, model), BF16),
            shape((own, 2, rows, model), BF16),
            shape((own, tp_size, 2 * rows, 2 * width), F32),
            shape((2, PARTS, 2 * tok, part // 2), F32),
            shape((2, PARTS, 2 * tok, part // 2), F32),
            shape((2, 2, PARTS, 2 * tok, part // 2), F32),
            shape((tok, model), BF16),
            shape((own, PARTS, part, width), BF16),
            shape((own, PARTS, part, width), BF16),
            shape((own, width, model), BF16),
        ],
        scratch_shapes=[
            vector(routes, F32),
            vector(ids.shape, jnp.int32),
            vector((own, PARTS, part, 2 * width), BF16),
            vector((own, width, model), BF16),
            vector((2, half // 2, tok, model), BF16),
            vector((2, half // 2, tok, model), BF16),
            vector((2, half // 2) + routes, F32),
            vector((ep_size,) + routes, F32),
            vector((tok, tok), BF16),
            vector((own, rows, model), BF16),
            vector((own, rows, model), BF16),
            vector((own, 2 * width, model), F32),
            vector((own, width, model), F32),
            vector((tp_size, own, part, 2 * width), BF16),
            vector((PARTS, tp_size, own, width, part), BF16),
            vector((tp_size, 2 * rows, 2 * width), F32),
            vector((own, tp_size, 2 * rows, 2 * width), BF16),
            vector((ep_size, own, cap, part), BF16),
            vector((4, 2 * tok, part // 2), F32),
            vector((2, 4, 2 * tok, part // 2), F32),
            vector((4, 2 * tok, part // 2), F32),
            vector((2 * tok, part // 2), F32),
            dma((copies,)),
            dma((copies,)),
            dma((4,)),
            dma((3, 2)),
            dma((2 * PARTS + 1,)),
            dma((2,)),
            dma((1 + tp_size,)),
            dma((tp_size,)),
            dma((3,)),
            dma((2 * PARTS,)),
            dma((2, 3)),
            pltpu.SemaphoreType.REGULAR,
        ],
        compiler_params=pltpu.CompilerParams(vmem_limit_bytes=VMEM_LIMIT, collective_id=0, has_side_effects=True),
        cost_estimate=pl.CostEstimate(
            flops=2 * slot_rows * model * (2 * tok + 12 * width),
            bytes_accessed=4 * ep_size * tp_size * tok * model,
            transcendentals=0,
        ),
        name="layer",
    )(tokens, d_out, ids, gate_vals, w_one, w_three, w_two)
    g1, g3, g2 = outs[12:]
    return outs[8], outs[10], outs[11], (g1.reshape(own, model, width), g3.reshape(own, model, width), g2)


def result_kernel(sums, last_land, rows_in, g1, g3, g2, out, dx, o1, o3, o2, parts, rows, row_buf, b1, b3, b2, in_sem, out_sem):
    moves = ((g1, b1, o1), (g3, b3, o3), (g2, b2, o2), (rows_in, row_buf, out))
    takes = [pltpu.make_async_copy(src, buf, in_sem.at[k]) for k, (src, buf, _) in enumerate(moves)]
    terms = [pltpu.make_async_copy(src, parts.at[k], in_sem.at[4 + k])
             for k, src in enumerate((sums.at[1], last_land.at[1, 0], last_land.at[1, 1]))]
    for copy in terms + takes:
        copy.start()
    for copy in terms:
        copy.wait()
    tok, fold = rows.shape[0], parts.shape[3]
    for q in range(parts.shape[1]):
        for h in range(2):
            at, half = (2 * q + h) * fold, pl.ds(h * tok, tok)
            rows[:, at : at + fold] = (parts[0, q, half] + (parts[1, q, half] + parts[2, q, half])).astype(BF16)
    puts = [pltpu.make_async_copy(rows, dx, out_sem.at[4])]
    puts[0].start()
    for k, (take, (_, buf, to)) in enumerate(zip(takes, moves)):
        take.wait()
        puts.append(pltpu.make_async_copy(buf, to, out_sem.at[k]))
        puts[-1].start()
    for copy in puts:
        copy.wait()


def results(sums, last_land, out, grads):
    _, count, tall, fold = sums.shape
    tok, model = out.shape
    hbm = pl.BlockSpec(memory_space=pl.ANY)
    row = jax.ShapeDtypeStruct((tok, model), BF16)
    rows = pltpu.VMEM((tok, model), BF16)
    return pl.pallas_call(
        result_kernel,
        in_specs=[hbm] * 6,
        out_specs=[hbm] * 5,
        out_shape=[row, row] + [jax.ShapeDtypeStruct(g.shape, g.dtype) for g in grads],
        scratch_shapes=[pltpu.VMEM((3, count, tall, fold), F32), rows, rows]
        + [pltpu.VMEM(g.shape, g.dtype) for g in grads]
        + [pltpu.SemaphoreType.DMA((7,)), pltpu.SemaphoreType.DMA((5,))],
        compiler_params=pltpu.CompilerParams(vmem_limit_bytes=VMEM_LIMIT),
        name="results",
    )(sums, last_land, out, *grads)


def solution(mesh):
    ep_size, tp_size = mesh.shape["ep"], mesh.shape["tp"]
    row_spec = P(("dp", "ep", "tp"), None)
    col_spec = P("ep", None, "tp")
    down_spec = P("ep", "tp", None)
    grad_col = P(("dp", "ep"), None, "tp")
    grad_down = P(("dp", "ep"), "tp", None)

    def local_step(tokens, expert_ids, gate_vals, w_one, w_three, w_two, d_out):
        cap = slot_count(expert_ids.shape[1], tokens.shape[0], w_one.shape[0] * ep_size)
        sums, last_land, out, grads = layer(tokens, d_out, expert_ids.T, gate_vals.T, w_one, w_three, w_two, ep_size, tp_size, cap)
        return tuple(results(sums, last_land, out, grads))

    return jax.shard_map(local_step, mesh=mesh,
                         in_specs=(row_spec, row_spec, row_spec, col_spec, col_spec, down_spec, row_spec),
                         out_specs=(row_spec, row_spec, grad_col, grad_col, grad_down), check_vma=False)
```

```python
import functools

import jax
import jax.numpy as jnp
from jax import lax
from jax.experimental import pallas as pl
from jax.experimental.pallas import tpu as pltpu
from jax.sharding import PartitionSpec as P

BF16 = jnp.bfloat16
F32 = jnp.float32
MESH = pl.DeviceIdType.MESH
VMEM_LIMIT = 67_043_328
PARTS = 3


def slot_count(num_top, tok_dev, experts):
    return 8 * ((5 * num_top * tok_dev + 32 * experts - 1) // (32 * experts))


def dot(a, b):
    return jnp.dot(a, b, preferred_element_type=F32)


def dot_tb(a, b):
    return lax.dot_general(a, b, (((1,), (1,)), ((), ())), preferred_element_type=F32)


def dot_ta(a, b):
    return lax.dot_general(a, b, (((0,), (0,)), ((), ())), preferred_element_type=F32)


def earlier_rows(tok):
    row = lax.broadcasted_iota(jnp.int32, (tok, tok), 0)
    col = lax.broadcasted_iota(jnp.int32, (tok, tok), 1)
    return jnp.where(row < col, 1.0, 0.0).astype(BF16)


def expert_rows(routes, first, own, earlier):
    top = routes.shape[0] // 2
    ids, gates = routes[:top], routes[top:]
    hits = [ids == (first + e).astype(F32) for e in range(own)]
    routed = jnp.concatenate([jnp.sum(jnp.where(m, 1.0, 0.0), axis=0, keepdims=True) for m in hits], axis=0)
    gate = jnp.concatenate([jnp.sum(jnp.where(m, gates, 0.0), axis=0, keepdims=True) for m in hits], axis=0)
    return jnp.where(routed > 0.0, dot(routed.astype(BF16), earlier), -1.0), gate


def hit_masks(pos, cap):
    slot = lax.broadcasted_iota(jnp.int32, (cap, pos.shape[1]), 0).astype(F32)
    return [pos[e : e + 1, :] == slot for e in range(pos.shape[0])]


def one_hot(masks):
    return jnp.concatenate([jnp.where(m, 1.0, 0.0) for m in masks], axis=0).astype(BF16)


def slot_gates(masks, gate):
    return jnp.concatenate([jnp.where(m, gate[e : e + 1, :], 0.0) for e, m in enumerate(masks)], axis=0)


def three_parts(x):
    hi = x.astype(BF16)
    rest = x - hi.astype(F32)
    mid = rest.astype(BF16)
    return hi, mid, (rest - mid.astype(F32)).astype(BF16)


class Links:
    def __init__(self, send_sem, recv_sem):
        self.send_sem, self.recv_sem, self.sent, self.finished = send_sem, recv_sem, [], set()

    def copy(self, k, src, dst, to):
        return pltpu.make_async_remote_copy(src_ref=src, dst_ref=dst, send_sem=self.send_sem.at[k],
                                            recv_sem=self.recv_sem.at[k], device_id=to, device_id_type=MESH)

    def send(self, src, dst, to):
        k = len(self.sent)
        copy = self.copy(k, src, dst, to)
        copy.start()
        self.sent.append(copy)
        return k

    def arrive(self, k, dst, to):
        self.copy(k, dst, dst, to).wait_recv()

    def finish(self, k):
        self.finished.add(k)
        self.sent[k].wait_send()

    def drain(self):
        for k in range(len(self.sent)):
            if k not in self.finished:
                self.finish(k)


def copy_count(own):
    return 6 + 21 * 3 + 24 + 4 * own + 4 * (PARTS + 1) + 2 * PARTS * 8


def layer_kernel(own, cap, width, tokens, d_out, ids, gate_vals, w1, w3, w2, x_all, dy_all, r_all, w13_all, w2_all, xs_all,
                 us_all, ab_all, sums, far_land, last_land, out, g1, g3, g2, r_own, i_own, w13, w2s, xb,
                 dyb, rb, routes, earlier, xs, us, acc13, acc2, wide_buf, w2v, ab_buf, d_all, y_buf, give, keep_sum, mate_sum,
                 far_sum, send_sem, recv_sem, row_sem, load_sem, w_sem, slot_sem, in_sem, ab_sem, sum_sem, own_sem, g_sem, free_sem):
    ep, tp = lax.axis_index("ep"), lax.axis_index("tp")
    eps, tps = x_all.shape[0], x_all.shape[1]
    model = x_all.shape[3]
    part = model // PARTS
    half = eps // 2
    x_own, dy_own = xs.at[0], xs.at[1]
    step = lambda n: lax.rem(ep + (n + eps), eps)
    turn = lambda n: lax.rem(tp + (n + tps), tps)
    right, left, far = step(2), step(-2), step(4)
    mate = ep + 1 - 2 * lax.rem(ep, 2)
    mate_step = lambda n: lax.rem(mate + (n + eps), eps)
    up, down, over = turn(1), turn(-1), turn(2)
    to_right, to_left, to_mate = {"ep": right}, {"ep": left}, {"ep": mate}
    to_up, to_down = {"tp": up}, {"tp": down}
    links = Links(send_sem, recv_sem)

    barrier = pltpu.get_barrier_semaphore()
    for to in (to_right, to_left, to_mate, to_up, to_down):
        pl.semaphore_signal(barrier, inc=1, device_id=to, device_id_type=MESH)
    top = ids.shape[0]
    firsts = [pltpu.make_async_copy(ids, i_own, row_sem.at[0]), pltpu.make_async_copy(gate_vals, r_own.at[pl.ds(top, top)], row_sem.at[1]),
              pltpu.make_async_copy(tokens, x_own, row_sem.at[2]), pltpu.make_async_copy(d_out, dy_own, row_sem.at[3])]
    loads = [pltpu.make_async_copy(src.at[:, pl.ds(m * part, part)], w13.at[:, m, :, pl.ds(k * width, width)], w_sem.at[PARTS * k + m])
             for k, src in ((0, w1), (1, w3)) for m in range(PARTS)]
    loads.append(pltpu.make_async_copy(w2, w2s, w_sem.at[2 * PARTS]))
    for copy in firsts + loads:
        copy.start()
    firsts[0].wait()
    r_own[0:top] = i_own[...].astype(F32)
    for copy in firsts[1:]:
        copy.wait()
    with jax.named_scope("barrier"):
        pl.semaphore_wait(barrier, 5)

    own_refs, all_refs = (x_own, dy_own, r_own), (x_all, dy_all, r_all)
    upward = (True, False, True)
    kinds = (0, 1, 2)

    def spread(t, srcs):
        out = {}
        for kind in kinds:
            to = to_right if upward[kind] else to_left
            out[kind, upward[kind]] = links.send(srcs[kind], all_refs[kind].at[ep, t], to)
        for kind in kinds:
            to = to_left if upward[kind] else to_right
            out[kind, not upward[kind]] = links.send(srcs[kind], all_refs[kind].at[ep, t], to)
        for kind in kinds:
            out[kind, "mate"] = links.send(srcs[kind], all_refs[kind].at[ep, t], to_mate)
        return out

    def pass_on(g):
        state, t = states[g], groups[g]
        for kind in kinds:
            got, to = (left, to_right) if upward[kind] else (right, to_left)
            block = all_refs[kind].at[got, t]
            links.arrive(state[kind, upward[kind]], block, to)
            state[kind, "far"] = links.send(block, block, to)
            state[kind, "mate1"] = links.send(block, block, to_mate)

    def share(g):
        state, t = states[g], groups[g]
        for kind in kinds:
            got, to = (right, to_left) if upward[kind] else (left, to_right)
            block = all_refs[kind].at[got, t]
            links.arrive(state[kind, not upward[kind]], block, to)
            state[kind, "mate2"] = links.send(block, block, to_mate)

    def last(g):
        state, t = states[g], groups[g]
        for kind in kinds:
            block = all_refs[kind].at[far, t]
            links.arrive(state[kind, "far"], block, to_right if upward[kind] else to_left)
            state[kind, "mate3"] = links.send(block, block, to_mate)

    def from_mate(g):
        state, t = states[g], groups[g]
        for kind in kinds:
            one, two = (mate_step(-2), mate_step(2)) if upward[kind] else (mate_step(2), mate_step(-2))
            for name, at in (("mate", mate), ("mate1", one), ("mate2", two), ("mate3", mate_step(4))):
                links.arrive(state[kind, name], all_refs[kind].at[at, t], to_mate)

    core = lax.rem(ep, 2)

    def send_over():
        return [{kind: links.send(all_refs[kind].at[core + 2 * m, down if upward[kind] else up],
                                  all_refs[kind].at[core + 2 * m, down if upward[kind] else up],
                                  to_up if upward[kind] else to_down) for kind in kinds} for m in range(half)]

    def share_over(m):
        for kind in kinds:
            block = all_refs[kind].at[core + 2 * m, over]
            links.arrive(over_state[m][kind], block, to_up if upward[kind] else to_down)
            over_state[m][kind, "mate"] = links.send(block, block, to_mate)

    def have_over(m):
        for kind in kinds:
            links.arrive(over_state[m][kind, "mate"], all_refs[kind].at[1 - core + 2 * m, over], to_mate)

    def both_ways(src, dst):
        return {True: links.send(src, dst, to_up), False: links.send(src, dst, to_down)}

    def pass_halves(state, below, above, split):
        links.arrive(state[True], below, to_up)
        state["first"] = links.send(split(below, 0), split(below, 0), to_up)
        links.arrive(state[False], above, to_down)
        state["second"] = links.send(split(above, 1), split(above, 1), to_down)

    def have_halves(state, block, split):
        links.arrive(state["first"], split(block, 0), to_up)
        links.arrive(state["second"], split(block, 1), to_down)

    w13_state, w2_state = [None] * own, [None] * (PARTS + 1)
    split13 = lambda ref, k: ref.at[:, pl.ds(k * (part // 2), part // 2)]
    split2 = lambda ref, k: ref.at[:, pl.ds(k * (width // 2), width // 2)]

    def send13(e):
        w13_state[e] = both_ways(w13.at[e], w13_all.at[tp, e])

    def pass13(e):
        pass_halves(w13_state[e], w13_all.at[down, e], w13_all.at[up, e], split13)

    def have13(e):
        have_halves(w13_state[e], w13_all.at[over, e], split13)

    pieces = [(q, pl.ds(0, own)) for q in range(PARTS - 1)] + [(PARTS - 1, pl.ds(0, 2)), (PARTS - 1, pl.ds(2, own - 2))]

    def piece(j, p):
        q, experts = pieces[p]
        return w2_all.at[j, q, experts]

    def send2(p):
        q, experts = pieces[p]
        w2_state[p] = both_ways(w2s.at[experts, :, pl.ds(q * part, part)], piece(tp, p))

    def pass2(p):
        pass_halves(w2_state[p], piece(down, p), piece(up, p), split2)

    def have2(p):
        have_halves(w2_state[p], piece(over, p), split2)

    def pair_loads(t, h, p):
        at = pl.ds(h * half + p * (half // 2), half // 2)
        return [pltpu.make_async_copy(src.at[at, t], dst.at[p], load_sem.at[k, p])
                for k, (src, dst) in enumerate(((x_all, xb), (dy_all, dyb), (r_all, rb)))]

    def half_group(t, h, keep, ahead, pairs=(0, 2), grads=True):
        def gather(p, b):
            pos, gate = expert_rows(rb[p, b], ep * own, own, earlier[...])
            masks = hit_masks(pos, cap)
            pick = one_hot(masks)
            gates = jnp.sum(slot_gates(masks, gate), axis=1, keepdims=True)
            rows = pl.ds(pl.multiple_of((p * (half // 2) + b) * cap, cap), cap)
            picked = dot(pick, xb[p, b]).astype(BF16)
            for e in range(own):
                xs[e, rows, :] = picked[e * cap : (e + 1) * cap]
            scaled = (gates * dot(pick, dyb[p, b])).astype(BF16)
            for e in range(own):
                us[e, rows, :] = scaled[e * cap : (e + 1) * cap]

        def pair(p, carry):
            for copy in pair_loads(t, h, p):
                copy.wait()
            for b in range(half // 2):
                gather(p, b)

            @pl.when(ahead)
            def _():
                for copy in pair_loads(t, 1, p):
                    copy.start()

            return carry

        lax.fori_loop(pairs[0], pairs[1], pair, 0)
        if not grads:
            return

        stores = []
        if keep:
            stores = [pltpu.make_async_copy(xs, xs_all.at[:, h], slot_sem.at[0]),
                      pltpu.make_async_copy(us, us_all.at[:, h], slot_sem.at[1])]
        for copy in stores:
            copy.start()

        def expert(e, carry):
            ab = dot(xs[e], w13[e].reshape(model, 2 * width))
            a, b = ab[:, :width], ab[:, width:]
            dh = dot_tb(us[e], w2s[e])
            sig = jax.nn.sigmoid(a)
            silu = a * sig
            hid = (silu * b).astype(BF16)
            da = (dh * b * sig * (1.0 + a * (1.0 - sig))).astype(BF16)
            db = (dh * silu).astype(BF16)
            acc13[e] += dot_ta(jnp.concatenate([da, db], axis=1), xs[e])
            acc2[e] += dot_ta(hid, us[e])
            return carry

        lax.fori_loop(0, own, expert, 0)
        for copy in stores:
            copy.wait()

    def start_loads(t, h, pairs=(0, 1)):
        for p in pairs:
            for copy in pair_loads(t, h, p):
                copy.start()

    def compute(t, keep):
        start_loads(t, 0)

        def one_half(h, carry):
            half_group(t, h, keep, h == 0)
            return carry

        lax.fori_loop(0, 2, one_half, 0)

    slots = eps * cap
    pending = []

    def settle():
        while pending:
            pending.pop().wait()

    def hidden(e):
        rows = pltpu.make_async_copy(xs_all.at[e], xs.at[pl.ds(0, 2)], in_sem.at[tps])
        rows.start()
        for j in range(tps):
            pltpu.make_async_copy(w13_all.at[j, e], wide_buf.at[pl.ds(0, PARTS), j], in_sem.at[j]).start()
        settle()
        rows.wait()

        def shard(j, carry):
            pltpu.make_async_copy(w13_all.at[j, e], wide_buf.at[pl.ds(0, PARTS), j], in_sem.at[j]).wait()
            ab = dot(xs[0:2].reshape(slots, model), wide_buf[0:PARTS, j].reshape(model, 2 * width))
            ab_buf[j] = ab
            a, b = ab[:, :width], ab[:, width:]
            at = pl.ds(pl.multiple_of(lax.rem(j, 2) * width, width), width)
            d_all[e, j // 2, :, at] = (a * jax.nn.sigmoid(a) * b).astype(BF16)
            return carry

        lax.fori_loop(0, tps, shard, 0)
        pending.append(pltpu.make_async_copy(ab_buf, ab_all.at[e], ab_sem.at[0]))
        pending[-1].start()

    def put_rows(e, value):
        for k in range(eps):
            y_buf[k, e] = value[k * cap : (k + 1) * cap]

    def y_part(q):
        load = pltpu.make_async_copy(w2_all.at[:, q], w2v.at[q], in_sem.at[0])
        load.start()
        load.wait()

        def one(e, carry):
            y = dot(d_all[e, 0], w2v[q, 0:2, e].reshape(2 * width, part)) + dot(d_all[e, 1], w2v[q, 2:4, e].reshape(2 * width, part))
            put_rows(e, y.astype(BF16))
            return carry

        lax.fori_loop(0, own, one, 0)

    def ab_load(e, j):
        return pltpu.make_async_copy(ab_all.at[e, j], ab_buf.at[j], ab_sem.at[j])

    def u_load(e, slot):
        return pltpu.make_async_copy(us_all.at[e], us.at[pl.ds(2 * slot, 2)], in_sem.at[1 + slot])

    def hidden_grads():
        settle()
        u_load(0, 0).start()
        for j in range(tps):
            ab_load(0, j).start()

        def one(e, carry):
            slot = lax.rem(e, 2)
            u_load(e, slot).wait()

            @pl.when(e + 1 < own)
            def _():
                u_load(e + 1, 1 - slot).start()

            def two(k, carry):
                dh = None
                for q in range(PARTS):
                    at = pl.ds(q * part, part)
                    u = us[pl.ds(2 * slot, 2), :, at].reshape(slots, part)
                    term = dot_tb(u, w2v[q, pl.ds(2 * k, 2), e].reshape(2 * width, part))
                    dh = term if dh is None else dh + term
                for i in range(2):
                    j = 2 * k + i
                    ab_load(e, j).wait()
                    a, b, d = ab_buf[j, :, :width], ab_buf[j, :, width:], dh[:, i * width : (i + 1) * width]
                    sig = jax.nn.sigmoid(a)
                    d_all[e, j, :, :width] = (d * b * sig * (1.0 + a * (1.0 - sig))).astype(BF16)
                    d_all[e, j, :, width:] = (d * (a * sig)).astype(BF16)

                    @pl.when(e + 1 < own)
                    def _():
                        ab_load(e + 1, j).start()
                return carry

            lax.fori_loop(0, tps // 2, two, 0)
            return carry

        lax.fori_loop(0, own, one, 0)

    def v_load(q):
        return pltpu.make_async_copy(w13_all.at[:, :, q], wide_buf, in_sem.at[0])

    def v_part(q):
        v_load(q).wait()

        def one(e, carry):
            v = dot_tb(d_all[e, 0], wide_buf[0, e])
            for j in range(1, tps):
                v = v + dot_tb(d_all[e, j], wide_buf[j, e])
            put_rows(e, v.astype(BF16))
            return carry

        lax.fori_loop(0, own, one, 0)
        if q + 1 < PARTS:
            v_load(q + 1).start()

    gifts, writes, stages = {}, {}, {}

    def combine(kind, block):
        masks = hit_masks(routes[block, 0:own], cap)
        rows = y_buf[block].reshape(own * cap, part)
        if kind == 1:
            return dot_ta(one_hot(masks), rows)
        hi, mid, low = three_parts(slot_gates(masks, routes[block, top : top + own]))
        return dot_ta(hi, rows) + (dot_ta(mid, rows) + dot_ta(low, rows))

    numbers, ready = {}, {}
    tok = far_sum.shape[0] // 2
    fold = part // 2
    buffers = [keep_sum.at[0], keep_sum.at[1], keep_sum.at[0], ab_buf, keep_sum.at[1], keep_sum.at[0]]
    earlier_user = {2: 0, 4: 1, 5: 2}
    assert ab_buf.shape == give.shape and len(buffers) == 2 * PARTS
    halves = (pl.ds(0, tok), pl.ds(tok, tok))

    def put_tile(ref, i, value):
        ref[i, 0:tok] = value[:, :fold]
        ref[i, tok : 2 * tok] = value[:, fold:]

    def sum_begin(kind, q):
        n = numbers[kind, q] = len(numbers)
        tiles = buffers[n]
        for k in gifts.get(n - 1, ()):
            links.finish(k)
        if n in earlier_user:
            for k in ready[earlier_user[n]]:
                links.finish(k)
            writes.pop(earlier_user[n]).wait()

        def to_other(i, carry):
            for k in range(2):
                put_tile(give, 2 * i + k, combine(kind, lax.rem(mate + 4 - 2 * (2 * i + k) + eps, eps)))
            return carry

        def to_own(i, carry):
            for k in range(2):
                put_tile(tiles, 2 * i + k, combine(kind, lax.rem(ep + 4 - 2 * (2 * i + k) + eps, eps)))
            return carry

        for i in range(2):
            to_other(i, 0)
            if n and not i:
                pl.semaphore_wait(free_sem, 1)
            pair = pl.ds(2 * i, 2)
            gifts.setdefault(n, []).append(links.send(give.at[pair], mate_sum.at[pair], to_mate))
        lax.fori_loop(0, 2, to_own, 0)

    def take_pair(n, i):
        pair = pl.ds(2 * i, 2)
        links.arrive(gifts[n][i], mate_sum.at[pair], to_mate)
        buffers[n][pair] += mate_sum[pair]

    def sum_far(kind, q):
        n = numbers[kind, q]
        tiles = buffers[n]
        take_pair(n, 0)
        stages[n] = [links.send(tiles.at[0, halves[h]], far_land.at[kind, q, halves[h]], to) for h, to in ((0, to_right), (1, to_left))]
        stages[n].append(links.send(tiles.at[1, halves[1]], last_land.at[kind, 0, q, halves[1]], to_right))

    def sum_near(kind, q):
        n = numbers[kind, q]
        tiles = buffers[n]
        take_pair(n, 1)
        if n + 1 < 2 * PARTS:
            pl.semaphore_signal(free_sem, inc=1, device_id=to_mate, device_id_type=MESH)
        stages[n].append(links.send(tiles.at[3, halves[0]], last_land.at[kind, 1, q, halves[0]], to_left))
        writes[n] = pltpu.make_async_copy(tiles.at[2], sums.at[kind, q], own_sem.at[n])
        writes[n].start()

    def sum_end(kind, q):
        sum_far(kind, q)
        sum_near(kind, q)

    def sum_turn(kind, q):
        n = numbers[kind, q]
        tiles = buffers[n]
        for h, to in ((0, to_right), (1, to_left)):
            links.arrive(stages[n][h], far_land.at[kind, q, halves[h]], to)
        load = pltpu.make_async_copy(far_land.at[kind, q], far_sum, sum_sem.at[2])
        load.start()
        load.wait()
        for i, h, side, to in ((1, 0, 0, to_right), (3, 1, 1, to_left)):
            tiles[i, halves[h]] += far_sum[halves[h]]
            stages[n].append(links.send(tiles.at[i, halves[h]], last_land.at[kind, side, q, halves[h]], to))
        ready[n] = tuple(stages[n])

    def sums_here(kind):
        for q in range(PARTS):
            sent = stages[numbers[kind, q]]
            for k, h, side, to in ((2, 1, 0, to_right), (3, 0, 1, to_left), (4, 0, 0, to_right), (5, 1, 1, to_left)):
                links.arrive(sent[k], last_land.at[kind, side, q, halves[h]], to)

    three = pl.ds(0, PARTS)
    out_loads = [pltpu.make_async_copy(sums.at[0], give.at[three], sum_sem.at[0]),
                 pltpu.make_async_copy(last_land.at[0, 0], mate_sum.at[three], sum_sem.at[1]),
                 pltpu.make_async_copy(last_land.at[0, 1], mate_sum.at[three], sum_sem.at[1])]
    out_store = pltpu.make_async_copy(xb.at[0, 0], out, sum_sem.at[0])

    def out_start():
        sums_here(0)
        for k in gifts[2 * PARTS - 1]:
            links.finish(k)
        out_loads[0].start()
        out_loads[1].start()

    def out_middle():
        out_loads[0].wait()
        out_loads[1].wait()
        give[three] += mate_sum[three]
        out_loads[2].start()

    def out_finish():
        out_loads[2].wait()
        for q in range(PARTS):
            for h in range(2):
                at = q * part + h * fold
                xb[0, 0, :, at : at + fold] = (give[q, halves[h]] + mate_sum[q, halves[h]]).astype(BF16)
        out_store.start()

    y_state = {}
    for way in (True, False):
        for kind in kinds:
            go_up = upward[kind] == way
            y_state[kind, go_up] = links.send(own_refs[kind], all_refs[kind].at[ep, tp], to_up if go_up else to_down)
    groups = (tp, down, up)
    states = [spread(tp, own_refs)]
    first_sends = range(len(links.sent))
    hold = [pltpu.make_async_copy(own_refs[kind], all_refs[kind].at[ep, tp], row_sem.at[kind]) for kind in range(3)]
    for copy in hold:
        copy.start()
    for copy in loads:
        copy.wait()
    stow = [pltpu.make_async_copy(w13, w13_all.at[tp], w_sem.at[0])]
    stow += [pltpu.make_async_copy(w2s.at[:, :, pl.ds(q * part, part)], w2_all.at[tp, q], w_sem.at[1 + q]) for q in range(PARTS)]
    for copy in stow:
        copy.start()
    earlier[...] = earlier_rows(earlier.shape[0])
    with jax.named_scope("zeros"):
        acc13[...] = jnp.zeros_like(acc13)
        acc2[...] = jnp.zeros_like(acc2)

    def y_arrive(kind, way):
        block = all_refs[kind].at[ep, down if way else up]
        links.arrive(y_state[kind, way], block, to_up if way else to_down)
        return block

    with jax.named_scope("pass_on_0"):
        pass_on(0)
    with jax.named_scope("y_arrive"):
        for way in (True, False):
            for kind in kinds:
                y_arrive(kind, way)
    with jax.named_scope("send13_0"):
        send13(0)
    with jax.named_scope("send13_1"):
        send13(1)
    with jax.named_scope("send13_2"):
        send13(2)
    states.append(spread(down, [ref.at[ep, down] for ref in all_refs]))
    with jax.named_scope("share_0"):
        share(0)
    with jax.named_scope("last_0"):
        last(0)
    for copy in hold + stow:
        copy.wait()
    with jax.named_scope("from_mate_0"):
        from_mate(0)
    route_copy = pltpu.make_async_copy(r_all.at[:, tp], routes, row_sem.at[0])
    route_copy.start()
    route_copy.wait()

    def tabulate(b, carry):
        pos, gate = expert_rows(routes[b], ep * own, own, earlier[...])
        routes[b, 0:own] = pos
        routes[b, top : top + own] = gate
        return carry

    lax.fori_loop(0, eps, tabulate, 0)
    for k in first_sends:
        links.finish(k)
    with jax.named_scope("compute_tp_True"):
        compute(tp, True)
    with jax.named_scope("pass13_0"):
        pass13(0)
    with jax.named_scope("send13_3"):
        send13(3)
    with jax.named_scope("pass_on_1"):
        pass_on(1)
    states.append(spread(up, [ref.at[ep, up] for ref in all_refs]))
    with jax.named_scope("share_1"):
        share(1)
    with jax.named_scope("pass13_1"):
        pass13(1)
    with jax.named_scope("send13_4"):
        send13(4)
    with jax.named_scope("have13_0"):
        have13(0)
    with jax.named_scope("hidden_0"):
        hidden(0)
    with jax.named_scope("pass13_2"):
        pass13(2)
    with jax.named_scope("last_1"):
        last(1)
    with jax.named_scope("from_mate_1"):
        from_mate(1)
    with jax.named_scope("compute_down_False"):
        compute(down, False)
    with jax.named_scope("pass13_3"):
        pass13(3)
    with jax.named_scope("send2_0"):
        send2(0)
    with jax.named_scope("pass_on_2"):
        pass_on(2)
    with jax.named_scope("have13_1"):
        have13(1)
    with jax.named_scope("hidden_1"):
        hidden(1)
    with jax.named_scope("share_2"):
        share(2)
    with jax.named_scope("pass13_4"):
        pass13(4)
    with jax.named_scope("have13_2"):
        have13(2)
    with jax.named_scope("hidden_2"):
        hidden(2)
    with jax.named_scope("last_2"):
        last(2)
    with jax.named_scope("from_mate_2"):
        from_mate(2)
    with jax.named_scope("have13_3"):
        have13(3)
    with jax.named_scope("hidden_3"):
        hidden(3)
    with jax.named_scope("start_loads_up_0"):
        start_loads(up, 0)
    with jax.named_scope("half_group_up_0_False_True"):
        half_group(up, 0, False, True)
    with jax.named_scope("pass2_0"):
        pass2(0)
    with jax.named_scope("send2_1"):
        send2(1)
        send2(2)
    with jax.named_scope("half_group_up_1_False_False"):
        half_group(up, 1, False, False)
    with jax.named_scope("have13_4"):
        have13(4)
    with jax.named_scope("hidden_4"):
        hidden(4)

    with jax.named_scope("have2_0"):
        have2(0)
    with jax.named_scope("y_part_0"):
        y_part(0)
    with jax.named_scope("sum_begin_0_0"):
        sum_begin(0, 0)
    with jax.named_scope("sum_end_0_0"):
        sum_end(0, 0)
    with jax.named_scope("pass2_1"):
        pass2(1)
    with jax.named_scope("send2_3"):
        send2(3)
    with jax.named_scope("pass2_2"):
        pass2(2)
    with jax.named_scope("sum_turn_0_0"):
        sum_turn(0, 0)
    with jax.named_scope("have2_1"):
        have2(1)
    with jax.named_scope("y_part_1"):
        y_part(1)
    with jax.named_scope("sum_begin_0_1"):
        sum_begin(0, 1)
    with jax.named_scope("pass2_3"):
        pass2(3)
    over_state = send_over()
    with jax.named_scope("sum_end_0_1"):
        sum_end(0, 1)
    with jax.named_scope("have2_2"):
        have2(2)
        have2(3)
    with jax.named_scope("y_part_2"):
        y_part(2)
    with jax.named_scope("sum_begin_0_2"):
        sum_begin(0, 2)
    with jax.named_scope("sum_end_0_2"):
        sum_end(0, 2)
    v_load(0).start()
    with jax.named_scope("sum_turn_0_1"):
        sum_turn(0, 1)
    with jax.named_scope("hidden_grads"):
        hidden_grads()
    with jax.named_scope("sum_turn_0_2"):
        sum_turn(0, 2)
    with jax.named_scope("share_over_0"):
        share_over(0)
    with jax.named_scope("v_part_0"):
        v_part(0)
    with jax.named_scope("sum_begin_1_0"):
        sum_begin(1, 0)
    with jax.named_scope("sum_far_1_0"):
        sum_far(1, 0)
    with jax.named_scope("v_part_1"):
        v_part(1)
    with jax.named_scope("sum_near_1_0"):
        sum_near(1, 0)
    with jax.named_scope("sum_begin_1_1"):
        sum_begin(1, 1)
    with jax.named_scope("sum_far_1_1"):
        sum_far(1, 1)
    with jax.named_scope("share_over_1"):
        share_over(1)
    with jax.named_scope("v_part_2"):
        v_part(2)
    with jax.named_scope("sum_near_1_1"):
        sum_near(1, 1)
    with jax.named_scope("sum_begin_1_2"):
        sum_begin(1, 2)
    with jax.named_scope("sum_far_1_2"):
        sum_far(1, 2)
    with jax.named_scope("sum_turn_1_0"):
        sum_turn(1, 0)
    with jax.named_scope("have_over_0"):
        have_over(0)
    with jax.named_scope("have_over_1"):
        have_over(1)
    with jax.named_scope("start_loads_over_0"):
        start_loads(over, 0)
    with jax.named_scope("sum_near_1_2"):
        sum_near(1, 2)
    with jax.named_scope("out_start"):
        out_start()
    with jax.named_scope("half_group_over_0_False_False"):
        half_group(over, 0, False, False)
    with jax.named_scope("sum_turn_1_1"):
        sum_turn(1, 1)
    with jax.named_scope("share_over_2"):
        share_over(2)
    with jax.named_scope("out_middle"):
        out_middle()
    with jax.named_scope("have_over_2"):
        have_over(2)
    with jax.named_scope("start_loads_over_1_0"):
        start_loads(over, 1, (0,))
    with jax.named_scope("sum_turn_1_2"):
        sum_turn(1, 2)
    with jax.named_scope("half_group_over_1_False_False_0_1_False"):
        half_group(over, 1, False, False, (0, 1), False)
    with jax.named_scope("share_over_3"):
        share_over(3)
    with jax.named_scope("have_over_3"):
        have_over(3)
    with jax.named_scope("start_loads_over_1_1"):
        start_loads(over, 1, (1,))
    with jax.named_scope("half_group_over_1_False_False_1_2"):
        half_group(over, 1, False, False, (1, 2))

    def grad_stores(e, slot):
        rows = pl.ds(0, PARTS)
        return [pltpu.make_async_copy(wide_buf.at[slot, rows, :, pl.ds(0, width)], g1.at[e], g_sem.at[slot, 0]),
                pltpu.make_async_copy(wide_buf.at[slot, rows, :, pl.ds(width, width)], g3.at[e], g_sem.at[slot, 1]),
                pltpu.make_async_copy(xs.at[slot, pl.ds(0, width)], g2.at[e], g_sem.at[slot, 2])]

    def finish(e, carry):
        slot = lax.rem(e, 2)

        @pl.when(e >= 2)
        def _():
            for copy in grad_stores(e - 2, slot):
                copy.wait()

        for m in range(PARTS):
            wide_buf[slot, m] = acc13[e, :, m * part : (m + 1) * part].T.astype(BF16)
        xs[slot, pl.ds(0, width), :] = acc2[e].astype(BF16)
        for copy in grad_stores(e, slot):
            copy.start()
        return carry

    with jax.named_scope("finish"):
        lax.fori_loop(0, own, finish, 0)
    with jax.named_scope("out_finish"):
        out_finish()
    with jax.named_scope("sums_here_1"):
        sums_here(1)
    out_store.wait()
    for e in range(max(own - 2, 0), own):
        for copy in grad_stores(e, e % 2):
            copy.wait()
    for n in sorted(writes):
        writes[n].wait()
    with jax.named_scope("drain"):
        links.drain()


def layer(tokens, d_out, ids, gate_vals, w_one, w_three, w_two, ep_size, tp_size, cap):
    tok, model = tokens.shape
    own, width, _ = w_two.shape
    half = ep_size // 2
    rows = half * cap
    part = model // PARTS
    hbm = pl.BlockSpec(memory_space=pl.ANY)
    shape = jax.ShapeDtypeStruct
    routes = (2 * ids.shape[0], tok)
    copies = copy_count(own)
    slot_rows = ep_size * tp_size * cap * own
    vector = pltpu.VMEM
    dma = pltpu.SemaphoreType.DMA
    outs = pl.pallas_call(
        functools.partial(layer_kernel, own, cap, width),
        in_specs=[hbm] * 7,
        out_specs=[hbm] * 15,
        out_shape=[
            shape((ep_size, tp_size, tok, model), BF16),
            shape((ep_size, tp_size, tok, model), BF16),
            shape((ep_size, tp_size) + routes, F32),
            shape((tp_size, own, PARTS, part, 2 * width), BF16),
            shape((tp_size, PARTS, own, width, part), BF16),
            shape((own, 2, rows, model), BF16),
            shape((own, 2, rows, model), BF16),
            shape((own, tp_size, 2 * rows, 2 * width), F32),
            shape((2, PARTS, 2 * tok, part // 2), F32),
            shape((2, PARTS, 2 * tok, part // 2), F32),
            shape((2, 2, PARTS, 2 * tok, part // 2), F32),
            shape((tok, model), BF16),
            shape((own, PARTS, part, width), BF16),
            shape((own, PARTS, part, width), BF16),
            shape((own, width, model), BF16),
        ],
        scratch_shapes=[
            vector(routes, F32),
            vector(ids.shape, jnp.int32),
            vector((own, PARTS, part, 2 * width), BF16),
            vector((own, width, model), BF16),
            vector((2, half // 2, tok, model), BF16),
            vector((2, half // 2, tok, model), BF16),
            vector((2, half // 2) + routes, F32),
            vector((ep_size,) + routes, F32),
            vector((tok, tok), BF16),
            vector((own, rows, model), BF16),
            vector((own, rows, model), BF16),
            vector((own, 2 * width, model), F32),
            vector((own, width, model), F32),
            vector((tp_size, own, part, 2 * width), BF16),
            vector((PARTS, tp_size, own, width, part), BF16),
            vector((tp_size, 2 * rows, 2 * width), F32),
            vector((own, tp_size, 2 * rows, 2 * width), BF16),
            vector((ep_size, own, cap, part), BF16),
            vector((4, 2 * tok, part // 2), F32),
            vector((2, 4, 2 * tok, part // 2), F32),
            vector((4, 2 * tok, part // 2), F32),
            vector((2 * tok, part // 2), F32),
            dma((copies,)),
            dma((copies,)),
            dma((4,)),
            dma((3, 2)),
            dma((2 * PARTS + 1,)),
            dma((2,)),
            dma((1 + tp_size,)),
            dma((tp_size,)),
            dma((3,)),
            dma((2 * PARTS,)),
            dma((2, 3)),
            pltpu.SemaphoreType.REGULAR,
        ],
        compiler_params=pltpu.CompilerParams(vmem_limit_bytes=VMEM_LIMIT, collective_id=0, has_side_effects=True),
        cost_estimate=pl.CostEstimate(
            flops=2 * slot_rows * model * (2 * tok + 12 * width),
            bytes_accessed=4 * ep_size * tp_size * tok * model,
            transcendentals=0,
        ),
        name="layer",
    )(tokens, d_out, ids, gate_vals, w_one, w_three, w_two)
    g1, g3, g2 = outs[12:]
    return outs[8], outs[10], outs[11], (g1.reshape(own, model, width), g3.reshape(own, model, width), g2)


def result_kernel(sums, last_land, rows_in, g1, g3, g2, out, dx, o1, o3, o2, parts, rows, row_buf, b1, b3, b2, in_sem, out_sem):
    moves = ((g1, b1, o1), (g3, b3, o3), (g2, b2, o2), (rows_in, row_buf, out))
    takes = [pltpu.make_async_copy(src, buf, in_sem.at[k]) for k, (src, buf, _) in enumerate(moves)]
    terms = [pltpu.make_async_copy(src, parts.at[k], in_sem.at[4 + k])
             for k, src in enumerate((sums.at[1], last_land.at[1, 0], last_land.at[1, 1]))]
    for copy in terms + takes:
        copy.start()
    for copy in terms:
        copy.wait()
    tok, fold = rows.shape[0], parts.shape[3]
    for q in range(parts.shape[1]):
        for h in range(2):
            at, half = (2 * q + h) * fold, pl.ds(h * tok, tok)
            rows[:, at : at + fold] = (parts[0, q, half] + (parts[1, q, half] + parts[2, q, half])).astype(BF16)
    puts = [pltpu.make_async_copy(rows, dx, out_sem.at[4])]
    puts[0].start()
    for k, (take, (_, buf, to)) in enumerate(zip(takes, moves)):
        take.wait()
        puts.append(pltpu.make_async_copy(buf, to, out_sem.at[k]))
        puts[-1].start()
    for copy in puts:
        copy.wait()


def results(sums, last_land, out, grads):
    _, count, tall, fold = sums.shape
    tok, model = out.shape
    hbm = pl.BlockSpec(memory_space=pl.ANY)
    row = jax.ShapeDtypeStruct((tok, model), BF16)
    rows = pltpu.VMEM((tok, model), BF16)
    return pl.pallas_call(
        result_kernel,
        in_specs=[hbm] * 6,
        out_specs=[hbm] * 5,
        out_shape=[row, row] + [jax.ShapeDtypeStruct(g.shape, g.dtype) for g in grads],
        scratch_shapes=[pltpu.VMEM((3, count, tall, fold), F32), rows, rows]
        + [pltpu.VMEM(g.shape, g.dtype) for g in grads]
        + [pltpu.SemaphoreType.DMA((7,)), pltpu.SemaphoreType.DMA((5,))],
        compiler_params=pltpu.CompilerParams(vmem_limit_bytes=VMEM_LIMIT),
        name="results",
    )(sums, last_land, out, *grads)


def solution(mesh):
    ep_size, tp_size = mesh.shape["ep"], mesh.shape["tp"]
    row_spec = P(("dp", "ep", "tp"), None)
    col_spec = P("ep", None, "tp")
    down_spec = P("ep", "tp", None)
    grad_col = P(("dp", "ep"), None, "tp")
    grad_down = P(("dp", "ep"), "tp", None)

    def local_step(tokens, expert_ids, gate_vals, w_one, w_three, w_two, d_out):
        cap = slot_count(expert_ids.shape[1], tokens.shape[0], w_one.shape[0] * ep_size)
        sums, last_land, out, grads = layer(tokens, d_out, expert_ids.T, gate_vals.T, w_one, w_three, w_two, ep_size, tp_size, cap)
        return tuple(results(sums, last_land, out, grads))

    return jax.shard_map(local_step, mesh=mesh,
                         in_specs=(row_spec, row_spec, row_spec, col_spec, col_spec, down_spec, row_spec),
                         out_specs=(row_spec, row_spec, grad_col, grad_col, grad_down), check_vma=False)
```

```python
import functools

import jax
import jax.numpy as jnp
from jax import lax
from jax.experimental import pallas as pl
from jax.experimental.pallas import tpu as pltpu
from jax.sharding import PartitionSpec as P

BF16 = jnp.bfloat16
F32 = jnp.float32
MESH = pl.DeviceIdType.MESH
VMEM_LIMIT = 67_043_328
PARTS = 3


def slot_count(num_top, tok_dev, experts):
    return 8 * ((5 * num_top * tok_dev + 32 * experts - 1) // (32 * experts))


def dot(a, b):
    return jnp.dot(a, b, preferred_element_type=F32)


def dot_tb(a, b):
    return lax.dot_general(a, b, (((1,), (1,)), ((), ())), preferred_element_type=F32)


def dot_ta(a, b):
    return lax.dot_general(a, b, (((0,), (0,)), ((), ())), preferred_element_type=F32)


def earlier_rows(tok):
    row = lax.broadcasted_iota(jnp.int32, (tok, tok), 0)
    col = lax.broadcasted_iota(jnp.int32, (tok, tok), 1)
    return jnp.where(row < col, 1.0, 0.0).astype(BF16)


def expert_rows(routes, first, own, earlier):
    top = routes.shape[0] // 2
    ids, gates = routes[:top], routes[top:]
    hits = [ids == (first + e).astype(F32) for e in range(own)]
    routed = jnp.concatenate([jnp.sum(jnp.where(m, 1.0, 0.0), axis=0, keepdims=True) for m in hits], axis=0)
    gate = jnp.concatenate([jnp.sum(jnp.where(m, gates, 0.0), axis=0, keepdims=True) for m in hits], axis=0)
    return jnp.where(routed > 0.0, dot(routed.astype(BF16), earlier), -1.0), gate


def hit_masks(pos, cap):
    slot = lax.broadcasted_iota(jnp.int32, (cap, pos.shape[1]), 0).astype(F32)
    return [pos[e : e + 1, :] == slot for e in range(pos.shape[0])]


def one_hot(masks):
    return jnp.concatenate([jnp.where(m, 1.0, 0.0) for m in masks], axis=0).astype(BF16)


def slot_gates(masks, gate):
    return jnp.concatenate([jnp.where(m, gate[e : e + 1, :], 0.0) for e, m in enumerate(masks)], axis=0)


def three_parts(x):
    hi = x.astype(BF16)
    rest = x - hi.astype(F32)
    mid = rest.astype(BF16)
    return hi, mid, (rest - mid.astype(F32)).astype(BF16)


class Links:
    def __init__(self, send_sem, recv_sem):
        self.send_sem, self.recv_sem, self.sent, self.finished = send_sem, recv_sem, [], set()
        self.send_of, self.recv_of = {}, {}

    def copy(self, s, r, src, dst, to):
        return pltpu.make_async_remote_copy(src_ref=src, dst_ref=dst, send_sem=self.send_sem.at[s],
                                            recv_sem=self.recv_sem.at[r], device_id=to, device_id_type=MESH)

    def send(self, src, dst, to, together=None, landing=None):
        k = len(self.sent)
        s = self.send_of.setdefault(k if together is None else together, len(self.send_of))
        r = self.recv_of.setdefault(k if landing is None else landing, len(self.recv_of))
        copy = self.copy(s, r, src, dst, to)
        copy.start()
        self.sent.append((s, r, copy))
        if together is not None:
            self.finished.add(k)
        return k

    def arrive(self, k, dst, to):
        s, r, _ = self.sent[k]
        self.copy(s, r, dst, dst, to).wait_recv()

    def arrive_all(self, landing, ref, to):
        self.copy(0, self.recv_of[landing], ref, ref, to).wait_recv()

    def finish(self, k):
        self.finished.add(k)
        self.sent[k][2].wait_send()

    def finish_all(self, together, ref, to):
        self.copy(self.send_of[together], 0, ref, ref, to).wait_send()

    def drain(self):
        for k in range(len(self.sent)):
            if k not in self.finished:
                self.finish(k)


def copy_counts(own):
    sums = 2 * PARTS * 8
    return 3 * 5 + 2 + sums, 6 + 3 * 3 * 4 + 24 + 4 * own + 4 * (PARTS + 1) + sums


def layer_kernel(own, cap, width, tokens, d_out, ids, gate_vals, w1, w3, w2, x_all, dy_all, r_all, w13_all, w2_all, xs_all,
                 us_all, ab_all, dh_all, sums, far_land, last_land, out, g1, g3, g2, r_own, i_own, w13, w2s, xb,
                 dyb, rb, routes, earlier, xs, us, acc13, acc2, wide_buf, w2v, ab_buf, d_all, y_buf, give, keep_sum, mate_sum,
                 far_sum, send_sem, recv_sem, row_sem, load_sem, w_sem, slot_sem, in_sem, ab_sem, sum_sem, own_sem, g_sem, dh_sem, free_sem):
    ep, tp = lax.axis_index("ep"), lax.axis_index("tp")
    eps, tps = x_all.shape[0], x_all.shape[1]
    model = x_all.shape[3]
    part = model // PARTS
    half = eps // 2
    x_own, dy_own = xs.at[0], xs.at[1]
    step = lambda n: lax.rem(ep + (n + eps), eps)
    turn = lambda n: lax.rem(tp + (n + tps), tps)
    right, left, far = step(2), step(-2), step(4)
    mate = ep + 1 - 2 * lax.rem(ep, 2)
    mate_step = lambda n: lax.rem(mate + (n + eps), eps)
    up, down, over = turn(1), turn(-1), turn(2)
    to_right, to_left, to_mate = {"ep": right}, {"ep": left}, {"ep": mate}
    to_up, to_down = {"tp": up}, {"tp": down}
    links = Links(send_sem, recv_sem)

    barrier = pltpu.get_barrier_semaphore()
    for to in (to_right, to_left, to_mate, to_up, to_down):
        pl.semaphore_signal(barrier, inc=1, device_id=to, device_id_type=MESH)
    top = ids.shape[0]
    firsts = [pltpu.make_async_copy(ids, i_own, row_sem.at[0]), pltpu.make_async_copy(gate_vals, r_own.at[pl.ds(top, top)], row_sem.at[1]),
              pltpu.make_async_copy(tokens, x_own, row_sem.at[2]), pltpu.make_async_copy(d_out, dy_own, row_sem.at[3])]
    loads = [pltpu.make_async_copy(src.at[:, pl.ds(m * part, part)], w13.at[:, m, :, pl.ds(k * width, width)], w_sem.at[PARTS * k + m])
             for k, src in ((0, w1), (1, w3)) for m in range(PARTS)]
    loads.append(pltpu.make_async_copy(w2, w2s, w_sem.at[2 * PARTS]))
    for copy in firsts + loads:
        copy.start()
    firsts[0].wait()
    r_own[0:top] = i_own[...].astype(F32)
    for copy in firsts[1:]:
        copy.wait()
    with jax.named_scope("barrier"):
        pl.semaphore_wait(barrier, 5)

    own_refs, all_refs = (x_own, dy_own, r_own), (x_all, dy_all, r_all)
    upward = (True, False, True)
    kinds = (0, 1, 2)

    def spread(g, srcs):
        out, t = {}, groups[g]
        set_of = lambda kind: ("rows", kind, g) if g else ("first", kind)
        for kind in kinds:
            to = to_right if upward[kind] else to_left
            out[kind, upward[kind]] = links.send(srcs[kind], all_refs[kind].at[ep, t], to, set_of(kind))
        for kind in kinds:
            to = to_left if upward[kind] else to_right
            out[kind, not upward[kind]] = links.send(srcs[kind], all_refs[kind].at[ep, t], to, set_of(kind))
        for kind in kinds:
            links.send(srcs[kind], all_refs[kind].at[ep, t], to_mate, set_of(kind), ("mate", kind, g))
        return out

    def pass_on(g):
        state, t = states[g], groups[g]
        for kind in kinds:
            got, to = (left, to_right) if upward[kind] else (right, to_left)
            block = all_refs[kind].at[got, t]
            links.arrive(state[kind, upward[kind]], block, to)
            state[kind, "far"] = links.send(block, block, to, ("rows", kind, g))
            links.send(block, block, to_mate, ("rows", kind, g), ("mate", kind, g))

    def share(g):
        state, t = states[g], groups[g]
        for kind in kinds:
            got, to = (right, to_left) if upward[kind] else (left, to_right)
            block = all_refs[kind].at[got, t]
            links.arrive(state[kind, not upward[kind]], block, to)
            links.send(block, block, to_mate, ("rows", kind, g), ("mate", kind, g))

    def last(g):
        state, t = states[g], groups[g]
        for kind in kinds:
            block = all_refs[kind].at[far, t]
            links.arrive(state[kind, "far"], block, to_right if upward[kind] else to_left)
            links.send(block, block, to_mate, ("rows", kind, g), ("mate", kind, g))

    def from_mate(g):
        for kind in kinds:
            links.arrive_all(("mate", kind, g), all_refs[kind].at[pl.ds(0, half), groups[g]], to_mate)

    core = lax.rem(ep, 2)

    def send_over():
        return [{kind: links.send(all_refs[kind].at[core + 2 * m, down if upward[kind] else up],
                                  all_refs[kind].at[core + 2 * m, down if upward[kind] else up],
                                  to_up if upward[kind] else to_down, ("over", kind)) for kind in kinds} for m in range(half)]

    def share_over(m):
        for kind in kinds:
            block = all_refs[kind].at[core + 2 * m, over]
            links.arrive(over_state[m][kind], block, to_up if upward[kind] else to_down)
            over_state[m][kind, "mate"] = links.send(block, block, to_mate, ("over", kind))

    def have_over(m):
        for kind in kinds:
            links.arrive(over_state[m][kind, "mate"], all_refs[kind].at[1 - core + 2 * m, over], to_mate)

    def both_ways(src, dst, which):
        return {True: links.send(src, dst, to_up, which), False: links.send(src, dst, to_down, which)}

    def pass_halves(state, below, above, split, which):
        links.arrive(state[True], below, to_up)
        state["first"] = links.send(split(below, 0), split(below, 0), to_up, which)
        links.arrive(state[False], above, to_down)
        state["second"] = links.send(split(above, 1), split(above, 1), to_down, which)

    def have_halves(state, block, split):
        links.arrive(state["first"], split(block, 0), to_up)
        links.arrive(state["second"], split(block, 1), to_down)

    w13_state, w2_state = [None] * own, [None] * (PARTS + 1)
    split13 = lambda ref, k: ref.at[:, pl.ds(k * (part // 2), part // 2)]
    split2 = lambda ref, k: ref.at[:, pl.ds(k * (width // 2), width // 2)]

    def send13(e):
        w13_state[e] = both_ways(w13.at[e], w13_all.at[tp, e], "w13")

    def pass13(e):
        pass_halves(w13_state[e], w13_all.at[down, e], w13_all.at[up, e], split13, "w13")

    def have13(e):
        have_halves(w13_state[e], w13_all.at[over, e], split13)

    pieces = [(q, pl.ds(0, own)) for q in range(PARTS - 1)] + [(PARTS - 1, pl.ds(0, 2)), (PARTS - 1, pl.ds(2, own - 2))]

    def piece(j, p):
        q, experts = pieces[p]
        return w2_all.at[j, q, experts]

    def send2(p):
        q, experts = pieces[p]
        w2_state[p] = both_ways(w2s.at[experts, :, pl.ds(q * part, part)], piece(tp, p), "w2")

    def pass2(p):
        pass_halves(w2_state[p], piece(down, p), piece(up, p), split2, "w2")

    def have2(p):
        have_halves(w2_state[p], piece(over, p), split2)

    def pair_loads(t, h, p):
        at = pl.ds(h * half + p * (half // 2), half // 2)
        return [pltpu.make_async_copy(src.at[at, t], dst.at[p], load_sem.at[k, p])
                for k, (src, dst) in enumerate(((x_all, xb), (dy_all, dyb), (r_all, rb)))]

    def half_group(t, h, keep, ahead, pairs=(0, 2), grads=True):
        def gather(p, b):
            pos, gate = expert_rows(rb[p, b], ep * own, own, earlier[...])
            masks = hit_masks(pos, cap)
            pick = one_hot(masks)
            gates = jnp.sum(slot_gates(masks, gate), axis=1, keepdims=True)
            rows = pl.ds(pl.multiple_of((p * (half // 2) + b) * cap, cap), cap)
            picked = dot(pick, xb[p, b]).astype(BF16)
            for e in range(own):
                xs[e, rows, :] = picked[e * cap : (e + 1) * cap]
            scaled = (gates * dot(pick, dyb[p, b])).astype(BF16)
            for e in range(own):
                us[e, rows, :] = scaled[e * cap : (e + 1) * cap]

        def pair(p, carry):
            for copy in pair_loads(t, h, p):
                copy.wait()
            for b in range(half // 2):
                gather(p, b)

            @pl.when(ahead)
            def _():
                for copy in pair_loads(t, 1, p):
                    copy.start()

            return carry

        lax.fori_loop(pairs[0], pairs[1], pair, 0)
        if not grads:
            return

        stores = []
        if keep:
            stores = [pltpu.make_async_copy(xs, xs_all.at[:, h], slot_sem.at[0]),
                      pltpu.make_async_copy(us, us_all.at[:, h], slot_sem.at[1])]
        for copy in stores:
            copy.start()

        def expert(e, carry):
            ab = dot(xs[e], w13[e].reshape(model, 2 * width))
            a, b = ab[:, :width], ab[:, width:]
            dh = dot_tb(us[e], w2s[e])
            sig = jax.nn.sigmoid(a)
            silu = a * sig
            hid = (silu * b).astype(BF16)
            da = (dh * b * sig * (1.0 + a * (1.0 - sig))).astype(BF16)
            db = (dh * silu).astype(BF16)
            acc13[e] += dot_ta(jnp.concatenate([da, db], axis=1), xs[e])
            acc2[e] += dot_ta(hid, us[e])
            return carry

        lax.fori_loop(0, own, expert, 0)
        for copy in stores:
            copy.wait()

    def start_loads(t, h, pairs=(0, 1)):
        for p in pairs:
            for copy in pair_loads(t, h, p):
                copy.start()

    def compute(t, keep):
        start_loads(t, 0)

        def one_half(h, carry):
            half_group(t, h, keep, h == 0)
            return carry

        lax.fori_loop(0, 2, one_half, 0)

    slots = eps * cap
    pending = []

    def settle():
        while pending:
            pending.pop().wait()

    def hidden(e):
        rows = pltpu.make_async_copy(xs_all.at[e], xs.at[pl.ds(0, 2)], in_sem.at[tps])
        rows.start()
        for j in range(tps):
            pltpu.make_async_copy(w13_all.at[j, e], wide_buf.at[pl.ds(0, PARTS), j], in_sem.at[j]).start()
        settle()
        rows.wait()

        def shard(j, carry):
            pltpu.make_async_copy(w13_all.at[j, e], wide_buf.at[pl.ds(0, PARTS), j], in_sem.at[j]).wait()
            ab = dot(xs[0:2].reshape(slots, model), wide_buf[0:PARTS, j].reshape(model, 2 * width))
            ab_buf[j] = ab
            a, b = ab[:, :width], ab[:, width:]
            at = pl.ds(pl.multiple_of(lax.rem(j, 2) * width, width), width)
            d_all[e, j // 2, :, at] = (a * jax.nn.sigmoid(a) * b).astype(BF16)
            return carry

        lax.fori_loop(0, tps, shard, 0)
        pending.append(pltpu.make_async_copy(ab_buf, ab_all.at[e], ab_sem.at[0]))
        pending[-1].start()

    def put_rows(e, value):
        for k in range(eps):
            y_buf[k, e] = value[k * cap : (k + 1) * cap]

    def down_load(q, j):
        return pltpu.make_async_copy(w2_all.at[j, q], w2v.at[q, j], in_sem.at[j])

    def load_down(q):
        for j in (tp, up, down):
            down_load(q, j).start()

    def y_part(q):
        down_load(q, over).start()
        for j in range(tps):
            down_load(q, j).wait()

        def one(e, carry):
            y = dot(d_all[e, 0], w2v[q, 0:2, e].reshape(2 * width, part)) + dot(d_all[e, 1], w2v[q, 2:4, e].reshape(2 * width, part))
            put_rows(e, y.astype(BF16))
            return carry

        lax.fori_loop(0, own, one, 0)

    def ab_load(e, j):
        return pltpu.make_async_copy(ab_all.at[e, j], ab_buf.at[j], ab_sem.at[j])

    most, final = pl.ds(0, (PARTS - 1) * part), pl.ds((PARTS - 1) * part, part)

    def u_load(e, slot, columns):
        rows = pl.ds(2 * slot, 2)
        return pltpu.make_async_copy(us_all.at[e, :, :, columns], us.at[rows, :, columns], slot_sem.at[slot])

    def dh_term(e, slot, k, q):
        u = us[pl.ds(2 * slot, 2), :, pl.ds(q * part, part)].reshape(slots, part)
        return dot_tb(u, w2v[q, pl.ds(2 * k, 2), e].reshape(2 * width, part))

    def dh_store(e, k, at):
        return pltpu.make_async_copy(give.at[at], dh_all.at[e, k], dh_sem.at[at])

    def dh_load(e, k, at):
        return pltpu.make_async_copy(dh_all.at[e, k], mate_sum.at[at], dh_sem.at[at])

    def dh_early():
        for k in gifts[PARTS - 2]:
            links.finish(k)
        u_load(0, 0, most).start()

        def one(e, carry):
            slot = lax.rem(e, 2)
            u_load(e, slot, most).wait()

            @pl.when(e + 1 < own)
            def _():
                u_load(e + 1, 1 - slot, most).start()

            for k in range(2):
                at = 2 * slot + k

                @pl.when(e >= 2)
                def _():
                    dh_store(e - 2, k, at).wait()

                total = dh_term(e, slot, k, 0)
                for q in range(1, PARTS - 1):
                    total = total + dh_term(e, slot, k, q)
                give[at] = total
                dh_store(e, k, at).start()
            return carry

        lax.fori_loop(0, own, one, 0)
        for e in (own - 2, own - 1):
            for k in range(2):
                dh_store(e, k, 2 * (e % 2) + k).wait()

    def hidden_grads():
        settle()
        u_load(0, 0, final).start()
        for k in range(2):
            dh_load(0, k, k).start()
        for j in range(tps):
            ab_load(0, j).start()

        def one(e, carry):
            slot = lax.rem(e, 2)
            u_load(e, slot, final).wait()

            @pl.when(e + 1 < own)
            def _():
                u_load(e + 1, 1 - slot, final).start()
                for k in range(2):
                    dh_load(e + 1, k, 2 * (1 - slot) + k).start()

            def two(k, carry):
                at = 2 * slot + k
                dh_load(e, k, at).wait()
                dh = mate_sum[at] + dh_term(e, slot, k, PARTS - 1)
                for i in range(2):
                    j = 2 * k + i
                    ab_load(e, j).wait()
                    a, b, d = ab_buf[j, :, :width], ab_buf[j, :, width:], dh[:, i * width : (i + 1) * width]
                    sig = jax.nn.sigmoid(a)
                    d_all[e, j, :, :width] = (d * b * sig * (1.0 + a * (1.0 - sig))).astype(BF16)
                    d_all[e, j, :, width:] = (d * (a * sig)).astype(BF16)

                    @pl.when(e + 1 < own)
                    def _():
                        ab_load(e + 1, j).start()
                return carry

            lax.fori_loop(0, tps // 2, two, 0)
            return carry

        lax.fori_loop(0, own, one, 0)
        free_mate()

    def v_load(q):
        return pltpu.make_async_copy(w13_all.at[:, :, q], wide_buf, in_sem.at[0])

    def v_part(q):
        v_load(q).wait()

        def one(e, carry):
            v = dot_tb(d_all[e, 0], wide_buf[0, e])
            for j in range(1, tps):
                v = v + dot_tb(d_all[e, j], wide_buf[j, e])
            put_rows(e, v.astype(BF16))
            return carry

        lax.fori_loop(0, own, one, 0)
        if q + 1 < PARTS:
            v_load(q + 1).start()

    gifts, writes, stages = {}, {}, {}

    def combine(kind, block):
        masks = hit_masks(routes[block, 0:own], cap)
        rows = y_buf[block].reshape(own * cap, part)
        if kind == 1:
            return dot_ta(one_hot(masks), rows)
        hi, mid, low = three_parts(slot_gates(masks, routes[block, top : top + own]))
        return dot_ta(hi, rows) + (dot_ta(mid, rows) + dot_ta(low, rows))

    numbers, ready = {}, {}
    tok = far_sum.shape[0] // 2
    fold = part // 2
    buffers = [keep_sum.at[0], keep_sum.at[1], keep_sum.at[0], ab_buf, keep_sum.at[1], keep_sum.at[0]]
    earlier_user = {2: 0, 4: 1, 5: 2}
    assert ab_buf.shape == give.shape and len(buffers) == 2 * PARTS
    halves = (pl.ds(0, tok), pl.ds(tok, tok))

    def put_tile(ref, i, value):
        ref[i, 0:tok] = value[:, :fold]
        ref[i, tok : 2 * tok] = value[:, fold:]

    def sum_begin(kind, q):
        n = numbers[kind, q] = len(numbers)
        tiles = buffers[n]
        for k in gifts.get(n - 1, ()):
            if k not in links.finished:
                links.finish(k)
        if n in earlier_user:
            for k in ready[earlier_user[n]]:
                links.finish(k)
            writes.pop(earlier_user[n]).wait()

        def to_other(i, carry):
            for k in range(2):
                put_tile(give, 2 * i + k, combine(kind, lax.rem(mate + 4 - 2 * (2 * i + k) + eps, eps)))
            return carry

        def to_own(i, carry):
            for k in range(2):
                put_tile(tiles, 2 * i + k, combine(kind, lax.rem(ep + 4 - 2 * (2 * i + k) + eps, eps)))
            return carry

        for i in range(2):
            to_other(i, 0)
            if n and not i:
                pl.semaphore_wait(free_sem, 1)
            pair = pl.ds(2 * i, 2)
            gifts.setdefault(n, []).append(links.send(give.at[pair], mate_sum.at[pair], to_mate))
        lax.fori_loop(0, 2, to_own, 0)

    def take_pair(n, i):
        pair = pl.ds(2 * i, 2)
        links.arrive(gifts[n][i], mate_sum.at[pair], to_mate)
        buffers[n][pair] += mate_sum[pair]

    def sum_far(kind, q):
        n = numbers[kind, q]
        tiles = buffers[n]
        take_pair(n, 0)
        stages[n] = [links.send(tiles.at[0, halves[h]], far_land.at[kind, q, halves[h]], to) for h, to in ((0, to_right), (1, to_left))]
        stages[n].append(links.send(tiles.at[1, halves[1]], last_land.at[kind, 0, q, halves[1]], to_right))

    def free_mate():
        pl.semaphore_signal(free_sem, inc=1, device_id=to_mate, device_id_type=MESH)

    def sum_near(kind, q):
        n = numbers[kind, q]
        tiles = buffers[n]
        take_pair(n, 1)
        if n + 1 not in (PARTS, 2 * PARTS):
            free_mate()
        stages[n].append(links.send(tiles.at[3, halves[0]], last_land.at[kind, 1, q, halves[0]], to_left))
        writes[n] = pltpu.make_async_copy(tiles.at[2], sums.at[kind, q], own_sem.at[n])
        writes[n].start()

    def sum_end(kind, q):
        sum_far(kind, q)
        sum_near(kind, q)

    def sum_turn(kind, q):
        n = numbers[kind, q]
        tiles = buffers[n]
        for h, to in ((0, to_right), (1, to_left)):
            links.arrive(stages[n][h], far_land.at[kind, q, halves[h]], to)
        load = pltpu.make_async_copy(far_land.at[kind, q], far_sum, sum_sem.at[2])
        load.start()
        load.wait()
        for i, h, side, to in ((1, 0, 0, to_right), (3, 1, 1, to_left)):
            tiles[i, halves[h]] += far_sum[halves[h]]
            stages[n].append(links.send(tiles.at[i, halves[h]], last_land.at[kind, side, q, halves[h]], to))
        ready[n] = tuple(stages[n])

    def sums_here(kind):
        for q in range(PARTS):
            sent = stages[numbers[kind, q]]
            for k, h, side, to in ((2, 1, 0, to_right), (3, 0, 1, to_left), (4, 0, 0, to_right), (5, 1, 1, to_left)):
                links.arrive(sent[k], last_land.at[kind, side, q, halves[h]], to)

    three = pl.ds(0, PARTS)
    out_loads = [pltpu.make_async_copy(sums.at[0], give.at[three], sum_sem.at[0]),
                 pltpu.make_async_copy(last_land.at[0, 0], mate_sum.at[three], sum_sem.at[1]),
                 pltpu.make_async_copy(last_land.at[0, 1], mate_sum.at[three], sum_sem.at[1])]
    out_store = pltpu.make_async_copy(xb.at[0, 0], out, sum_sem.at[0])

    def out_start():
        sums_here(0)
        for k in gifts[2 * PARTS - 1]:
            links.finish(k)
        out_loads[0].start()
        out_loads[1].start()

    def out_middle():
        out_loads[0].wait()
        out_loads[1].wait()
        give[three] += mate_sum[three]
        out_loads[2].start()

    def out_finish():
        out_loads[2].wait()
        for q in range(PARTS):
            for h in range(2):
                at = q * part + h * fold
                xb[0, 0, :, at : at + fold] = (give[q, halves[h]] + mate_sum[q, halves[h]]).astype(BF16)
        out_store.start()

    y_state = {}
    for way in (True, False):
        for kind in kinds:
            go_up = upward[kind] == way
            y_state[kind, go_up] = links.send(own_refs[kind], all_refs[kind].at[ep, tp], to_up if go_up else to_down, ("first", kind))
    groups = (tp, down, up)
    states = [spread(0, own_refs)]
    hold = [pltpu.make_async_copy(own_refs[kind], all_refs[kind].at[ep, tp], row_sem.at[kind]) for kind in range(3)]
    for copy in hold:
        copy.start()
    for copy in loads:
        copy.wait()
    stow = [pltpu.make_async_copy(w13, w13_all.at[tp], w_sem.at[0])]
    stow += [pltpu.make_async_copy(w2s.at[:, :, pl.ds(q * part, part)], w2_all.at[tp, q], w_sem.at[1 + q]) for q in range(PARTS)]
    for copy in stow:
        copy.start()
    earlier[...] = earlier_rows(earlier.shape[0])
    with jax.named_scope("zeros"):
        acc13[...] = jnp.zeros_like(acc13)
        acc2[...] = jnp.zeros_like(acc2)

    def y_arrive(kind, way):
        block = all_refs[kind].at[ep, down if way else up]
        links.arrive(y_state[kind, way], block, to_up if way else to_down)
        return block

    with jax.named_scope("pass_on_0"):
        pass_on(0)
    with jax.named_scope("y_arrive"):
        for way in (True, False):
            for kind in kinds:
                y_arrive(kind, way)
    with jax.named_scope("send13_0"):
        send13(0)
    with jax.named_scope("send13_1"):
        send13(1)
    with jax.named_scope("send13_2"):
        send13(2)
    states.append(spread(1, [ref.at[ep, down] for ref in all_refs]))
    with jax.named_scope("share_0"):
        share(0)
    with jax.named_scope("last_0"):
        last(0)
    for copy in hold + stow:
        copy.wait()
    with jax.named_scope("from_mate_0"):
        from_mate(0)
    route_copy = pltpu.make_async_copy(r_all.at[:, tp], routes, row_sem.at[0])
    route_copy.start()
    route_copy.wait()

    def tabulate(b, carry):
        pos, gate = expert_rows(routes[b], ep * own, own, earlier[...])
        routes[b, 0:own] = pos
        routes[b, top : top + own] = gate
        return carry

    lax.fori_loop(0, eps, tabulate, 0)
    for kind in kinds:
        links.finish_all(("first", kind), all_refs[kind].at[pl.ds(0, 5), tp], to_mate)
    with jax.named_scope("compute_tp_True"):
        compute(tp, True)
    with jax.named_scope("pass13_0"):
        pass13(0)
    with jax.named_scope("send13_3"):
        send13(3)
    with jax.named_scope("pass_on_1"):
        pass_on(1)
    states.append(spread(2, [ref.at[ep, up] for ref in all_refs]))
    with jax.named_scope("share_1"):
        share(1)
    with jax.named_scope("pass13_1"):
        pass13(1)
    with jax.named_scope("send13_4"):
        send13(4)
    with jax.named_scope("have13_0"):
        have13(0)
    with jax.named_scope("hidden_0"):
        hidden(0)
    with jax.named_scope("pass13_2"):
        pass13(2)
    with jax.named_scope("last_1"):
        last(1)
    with jax.named_scope("from_mate_1"):
        from_mate(1)
    with jax.named_scope("compute_down_False"):
        compute(down, False)
    with jax.named_scope("pass13_3"):
        pass13(3)
    with jax.named_scope("send2_0"):
        send2(0)
    with jax.named_scope("pass_on_2"):
        pass_on(2)
    with jax.named_scope("have13_1"):
        have13(1)
    with jax.named_scope("hidden_1"):
        hidden(1)
    with jax.named_scope("share_2"):
        share(2)
    with jax.named_scope("pass13_4"):
        pass13(4)
    with jax.named_scope("have13_2"):
        have13(2)
    with jax.named_scope("hidden_2"):
        hidden(2)
    with jax.named_scope("last_2"):
        last(2)
    with jax.named_scope("from_mate_2"):
        from_mate(2)
    with jax.named_scope("have13_3"):
        have13(3)
    with jax.named_scope("hidden_3"):
        hidden(3)
    with jax.named_scope("start_loads_up_0"):
        start_loads(up, 0)
    with jax.named_scope("half_group_up_0_False_True"):
        half_group(up, 0, False, True)
    with jax.named_scope("pass2_0"):
        pass2(0)
    with jax.named_scope("send2_1"):
        send2(1)
        send2(2)
    with jax.named_scope("half_group_up_1_False_False"):
        half_group(up, 1, False, False)
    with jax.named_scope("have13_4"):
        have13(4)
    with jax.named_scope("hidden_4"):
        hidden(4)

    with jax.named_scope("have2_0"):
        have2(0)
    load_down(0)
    with jax.named_scope("y_part_0"):
        y_part(0)
    with jax.named_scope("sum_begin_0_0"):
        sum_begin(0, 0)
    with jax.named_scope("sum_end_0_0"):
        sum_end(0, 0)
    with jax.named_scope("pass2_1"):
        pass2(1)
    with jax.named_scope("send2_3"):
        send2(3)
    with jax.named_scope("pass2_2"):
        pass2(2)
    with jax.named_scope("sum_turn_0_0"):
        sum_turn(0, 0)
    load_down(1)
    with jax.named_scope("have2_1"):
        have2(1)
    with jax.named_scope("y_part_1"):
        y_part(1)
    with jax.named_scope("sum_begin_0_1"):
        sum_begin(0, 1)
    with jax.named_scope("pass2_3"):
        pass2(3)
    over_state = send_over()
    with jax.named_scope("sum_end_0_1"):
        sum_end(0, 1)
    load_down(2)
    with jax.named_scope("dh_early"):
        dh_early()
    with jax.named_scope("have2_2"):
        have2(2)
        have2(3)
    with jax.named_scope("y_part_2"):
        y_part(2)
    with jax.named_scope("sum_begin_0_2"):
        sum_begin(0, 2)
    with jax.named_scope("sum_end_0_2"):
        sum_end(0, 2)
    with jax.named_scope("sum_turn_0_1"):
        sum_turn(0, 1)
    v_load(0).start()
    with jax.named_scope("hidden_grads"):
        hidden_grads()
    with jax.named_scope("sum_turn_0_2"):
        sum_turn(0, 2)
    with jax.named_scope("share_over_0"):
        share_over(0)
    with jax.named_scope("v_part_0"):
        v_part(0)
    with jax.named_scope("sum_begin_1_0"):
        sum_begin(1, 0)
    with jax.named_scope("sum_far_1_0"):
        sum_far(1, 0)
    with jax.named_scope("v_part_1"):
        v_part(1)
    with jax.named_scope("sum_near_1_0"):
        sum_near(1, 0)
    with jax.named_scope("sum_begin_1_1"):
        sum_begin(1, 1)
    with jax.named_scope("sum_far_1_1"):
        sum_far(1, 1)
    with jax.named_scope("share_over_1"):
        share_over(1)
    with jax.named_scope("v_part_2"):
        v_part(2)
    with jax.named_scope("sum_near_1_1"):
        sum_near(1, 1)
    with jax.named_scope("sum_begin_1_2"):
        sum_begin(1, 2)
    with jax.named_scope("sum_far_1_2"):
        sum_far(1, 2)
    with jax.named_scope("sum_turn_1_0"):
        sum_turn(1, 0)
    with jax.named_scope("have_over_0"):
        have_over(0)
    with jax.named_scope("have_over_1"):
        have_over(1)
    with jax.named_scope("start_loads_over_0"):
        start_loads(over, 0)
    with jax.named_scope("sum_near_1_2"):
        sum_near(1, 2)
    with jax.named_scope("out_start"):
        out_start()
    with jax.named_scope("half_group_over_0_False_False"):
        half_group(over, 0, False, False)
    with jax.named_scope("sum_turn_1_1"):
        sum_turn(1, 1)
    with jax.named_scope("share_over_2"):
        share_over(2)
    with jax.named_scope("out_middle"):
        out_middle()
    with jax.named_scope("have_over_2"):
        have_over(2)
    with jax.named_scope("start_loads_over_1_0"):
        start_loads(over, 1, (0,))
    with jax.named_scope("sum_turn_1_2"):
        sum_turn(1, 2)
    with jax.named_scope("half_group_over_1_False_False_0_1_False"):
        half_group(over, 1, False, False, (0, 1), False)
    with jax.named_scope("share_over_3"):
        share_over(3)
    with jax.named_scope("have_over_3"):
        have_over(3)
    with jax.named_scope("start_loads_over_1_1"):
        start_loads(over, 1, (1,))
    with jax.named_scope("half_group_over_1_False_False_1_2"):
        half_group(over, 1, False, False, (1, 2))

    def grad_stores(e, slot):
        rows = pl.ds(0, PARTS)
        return [pltpu.make_async_copy(wide_buf.at[slot, rows, :, pl.ds(0, width)], g1.at[e], g_sem.at[slot, 0]),
                pltpu.make_async_copy(wide_buf.at[slot, rows, :, pl.ds(width, width)], g3.at[e], g_sem.at[slot, 1]),
                pltpu.make_async_copy(xs.at[slot, pl.ds(0, width)], g2.at[e], g_sem.at[slot, 2])]

    def finish(e, carry):
        slot = lax.rem(e, 2)

        @pl.when(e >= 2)
        def _():
            for copy in grad_stores(e - 2, slot):
                copy.wait()

        for m in range(PARTS):
            wide_buf[slot, m] = acc13[e, :, m * part : (m + 1) * part].T.astype(BF16)
        xs[slot, pl.ds(0, width), :] = acc2[e].astype(BF16)
        for copy in grad_stores(e, slot):
            copy.start()
        return carry

    with jax.named_scope("finish"):
        lax.fori_loop(0, own, finish, 0)
    with jax.named_scope("out_finish"):
        out_finish()
    with jax.named_scope("sums_here_1"):
        sums_here(1)
    out_store.wait()
    for e in range(max(own - 2, 0), own):
        for copy in grad_stores(e, e % 2):
            copy.wait()
    for n in sorted(writes):
        writes[n].wait()
    for kind in kinds:
        for g, count in ((0, half), (1, 3 + half), (2, 3 + half)):
            links.finish_all(("rows", kind, g), all_refs[kind].at[pl.ds(0, count), tp], to_mate)
        links.finish_all(("over", kind), all_refs[kind].at[pl.ds(0, 2 * half), tp], to_mate)
    links.finish_all("w13", w13_all.at[pl.ds(0, 3)], to_up)
    links.finish_all("w2", w2_all.at[pl.ds(0, 3)], to_up)
    with jax.named_scope("drain"):
        links.drain()


def layer(tokens, d_out, ids, gate_vals, w_one, w_three, w_two, ep_size, tp_size, cap):
    tok, model = tokens.shape
    own, width, _ = w_two.shape
    half = ep_size // 2
    rows = half * cap
    part = model // PARTS
    hbm = pl.BlockSpec(memory_space=pl.ANY)
    shape = jax.ShapeDtypeStruct
    routes = (2 * ids.shape[0], tok)
    sends, receives = copy_counts(own)
    slot_rows = ep_size * tp_size * cap * own
    vector = pltpu.VMEM
    dma = pltpu.SemaphoreType.DMA
    outs = pl.pallas_call(
        functools.partial(layer_kernel, own, cap, width),
        in_specs=[hbm] * 7,
        out_specs=[hbm] * 16,
        out_shape=[
            shape((ep_size, tp_size, tok, model), BF16),
            shape((ep_size, tp_size, tok, model), BF16),
            shape((ep_size, tp_size) + routes, F32),
            shape((tp_size, own, PARTS, part, 2 * width), BF16),
            shape((tp_size, PARTS, own, width, part), BF16),
            shape((own, 2, rows, model), BF16),
            shape((own, 2, rows, model), BF16),
            shape((own, tp_size, 2 * rows, 2 * width), F32),
            shape((own, 2, 2 * rows, 2 * width), F32),
            shape((2, PARTS, 2 * tok, part // 2), F32),
            shape((2, PARTS, 2 * tok, part // 2), F32),
            shape((2, 2, PARTS, 2 * tok, part // 2), F32),
            shape((tok, model), BF16),
            shape((own, PARTS, part, width), BF16),
            shape((own, PARTS, part, width), BF16),
            shape((own, width, model), BF16),
        ],
        scratch_shapes=[
            vector(routes, F32),
            vector(ids.shape, jnp.int32),
            vector((own, PARTS, part, 2 * width), BF16),
            vector((own, width, model), BF16),
            vector((2, half // 2, tok, model), BF16),
            vector((2, half // 2, tok, model), BF16),
            vector((2, half // 2) + routes, F32),
            vector((ep_size,) + routes, F32),
            vector((tok, tok), BF16),
            vector((own, rows, model), BF16),
            vector((own, rows, model), BF16),
            vector((own, 2 * width, model), F32),
            vector((own, width, model), F32),
            vector((tp_size, own, part, 2 * width), BF16),
            vector((PARTS, tp_size, own, width, part), BF16),
            vector((tp_size, 2 * rows, 2 * width), F32),
            vector((own, tp_size, 2 * rows, 2 * width), BF16),
            vector((ep_size, own, cap, part), BF16),
            vector((4, 2 * tok, part // 2), F32),
            vector((2, 4, 2 * tok, part // 2), F32),
            vector((4, 2 * tok, part // 2), F32),
            vector((2 * tok, part // 2), F32),
            dma((sends,)),
            dma((receives,)),
            dma((4,)),
            dma((3, 2)),
            dma((2 * PARTS + 1,)),
            dma((2,)),
            dma((1 + tp_size,)),
            dma((tp_size,)),
            dma((3,)),
            dma((2 * PARTS,)),
            dma((2, 3)),
            dma((4,)),
            pltpu.SemaphoreType.REGULAR,
        ],
        compiler_params=pltpu.CompilerParams(vmem_limit_bytes=VMEM_LIMIT, collective_id=0, has_side_effects=True),
        cost_estimate=pl.CostEstimate(
            flops=2 * slot_rows * model * (2 * tok + 12 * width),
            bytes_accessed=4 * ep_size * tp_size * tok * model,
            transcendentals=0,
        ),
        name="layer",
    )(tokens, d_out, ids, gate_vals, w_one, w_three, w_two)
    g1, g3, g2 = outs[13:]
    return outs[9], outs[11], outs[12], (g1.reshape(own, model, width), g3.reshape(own, model, width), g2)


def result_kernel(sums, last_land, rows_in, g1, g3, g2, out, dx, o1, o3, o2, parts, rows, row_buf, b1, b3, b2, in_sem, out_sem):
    moves = ((g1, b1, o1), (g3, b3, o3), (g2, b2, o2), (rows_in, row_buf, out))
    takes = [pltpu.make_async_copy(src, buf, in_sem.at[k]) for k, (src, buf, _) in enumerate(moves)]
    terms = [pltpu.make_async_copy(src, parts.at[k], in_sem.at[4 + k])
             for k, src in enumerate((sums.at[1], last_land.at[1, 0], last_land.at[1, 1]))]
    for copy in terms + takes:
        copy.start()
    for copy in terms:
        copy.wait()
    tok, fold = rows.shape[0], parts.shape[3]
    for q in range(parts.shape[1]):
        for h in range(2):
            at, half = (2 * q + h) * fold, pl.ds(h * tok, tok)
            rows[:, at : at + fold] = (parts[0, q, half] + (parts[1, q, half] + parts[2, q, half])).astype(BF16)
    puts = [pltpu.make_async_copy(rows, dx, out_sem.at[4])]
    puts[0].start()
    for k, (take, (_, buf, to)) in enumerate(zip(takes, moves)):
        take.wait()
        puts.append(pltpu.make_async_copy(buf, to, out_sem.at[k]))
        puts[-1].start()
    for copy in puts:
        copy.wait()


def results(sums, last_land, out, grads):
    _, count, tall, fold = sums.shape
    tok, model = out.shape
    hbm = pl.BlockSpec(memory_space=pl.ANY)
    row = jax.ShapeDtypeStruct((tok, model), BF16)
    rows = pltpu.VMEM((tok, model), BF16)
    return pl.pallas_call(
        result_kernel,
        in_specs=[hbm] * 6,
        out_specs=[hbm] * 5,
        out_shape=[row, row] + [jax.ShapeDtypeStruct(g.shape, g.dtype) for g in grads],
        scratch_shapes=[pltpu.VMEM((3, count, tall, fold), F32), rows, rows]
        + [pltpu.VMEM(g.shape, g.dtype) for g in grads]
        + [pltpu.SemaphoreType.DMA((7,)), pltpu.SemaphoreType.DMA((5,))],
        compiler_params=pltpu.CompilerParams(vmem_limit_bytes=VMEM_LIMIT),
        name="results",
    )(sums, last_land, out, *grads)


def solution(mesh):
    ep_size, tp_size = mesh.shape["ep"], mesh.shape["tp"]
    row_spec = P(("dp", "ep", "tp"), None)
    col_spec = P("ep", None, "tp")
    down_spec = P("ep", "tp", None)
    grad_col = P(("dp", "ep"), None, "tp")
    grad_down = P(("dp", "ep"), "tp", None)

    def local_step(tokens, expert_ids, gate_vals, w_one, w_three, w_two, d_out):
        cap = slot_count(expert_ids.shape[1], tokens.shape[0], w_one.shape[0] * ep_size)
        sums, last_land, out, grads = layer(tokens, d_out, expert_ids.T, gate_vals.T, w_one, w_three, w_two, ep_size, tp_size, cap)
        return tuple(results(sums, last_land, out, grads))

    return jax.shard_map(local_step, mesh=mesh,
                         in_specs=(row_spec, row_spec, row_spec, col_spec, col_spec, down_spec, row_spec),
                         out_specs=(row_spec, row_spec, grad_col, grad_col, grad_down), check_vma=False)
```

```python
import functools

import jax
import jax.numpy as jnp
from jax import lax
from jax.experimental import pallas as pl
from jax.experimental.pallas import tpu as pltpu
from jax.sharding import PartitionSpec as P

BF16 = jnp.bfloat16
F32 = jnp.float32
MESH = pl.DeviceIdType.MESH
VMEM_LIMIT = 67_043_328
PARTS = 3


def slot_count(num_top, tok_dev, experts):
    return 8 * ((5 * num_top * tok_dev + 32 * experts - 1) // (32 * experts))


def dot(a, b):
    return jnp.dot(a, b, preferred_element_type=F32)


def dot_tb(a, b):
    return lax.dot_general(a, b, (((1,), (1,)), ((), ())), preferred_element_type=F32)


def dot_ta(a, b):
    return lax.dot_general(a, b, (((0,), (0,)), ((), ())), preferred_element_type=F32)


def earlier_rows(tok):
    row = lax.broadcasted_iota(jnp.int32, (tok, tok), 0)
    col = lax.broadcasted_iota(jnp.int32, (tok, tok), 1)
    return jnp.where(row < col, 1.0, 0.0).astype(BF16)


def expert_rows(routes, first, own, earlier):
    top = routes.shape[0] // 2
    ids, gates = routes[:top], routes[top:]
    hits = [ids == (first + e).astype(F32) for e in range(own)]
    routed = jnp.concatenate([jnp.sum(jnp.where(m, 1.0, 0.0), axis=0, keepdims=True) for m in hits], axis=0)
    gate = jnp.concatenate([jnp.sum(jnp.where(m, gates, 0.0), axis=0, keepdims=True) for m in hits], axis=0)
    return jnp.where(routed > 0.0, dot(routed.astype(BF16), earlier), -1.0), gate


def hit_masks(pos, cap):
    slot = lax.broadcasted_iota(jnp.int32, (cap, pos.shape[1]), 0).astype(F32)
    return [pos[e : e + 1, :] == slot for e in range(pos.shape[0])]


def one_hot(masks):
    return jnp.concatenate([jnp.where(m, 1.0, 0.0) for m in masks], axis=0).astype(BF16)


def slot_gates(masks, gate):
    return jnp.concatenate([jnp.where(m, gate[e : e + 1, :], 0.0) for e, m in enumerate(masks)], axis=0)


def three_parts(x):
    hi = x.astype(BF16)
    rest = x - hi.astype(F32)
    mid = rest.astype(BF16)
    return hi, mid, (rest - mid.astype(F32)).astype(BF16)


class Links:
    def __init__(self, send_sem, recv_sem):
        self.send_sem, self.recv_sem, self.sent, self.finished = send_sem, recv_sem, [], set()
        self.send_of, self.recv_of = {}, {}

    def copy(self, s, r, src, dst, to):
        return pltpu.make_async_remote_copy(src_ref=src, dst_ref=dst, send_sem=self.send_sem.at[s],
                                            recv_sem=self.recv_sem.at[r], device_id=to, device_id_type=MESH)

    def send(self, src, dst, to, together=None, landing=None):
        k = len(self.sent)
        s = self.send_of.setdefault(k if together is None else together, len(self.send_of))
        r = self.recv_of.setdefault(k if landing is None else landing, len(self.recv_of))
        copy = self.copy(s, r, src, dst, to)
        copy.start()
        self.sent.append((s, r, copy))
        if together is not None:
            self.finished.add(k)
        return k

    def arrive(self, k, dst, to):
        s, r, _ = self.sent[k]
        self.copy(s, r, dst, dst, to).wait_recv()

    def arrive_all(self, landing, ref, to):
        self.copy(0, self.recv_of[landing], ref, ref, to).wait_recv()

    def finish(self, k):
        self.finished.add(k)
        self.sent[k][2].wait_send()

    def finish_all(self, together, ref, to):
        self.copy(self.send_of[together], 0, ref, ref, to).wait_send()

    def drain(self):
        for k in range(len(self.sent)):
            if k not in self.finished:
                self.finish(k)


def copy_counts(own):
    sums = 2 * PARTS * 8
    return 3 * 5 + 2 + sums, 6 + 3 * 3 * 4 + 24 + 4 * own + 4 * (PARTS + 1) + sums


def layer_kernel(own, cap, width, tokens, d_out, ids, gate_vals, w1, w3, w2, x_all, dy_all, r_all, w13_all, w2_all, xs_all,
                 us_all, ab_all, sums, far_land, last_land, out, g1, g3, g2, r_own, i_own, w13, w2s, xb,
                 dyb, rb, routes, earlier, xs, us, acc13, acc2, wide_buf, w2v, ab_buf, d_all, y_buf, give, keep_sum, mate_sum,
                 far_sum, send_sem, recv_sem, row_sem, load_sem, w_sem, slot_sem, in_sem, ab_sem, sum_sem, own_sem, g_sem, free_sem):
    ep, tp = lax.axis_index("ep"), lax.axis_index("tp")
    eps, tps = x_all.shape[0], x_all.shape[1]
    model = x_all.shape[3]
    part = model // PARTS
    half = eps // 2
    x_own, dy_own = xs.at[0], xs.at[1]
    step = lambda n: lax.rem(ep + (n + eps), eps)
    turn = lambda n: lax.rem(tp + (n + tps), tps)
    right, left, far = step(2), step(-2), step(4)
    mate = ep + 1 - 2 * lax.rem(ep, 2)
    mate_step = lambda n: lax.rem(mate + (n + eps), eps)
    up, down, over = turn(1), turn(-1), turn(2)
    to_right, to_left, to_mate = {"ep": right}, {"ep": left}, {"ep": mate}
    to_up, to_down = {"tp": up}, {"tp": down}
    links = Links(send_sem, recv_sem)

    barrier = pltpu.get_barrier_semaphore()
    for to in (to_right, to_left, to_mate, to_up, to_down):
        pl.semaphore_signal(barrier, inc=1, device_id=to, device_id_type=MESH)
    top = ids.shape[0]
    firsts = [pltpu.make_async_copy(ids, i_own, row_sem.at[0]), pltpu.make_async_copy(gate_vals, r_own.at[pl.ds(top, top)], row_sem.at[1]),
              pltpu.make_async_copy(tokens, x_own, row_sem.at[2]), pltpu.make_async_copy(d_out, dy_own, row_sem.at[3])]
    loads = [pltpu.make_async_copy(src.at[:, pl.ds(m * part, part)], w13.at[:, m, :, pl.ds(k * width, width)], w_sem.at[PARTS * k + m])
             for k, src in ((0, w1), (1, w3)) for m in range(PARTS)]
    loads.append(pltpu.make_async_copy(w2, w2s, w_sem.at[2 * PARTS]))
    for copy in firsts + loads:
        copy.start()
    firsts[0].wait()
    r_own[0:top] = i_own[...].astype(F32)
    for copy in firsts[1:]:
        copy.wait()
    with jax.named_scope("barrier"):
        pl.semaphore_wait(barrier, 5)

    own_refs, all_refs = (x_own, dy_own, r_own), (x_all, dy_all, r_all)
    upward = (True, False, True)
    kinds = (0, 1, 2)

    def spread(g, srcs):
        out, t = {}, groups[g]
        set_of = lambda kind: ("rows", kind, g) if g else ("first", kind)
        for kind in kinds:
            to = to_right if upward[kind] else to_left
            out[kind, upward[kind]] = links.send(srcs[kind], all_refs[kind].at[ep, t], to, set_of(kind))
        for kind in kinds:
            to = to_left if upward[kind] else to_right
            out[kind, not upward[kind]] = links.send(srcs[kind], all_refs[kind].at[ep, t], to, set_of(kind))
        for kind in kinds:
            links.send(srcs[kind], all_refs[kind].at[ep, t], to_mate, set_of(kind), ("mate", kind, g))
        return out

    def pass_on(g):
        state, t = states[g], groups[g]
        for kind in kinds:
            got, to = (left, to_right) if upward[kind] else (right, to_left)
            block = all_refs[kind].at[got, t]
            links.arrive(state[kind, upward[kind]], block, to)
            state[kind, "far"] = links.send(block, block, to, ("rows", kind, g))
            links.send(block, block, to_mate, ("rows", kind, g), ("mate", kind, g))

    def share(g):
        state, t = states[g], groups[g]
        for kind in kinds:
            got, to = (right, to_left) if upward[kind] else (left, to_right)
            block = all_refs[kind].at[got, t]
            links.arrive(state[kind, not upward[kind]], block, to)
            links.send(block, block, to_mate, ("rows", kind, g), ("mate", kind, g))

    def last(g):
        state, t = states[g], groups[g]
        for kind in kinds:
            block = all_refs[kind].at[far, t]
            links.arrive(state[kind, "far"], block, to_right if upward[kind] else to_left)
            links.send(block, block, to_mate, ("rows", kind, g), ("mate", kind, g))

    def from_mate(g):
        for kind in kinds:
            links.arrive_all(("mate", kind, g), all_refs[kind].at[pl.ds(0, half), groups[g]], to_mate)

    core = lax.rem(ep, 2)

    def send_over():
        return [{kind: links.send(all_refs[kind].at[core + 2 * m, down if upward[kind] else up],
                                  all_refs[kind].at[core + 2 * m, down if upward[kind] else up],
                                  to_up if upward[kind] else to_down, ("over", kind)) for kind in kinds} for m in range(half)]

    def share_over(m):
        for kind in kinds:
            block = all_refs[kind].at[core + 2 * m, over]
            links.arrive(over_state[m][kind], block, to_up if upward[kind] else to_down)
            over_state[m][kind, "mate"] = links.send(block, block, to_mate, ("over", kind))

    def have_over(m):
        for kind in kinds:
            links.arrive(over_state[m][kind, "mate"], all_refs[kind].at[1 - core + 2 * m, over], to_mate)

    def both_ways(src, dst, which):
        return {True: links.send(src, dst, to_up, which), False: links.send(src, dst, to_down, which)}

    def pass_halves(state, below, above, split, which):
        links.arrive(state[True], below, to_up)
        state["first"] = links.send(split(below, 0), split(below, 0), to_up, which)
        links.arrive(state[False], above, to_down)
        state["second"] = links.send(split(above, 1), split(above, 1), to_down, which)

    def have_halves(state, block, split):
        links.arrive(state["first"], split(block, 0), to_up)
        links.arrive(state["second"], split(block, 1), to_down)

    w13_state, w2_state = [None] * own, [None] * (PARTS + 1)
    split13 = lambda ref, k: ref.at[:, pl.ds(k * (part // 2), part // 2)]
    split2 = lambda ref, k: ref.at[:, pl.ds(k * (width // 2), width // 2)]

    def send13(e):
        w13_state[e] = both_ways(w13.at[e], w13_all.at[tp, e], "w13")

    def pass13(e):
        pass_halves(w13_state[e], w13_all.at[down, e], w13_all.at[up, e], split13, "w13")

    def have13(e):
        have_halves(w13_state[e], w13_all.at[over, e], split13)

    pieces = [(q, pl.ds(0, own)) for q in range(PARTS - 1)] + [(PARTS - 1, pl.ds(0, 2)), (PARTS - 1, pl.ds(2, own - 2))]

    def piece(j, p):
        q, experts = pieces[p]
        return w2_all.at[j, q, experts]

    def send2(p):
        q, experts = pieces[p]
        w2_state[p] = both_ways(w2s.at[experts, :, pl.ds(q * part, part)], piece(tp, p), "w2")

    def pass2(p):
        pass_halves(w2_state[p], piece(down, p), piece(up, p), split2, "w2")

    def have2(p):
        have_halves(w2_state[p], piece(over, p), split2)

    def pair_loads(t, h, p):
        at = pl.ds(h * half + p * (half // 2), half // 2)
        return [pltpu.make_async_copy(src.at[at, t], dst.at[p], load_sem.at[k, p])
                for k, (src, dst) in enumerate(((x_all, xb), (dy_all, dyb), (r_all, rb)))]

    def half_group(t, h, keep, ahead, pairs=(0, 2), grads=True):
        def gather(p, b):
            pos, gate = expert_rows(rb[p, b], ep * own, own, earlier[...])
            masks = hit_masks(pos, cap)
            pick = one_hot(masks)
            gates = jnp.sum(slot_gates(masks, gate), axis=1, keepdims=True)
            rows = pl.ds(pl.multiple_of((p * (half // 2) + b) * cap, cap), cap)
            picked = dot(pick, xb[p, b]).astype(BF16)
            for e in range(own):
                xs[e, rows, :] = picked[e * cap : (e + 1) * cap]
            scaled = (gates * dot(pick, dyb[p, b])).astype(BF16)
            for e in range(own):
                us[e, rows, :] = scaled[e * cap : (e + 1) * cap]

        def pair(p, carry):
            for copy in pair_loads(t, h, p):
                copy.wait()
            for b in range(half // 2):
                gather(p, b)

            @pl.when(ahead)
            def _():
                for copy in pair_loads(t, 1, p):
                    copy.start()

            return carry

        lax.fori_loop(pairs[0], pairs[1], pair, 0)
        if not grads:
            return

        stores = []
        if keep:
            stores = [pltpu.make_async_copy(xs, xs_all.at[:, h], slot_sem.at[0]),
                      pltpu.make_async_copy(us, us_all.at[:, h], slot_sem.at[1])]
        for copy in stores:
            copy.start()

        def expert(e, carry):
            ab = dot(xs[e], w13[e].reshape(model, 2 * width))
            a, b = ab[:, :width], ab[:, width:]
            dh = dot_tb(us[e], w2s[e])
            sig = jax.nn.sigmoid(a)
            silu = a * sig
            hid = (silu * b).astype(BF16)
            da = (dh * b * sig * (1.0 + a * (1.0 - sig))).astype(BF16)
            db = (dh * silu).astype(BF16)
            acc13[e] += dot_ta(jnp.concatenate([da, db], axis=1), xs[e])
            acc2[e] += dot_ta(hid, us[e])
            return carry

        lax.fori_loop(0, own, expert, 0)
        for copy in stores:
            copy.wait()

    def start_loads(t, h, pairs=(0, 1)):
        for p in pairs:
            for copy in pair_loads(t, h, p):
                copy.start()

    def compute(t, keep):
        start_loads(t, 0)

        def one_half(h, carry):
            half_group(t, h, keep, h == 0)
            return carry

        lax.fori_loop(0, 2, one_half, 0)

    slots = eps * cap
    pending = []

    def settle():
        while pending:
            pending.pop().wait()

    def hidden(e):
        rows = pltpu.make_async_copy(xs_all.at[e], xs.at[pl.ds(0, 2)], in_sem.at[tps])
        rows.start()
        for j in range(tps):
            pltpu.make_async_copy(w13_all.at[j, e], wide_buf.at[pl.ds(0, PARTS), j], in_sem.at[j]).start()
        settle()
        rows.wait()

        def shard(j, carry):
            pltpu.make_async_copy(w13_all.at[j, e], wide_buf.at[pl.ds(0, PARTS), j], in_sem.at[j]).wait()
            ab = dot(xs[0:2].reshape(slots, model), wide_buf[0:PARTS, j].reshape(model, 2 * width))
            ab_buf[j] = ab
            a, b = ab[:, :width], ab[:, width:]
            at = pl.ds(pl.multiple_of(lax.rem(j, 2) * width, width), width)
            d_all[e, j // 2, :, at] = (a * jax.nn.sigmoid(a) * b).astype(BF16)
            return carry

        lax.fori_loop(0, tps, shard, 0)
        pending.append(pltpu.make_async_copy(ab_buf, ab_all.at[e], ab_sem.at[0]))
        pending[-1].start()

    def put_rows(e, value):
        for k in range(eps):
            y_buf[k, e] = value[k * cap : (k + 1) * cap]

    def down_load(q, j):
        return pltpu.make_async_copy(w2_all.at[j, q], w2v.at[q, j], in_sem.at[j])

    def load_down(q):
        for j in (tp, up, down):
            down_load(q, j).start()

    def y_part(q):
        down_load(q, over).start()
        for j in range(tps):
            down_load(q, j).wait()

        def one(e, carry):
            y = dot(d_all[e, 0], w2v[q, 0:2, e].reshape(2 * width, part)) + dot(d_all[e, 1], w2v[q, 2:4, e].reshape(2 * width, part))
            put_rows(e, y.astype(BF16))
            return carry

        lax.fori_loop(0, own, one, 0)

    def ab_load(e, j):
        return pltpu.make_async_copy(ab_all.at[e, j], ab_buf.at[j], ab_sem.at[j])

    def u_load(e, slot):
        return pltpu.make_async_copy(us_all.at[e], us.at[pl.ds(2 * slot, 2)], slot_sem.at[slot])

    def hidden_grads():
        settle()
        u_load(0, 0).start()
        for j in range(tps):
            ab_load(0, j).start()

        def one(e, carry):
            slot = lax.rem(e, 2)
            u_load(e, slot).wait()

            @pl.when(e + 1 < own)
            def _():
                u_load(e + 1, 1 - slot).start()

            def two(k, carry):
                dh = None
                for q in range(PARTS):
                    at = pl.ds(q * part, part)
                    u = us[pl.ds(2 * slot, 2), :, at].reshape(slots, part)
                    term = dot_tb(u, w2v[q, pl.ds(2 * k, 2), e].reshape(2 * width, part))
                    dh = term if dh is None else dh + term
                for i in range(2):
                    j = 2 * k + i
                    ab_load(e, j).wait()
                    a, b, d = ab_buf[j, :, :width], ab_buf[j, :, width:], dh[:, i * width : (i + 1) * width]
                    sig = jax.nn.sigmoid(a)
                    d_all[e, j, :, :width] = (d * b * sig * (1.0 + a * (1.0 - sig))).astype(BF16)
                    d_all[e, j, :, width:] = (d * (a * sig)).astype(BF16)

                    @pl.when(e + 1 < own)
                    def _():
                        ab_load(e + 1, j).start()
                return carry

            lax.fori_loop(0, tps // 2, two, 0)
            return carry

        lax.fori_loop(0, own, one, 0)

    def v_load(q):
        return pltpu.make_async_copy(w13_all.at[:, :, q], wide_buf, in_sem.at[0])

    def v_part(q):
        v_load(q).wait()

        def one(e, carry):
            v = dot_tb(d_all[e, 0], wide_buf[0, e])
            for j in range(1, tps):
                v = v + dot_tb(d_all[e, j], wide_buf[j, e])
            put_rows(e, v.astype(BF16))
            return carry

        lax.fori_loop(0, own, one, 0)
        if q + 1 < PARTS:
            v_load(q + 1).start()

    gifts, writes, stages = {}, {}, {}

    def combine(kind, block):
        masks = hit_masks(routes[block, 0:own], cap)
        rows = y_buf[block].reshape(own * cap, part)
        if kind == 1:
            return dot_ta(one_hot(masks), rows)
        hi, mid, low = three_parts(slot_gates(masks, routes[block, top : top + own]))
        return dot_ta(hi, rows) + (dot_ta(mid, rows) + dot_ta(low, rows))

    numbers, ready = {}, {}
    tok = far_sum.shape[0] // 2
    fold = part // 2
    buffers = [keep_sum.at[0], keep_sum.at[1], keep_sum.at[0], ab_buf, keep_sum.at[1], keep_sum.at[0]]
    earlier_user = {2: 0, 4: 1, 5: 2}
    assert ab_buf.shape == give.shape and len(buffers) == 2 * PARTS
    halves = (pl.ds(0, tok), pl.ds(tok, tok))

    def put_tile(ref, i, value):
        ref[i, 0:tok] = value[:, :fold]
        ref[i, tok : 2 * tok] = value[:, fold:]

    def sum_begin(kind, q):
        n = numbers[kind, q] = len(numbers)
        tiles = buffers[n]
        for k in gifts.get(n - 1, ()):
            links.finish(k)
        if n in earlier_user:
            for k in ready[earlier_user[n]]:
                links.finish(k)
            writes.pop(earlier_user[n]).wait()

        def to_other(i, carry):
            for k in range(2):
                put_tile(give, 2 * i + k, combine(kind, lax.rem(mate + 4 - 2 * (2 * i + k) + eps, eps)))
            return carry

        def to_own(i, carry):
            put_tile(tiles, i, combine(kind, lax.rem(ep + 4 - 2 * i + eps, eps)))
            return carry

        for i in range(2):
            to_other(i, 0)
            if n and not i:
                pl.semaphore_wait(free_sem, 1)
            pair = pl.ds(2 * i, 2)
            gifts.setdefault(n, []).append(links.send(give.at[pair], mate_sum.at[pair], to_mate))
        lax.fori_loop(0, 2, to_own, 0)
        second[n] = to_own

    second = {}

    def take_pair(n, i):
        pair = pl.ds(2 * i, 2)
        links.arrive(gifts[n][i], mate_sum.at[pair], to_mate)
        buffers[n][pair] += mate_sum[pair]

    def sum_far(kind, q):
        n = numbers[kind, q]
        tiles = buffers[n]
        take_pair(n, 0)
        stages[n] = [links.send(tiles.at[0, halves[h]], far_land.at[kind, q, halves[h]], to) for h, to in ((0, to_right), (1, to_left))]
        stages[n].append(links.send(tiles.at[1, halves[1]], last_land.at[kind, 0, q, halves[1]], to_right))
        lax.fori_loop(2, 4, second[n], 0)

    def free_mate():
        pl.semaphore_signal(free_sem, inc=1, device_id=to_mate, device_id_type=MESH)

    def sum_near(kind, q):
        n = numbers[kind, q]
        tiles = buffers[n]
        take_pair(n, 1)
        if n + 1 < 2 * PARTS:
            free_mate()
        stages[n].append(links.send(tiles.at[3, halves[0]], last_land.at[kind, 1, q, halves[0]], to_left))
        writes[n] = pltpu.make_async_copy(tiles.at[2], sums.at[kind, q], own_sem.at[n])
        writes[n].start()

    def sum_end(kind, q):
        sum_far(kind, q)
        sum_near(kind, q)

    def sum_turn(kind, q):
        n = numbers[kind, q]
        tiles = buffers[n]
        for h, to in ((0, to_right), (1, to_left)):
            links.arrive(stages[n][h], far_land.at[kind, q, halves[h]], to)
        load = pltpu.make_async_copy(far_land.at[kind, q], far_sum, sum_sem.at[2])
        load.start()
        load.wait()
        for i, h, side, to in ((1, 0, 0, to_right), (3, 1, 1, to_left)):
            tiles[i, halves[h]] += far_sum[halves[h]]
            stages[n].append(links.send(tiles.at[i, halves[h]], last_land.at[kind, side, q, halves[h]], to))
        ready[n] = tuple(stages[n])

    def sums_here(kind):
        for q in range(PARTS):
            sent = stages[numbers[kind, q]]
            for k, h, side, to in ((2, 1, 0, to_right), (3, 0, 1, to_left), (4, 0, 0, to_right), (5, 1, 1, to_left)):
                links.arrive(sent[k], last_land.at[kind, side, q, halves[h]], to)

    three = pl.ds(0, PARTS)
    out_loads = [pltpu.make_async_copy(sums.at[0], give.at[three], sum_sem.at[0]),
                 pltpu.make_async_copy(last_land.at[0, 0], mate_sum.at[three], sum_sem.at[1]),
                 pltpu.make_async_copy(last_land.at[0, 1], mate_sum.at[three], sum_sem.at[1])]
    out_store = pltpu.make_async_copy(xb.at[0, 0], out, sum_sem.at[0])

    def out_start():
        sums_here(0)
        for k in gifts[2 * PARTS - 1]:
            links.finish(k)
        out_loads[0].start()
        out_loads[1].start()

    def out_middle():
        out_loads[0].wait()
        out_loads[1].wait()
        give[three] += mate_sum[three]
        out_loads[2].start()

    def out_finish():
        out_loads[2].wait()
        for q in range(PARTS):
            for h in range(2):
                at = q * part + h * fold
                xb[0, 0, :, at : at + fold] = (give[q, halves[h]] + mate_sum[q, halves[h]]).astype(BF16)
        out_store.start()

    y_state = {}
    for way in (True, False):
        for kind in kinds:
            go_up = upward[kind] == way
            y_state[kind, go_up] = links.send(own_refs[kind], all_refs[kind].at[ep, tp], to_up if go_up else to_down, ("first", kind))
    groups = (tp, down, up)
    states = [spread(0, own_refs)]
    hold = [pltpu.make_async_copy(own_refs[kind], all_refs[kind].at[ep, tp], row_sem.at[kind]) for kind in range(3)]
    for copy in hold:
        copy.start()
    for copy in loads:
        copy.wait()
    stow = [pltpu.make_async_copy(w13, w13_all.at[tp], w_sem.at[0])]
    stow += [pltpu.make_async_copy(w2s.at[:, :, pl.ds(q * part, part)], w2_all.at[tp, q], w_sem.at[1 + q]) for q in range(PARTS)]
    for copy in stow:
        copy.start()
    earlier[...] = earlier_rows(earlier.shape[0])
    with jax.named_scope("zeros"):
        acc13[...] = jnp.zeros_like(acc13)
        acc2[...] = jnp.zeros_like(acc2)

    def y_arrive(kind, way):
        block = all_refs[kind].at[ep, down if way else up]
        links.arrive(y_state[kind, way], block, to_up if way else to_down)
        return block

    with jax.named_scope("pass_on_0"):
        pass_on(0)
    with jax.named_scope("y_arrive"):
        for way in (True, False):
            for kind in kinds:
                y_arrive(kind, way)
    with jax.named_scope("send13_0"):
        send13(0)
    with jax.named_scope("send13_1"):
        send13(1)
    with jax.named_scope("send13_2"):
        send13(2)
    states.append(spread(1, [ref.at[ep, down] for ref in all_refs]))
    with jax.named_scope("share_0"):
        share(0)
    with jax.named_scope("last_0"):
        last(0)
    for copy in hold + stow:
        copy.wait()
    with jax.named_scope("from_mate_0"):
        from_mate(0)
    route_copy = pltpu.make_async_copy(r_all.at[:, tp], routes, row_sem.at[0])
    route_copy.start()
    route_copy.wait()

    def tabulate(b, carry):
        pos, gate = expert_rows(routes[b], ep * own, own, earlier[...])
        routes[b, 0:own] = pos
        routes[b, top : top + own] = gate
        return carry

    lax.fori_loop(0, eps, tabulate, 0)
    for kind in kinds:
        links.finish_all(("first", kind), all_refs[kind].at[pl.ds(0, 5), tp], to_mate)
    with jax.named_scope("compute_tp_True"):
        compute(tp, True)
    with jax.named_scope("pass13_0"):
        pass13(0)
    with jax.named_scope("send13_3"):
        send13(3)
    with jax.named_scope("pass_on_1"):
        pass_on(1)
    states.append(spread(2, [ref.at[ep, up] for ref in all_refs]))
    with jax.named_scope("share_1"):
        share(1)
    with jax.named_scope("pass13_1"):
        pass13(1)
    with jax.named_scope("send13_4"):
        send13(4)
    with jax.named_scope("have13_0"):
        have13(0)
    with jax.named_scope("hidden_0"):
        hidden(0)
    with jax.named_scope("pass13_2"):
        pass13(2)
    with jax.named_scope("last_1"):
        last(1)
    with jax.named_scope("from_mate_1"):
        from_mate(1)
    with jax.named_scope("compute_down_False"):
        compute(down, False)
    with jax.named_scope("pass13_3"):
        pass13(3)
    with jax.named_scope("send2_0"):
        send2(0)
    with jax.named_scope("pass_on_2"):
        pass_on(2)
    with jax.named_scope("have13_1"):
        have13(1)
    with jax.named_scope("hidden_1"):
        hidden(1)
    with jax.named_scope("share_2"):
        share(2)
    with jax.named_scope("pass13_4"):
        pass13(4)
    with jax.named_scope("have13_2"):
        have13(2)
    with jax.named_scope("hidden_2"):
        hidden(2)
    with jax.named_scope("last_2"):
        last(2)
    with jax.named_scope("from_mate_2"):
        from_mate(2)
    with jax.named_scope("have13_3"):
        have13(3)
    with jax.named_scope("hidden_3"):
        hidden(3)
    with jax.named_scope("start_loads_up_0"):
        start_loads(up, 0)
    with jax.named_scope("half_group_up_0_False_True"):
        half_group(up, 0, False, True)
    with jax.named_scope("pass2_0"):
        pass2(0)
    with jax.named_scope("send2_1"):
        send2(1)
        send2(2)
    with jax.named_scope("half_group_up_1_False_False"):
        half_group(up, 1, False, False)
    with jax.named_scope("have13_4"):
        have13(4)
    with jax.named_scope("hidden_4"):
        hidden(4)

    with jax.named_scope("have2_0"):
        have2(0)
    load_down(0)
    with jax.named_scope("y_part_0"):
        y_part(0)
    with jax.named_scope("sum_begin_0_0"):
        sum_begin(0, 0)
    with jax.named_scope("sum_end_0_0"):
        sum_end(0, 0)
    with jax.named_scope("pass2_1"):
        pass2(1)
    with jax.named_scope("send2_3"):
        send2(3)
    with jax.named_scope("pass2_2"):
        pass2(2)
    with jax.named_scope("sum_turn_0_0"):
        sum_turn(0, 0)
    load_down(1)
    with jax.named_scope("have2_1"):
        have2(1)
    with jax.named_scope("y_part_1"):
        y_part(1)
    with jax.named_scope("sum_begin_0_1"):
        sum_begin(0, 1)
    with jax.named_scope("pass2_3"):
        pass2(3)
    over_state = send_over()
    with jax.named_scope("sum_end_0_1"):
        sum_end(0, 1)
    load_down(2)
    with jax.named_scope("sum_turn_0_1"):
        sum_turn(0, 1)
    with jax.named_scope("have2_2"):
        have2(2)
        have2(3)
    with jax.named_scope("y_part_2"):
        y_part(2)
    with jax.named_scope("sum_begin_0_2"):
        sum_begin(0, 2)
    with jax.named_scope("sum_end_0_2"):
        sum_end(0, 2)
    v_load(0).start()
    with jax.named_scope("hidden_grads"):
        hidden_grads()
    with jax.named_scope("sum_turn_0_2"):
        sum_turn(0, 2)
    with jax.named_scope("share_over_0"):
        share_over(0)
    with jax.named_scope("v_part_0"):
        v_part(0)
    with jax.named_scope("sum_begin_1_0"):
        sum_begin(1, 0)
    with jax.named_scope("sum_far_1_0"):
        sum_far(1, 0)
    with jax.named_scope("v_part_1"):
        v_part(1)
    with jax.named_scope("sum_near_1_0"):
        sum_near(1, 0)
    with jax.named_scope("sum_begin_1_1"):
        sum_begin(1, 1)
    with jax.named_scope("sum_far_1_1"):
        sum_far(1, 1)
    with jax.named_scope("share_over_1"):
        share_over(1)
    with jax.named_scope("v_part_2"):
        v_part(2)
    with jax.named_scope("sum_near_1_1"):
        sum_near(1, 1)
    with jax.named_scope("sum_begin_1_2"):
        sum_begin(1, 2)
    with jax.named_scope("sum_far_1_2"):
        sum_far(1, 2)
    with jax.named_scope("sum_turn_1_0"):
        sum_turn(1, 0)
    with jax.named_scope("have_over_0"):
        have_over(0)
    with jax.named_scope("have_over_1"):
        have_over(1)
    with jax.named_scope("start_loads_over_0"):
        start_loads(over, 0)
    with jax.named_scope("sum_near_1_2"):
        sum_near(1, 2)
    with jax.named_scope("out_start"):
        out_start()
    with jax.named_scope("half_group_over_0_False_False"):
        half_group(over, 0, False, False)
    with jax.named_scope("sum_turn_1_1"):
        sum_turn(1, 1)
    with jax.named_scope("share_over_2"):
        share_over(2)
    with jax.named_scope("out_middle"):
        out_middle()
    with jax.named_scope("have_over_2"):
        have_over(2)
    with jax.named_scope("start_loads_over_1_0"):
        start_loads(over, 1, (0,))
    with jax.named_scope("sum_turn_1_2"):
        sum_turn(1, 2)
    with jax.named_scope("half_group_over_1_False_False_0_1_False"):
        half_group(over, 1, False, False, (0, 1), False)
    with jax.named_scope("share_over_3"):
        share_over(3)
    with jax.named_scope("have_over_3"):
        have_over(3)
    with jax.named_scope("start_loads_over_1_1"):
        start_loads(over, 1, (1,))
    with jax.named_scope("half_group_over_1_False_False_1_2"):
        half_group(over, 1, False, False, (1, 2))

    def grad_stores(e, slot):
        rows = pl.ds(0, PARTS)
        return [pltpu.make_async_copy(wide_buf.at[slot, rows, :, pl.ds(0, width)], g1.at[e], g_sem.at[slot, 0]),
                pltpu.make_async_copy(wide_buf.at[slot, rows, :, pl.ds(width, width)], g3.at[e], g_sem.at[slot, 1]),
                pltpu.make_async_copy(xs.at[slot, pl.ds(0, width)], g2.at[e], g_sem.at[slot, 2])]

    def finish(e, carry):
        slot = lax.rem(e, 2)

        @pl.when(e >= 2)
        def _():
            for copy in grad_stores(e - 2, slot):
                copy.wait()

        for m in range(PARTS):
            wide_buf[slot, m] = acc13[e, :, m * part : (m + 1) * part].T.astype(BF16)
        xs[slot, pl.ds(0, width), :] = acc2[e].astype(BF16)
        for copy in grad_stores(e, slot):
            copy.start()
        return carry

    with jax.named_scope("finish"):
        lax.fori_loop(0, own, finish, 0)
    with jax.named_scope("out_finish"):
        out_finish()
    with jax.named_scope("sums_here_1"):
        sums_here(1)
    out_store.wait()
    for e in range(max(own - 2, 0), own):
        for copy in grad_stores(e, e % 2):
            copy.wait()
    for n in sorted(writes):
        writes[n].wait()
    for kind in kinds:
        for g, count in ((0, half), (1, 3 + half), (2, 3 + half)):
            links.finish_all(("rows", kind, g), all_refs[kind].at[pl.ds(0, count), tp], to_mate)
        links.finish_all(("over", kind), all_refs[kind].at[pl.ds(0, 2 * half), tp], to_mate)
    links.finish_all("w13", w13_all.at[pl.ds(0, 3)], to_up)
    links.finish_all("w2", w2_all.at[pl.ds(0, 3)], to_up)
    with jax.named_scope("drain"):
        links.drain()


def layer(tokens, d_out, ids, gate_vals, w_one, w_three, w_two, ep_size, tp_size, cap):
    tok, model = tokens.shape
    own, width, _ = w_two.shape
    half = ep_size // 2
    rows = half * cap
    part = model // PARTS
    hbm = pl.BlockSpec(memory_space=pl.ANY)
    shape = jax.ShapeDtypeStruct
    routes = (2 * ids.shape[0], tok)
    sends, receives = copy_counts(own)
    slot_rows = ep_size * tp_size * cap * own
    vector = pltpu.VMEM
    dma = pltpu.SemaphoreType.DMA
    outs = pl.pallas_call(
        functools.partial(layer_kernel, own, cap, width),
        in_specs=[hbm] * 7,
        out_specs=[hbm] * 15,
        out_shape=[
            shape((ep_size, tp_size, tok, model), BF16),
            shape((ep_size, tp_size, tok, model), BF16),
            shape((ep_size, tp_size) + routes, F32),
            shape((tp_size, own, PARTS, part, 2 * width), BF16),
            shape((tp_size, PARTS, own, width, part), BF16),
            shape((own, 2, rows, model), BF16),
            shape((own, 2, rows, model), BF16),
            shape((own, tp_size, 2 * rows, 2 * width), F32),
            shape((2, PARTS, 2 * tok, part // 2), F32),
            shape((2, PARTS, 2 * tok, part // 2), F32),
            shape((2, 2, PARTS, 2 * tok, part // 2), F32),
            shape((tok, model), BF16),
            shape((own, PARTS, part, width), BF16),
            shape((own, PARTS, part, width), BF16),
            shape((own, width, model), BF16),
        ],
        scratch_shapes=[
            vector(routes, F32),
            vector(ids.shape, jnp.int32),
            vector((own, PARTS, part, 2 * width), BF16),
            vector((own, width, model), BF16),
            vector((2, half // 2, tok, model), BF16),
            vector((2, half // 2, tok, model), BF16),
            vector((2, half // 2) + routes, F32),
            vector((ep_size,) + routes, F32),
            vector((tok, tok), BF16),
            vector((own, rows, model), BF16),
            vector((own, rows, model), BF16),
            vector((own, 2 * width, model), F32),
            vector((own, width, model), F32),
            vector((tp_size, own, part, 2 * width), BF16),
            vector((PARTS, tp_size, own, width, part), BF16),
            vector((tp_size, 2 * rows, 2 * width), F32),
            vector((own, tp_size, 2 * rows, 2 * width), BF16),
            vector((ep_size, own, cap, part), BF16),
            vector((4, 2 * tok, part // 2), F32),
            vector((2, 4, 2 * tok, part // 2), F32),
            vector((4, 2 * tok, part // 2), F32),
            vector((2 * tok, part // 2), F32),
            dma((sends,)),
            dma((receives,)),
            dma((4,)),
            dma((3, 2)),
            dma((2 * PARTS + 1,)),
            dma((2,)),
            dma((1 + tp_size,)),
            dma((tp_size,)),
            dma((3,)),
            dma((2 * PARTS,)),
            dma((2, 3)),
            pltpu.SemaphoreType.REGULAR,
        ],
        compiler_params=pltpu.CompilerParams(vmem_limit_bytes=VMEM_LIMIT, collective_id=0, has_side_effects=True),
        cost_estimate=pl.CostEstimate(
            flops=2 * slot_rows * model * (2 * tok + 12 * width),
            bytes_accessed=4 * ep_size * tp_size * tok * model,
            transcendentals=0,
        ),
        name="layer",
    )(tokens, d_out, ids, gate_vals, w_one, w_three, w_two)
    g1, g3, g2 = outs[12:]
    return outs[8], outs[10], outs[11], (g1.reshape(own, model, width), g3.reshape(own, model, width), g2)


def result_kernel(sums, last_land, rows_in, g1, g3, g2, out, dx, o1, o3, o2, parts, rows, row_buf, b1, b3, b2, in_sem, out_sem):
    moves = ((g1, b1, o1), (g3, b3, o3), (g2, b2, o2), (rows_in, row_buf, out))
    takes = [pltpu.make_async_copy(src, buf, in_sem.at[k]) for k, (src, buf, _) in enumerate(moves)]
    terms = [pltpu.make_async_copy(src, parts.at[k], in_sem.at[4 + k])
             for k, src in enumerate((sums.at[1], last_land.at[1, 0], last_land.at[1, 1]))]
    for copy in terms + takes:
        copy.start()
    for copy in terms:
        copy.wait()
    tok, fold = rows.shape[0], parts.shape[3]
    for q in range(parts.shape[1]):
        for h in range(2):
            at, half = (2 * q + h) * fold, pl.ds(h * tok, tok)
            rows[:, at : at + fold] = (parts[0, q, half] + (parts[1, q, half] + parts[2, q, half])).astype(BF16)
    puts = [pltpu.make_async_copy(rows, dx, out_sem.at[4])]
    puts[0].start()
    for k, (take, (_, buf, to)) in enumerate(zip(takes, moves)):
        take.wait()
        puts.append(pltpu.make_async_copy(buf, to, out_sem.at[k]))
        puts[-1].start()
    for copy in puts:
        copy.wait()


def results(sums, last_land, out, grads):
    _, count, tall, fold = sums.shape
    tok, model = out.shape
    hbm = pl.BlockSpec(memory_space=pl.ANY)
    row = jax.ShapeDtypeStruct((tok, model), BF16)
    rows = pltpu.VMEM((tok, model), BF16)
    return pl.pallas_call(
        result_kernel,
        in_specs=[hbm] * 6,
        out_specs=[hbm] * 5,
        out_shape=[row, row] + [jax.ShapeDtypeStruct(g.shape, g.dtype) for g in grads],
        scratch_shapes=[pltpu.VMEM((3, count, tall, fold), F32), rows, rows]
        + [pltpu.VMEM(g.shape, g.dtype) for g in grads]
        + [pltpu.SemaphoreType.DMA((7,)), pltpu.SemaphoreType.DMA((5,))],
        compiler_params=pltpu.CompilerParams(vmem_limit_bytes=VMEM_LIMIT),
        name="results",
    )(sums, last_land, out, *grads)


def solution(mesh):
    ep_size, tp_size = mesh.shape["ep"], mesh.shape["tp"]
    row_spec = P(("dp", "ep", "tp"), None)
    col_spec = P("ep", None, "tp")
    down_spec = P("ep", "tp", None)
    grad_col = P(("dp", "ep"), None, "tp")
    grad_down = P(("dp", "ep"), "tp", None)

    def local_step(tokens, expert_ids, gate_vals, w_one, w_three, w_two, d_out):
        cap = slot_count(expert_ids.shape[1], tokens.shape[0], w_one.shape[0] * ep_size)
        sums, last_land, out, grads = layer(tokens, d_out, expert_ids.T, gate_vals.T, w_one, w_three, w_two, ep_size, tp_size, cap)
        return tuple(results(sums, last_land, out, grads))

    return jax.shard_map(local_step, mesh=mesh,
                         in_specs=(row_spec, row_spec, row_spec, col_spec, col_spec, down_spec, row_spec),
                         out_specs=(row_spec, row_spec, grad_col, grad_col, grad_down), check_vma=False)
```

```python
import functools

import jax
import jax.numpy as jnp
from jax import lax
from jax.experimental import pallas as pl
from jax.experimental.pallas import tpu as pltpu
from jax.sharding import PartitionSpec as P

BF16 = jnp.bfloat16
F32 = jnp.float32
MESH = pl.DeviceIdType.MESH
VMEM_LIMIT = 67_043_328
PARTS = 3


def slot_count(num_top, tok_dev, experts):
    return 8 * ((5 * num_top * tok_dev + 32 * experts - 1) // (32 * experts))


def dot(a, b):
    return jnp.dot(a, b, preferred_element_type=F32)


def dot_tb(a, b):
    return lax.dot_general(a, b, (((1,), (1,)), ((), ())), preferred_element_type=F32)


def dot_ta(a, b):
    return lax.dot_general(a, b, (((0,), (0,)), ((), ())), preferred_element_type=F32)


def earlier_rows(tok):
    row = lax.broadcasted_iota(jnp.int32, (tok, tok), 0)
    col = lax.broadcasted_iota(jnp.int32, (tok, tok), 1)
    return jnp.where(row < col, 1.0, 0.0).astype(BF16)


def expert_rows(routes, first, own, earlier):
    top = routes.shape[0] // 2
    ids, gates = routes[:top], routes[top:]
    hits = [ids == (first + e).astype(F32) for e in range(own)]
    routed = jnp.concatenate([jnp.sum(jnp.where(m, 1.0, 0.0), axis=0, keepdims=True) for m in hits], axis=0)
    gate = jnp.concatenate([jnp.sum(jnp.where(m, gates, 0.0), axis=0, keepdims=True) for m in hits], axis=0)
    return jnp.where(routed > 0.0, dot(routed.astype(BF16), earlier), -1.0), gate


def hit_masks(pos, cap):
    slot = lax.broadcasted_iota(jnp.int32, (cap, pos.shape[1]), 0).astype(F32)
    return [pos[e : e + 1, :] == slot for e in range(pos.shape[0])]


def one_hot(masks):
    return jnp.concatenate([jnp.where(m, 1.0, 0.0) for m in masks], axis=0).astype(BF16)


def slot_gates(masks, gate):
    return jnp.concatenate([jnp.where(m, gate[e : e + 1, :], 0.0) for e, m in enumerate(masks)], axis=0)


def three_parts(x):
    hi = x.astype(BF16)
    rest = x - hi.astype(F32)
    mid = rest.astype(BF16)
    return hi, mid, (rest - mid.astype(F32)).astype(BF16)


class Links:
    def __init__(self, send_sem, recv_sem):
        self.send_sem, self.recv_sem, self.sent, self.finished = send_sem, recv_sem, [], set()
        self.send_of, self.recv_of = {}, {}

    def copy(self, s, r, src, dst, to):
        return pltpu.make_async_remote_copy(src_ref=src, dst_ref=dst, send_sem=self.send_sem.at[s],
                                            recv_sem=self.recv_sem.at[r], device_id=to, device_id_type=MESH)

    def send(self, src, dst, to, together=None, landing=None):
        k = len(self.sent)
        s = self.send_of.setdefault(k if together is None else together, len(self.send_of))
        r = self.recv_of.setdefault(k if landing is None else landing, len(self.recv_of))
        copy = self.copy(s, r, src, dst, to)
        copy.start()
        self.sent.append((s, r, copy))
        if together is not None:
            self.finished.add(k)
        return k

    def arrive(self, k, dst, to):
        s, r, _ = self.sent[k]
        self.copy(s, r, dst, dst, to).wait_recv()

    def arrive_all(self, landing, ref, to):
        self.copy(0, self.recv_of[landing], ref, ref, to).wait_recv()

    def finish(self, k):
        self.finished.add(k)
        self.sent[k][2].wait_send()

    def finish_all(self, together, ref, to):
        self.copy(self.send_of[together], 0, ref, ref, to).wait_send()

    def drain(self):
        for k in range(len(self.sent)):
            if k not in self.finished:
                self.finish(k)


def copy_counts(own):
    sums = 2 * PARTS * 8
    return 3 * 5 + 2 + sums, 6 + 3 * 3 * 4 + 24 + 4 * own + 4 * (PARTS + 1) + sums


def layer_kernel(own, cap, width, tokens, d_out, ids, gate_vals, w1, w3, w2, x_all, dy_all, r_all, w13_all, w2_all, xs_all,
                 us_all, ab_all, sums, far_land, last_land, out, g1, g3, g2, r_own, i_own, w13, w2s, xb,
                 dyb, rb, routes, earlier, xs, us, acc13, acc2, wide_buf, w2v, ab_buf, d_all, y_buf, give, keep_sum, mate_sum,
                 far_sum, send_sem, recv_sem, row_sem, load_sem, w_sem, slot_sem, in_sem, ab_sem, sum_sem, own_sem, g_sem, free_sem):
    ep, tp = lax.axis_index("ep"), lax.axis_index("tp")
    eps, tps = x_all.shape[0], x_all.shape[1]
    model = x_all.shape[3]
    part = model // PARTS
    half = eps // 2
    x_own, dy_own = xs.at[0], xs.at[1]
    step = lambda n: lax.rem(ep + (n + eps), eps)
    turn = lambda n: lax.rem(tp + (n + tps), tps)
    right, left, far = step(2), step(-2), step(4)
    mate = ep + 1 - 2 * lax.rem(ep, 2)
    mate_step = lambda n: lax.rem(mate + (n + eps), eps)
    up, down, over = turn(1), turn(-1), turn(2)
    to_right, to_left, to_mate = {"ep": right}, {"ep": left}, {"ep": mate}
    to_up, to_down = {"tp": up}, {"tp": down}
    links = Links(send_sem, recv_sem)

    barrier = pltpu.get_barrier_semaphore()
    for to in (to_right, to_left, to_mate, to_up, to_down):
        pl.semaphore_signal(barrier, inc=1, device_id=to, device_id_type=MESH)
    top = ids.shape[0]
    firsts = [pltpu.make_async_copy(ids, i_own, row_sem.at[0]), pltpu.make_async_copy(gate_vals, r_own.at[pl.ds(top, top)], row_sem.at[1]),
              pltpu.make_async_copy(tokens, x_own, row_sem.at[2]), pltpu.make_async_copy(d_out, dy_own, row_sem.at[3])]
    loads = [pltpu.make_async_copy(src.at[:, pl.ds(m * part, part)], w13.at[:, m, :, pl.ds(k * width, width)], w_sem.at[PARTS * k + m])
             for k, src in ((0, w1), (1, w3)) for m in range(PARTS)]
    loads.append(pltpu.make_async_copy(w2, w2s, w_sem.at[2 * PARTS]))
    for copy in firsts + loads:
        copy.start()
    firsts[0].wait()
    r_own[0:top] = i_own[...].astype(F32)
    for copy in firsts[1:]:
        copy.wait()
    with jax.named_scope("barrier"):
        pl.semaphore_wait(barrier, 5)

    own_refs, all_refs = (x_own, dy_own, r_own), (x_all, dy_all, r_all)
    upward = (True, False, True)
    kinds = (0, 1, 2)

    def spread(g, srcs):
        out, t = {}, groups[g]
        set_of = lambda kind: ("rows", kind, g) if g else ("first", kind)
        for kind in kinds:
            to = to_right if upward[kind] else to_left
            out[kind, upward[kind]] = links.send(srcs[kind], all_refs[kind].at[ep, t], to, set_of(kind))
        for kind in kinds:
            to = to_left if upward[kind] else to_right
            out[kind, not upward[kind]] = links.send(srcs[kind], all_refs[kind].at[ep, t], to, set_of(kind))
        for kind in kinds:
            links.send(srcs[kind], all_refs[kind].at[ep, t], to_mate, set_of(kind), ("mate", kind, g))
        return out

    def pass_on(g):
        state, t = states[g], groups[g]
        for kind in kinds:
            got, to = (left, to_right) if upward[kind] else (right, to_left)
            block = all_refs[kind].at[got, t]
            links.arrive(state[kind, upward[kind]], block, to)
            state[kind, "far"] = links.send(block, block, to, ("rows", kind, g))
            links.send(block, block, to_mate, ("rows", kind, g), ("mate", kind, g))

    def share(g):
        state, t = states[g], groups[g]
        for kind in kinds:
            got, to = (right, to_left) if upward[kind] else (left, to_right)
            block = all_refs[kind].at[got, t]
            links.arrive(state[kind, not upward[kind]], block, to)
            links.send(block, block, to_mate, ("rows", kind, g), ("mate", kind, g))

    def last(g):
        state, t = states[g], groups[g]
        for kind in kinds:
            block = all_refs[kind].at[far, t]
            links.arrive(state[kind, "far"], block, to_right if upward[kind] else to_left)
            links.send(block, block, to_mate, ("rows", kind, g), ("mate", kind, g))

    def from_mate(g):
        for kind in kinds:
            links.arrive_all(("mate", kind, g), all_refs[kind].at[pl.ds(0, half), groups[g]], to_mate)

    core = lax.rem(ep, 2)

    def send_over():
        return [{kind: links.send(all_refs[kind].at[core + 2 * m, down if upward[kind] else up],
                                  all_refs[kind].at[core + 2 * m, down if upward[kind] else up],
                                  to_up if upward[kind] else to_down, ("over", kind)) for kind in kinds} for m in range(half)]

    def share_over(m):
        for kind in kinds:
            block = all_refs[kind].at[core + 2 * m, over]
            links.arrive(over_state[m][kind], block, to_up if upward[kind] else to_down)
            over_state[m][kind, "mate"] = links.send(block, block, to_mate, ("over", kind))

    def have_over(m):
        for kind in kinds:
            links.arrive(over_state[m][kind, "mate"], all_refs[kind].at[1 - core + 2 * m, over], to_mate)

    def both_ways(src, dst, which):
        return {True: links.send(src, dst, to_up, which), False: links.send(src, dst, to_down, which)}

    def pass_halves(state, below, above, split, which):
        links.arrive(state[True], below, to_up)
        state["first"] = links.send(split(below, 0), split(below, 0), to_up, which)
        links.arrive(state[False], above, to_down)
        state["second"] = links.send(split(above, 1), split(above, 1), to_down, which)

    def have_halves(state, block, split):
        links.arrive(state["first"], split(block, 0), to_up)
        links.arrive(state["second"], split(block, 1), to_down)

    w13_state, w2_state = [None] * own, [None] * (PARTS + 1)
    split13 = lambda ref, k: ref.at[:, pl.ds(k * (part // 2), part // 2)]
    split2 = lambda ref, k: ref.at[:, pl.ds(k * (width // 2), width // 2)]

    def send13(e):
        w13_state[e] = both_ways(w13.at[e], w13_all.at[tp, e], "w13")

    def pass13(e):
        pass_halves(w13_state[e], w13_all.at[down, e], w13_all.at[up, e], split13, "w13")

    def have13(e):
        have_halves(w13_state[e], w13_all.at[over, e], split13)

    pieces = [(q, pl.ds(0, own)) for q in range(PARTS - 1)] + [(PARTS - 1, pl.ds(0, 2)), (PARTS - 1, pl.ds(2, own - 2))]

    def piece(j, p):
        q, experts = pieces[p]
        return w2_all.at[j, q, experts]

    def send2(p):
        q, experts = pieces[p]
        w2_state[p] = both_ways(w2s.at[experts, :, pl.ds(q * part, part)], piece(tp, p), "w2")

    def pass2(p):
        pass_halves(w2_state[p], piece(down, p), piece(up, p), split2, "w2")

    def have2(p):
        have_halves(w2_state[p], piece(over, p), split2)

    def grad_stores(e, slot):
        rows = pl.ds(0, PARTS)
        return [pltpu.make_async_copy(wide_buf.at[slot, rows, :, pl.ds(0, width)], g1.at[e], g_sem.at[slot, 0]),
                pltpu.make_async_copy(wide_buf.at[slot, rows, :, pl.ds(width, width)], g3.at[e], g_sem.at[slot, 1]),
                pltpu.make_async_copy(xs.at[slot, pl.ds(0, width)], g2.at[e], g_sem.at[slot, 2])]

    def write_grads(e):
        slot = lax.rem(e, 2)

        @pl.when(e >= 2)
        def _():
            for copy in grad_stores(e - 2, slot):
                copy.wait()

        for m in range(PARTS):
            wide_buf[slot, m] = acc13[e, :, m * part : (m + 1) * part].T.astype(BF16)
        xs[slot, pl.ds(0, width), :] = acc2[e].astype(BF16)
        for copy in grad_stores(e, slot):
            copy.start()

    def pair_loads(t, h, p):
        at = pl.ds(h * half + p * (half // 2), half // 2)
        return [pltpu.make_async_copy(src.at[at, t], dst.at[p], load_sem.at[k, p])
                for k, (src, dst) in enumerate(((x_all, xb), (dy_all, dyb), (r_all, rb)))]

    def half_group(t, h, keep, ahead, pairs=(0, 2), grads=True, write=False):
        def gather(p, b):
            pos, gate = expert_rows(rb[p, b], ep * own, own, earlier[...])
            masks = hit_masks(pos, cap)
            pick = one_hot(masks)
            gates = jnp.sum(slot_gates(masks, gate), axis=1, keepdims=True)
            rows = pl.ds(pl.multiple_of((p * (half // 2) + b) * cap, cap), cap)
            picked = dot(pick, xb[p, b]).astype(BF16)
            for e in range(own):
                xs[e, rows, :] = picked[e * cap : (e + 1) * cap]
            scaled = (gates * dot(pick, dyb[p, b])).astype(BF16)
            for e in range(own):
                us[e, rows, :] = scaled[e * cap : (e + 1) * cap]

        def pair(p, carry):
            for copy in pair_loads(t, h, p):
                copy.wait()
            for b in range(half // 2):
                gather(p, b)

            @pl.when(ahead)
            def _():
                for copy in pair_loads(t, 1, p):
                    copy.start()

            return carry

        lax.fori_loop(pairs[0], pairs[1], pair, 0)
        if not grads:
            return

        stores = []
        if keep:
            stores = [pltpu.make_async_copy(xs, xs_all.at[:, h], slot_sem.at[0]),
                      pltpu.make_async_copy(us, us_all.at[:, h], slot_sem.at[1])]
        for copy in stores:
            copy.start()

        def expert(e, carry):
            ab = dot(xs[e], w13[e].reshape(model, 2 * width))
            a, b = ab[:, :width], ab[:, width:]
            dh = dot_tb(us[e], w2s[e])
            sig = jax.nn.sigmoid(a)
            silu = a * sig
            hid = (silu * b).astype(BF16)
            da = (dh * b * sig * (1.0 + a * (1.0 - sig))).astype(BF16)
            db = (dh * silu).astype(BF16)
            acc13[e] += dot_ta(jnp.concatenate([da, db], axis=1), xs[e])
            acc2[e] += dot_ta(hid, us[e])
            if write:
                write_grads(e)
            return carry

        lax.fori_loop(0, own, expert, 0)
        for copy in stores:
            copy.wait()

    def start_loads(t, h, pairs=(0, 1)):
        for p in pairs:
            for copy in pair_loads(t, h, p):
                copy.start()

    def compute(t, keep):
        start_loads(t, 0)

        def one_half(h, carry):
            half_group(t, h, keep, h == 0)
            return carry

        lax.fori_loop(0, 2, one_half, 0)

    slots = eps * cap
    pending = []

    def settle():
        while pending:
            pending.pop().wait()

    def hidden(e):
        rows = pltpu.make_async_copy(xs_all.at[e], xs.at[pl.ds(0, 2)], in_sem.at[tps])
        rows.start()
        for j in range(tps):
            pltpu.make_async_copy(w13_all.at[j, e], wide_buf.at[pl.ds(0, PARTS), j], in_sem.at[j]).start()
        settle()
        rows.wait()

        def shard(j, carry):
            pltpu.make_async_copy(w13_all.at[j, e], wide_buf.at[pl.ds(0, PARTS), j], in_sem.at[j]).wait()
            ab = dot(xs[0:2].reshape(slots, model), wide_buf[0:PARTS, j].reshape(model, 2 * width))
            ab_buf[j] = ab
            a, b = ab[:, :width], ab[:, width:]
            at = pl.ds(pl.multiple_of(lax.rem(j, 2) * width, width), width)
            d_all[e, j // 2, :, at] = (a * jax.nn.sigmoid(a) * b).astype(BF16)
            return carry

        lax.fori_loop(0, tps, shard, 0)
        pending.append(pltpu.make_async_copy(ab_buf, ab_all.at[e], ab_sem.at[0]))
        pending[-1].start()

    def put_rows(e, value):
        for k in range(eps):
            y_buf[k, e] = value[k * cap : (k + 1) * cap]

    def down_load(q, j):
        return pltpu.make_async_copy(w2_all.at[j, q], w2v.at[q, j], in_sem.at[j])

    def load_down(q):
        for j in (tp, up, down):
            down_load(q, j).start()

    def y_part(q):
        down_load(q, over).start()
        for j in range(tps):
            down_load(q, j).wait()

        def one(e, carry):
            y = dot(d_all[e, 0], w2v[q, 0:2, e].reshape(2 * width, part)) + dot(d_all[e, 1], w2v[q, 2:4, e].reshape(2 * width, part))
            put_rows(e, y.astype(BF16))
            return carry

        lax.fori_loop(0, own, one, 0)

    def ab_load(e, j):
        return pltpu.make_async_copy(ab_all.at[e, j], ab_buf.at[j], ab_sem.at[j])

    def u_load(e, slot):
        return pltpu.make_async_copy(us_all.at[e], us.at[pl.ds(2 * slot, 2)], slot_sem.at[slot])

    def hidden_grads():
        settle()
        u_load(0, 0).start()
        for j in range(tps):
            ab_load(0, j).start()

        def one(e, carry):
            slot = lax.rem(e, 2)
            u_load(e, slot).wait()

            @pl.when(e + 1 < own)
            def _():
                u_load(e + 1, 1 - slot).start()

            def two(k, carry):
                dh = None
                for q in range(PARTS):
                    at = pl.ds(q * part, part)
                    u = us[pl.ds(2 * slot, 2), :, at].reshape(slots, part)
                    term = dot_tb(u, w2v[q, pl.ds(2 * k, 2), e].reshape(2 * width, part))
                    dh = term if dh is None else dh + term
                for i in range(2):
                    j = 2 * k + i
                    ab_load(e, j).wait()
                    a, b, d = ab_buf[j, :, :width], ab_buf[j, :, width:], dh[:, i * width : (i + 1) * width]
                    sig = jax.nn.sigmoid(a)
                    d_all[e, j, :, :width] = (d * b * sig * (1.0 + a * (1.0 - sig))).astype(BF16)
                    d_all[e, j, :, width:] = (d * (a * sig)).astype(BF16)

                    @pl.when(e + 1 < own)
                    def _():
                        ab_load(e + 1, j).start()
                return carry

            lax.fori_loop(0, tps // 2, two, 0)
            return carry

        lax.fori_loop(0, own, one, 0)

    def v_load(q):
        return pltpu.make_async_copy(w13_all.at[:, :, q], wide_buf, in_sem.at[tps])

    def v_part(q):
        v_load(q).wait()

        def one(e, carry):
            v = dot_tb(d_all[e, 0], wide_buf[0, e])
            for j in range(1, tps):
                v = v + dot_tb(d_all[e, j], wide_buf[j, e])
            put_rows(e, v.astype(BF16))
            return carry

        lax.fori_loop(0, own, one, 0)
        if q + 1 < PARTS:
            v_load(q + 1).start()

    gifts, writes, stages = {}, {}, {}

    def combine(kind, block):
        masks = hit_masks(routes[block, 0:own], cap)
        rows = y_buf[block].reshape(own * cap, part)
        if kind == 1:
            return dot_ta(one_hot(masks), rows)
        hi, mid, low = three_parts(slot_gates(masks, routes[block, top : top + own]))
        return dot_ta(hi, rows) + (dot_ta(mid, rows) + dot_ta(low, rows))

    numbers, ready = {}, {}
    tok = far_sum.shape[0] // 2
    fold = part // 2
    buffers = [keep_sum.at[0], keep_sum.at[1], keep_sum.at[0], ab_buf, keep_sum.at[1], keep_sum.at[0]]
    earlier_user = {2: 0, 4: 1, 5: 2}
    assert ab_buf.shape == give.shape and len(buffers) == 2 * PARTS
    halves = (pl.ds(0, tok), pl.ds(tok, tok))

    def put_tile(ref, i, value):
        ref[i, 0:tok] = value[:, :fold]
        ref[i, tok : 2 * tok] = value[:, fold:]

    def sum_begin(kind, q):
        n = numbers[kind, q] = len(numbers)
        tiles = buffers[n]
        for k in gifts.get(n - 1, ()):
            links.finish(k)
        if n in earlier_user:
            for k in ready[earlier_user[n]]:
                links.finish(k)
            writes.pop(earlier_user[n]).wait()

        def to_other(i, carry):
            for k in range(2):
                put_tile(give, 2 * i + k, combine(kind, lax.rem(mate + 4 - 2 * (2 * i + k) + eps, eps)))
            return carry

        def to_own(i, carry):
            put_tile(tiles, i, combine(kind, lax.rem(ep + 4 - 2 * i + eps, eps)))
            return carry

        for i in range(2):
            to_other(i, 0)
            if n and not i:
                pl.semaphore_wait(free_sem, 1)
            pair = pl.ds(2 * i, 2)
            gifts.setdefault(n, []).append(links.send(give.at[pair], mate_sum.at[pair], to_mate))
        lax.fori_loop(0, 2, to_own, 0)
        second[n] = to_own

    second = {}

    def take_pair(n, i):
        pair = pl.ds(2 * i, 2)
        links.arrive(gifts[n][i], mate_sum.at[pair], to_mate)
        buffers[n][pair] += mate_sum[pair]

    def sum_far(kind, q):
        n = numbers[kind, q]
        tiles = buffers[n]
        take_pair(n, 0)
        stages[n] = [links.send(tiles.at[0, halves[h]], far_land.at[kind, q, halves[h]], to) for h, to in ((0, to_right), (1, to_left))]
        stages[n].append(links.send(tiles.at[1, halves[1]], last_land.at[kind, 0, q, halves[1]], to_right))
        lax.fori_loop(2, 4, second[n], 0)

    def free_mate():
        pl.semaphore_signal(free_sem, inc=1, device_id=to_mate, device_id_type=MESH)

    def sum_near(kind, q):
        n = numbers[kind, q]
        tiles = buffers[n]
        take_pair(n, 1)
        if n + 1 < 2 * PARTS:
            free_mate()
        stages[n].append(links.send(tiles.at[3, halves[0]], last_land.at[kind, 1, q, halves[0]], to_left))
        writes[n] = pltpu.make_async_copy(tiles.at[2], sums.at[kind, q], own_sem.at[n])
        writes[n].start()

    def sum_end(kind, q):
        sum_far(kind, q)
        sum_near(kind, q)

    def sum_turn(kind, q):
        n = numbers[kind, q]
        tiles = buffers[n]
        for h, to in ((0, to_right), (1, to_left)):
            links.arrive(stages[n][h], far_land.at[kind, q, halves[h]], to)
        load = pltpu.make_async_copy(far_land.at[kind, q], far_sum, sum_sem.at[2])
        load.start()
        load.wait()
        for i, h, side, to in ((1, 0, 0, to_right), (3, 1, 1, to_left)):
            tiles[i, halves[h]] += far_sum[halves[h]]
            stages[n].append(links.send(tiles.at[i, halves[h]], last_land.at[kind, side, q, halves[h]], to))
        ready[n] = tuple(stages[n])

    def sums_here(kind):
        for q in range(PARTS):
            sent = stages[numbers[kind, q]]
            for k, h, side, to in ((2, 1, 0, to_right), (3, 0, 1, to_left), (4, 0, 0, to_right), (5, 1, 1, to_left)):
                links.arrive(sent[k], last_land.at[kind, side, q, halves[h]], to)

    three = pl.ds(0, PARTS)
    out_loads = [pltpu.make_async_copy(sums.at[0], give.at[three], sum_sem.at[0]),
                 pltpu.make_async_copy(last_land.at[0, 0], mate_sum.at[three], sum_sem.at[1]),
                 pltpu.make_async_copy(last_land.at[0, 1], mate_sum.at[three], sum_sem.at[1])]
    out_store = pltpu.make_async_copy(xb.at[0, 0], out, sum_sem.at[0])

    def out_start():
        sums_here(0)
        for k in gifts[2 * PARTS - 1]:
            links.finish(k)
        out_loads[0].start()
        out_loads[1].start()

    def out_middle():
        out_loads[0].wait()
        out_loads[1].wait()
        give[three] += mate_sum[three]
        out_loads[2].start()

    def out_finish():
        out_loads[2].wait()
        for q in range(PARTS):
            for h in range(2):
                at = q * part + h * fold
                xb[0, 0, :, at : at + fold] = (give[q, halves[h]] + mate_sum[q, halves[h]]).astype(BF16)
        out_store.start()

    y_state = {}
    for way in (True, False):
        for kind in kinds:
            go_up = upward[kind] == way
            y_state[kind, go_up] = links.send(own_refs[kind], all_refs[kind].at[ep, tp], to_up if go_up else to_down, ("first", kind))
    groups = (tp, down, up)
    states = [spread(0, own_refs)]
    hold = [pltpu.make_async_copy(own_refs[kind], all_refs[kind].at[ep, tp], row_sem.at[kind]) for kind in range(3)]
    for copy in hold:
        copy.start()
    for copy in loads:
        copy.wait()
    stow = [pltpu.make_async_copy(w13, w13_all.at[tp], w_sem.at[0])]
    stow += [pltpu.make_async_copy(w2s.at[:, :, pl.ds(q * part, part)], w2_all.at[tp, q], w_sem.at[1 + q]) for q in range(PARTS)]
    for copy in stow:
        copy.start()
    earlier[...] = earlier_rows(earlier.shape[0])
    with jax.named_scope("zeros"):
        acc13[...] = jnp.zeros_like(acc13)
        acc2[...] = jnp.zeros_like(acc2)

    def y_arrive(kind, way):
        block = all_refs[kind].at[ep, down if way else up]
        links.arrive(y_state[kind, way], block, to_up if way else to_down)
        return block

    with jax.named_scope("pass_on_0"):
        pass_on(0)
    with jax.named_scope("y_arrive"):
        for way in (True, False):
            for kind in kinds:
                y_arrive(kind, way)
    with jax.named_scope("send13_0"):
        send13(0)
    with jax.named_scope("send13_1"):
        send13(1)
    with jax.named_scope("send13_2"):
        send13(2)
    states.append(spread(1, [ref.at[ep, down] for ref in all_refs]))
    with jax.named_scope("share_0"):
        share(0)
    with jax.named_scope("last_0"):
        last(0)
    for copy in hold + stow:
        copy.wait()
    with jax.named_scope("from_mate_0"):
        from_mate(0)
    route_copy = pltpu.make_async_copy(r_all.at[:, tp], routes, row_sem.at[0])
    route_copy.start()
    route_copy.wait()

    def tabulate(b, carry):
        pos, gate = expert_rows(routes[b], ep * own, own, earlier[...])
        routes[b, 0:own] = pos
        routes[b, top : top + own] = gate
        return carry

    lax.fori_loop(0, eps, tabulate, 0)
    for kind in kinds:
        links.finish_all(("first", kind), all_refs[kind].at[pl.ds(0, 5), tp], to_mate)
    with jax.named_scope("compute_tp_True"):
        compute(tp, True)
    with jax.named_scope("pass13_0"):
        pass13(0)
    with jax.named_scope("send13_3"):
        send13(3)
    with jax.named_scope("pass_on_1"):
        pass_on(1)
    states.append(spread(2, [ref.at[ep, up] for ref in all_refs]))
    with jax.named_scope("share_1"):
        share(1)
    with jax.named_scope("pass13_1"):
        pass13(1)
    with jax.named_scope("send13_4"):
        send13(4)
    with jax.named_scope("have13_0"):
        have13(0)
    with jax.named_scope("hidden_0"):
        hidden(0)
    with jax.named_scope("pass13_2"):
        pass13(2)
    with jax.named_scope("last_1"):
        last(1)
    with jax.named_scope("from_mate_1"):
        from_mate(1)
    with jax.named_scope("compute_down_False"):
        compute(down, False)
    with jax.named_scope("pass13_3"):
        pass13(3)
    with jax.named_scope("send2_0"):
        send2(0)
    with jax.named_scope("pass_on_2"):
        pass_on(2)
    with jax.named_scope("have13_1"):
        have13(1)
    with jax.named_scope("hidden_1"):
        hidden(1)
    with jax.named_scope("share_2"):
        share(2)
    with jax.named_scope("pass13_4"):
        pass13(4)
    with jax.named_scope("have13_2"):
        have13(2)
    with jax.named_scope("hidden_2"):
        hidden(2)
    with jax.named_scope("last_2"):
        last(2)
    with jax.named_scope("from_mate_2"):
        from_mate(2)
    with jax.named_scope("have13_3"):
        have13(3)
    with jax.named_scope("hidden_3"):
        hidden(3)
    with jax.named_scope("start_loads_up_0"):
        start_loads(up, 0)
    with jax.named_scope("half_group_up_0_False_True"):
        half_group(up, 0, False, True)
    with jax.named_scope("pass2_0"):
        pass2(0)
    with jax.named_scope("send2_1"):
        send2(1)
        send2(2)
    with jax.named_scope("half_group_up_1_False_False"):
        half_group(up, 1, False, False)
    with jax.named_scope("have13_4"):
        have13(4)
    with jax.named_scope("hidden_4"):
        hidden(4)

    with jax.named_scope("have2_0"):
        have2(0)
    load_down(0)
    v_load(0).start()
    with jax.named_scope("y_part_0"):
        y_part(0)
    with jax.named_scope("sum_begin_0_0"):
        sum_begin(0, 0)
    with jax.named_scope("sum_end_0_0"):
        sum_end(0, 0)
    with jax.named_scope("pass2_1"):
        pass2(1)
    with jax.named_scope("send2_3"):
        send2(3)
    with jax.named_scope("pass2_2"):
        pass2(2)
    with jax.named_scope("sum_turn_0_0"):
        sum_turn(0, 0)
    load_down(1)
    with jax.named_scope("have2_1"):
        have2(1)
    with jax.named_scope("y_part_1"):
        y_part(1)
    with jax.named_scope("sum_begin_0_1"):
        sum_begin(0, 1)
    with jax.named_scope("pass2_3"):
        pass2(3)
    over_state = send_over()
    with jax.named_scope("sum_end_0_1"):
        sum_end(0, 1)
    load_down(2)
    with jax.named_scope("have2_2"):
        have2(2)
        have2(3)
    with jax.named_scope("y_part_2"):
        y_part(2)
    with jax.named_scope("sum_turn_0_1"):
        sum_turn(0, 1)
    with jax.named_scope("sum_begin_0_2"):
        sum_begin(0, 2)
    with jax.named_scope("sum_end_0_2"):
        sum_end(0, 2)
    with jax.named_scope("hidden_grads"):
        hidden_grads()
    with jax.named_scope("sum_turn_0_2"):
        sum_turn(0, 2)
    with jax.named_scope("share_over_0"):
        share_over(0)
    with jax.named_scope("v_part_0"):
        v_part(0)
    with jax.named_scope("sum_begin_1_0"):
        sum_begin(1, 0)
    with jax.named_scope("sum_far_1_0"):
        sum_far(1, 0)
    with jax.named_scope("v_part_1"):
        v_part(1)
    with jax.named_scope("sum_near_1_0"):
        sum_near(1, 0)
    with jax.named_scope("sum_begin_1_1"):
        sum_begin(1, 1)
    with jax.named_scope("sum_far_1_1"):
        sum_far(1, 1)
    with jax.named_scope("share_over_1"):
        share_over(1)
    with jax.named_scope("v_part_2"):
        v_part(2)
    with jax.named_scope("sum_near_1_1"):
        sum_near(1, 1)
    with jax.named_scope("sum_begin_1_2"):
        sum_begin(1, 2)
    with jax.named_scope("sum_far_1_2"):
        sum_far(1, 2)
    with jax.named_scope("sum_turn_1_0"):
        sum_turn(1, 0)
    with jax.named_scope("have_over_0"):
        have_over(0)
    with jax.named_scope("have_over_1"):
        have_over(1)
    with jax.named_scope("start_loads_over_0"):
        start_loads(over, 0)
    with jax.named_scope("sum_near_1_2"):
        sum_near(1, 2)
    with jax.named_scope("out_start"):
        out_start()
    with jax.named_scope("half_group_over_0_False_False"):
        half_group(over, 0, False, False)
    with jax.named_scope("sum_turn_1_1"):
        sum_turn(1, 1)
    with jax.named_scope("share_over_2"):
        share_over(2)
    with jax.named_scope("out_middle"):
        out_middle()
    with jax.named_scope("have_over_2"):
        have_over(2)
    with jax.named_scope("start_loads_over_1_0"):
        start_loads(over, 1, (0,))
    with jax.named_scope("sum_turn_1_2"):
        sum_turn(1, 2)
    with jax.named_scope("half_group_over_1_False_False_0_1_False"):
        half_group(over, 1, False, False, (0, 1), False)
    with jax.named_scope("share_over_3"):
        share_over(3)
    with jax.named_scope("have_over_3"):
        have_over(3)
    with jax.named_scope("start_loads_over_1_1"):
        start_loads(over, 1, (1,))
    with jax.named_scope("half_group_over_1_False_False_1_2"):
        half_group(over, 1, False, False, (1, 2), write=True)

    with jax.named_scope("out_finish"):
        out_finish()
    with jax.named_scope("sums_here_1"):
        sums_here(1)
    out_store.wait()
    for e in range(max(own - 2, 0), own):
        for copy in grad_stores(e, e % 2):
            copy.wait()
    for n in sorted(writes):
        writes[n].wait()
    for kind in kinds:
        for g, count in ((0, half), (1, 3 + half), (2, 3 + half)):
            links.finish_all(("rows", kind, g), all_refs[kind].at[pl.ds(0, count), tp], to_mate)
        links.finish_all(("over", kind), all_refs[kind].at[pl.ds(0, 2 * half), tp], to_mate)
    links.finish_all("w13", w13_all.at[pl.ds(0, 3)], to_up)
    links.finish_all("w2", w2_all.at[pl.ds(0, 3)], to_up)
    with jax.named_scope("drain"):
        links.drain()


def layer(tokens, d_out, ids, gate_vals, w_one, w_three, w_two, ep_size, tp_size, cap):
    tok, model = tokens.shape
    own, width, _ = w_two.shape
    half = ep_size // 2
    rows = half * cap
    part = model // PARTS
    hbm = pl.BlockSpec(memory_space=pl.ANY)
    shape = jax.ShapeDtypeStruct
    routes = (2 * ids.shape[0], tok)
    sends, receives = copy_counts(own)
    slot_rows = ep_size * tp_size * cap * own
    vector = pltpu.VMEM
    dma = pltpu.SemaphoreType.DMA
    outs = pl.pallas_call(
        functools.partial(layer_kernel, own, cap, width),
        in_specs=[hbm] * 7,
        out_specs=[hbm] * 15,
        out_shape=[
            shape((ep_size, tp_size, tok, model), BF16),
            shape((ep_size, tp_size, tok, model), BF16),
            shape((ep_size, tp_size) + routes, F32),
            shape((tp_size, own, PARTS, part, 2 * width), BF16),
            shape((tp_size, PARTS, own, width, part), BF16),
            shape((own, 2, rows, model), BF16),
            shape((own, 2, rows, model), BF16),
            shape((own, tp_size, 2 * rows, 2 * width), F32),
            shape((2, PARTS, 2 * tok, part // 2), F32),
            shape((2, PARTS, 2 * tok, part // 2), F32),
            shape((2, 2, PARTS, 2 * tok, part // 2), F32),
            shape((tok, model), BF16),
            shape((own, PARTS, part, width), BF16),
            shape((own, PARTS, part, width), BF16),
            shape((own, width, model), BF16),
        ],
        scratch_shapes=[
            vector(routes, F32),
            vector(ids.shape, jnp.int32),
            vector((own, PARTS, part, 2 * width), BF16),
            vector((own, width, model), BF16),
            vector((2, half // 2, tok, model), BF16),
            vector((2, half // 2, tok, model), BF16),
            vector((2, half // 2) + routes, F32),
            vector((ep_size,) + routes, F32),
            vector((tok, tok), BF16),
            vector((own, rows, model), BF16),
            vector((own, rows, model), BF16),
            vector((own, 2 * width, model), F32),
            vector((own, width, model), F32),
            vector((tp_size, own, part, 2 * width), BF16),
            vector((PARTS, tp_size, own, width, part), BF16),
            vector((tp_size, 2 * rows, 2 * width), F32),
            vector((own, tp_size, 2 * rows, 2 * width), BF16),
            vector((ep_size, own, cap, part), BF16),
            vector((4, 2 * tok, part // 2), F32),
            vector((2, 4, 2 * tok, part // 2), F32),
            vector((4, 2 * tok, part // 2), F32),
            vector((2 * tok, part // 2), F32),
            dma((sends,)),
            dma((receives,)),
            dma((4,)),
            dma((3, 2)),
            dma((2 * PARTS + 1,)),
            dma((2,)),
            dma((1 + tp_size,)),
            dma((tp_size,)),
            dma((3,)),
            dma((2 * PARTS,)),
            dma((2, 3)),
            pltpu.SemaphoreType.REGULAR,
        ],
        compiler_params=pltpu.CompilerParams(vmem_limit_bytes=VMEM_LIMIT, collective_id=0, has_side_effects=True),
        cost_estimate=pl.CostEstimate(
            flops=2 * slot_rows * model * (2 * tok + 12 * width),
            bytes_accessed=4 * ep_size * tp_size * tok * model,
            transcendentals=0,
        ),
        name="layer",
    )(tokens, d_out, ids, gate_vals, w_one, w_three, w_two)
    g1, g3, g2 = outs[12:]
    return outs[8], outs[10], outs[11], (g1.reshape(own, model, width), g3.reshape(own, model, width), g2)


def result_kernel(sums, last_land, rows_in, g1, g3, g2, out, dx, o1, o3, o2, parts, rows, row_buf, b1, b3, b2, in_sem, out_sem):
    moves = ((g1, b1, o1), (g3, b3, o3), (g2, b2, o2), (rows_in, row_buf, out))
    takes = [pltpu.make_async_copy(src, buf, in_sem.at[k]) for k, (src, buf, _) in enumerate(moves)]
    terms = [pltpu.make_async_copy(src, parts.at[k], in_sem.at[4 + k])
             for k, src in enumerate((sums.at[1], last_land.at[1, 0], last_land.at[1, 1]))]
    for copy in terms + takes:
        copy.start()
    for copy in terms:
        copy.wait()
    tok, fold = rows.shape[0], parts.shape[3]
    for q in range(parts.shape[1]):
        for h in range(2):
            at, half = (2 * q + h) * fold, pl.ds(h * tok, tok)
            rows[:, at : at + fold] = (parts[0, q, half] + (parts[1, q, half] + parts[2, q, half])).astype(BF16)
    puts = [pltpu.make_async_copy(rows, dx, out_sem.at[4])]
    puts[0].start()
    for k, (take, (_, buf, to)) in enumerate(zip(takes, moves)):
        take.wait()
        puts.append(pltpu.make_async_copy(buf, to, out_sem.at[k]))
        puts[-1].start()
    for copy in puts:
        copy.wait()


def results(sums, last_land, out, grads):
    _, count, tall, fold = sums.shape
    tok, model = out.shape
    hbm = pl.BlockSpec(memory_space=pl.ANY)
    row = jax.ShapeDtypeStruct((tok, model), BF16)
    rows = pltpu.VMEM((tok, model), BF16)
    return pl.pallas_call(
        result_kernel,
        in_specs=[hbm] * 6,
        out_specs=[hbm] * 5,
        out_shape=[row, row] + [jax.ShapeDtypeStruct(g.shape, g.dtype) for g in grads],
        scratch_shapes=[pltpu.VMEM((3, count, tall, fold), F32), rows, rows]
        + [pltpu.VMEM(g.shape, g.dtype) for g in grads]
        + [pltpu.SemaphoreType.DMA((7,)), pltpu.SemaphoreType.DMA((5,))],
        compiler_params=pltpu.CompilerParams(vmem_limit_bytes=VMEM_LIMIT),
        name="results",
    )(sums, last_land, out, *grads)


def solution(mesh):
    ep_size, tp_size = mesh.shape["ep"], mesh.shape["tp"]
    row_spec = P(("dp", "ep", "tp"), None)
    col_spec = P("ep", None, "tp")
    down_spec = P("ep", "tp", None)
    grad_col = P(("dp", "ep"), None, "tp")
    grad_down = P(("dp", "ep"), "tp", None)

    def local_step(tokens, expert_ids, gate_vals, w_one, w_three, w_two, d_out):
        cap = slot_count(expert_ids.shape[1], tokens.shape[0], w_one.shape[0] * ep_size)
        sums, last_land, out, grads = layer(tokens, d_out, expert_ids.T, gate_vals.T, w_one, w_three, w_two, ep_size, tp_size, cap)
        return tuple(results(sums, last_land, out, grads))

    return jax.shard_map(local_step, mesh=mesh,
                         in_specs=(row_spec, row_spec, row_spec, col_spec, col_spec, down_spec, row_spec),
                         out_specs=(row_spec, row_spec, grad_col, grad_col, grad_down), check_vma=False)
```

```python
import functools

import jax
import jax.numpy as jnp
from jax import lax
from jax.experimental import pallas as pl
from jax.experimental.pallas import tpu as pltpu
from jax.sharding import PartitionSpec as P

BF16 = jnp.bfloat16
F32 = jnp.float32
MESH = pl.DeviceIdType.MESH
VMEM_LIMIT = 67_043_328
PARTS = 3


def slot_count(num_top, tok_dev, experts):
    return 8 * ((5 * num_top * tok_dev + 32 * experts - 1) // (32 * experts))


def dot(a, b):
    return jnp.dot(a, b, preferred_element_type=F32)


def dot_tb(a, b):
    return lax.dot_general(a, b, (((1,), (1,)), ((), ())), preferred_element_type=F32)


def dot_ta(a, b):
    return lax.dot_general(a, b, (((0,), (0,)), ((), ())), preferred_element_type=F32)


def earlier_rows(tok):
    row = lax.broadcasted_iota(jnp.int32, (tok, tok), 0)
    col = lax.broadcasted_iota(jnp.int32, (tok, tok), 1)
    return jnp.where(row < col, 1.0, 0.0).astype(BF16)


def expert_rows(routes, first, own, earlier):
    top = routes.shape[0] // 2
    ids, gates = routes[:top], routes[top:]
    hits = [ids == (first + e).astype(F32) for e in range(own)]
    routed = jnp.concatenate([jnp.sum(jnp.where(m, 1.0, 0.0), axis=0, keepdims=True) for m in hits], axis=0)
    gate = jnp.concatenate([jnp.sum(jnp.where(m, gates, 0.0), axis=0, keepdims=True) for m in hits], axis=0)
    return jnp.where(routed > 0.0, dot(routed.astype(BF16), earlier), -1.0), gate


def hit_masks(pos, cap):
    slot = lax.broadcasted_iota(jnp.int32, (cap, pos.shape[1]), 0).astype(F32)
    return [pos[e : e + 1, :] == slot for e in range(pos.shape[0])]


def one_hot(masks):
    return jnp.concatenate([jnp.where(m, 1.0, 0.0) for m in masks], axis=0).astype(BF16)


def slot_gates(masks, gate):
    return jnp.concatenate([jnp.where(m, gate[e : e + 1, :], 0.0) for e, m in enumerate(masks)], axis=0)


def three_parts(x):
    hi = x.astype(BF16)
    rest = x - hi.astype(F32)
    mid = rest.astype(BF16)
    return hi, mid, (rest - mid.astype(F32)).astype(BF16)


class Links:
    def __init__(self, send_sem, recv_sem):
        self.send_sem, self.recv_sem, self.sent, self.finished = send_sem, recv_sem, [], set()
        self.send_of, self.recv_of = {}, {}

    def copy(self, s, r, src, dst, to):
        return pltpu.make_async_remote_copy(src_ref=src, dst_ref=dst, send_sem=self.send_sem.at[s],
                                            recv_sem=self.recv_sem.at[r], device_id=to, device_id_type=MESH)

    def send(self, src, dst, to, together=None, landing=None):
        k = len(self.sent)
        s = self.send_of.setdefault(k if together is None else together, len(self.send_of))
        r = self.recv_of.setdefault(k if landing is None else landing, len(self.recv_of))
        copy = self.copy(s, r, src, dst, to)
        copy.start()
        self.sent.append((s, r, copy))
        if together is not None:
            self.finished.add(k)
        return k

    def arrive(self, k, dst, to):
        s, r, _ = self.sent[k]
        self.copy(s, r, dst, dst, to).wait_recv()

    def arrive_all(self, landing, ref, to):
        self.copy(0, self.recv_of[landing], ref, ref, to).wait_recv()

    def finish(self, k):
        self.finished.add(k)
        self.sent[k][2].wait_send()

    def finish_all(self, together, ref, to):
        self.copy(self.send_of[together], 0, ref, ref, to).wait_send()

    def drain(self):
        for k in range(len(self.sent)):
            if k not in self.finished:
                self.finish(k)


def copy_counts(own):
    sums = 2 * PARTS * 8
    return 3 * 5 + 2 + sums, 6 + 3 * 3 * 4 + 24 + 4 * own + 4 * (PARTS + 1) + sums


def layer_kernel(own, cap, width, tokens, d_out, ids, gate_vals, w1, w3, w2, x_all, dy_all, r_all, w13_all, w2_all, xs_all,
                 us_all, ab_all, sums, far_land, last_land, out, g1, g3, g2, r_own, i_own, w13, w2s, xb,
                 dyb, rb, routes, earlier, xs, us, acc13, acc2, wide_buf, w2v, ab_buf, d_all, y_buf, give, keep_sum, mate_sum,
                 far_sum, send_sem, recv_sem, row_sem, load_sem, w_sem, slot_sem, in_sem, ab_sem, sum_sem, own_sem, g_sem, free_sem):
    ep, tp = lax.axis_index("ep"), lax.axis_index("tp")
    eps, tps = x_all.shape[0], x_all.shape[1]
    model = x_all.shape[3]
    part = model // PARTS
    half = eps // 2
    x_own, dy_own = xs.at[0], xs.at[1]
    step = lambda n: lax.rem(ep + (n + eps), eps)
    turn = lambda n: lax.rem(tp + (n + tps), tps)
    right, left, far = step(2), step(-2), step(4)
    mate = ep + 1 - 2 * lax.rem(ep, 2)
    mate_step = lambda n: lax.rem(mate + (n + eps), eps)
    up, down, over = turn(1), turn(-1), turn(2)
    to_right, to_left, to_mate = {"ep": right}, {"ep": left}, {"ep": mate}
    to_up, to_down = {"tp": up}, {"tp": down}
    links = Links(send_sem, recv_sem)

    barrier = pltpu.get_barrier_semaphore()
    for to in (to_right, to_left, to_mate, to_up, to_down):
        pl.semaphore_signal(barrier, inc=1, device_id=to, device_id_type=MESH)
    top = ids.shape[0]
    firsts = [pltpu.make_async_copy(ids, i_own, row_sem.at[0]), pltpu.make_async_copy(gate_vals, r_own.at[pl.ds(top, top)], row_sem.at[1]),
              pltpu.make_async_copy(tokens, x_own, row_sem.at[2]), pltpu.make_async_copy(d_out, dy_own, row_sem.at[3])]
    loads = [pltpu.make_async_copy(src.at[:, pl.ds(m * part, part)], w13.at[:, m, :, pl.ds(k * width, width)], w_sem.at[PARTS * k + m])
             for k, src in ((0, w1), (1, w3)) for m in range(PARTS)]
    loads.append(pltpu.make_async_copy(w2, w2s, w_sem.at[2 * PARTS]))
    for copy in firsts + loads:
        copy.start()
    firsts[0].wait()
    r_own[0:top] = i_own[...].astype(F32)
    for copy in firsts[1:]:
        copy.wait()
    with jax.named_scope("barrier"):
        pl.semaphore_wait(barrier, 5)

    own_refs, all_refs = (x_own, dy_own, r_own), (x_all, dy_all, r_all)
    upward = (True, False, True)
    kinds = (0, 1, 2)

    def spread(g, srcs):
        out, t = {}, groups[g]
        set_of = lambda kind: ("rows", kind, g) if g else ("first", kind)
        for kind in kinds:
            to = to_right if upward[kind] else to_left
            out[kind, upward[kind]] = links.send(srcs[kind], all_refs[kind].at[ep, t], to, set_of(kind))
        for kind in kinds:
            to = to_left if upward[kind] else to_right
            out[kind, not upward[kind]] = links.send(srcs[kind], all_refs[kind].at[ep, t], to, set_of(kind))
        for kind in kinds:
            links.send(srcs[kind], all_refs[kind].at[ep, t], to_mate, set_of(kind), ("mate", kind, g))
        return out

    def pass_on(g):
        state, t = states[g], groups[g]
        for kind in kinds:
            got, to = (left, to_right) if upward[kind] else (right, to_left)
            block = all_refs[kind].at[got, t]
            links.arrive(state[kind, upward[kind]], block, to)
            state[kind, "far"] = links.send(block, block, to, ("rows", kind, g))
            links.send(block, block, to_mate, ("rows", kind, g), ("mate", kind, g))

    def share(g):
        state, t = states[g], groups[g]
        for kind in kinds:
            got, to = (right, to_left) if upward[kind] else (left, to_right)
            block = all_refs[kind].at[got, t]
            links.arrive(state[kind, not upward[kind]], block, to)
            links.send(block, block, to_mate, ("rows", kind, g), ("mate", kind, g))

    def last(g):
        state, t = states[g], groups[g]
        for kind in kinds:
            block = all_refs[kind].at[far, t]
            links.arrive(state[kind, "far"], block, to_right if upward[kind] else to_left)
            links.send(block, block, to_mate, ("rows", kind, g), ("mate", kind, g))

    def from_mate(g):
        for kind in kinds:
            links.arrive_all(("mate", kind, g), all_refs[kind].at[pl.ds(0, half), groups[g]], to_mate)

    core = lax.rem(ep, 2)

    def send_over():
        return [{kind: links.send(all_refs[kind].at[core + 2 * m, down if upward[kind] else up],
                                  all_refs[kind].at[core + 2 * m, down if upward[kind] else up],
                                  to_up if upward[kind] else to_down, ("over", kind)) for kind in kinds} for m in range(half)]

    def share_over(m):
        for kind in kinds:
            block = all_refs[kind].at[core + 2 * m, over]
            links.arrive(over_state[m][kind], block, to_up if upward[kind] else to_down)
            over_state[m][kind, "mate"] = links.send(block, block, to_mate, ("over", kind))

    def have_over(m):
        for kind in kinds:
            links.arrive(over_state[m][kind, "mate"], all_refs[kind].at[1 - core + 2 * m, over], to_mate)

    def both_ways(src, dst, which):
        return {True: links.send(src, dst, to_up, which), False: links.send(src, dst, to_down, which)}

    def pass_halves(state, below, above, split, which):
        links.arrive(state[True], below, to_up)
        state["first"] = links.send(split(below, 0), split(below, 0), to_up, which)
        links.arrive(state[False], above, to_down)
        state["second"] = links.send(split(above, 1), split(above, 1), to_down, which)

    def have_halves(state, block, split):
        links.arrive(state["first"], split(block, 0), to_up)
        links.arrive(state["second"], split(block, 1), to_down)

    w13_state, w2_state = [None] * own, [None] * (PARTS + 1)
    split13 = lambda ref, k: ref.at[:, pl.ds(k * (part // 2), part // 2)]
    split2 = lambda ref, k: ref.at[:, pl.ds(k * (width // 2), width // 2)]

    def send13(e):
        w13_state[e] = both_ways(w13.at[e], w13_all.at[tp, e], "w13")

    def pass13(e):
        pass_halves(w13_state[e], w13_all.at[down, e], w13_all.at[up, e], split13, "w13")

    def have13(e):
        have_halves(w13_state[e], w13_all.at[over, e], split13)

    pieces = [(q, pl.ds(0, own)) for q in range(PARTS - 1)] + [(PARTS - 1, pl.ds(0, 2)), (PARTS - 1, pl.ds(2, own - 2))]

    def piece(j, p):
        q, experts = pieces[p]
        return w2_all.at[j, q, experts]

    def send2(p):
        q, experts = pieces[p]
        w2_state[p] = both_ways(w2s.at[experts, :, pl.ds(q * part, part)], piece(tp, p), "w2")

    def pass2(p):
        pass_halves(w2_state[p], piece(down, p), piece(up, p), split2, "w2")

    def have2(p):
        have_halves(w2_state[p], piece(over, p), split2)

    def grad_stores(e, slot):
        rows = pl.ds(0, PARTS)
        return [pltpu.make_async_copy(wide_buf.at[slot, rows, :, pl.ds(0, width)], g1.at[e], g_sem.at[slot, 0]),
                pltpu.make_async_copy(wide_buf.at[slot, rows, :, pl.ds(width, width)], g3.at[e], g_sem.at[slot, 1]),
                pltpu.make_async_copy(xs.at[slot, pl.ds(0, width)], g2.at[e], g_sem.at[slot, 2])]

    def write_grads(e):
        slot = lax.rem(e, 2)

        @pl.when(e >= 2)
        def _():
            for copy in grad_stores(e - 2, slot):
                copy.wait()

        for m in range(PARTS):
            wide_buf[slot, m] = acc13[e, :, m * part : (m + 1) * part].T.astype(BF16)
        xs[slot, pl.ds(0, width), :] = acc2[e].astype(BF16)
        for copy in grad_stores(e, slot):
            copy.start()

    def pair_loads(t, h, p):
        at = pl.ds(h * half + p * (half // 2), half // 2)
        return [pltpu.make_async_copy(src.at[at, t], dst.at[p], load_sem.at[k, p])
                for k, (src, dst) in enumerate(((x_all, xb), (dy_all, dyb), (r_all, rb)))]

    def half_group(t, h, keep, ahead, pairs=(0, 2), grads=True, write=False):
        def gather(p, b):
            pos, gate = expert_rows(rb[p, b], ep * own, own, earlier[...])
            masks = hit_masks(pos, cap)
            pick = one_hot(masks)
            gates = jnp.sum(slot_gates(masks, gate), axis=1, keepdims=True)
            rows = pl.ds(pl.multiple_of((p * (half // 2) + b) * cap, cap), cap)
            picked = dot(pick, xb[p, b]).astype(BF16)
            for e in range(own):
                xs[e, rows, :] = picked[e * cap : (e + 1) * cap]
            scaled = (gates * dot(pick, dyb[p, b])).astype(BF16)
            for e in range(own):
                us[e, rows, :] = scaled[e * cap : (e + 1) * cap]

        def pair(p, carry):
            for copy in pair_loads(t, h, p):
                copy.wait()
            for b in range(half // 2):
                gather(p, b)

            @pl.when(ahead)
            def _():
                for copy in pair_loads(t, 1, p):
                    copy.start()

            return carry

        lax.fori_loop(pairs[0], pairs[1], pair, 0)
        if not grads:
            return

        stores = []
        if keep:
            stores = [pltpu.make_async_copy(xs, xs_all.at[:, h], slot_sem.at[0]),
                      pltpu.make_async_copy(us, us_all.at[:, h], slot_sem.at[1])]
        for copy in stores:
            copy.start()

        def expert(e, carry):
            ab = dot(xs[e], w13[e].reshape(model, 2 * width))
            a, b = ab[:, :width], ab[:, width:]
            dh = dot_tb(us[e], w2s[e])
            sig = jax.nn.sigmoid(a)
            silu = a * sig
            hid = (silu * b).astype(BF16)
            da = (dh * b * sig * (1.0 + a * (1.0 - sig))).astype(BF16)
            db = (dh * silu).astype(BF16)
            acc13[e] += dot_ta(jnp.concatenate([da, db], axis=1), xs[e])
            acc2[e] += dot_ta(hid, us[e])
            if write:
                write_grads(e)
            return carry

        lax.fori_loop(0, own, expert, 0)
        for copy in stores:
            copy.wait()

    def start_loads(t, h, pairs=(0, 1)):
        for p in pairs:
            for copy in pair_loads(t, h, p):
                copy.start()

    def compute(t, keep):
        start_loads(t, 0)

        def one_half(h, carry):
            half_group(t, h, keep, h == 0)
            return carry

        lax.fori_loop(0, 2, one_half, 0)

    slots = eps * cap
    pending = []

    def settle():
        while pending:
            pending.pop().wait()

    def hidden(e):
        rows = pltpu.make_async_copy(xs_all.at[e], xs.at[pl.ds(0, 2)], in_sem.at[tps])
        rows.start()
        for j in range(tps):
            pltpu.make_async_copy(w13_all.at[j, e], wide_buf.at[pl.ds(0, PARTS), j], in_sem.at[j]).start()
        settle()
        rows.wait()

        def shard(j, carry):
            pltpu.make_async_copy(w13_all.at[j, e], wide_buf.at[pl.ds(0, PARTS), j], in_sem.at[j]).wait()
            ab = dot(xs[0:2].reshape(slots, model), wide_buf[0:PARTS, j].reshape(model, 2 * width))
            ab_buf[j] = ab
            a, b = ab[:, :width], ab[:, width:]
            at = pl.ds(pl.multiple_of(lax.rem(j, 2) * width, width), width)
            d_all[e, j // 2, :, at] = (a * jax.nn.sigmoid(a) * b).astype(BF16)
            return carry

        lax.fori_loop(0, tps, shard, 0)
        pending.append(pltpu.make_async_copy(ab_buf, ab_all.at[e], ab_sem.at[0]))
        pending[-1].start()

    def put_rows(e, value):
        for k in range(eps):
            y_buf[k, e] = value[k * cap : (k + 1) * cap]

    def down_load(q, j):
        return pltpu.make_async_copy(w2_all.at[j, q], w2v.at[q, j], in_sem.at[j])

    def load_down(q):
        for j in (tp, up, down):
            down_load(q, j).start()

    def y_part(q):
        down_load(q, over).start()
        for j in range(tps):
            down_load(q, j).wait()

        def one(e, carry):
            y = dot(d_all[e, 0], w2v[q, 0:2, e].reshape(2 * width, part)) + dot(d_all[e, 1], w2v[q, 2:4, e].reshape(2 * width, part))
            put_rows(e, y.astype(BF16))
            return carry

        lax.fori_loop(0, own, one, 0)

    def ab_load(e, j):
        return pltpu.make_async_copy(ab_all.at[e, j], ab_buf.at[j], ab_sem.at[j])

    def u_load(e, slot):
        return pltpu.make_async_copy(us_all.at[e], us.at[pl.ds(2 * slot, 2)], slot_sem.at[slot])

    def hidden_grads():
        settle()
        u_load(0, 0).start()
        for j in range(tps):
            ab_load(0, j).start()

        def one(e, carry):
            slot = lax.rem(e, 2)
            u_load(e, slot).wait()

            @pl.when(e + 1 < own)
            def _():
                u_load(e + 1, 1 - slot).start()

            def two(k, carry):
                dh = None
                for q in range(PARTS):
                    at = pl.ds(q * part, part)
                    u = us[pl.ds(2 * slot, 2), :, at].reshape(slots, part)
                    term = dot_tb(u, w2v[q, pl.ds(2 * k, 2), e].reshape(2 * width, part))
                    dh = term if dh is None else dh + term
                for i in range(2):
                    j = 2 * k + i
                    ab_load(e, j).wait()
                    a, b, d = ab_buf[j, :, :width], ab_buf[j, :, width:], dh[:, i * width : (i + 1) * width]
                    sig = jax.nn.sigmoid(a)
                    d_all[e, j, :, :width] = (d * b * sig * (1.0 + a * (1.0 - sig))).astype(BF16)
                    d_all[e, j, :, width:] = (d * (a * sig)).astype(BF16)

                    @pl.when(e + 1 < own)
                    def _():
                        ab_load(e + 1, j).start()
                return carry

            lax.fori_loop(0, tps // 2, two, 0)
            return carry

        lax.fori_loop(0, own, one, 0)

    def v_load(q):
        return pltpu.make_async_copy(w13_all.at[:, :, q], wide_buf, in_sem.at[tps])

    def v_part(q):
        v_load(q).wait()

        def one(e, carry):
            v = dot_tb(d_all[e, 0], wide_buf[0, e])
            for j in range(1, tps):
                v = v + dot_tb(d_all[e, j], wide_buf[j, e])
            put_rows(e, v.astype(BF16))
            return carry

        lax.fori_loop(0, own, one, 0)
        if q + 1 < PARTS:
            v_load(q + 1).start()

    gifts, writes, stages = {}, {}, {}

    def combine(kind, block):
        masks = hit_masks(routes[block, 0:own], cap)
        rows = y_buf[block].reshape(own * cap, part)
        if kind == 1:
            return dot_ta(one_hot(masks), rows)
        hi, mid, low = three_parts(slot_gates(masks, routes[block, top : top + own]))
        return dot_ta(hi, rows) + (dot_ta(mid, rows) + dot_ta(low, rows))

    numbers, ready = {}, {}
    tok = far_sum.shape[0] // 2
    fold = part // 2
    buffers = [keep_sum.at[0], keep_sum.at[1], keep_sum.at[0], ab_buf, keep_sum.at[1], keep_sum.at[0]]
    earlier_user = {2: 0, 4: 1, 5: 2}
    assert ab_buf.shape == give.shape and len(buffers) == 2 * PARTS
    halves = (pl.ds(0, tok), pl.ds(tok, tok))

    def put_tile(ref, i, value):
        ref[i, 0:tok] = value[:, :fold]
        ref[i, tok : 2 * tok] = value[:, fold:]

    def sum_begin(kind, q):
        n = numbers[kind, q] = len(numbers)
        tiles = buffers[n]
        for k in gifts.get(n - 1, ()):
            links.finish(k)
        if n in earlier_user:
            for k in ready[earlier_user[n]]:
                links.finish(k)
            writes.pop(earlier_user[n]).wait()

        def to_other(i, carry):
            for k in range(2):
                put_tile(give, 2 * i + k, combine(kind, lax.rem(mate + 4 - 2 * (2 * i + k) + eps, eps)))
            return carry

        def to_own(i, carry):
            put_tile(tiles, i, combine(kind, lax.rem(ep + 4 - 2 * i + eps, eps)))
            return carry

        for i in range(2):
            to_other(i, 0)
            if n and not i:
                pl.semaphore_wait(free_sem, 1)
            pair = pl.ds(2 * i, 2)
            gifts.setdefault(n, []).append(links.send(give.at[pair], mate_sum.at[pair], to_mate))
        lax.fori_loop(0, 2, to_own, 0)
        second[n] = to_own

    second = {}

    def take_pair(n, i):
        pair = pl.ds(2 * i, 2)
        links.arrive(gifts[n][i], mate_sum.at[pair], to_mate)
        buffers[n][pair] += mate_sum[pair]

    def sum_far(kind, q):
        n = numbers[kind, q]
        tiles = buffers[n]
        take_pair(n, 0)
        stages[n] = [links.send(tiles.at[0, halves[h]], far_land.at[kind, q, halves[h]], to) for h, to in ((0, to_right), (1, to_left))]
        stages[n].append(links.send(tiles.at[1, halves[1]], last_land.at[kind, 0, q, halves[1]], to_right))
        lax.fori_loop(2, 4, second[n], 0)

    def free_mate():
        pl.semaphore_signal(free_sem, inc=1, device_id=to_mate, device_id_type=MESH)

    def sum_near(kind, q):
        n = numbers[kind, q]
        tiles = buffers[n]
        take_pair(n, 1)
        if n + 1 < 2 * PARTS:
            free_mate()
        stages[n].append(links.send(tiles.at[3, halves[0]], last_land.at[kind, 1, q, halves[0]], to_left))
        writes[n] = pltpu.make_async_copy(tiles.at[2], sums.at[kind, q], own_sem.at[n])
        writes[n].start()

    def sum_end(kind, q):
        sum_far(kind, q)
        sum_near(kind, q)

    def sum_turn(kind, q):
        n = numbers[kind, q]
        tiles = buffers[n]
        for h, to in ((0, to_right), (1, to_left)):
            links.arrive(stages[n][h], far_land.at[kind, q, halves[h]], to)
        load = pltpu.make_async_copy(far_land.at[kind, q], far_sum, sum_sem.at[2])
        load.start()
        load.wait()
        for i, h, side, to in ((1, 0, 0, to_right), (3, 1, 1, to_left)):
            tiles[i, halves[h]] += far_sum[halves[h]]
            stages[n].append(links.send(tiles.at[i, halves[h]], last_land.at[kind, side, q, halves[h]], to))
        ready[n] = tuple(stages[n])

    def sums_here(kind):
        for q in range(PARTS):
            sent = stages[numbers[kind, q]]
            for k, h, side, to in ((2, 1, 0, to_right), (3, 0, 1, to_left), (4, 0, 0, to_right), (5, 1, 1, to_left)):
                links.arrive(sent[k], last_land.at[kind, side, q, halves[h]], to)

    three = pl.ds(0, PARTS)
    out_loads = [pltpu.make_async_copy(sums.at[0], give.at[three], sum_sem.at[0]),
                 pltpu.make_async_copy(last_land.at[0, 0], mate_sum.at[three], sum_sem.at[1]),
                 pltpu.make_async_copy(last_land.at[0, 1], mate_sum.at[three], sum_sem.at[1])]
    out_store = pltpu.make_async_copy(xb.at[0, 0], out, sum_sem.at[0])

    def out_start():
        sums_here(0)
        for k in gifts[2 * PARTS - 1]:
            links.finish(k)
        out_loads[0].start()
        out_loads[1].start()

    def out_middle():
        out_loads[0].wait()
        out_loads[1].wait()
        give[three] += mate_sum[three]
        out_loads[2].start()

    def out_finish():
        out_loads[2].wait()
        for q in range(PARTS):
            for h in range(2):
                at = q * part + h * fold
                xb[0, 0, :, at : at + fold] = (give[q, halves[h]] + mate_sum[q, halves[h]]).astype(BF16)
        out_store.start()

    y_state = {}
    for way in (True, False):
        for kind in kinds:
            go_up = upward[kind] == way
            y_state[kind, go_up] = links.send(own_refs[kind], all_refs[kind].at[ep, tp], to_up if go_up else to_down, ("first", kind))
    groups = (tp, down, up)
    states = [spread(0, own_refs)]
    hold = [pltpu.make_async_copy(own_refs[kind], all_refs[kind].at[ep, tp], row_sem.at[kind]) for kind in range(3)]
    for copy in hold:
        copy.start()
    for copy in loads:
        copy.wait()
    stow = [pltpu.make_async_copy(w13, w13_all.at[tp], w_sem.at[0])]
    stow += [pltpu.make_async_copy(w2s.at[:, :, pl.ds(q * part, part)], w2_all.at[tp, q], w_sem.at[1 + q]) for q in range(PARTS)]
    for copy in stow:
        copy.start()
    with jax.named_scope("send13_0"):
        send13(0)
    with jax.named_scope("send13_1"):
        send13(1)
    with jax.named_scope("send13_2"):
        send13(2)
    earlier[...] = earlier_rows(earlier.shape[0])
    with jax.named_scope("zeros"):
        acc13[...] = jnp.zeros_like(acc13)
        acc2[...] = jnp.zeros_like(acc2)

    def y_arrive(kind, way):
        block = all_refs[kind].at[ep, down if way else up]
        links.arrive(y_state[kind, way], block, to_up if way else to_down)
        return block

    with jax.named_scope("pass_on_0"):
        pass_on(0)
    with jax.named_scope("y_arrive"):
        for way in (True, False):
            for kind in kinds:
                y_arrive(kind, way)
    states.append(spread(1, [ref.at[ep, down] for ref in all_refs]))
    with jax.named_scope("share_0"):
        share(0)
    with jax.named_scope("last_0"):
        last(0)
    for copy in hold + stow:
        copy.wait()
    with jax.named_scope("from_mate_0"):
        from_mate(0)
    route_copy = pltpu.make_async_copy(r_all.at[:, tp], routes, row_sem.at[0])
    route_copy.start()
    route_copy.wait()

    def tabulate(b, carry):
        pos, gate = expert_rows(routes[b], ep * own, own, earlier[...])
        routes[b, 0:own] = pos
        routes[b, top : top + own] = gate
        return carry

    lax.fori_loop(0, eps, tabulate, 0)
    for kind in kinds:
        links.finish_all(("first", kind), all_refs[kind].at[pl.ds(0, 5), tp], to_mate)
    with jax.named_scope("compute_tp_True"):
        compute(tp, True)
    with jax.named_scope("pass13_0"):
        pass13(0)
    with jax.named_scope("send13_3"):
        send13(3)
    with jax.named_scope("pass_on_1"):
        pass_on(1)
    states.append(spread(2, [ref.at[ep, up] for ref in all_refs]))
    with jax.named_scope("share_1"):
        share(1)
    with jax.named_scope("pass13_1"):
        pass13(1)
    with jax.named_scope("send13_4"):
        send13(4)
    with jax.named_scope("have13_0"):
        have13(0)
    with jax.named_scope("hidden_0"):
        hidden(0)
    with jax.named_scope("pass13_2"):
        pass13(2)
    with jax.named_scope("last_1"):
        last(1)
    with jax.named_scope("from_mate_1"):
        from_mate(1)
    with jax.named_scope("compute_down_False"):
        compute(down, False)
    with jax.named_scope("pass13_3"):
        pass13(3)
    with jax.named_scope("send2_0"):
        send2(0)
    with jax.named_scope("pass_on_2"):
        pass_on(2)
    with jax.named_scope("have13_1"):
        have13(1)
    with jax.named_scope("hidden_1"):
        hidden(1)
    with jax.named_scope("share_2"):
        share(2)
    with jax.named_scope("pass13_4"):
        pass13(4)
    with jax.named_scope("have13_2"):
        have13(2)
    with jax.named_scope("hidden_2"):
        hidden(2)
    with jax.named_scope("last_2"):
        last(2)
    with jax.named_scope("from_mate_2"):
        from_mate(2)
    with jax.named_scope("have13_3"):
        have13(3)
    with jax.named_scope("hidden_3"):
        hidden(3)
    with jax.named_scope("start_loads_up_0"):
        start_loads(up, 0)
    with jax.named_scope("half_group_up_0_False_True"):
        half_group(up, 0, False, True)
    with jax.named_scope("pass2_0"):
        pass2(0)
    with jax.named_scope("send2_1"):
        send2(1)
        send2(2)
    with jax.named_scope("half_group_up_1_False_False"):
        half_group(up, 1, False, False)
    with jax.named_scope("have13_4"):
        have13(4)
    with jax.named_scope("hidden_4"):
        hidden(4)

    with jax.named_scope("have2_0"):
        have2(0)
    load_down(0)
    v_load(0).start()
    with jax.named_scope("y_part_0"):
        y_part(0)
    with jax.named_scope("sum_begin_0_0"):
        sum_begin(0, 0)
    with jax.named_scope("sum_end_0_0"):
        sum_end(0, 0)
    with jax.named_scope("pass2_1"):
        pass2(1)
    with jax.named_scope("send2_3"):
        send2(3)
    with jax.named_scope("pass2_2"):
        pass2(2)
    with jax.named_scope("sum_turn_0_0"):
        sum_turn(0, 0)
    load_down(1)
    with jax.named_scope("have2_1"):
        have2(1)
    with jax.named_scope("y_part_1"):
        y_part(1)
    with jax.named_scope("sum_begin_0_1"):
        sum_begin(0, 1)
    with jax.named_scope("pass2_3"):
        pass2(3)
    over_state = send_over()
    with jax.named_scope("sum_end_0_1"):
        sum_end(0, 1)
    load_down(2)
    with jax.named_scope("have2_2"):
        have2(2)
        have2(3)
    with jax.named_scope("y_part_2"):
        y_part(2)
    with jax.named_scope("sum_turn_0_1"):
        sum_turn(0, 1)
    with jax.named_scope("sum_begin_0_2"):
        sum_begin(0, 2)
    with jax.named_scope("sum_end_0_2"):
        sum_end(0, 2)
    with jax.named_scope("hidden_grads"):
        hidden_grads()
    with jax.named_scope("sum_turn_0_2"):
        sum_turn(0, 2)
    with jax.named_scope("share_over_0"):
        share_over(0)
    with jax.named_scope("v_part_0"):
        v_part(0)
    with jax.named_scope("sum_begin_1_0"):
        sum_begin(1, 0)
    with jax.named_scope("sum_far_1_0"):
        sum_far(1, 0)
    with jax.named_scope("v_part_1"):
        v_part(1)
    with jax.named_scope("sum_near_1_0"):
        sum_near(1, 0)
    with jax.named_scope("sum_begin_1_1"):
        sum_begin(1, 1)
    with jax.named_scope("sum_far_1_1"):
        sum_far(1, 1)
    with jax.named_scope("share_over_1"):
        share_over(1)
    with jax.named_scope("v_part_2"):
        v_part(2)
    with jax.named_scope("sum_near_1_1"):
        sum_near(1, 1)
    with jax.named_scope("sum_begin_1_2"):
        sum_begin(1, 2)
    with jax.named_scope("sum_far_1_2"):
        sum_far(1, 2)
    with jax.named_scope("sum_turn_1_0"):
        sum_turn(1, 0)
    with jax.named_scope("have_over_0"):
        have_over(0)
    with jax.named_scope("have_over_1"):
        have_over(1)
    with jax.named_scope("start_loads_over_0"):
        start_loads(over, 0)
    with jax.named_scope("sum_near_1_2"):
        sum_near(1, 2)
    with jax.named_scope("out_start"):
        out_start()
    with jax.named_scope("half_group_over_0_False_False"):
        half_group(over, 0, False, False)
    with jax.named_scope("share_over_2"):
        share_over(2)
    with jax.named_scope("sum_turn_1_1"):
        sum_turn(1, 1)
    with jax.named_scope("out_middle"):
        out_middle()
    with jax.named_scope("sum_turn_1_2"):
        sum_turn(1, 2)
    with jax.named_scope("have_over_2"):
        have_over(2)
    with jax.named_scope("start_loads_over_1_0"):
        start_loads(over, 1, (0,))
    with jax.named_scope("half_group_over_1_False_False_0_1_False"):
        half_group(over, 1, False, False, (0, 1), False)
    with jax.named_scope("share_over_3"):
        share_over(3)
    with jax.named_scope("have_over_3"):
        have_over(3)
    with jax.named_scope("start_loads_over_1_1"):
        start_loads(over, 1, (1,))
    with jax.named_scope("half_group_over_1_False_False_1_2"):
        half_group(over, 1, False, False, (1, 2), write=True)

    with jax.named_scope("out_finish"):
        out_finish()
    with jax.named_scope("sums_here_1"):
        sums_here(1)
    out_store.wait()
    for e in range(max(own - 2, 0), own):
        for copy in grad_stores(e, e % 2):
            copy.wait()
    for n in sorted(writes):
        writes[n].wait()
    for kind in kinds:
        for g, count in ((0, half), (1, 3 + half), (2, 3 + half)):
            links.finish_all(("rows", kind, g), all_refs[kind].at[pl.ds(0, count), tp], to_mate)
        links.finish_all(("over", kind), all_refs[kind].at[pl.ds(0, 2 * half), tp], to_mate)
    links.finish_all("w13", w13_all.at[pl.ds(0, 3)], to_up)
    links.finish_all("w2", w2_all.at[pl.ds(0, 3)], to_up)
    with jax.named_scope("drain"):
        links.drain()


def layer(tokens, d_out, ids, gate_vals, w_one, w_three, w_two, ep_size, tp_size, cap):
    tok, model = tokens.shape
    own, width, _ = w_two.shape
    half = ep_size // 2
    rows = half * cap
    part = model // PARTS
    hbm = pl.BlockSpec(memory_space=pl.ANY)
    shape = jax.ShapeDtypeStruct
    routes = (2 * ids.shape[0], tok)
    sends, receives = copy_counts(own)
    slot_rows = ep_size * tp_size * cap * own
    vector = pltpu.VMEM
    dma = pltpu.SemaphoreType.DMA
    outs = pl.pallas_call(
        functools.partial(layer_kernel, own, cap, width),
        in_specs=[hbm] * 7,
        out_specs=[hbm] * 15,
        out_shape=[
            shape((ep_size, tp_size, tok, model), BF16),
            shape((ep_size, tp_size, tok, model), BF16),
            shape((ep_size, tp_size) + routes, F32),
            shape((tp_size, own, PARTS, part, 2 * width), BF16),
            shape((tp_size, PARTS, own, width, part), BF16),
            shape((own, 2, rows, model), BF16),
            shape((own, 2, rows, model), BF16),
            shape((own, tp_size, 2 * rows, 2 * width), F32),
            shape((2, PARTS, 2 * tok, part // 2), F32),
            shape((2, PARTS, 2 * tok, part // 2), F32),
            shape((2, 2, PARTS, 2 * tok, part // 2), F32),
            shape((tok, model), BF16),
            shape((own, PARTS, part, width), BF16),
            shape((own, PARTS, part, width), BF16),
            shape((own, width, model), BF16),
        ],
        scratch_shapes=[
            vector(routes, F32),
            vector(ids.shape, jnp.int32),
            vector((own, PARTS, part, 2 * width), BF16),
            vector((own, width, model), BF16),
            vector((2, half // 2, tok, model), BF16),
            vector((2, half // 2, tok, model), BF16),
            vector((2, half // 2) + routes, F32),
            vector((ep_size,) + routes, F32),
            vector((tok, tok), BF16),
            vector((own, rows, model), BF16),
            vector((own, rows, model), BF16),
            vector((own, 2 * width, model), F32),
            vector((own, width, model), F32),
            vector((tp_size, own, part, 2 * width), BF16),
            vector((PARTS, tp_size, own, width, part), BF16),
            vector((tp_size, 2 * rows, 2 * width), F32),
            vector((own, tp_size, 2 * rows, 2 * width), BF16),
            vector((ep_size, own, cap, part), BF16),
            vector((4, 2 * tok, part // 2), F32),
            vector((2, 4, 2 * tok, part // 2), F32),
            vector((4, 2 * tok, part // 2), F32),
            vector((2 * tok, part // 2), F32),
            dma((sends,)),
            dma((receives,)),
            dma((4,)),
            dma((3, 2)),
            dma((2 * PARTS + 1,)),
            dma((2,)),
            dma((1 + tp_size,)),
            dma((tp_size,)),
            dma((3,)),
            dma((2 * PARTS,)),
            dma((2, 3)),
            pltpu.SemaphoreType.REGULAR,
        ],
        compiler_params=pltpu.CompilerParams(vmem_limit_bytes=VMEM_LIMIT, collective_id=0, has_side_effects=True),
        cost_estimate=pl.CostEstimate(
            flops=2 * slot_rows * model * (2 * tok + 12 * width),
            bytes_accessed=4 * ep_size * tp_size * tok * model,
            transcendentals=0,
        ),
        name="layer",
    )(tokens, d_out, ids, gate_vals, w_one, w_three, w_two)
    g1, g3, g2 = outs[12:]
    return outs[8], outs[10], outs[11], (g1.reshape(own, model, width), g3.reshape(own, model, width), g2)


def result_kernel(sums, last_land, rows_in, g1, g3, g2, out, dx, o1, o3, o2, parts, rows, row_buf, b1, b3, b2, in_sem, out_sem):
    moves = ((g1, b1, o1), (g3, b3, o3), (g2, b2, o2), (rows_in, row_buf, out))
    takes = [pltpu.make_async_copy(src, buf, in_sem.at[k]) for k, (src, buf, _) in enumerate(moves)]
    terms = [pltpu.make_async_copy(src, parts.at[k], in_sem.at[4 + k])
             for k, src in enumerate((sums.at[1], last_land.at[1, 0], last_land.at[1, 1]))]
    for copy in terms + takes:
        copy.start()
    for copy in terms:
        copy.wait()
    tok, fold = rows.shape[0], parts.shape[3]
    for q in range(parts.shape[1]):
        for h in range(2):
            at, half = (2 * q + h) * fold, pl.ds(h * tok, tok)
            rows[:, at : at + fold] = (parts[0, q, half] + (parts[1, q, half] + parts[2, q, half])).astype(BF16)
    puts = [pltpu.make_async_copy(rows, dx, out_sem.at[4])]
    puts[0].start()
    for k, (take, (_, buf, to)) in enumerate(zip(takes, moves)):
        take.wait()
        puts.append(pltpu.make_async_copy(buf, to, out_sem.at[k]))
        puts[-1].start()
    for copy in puts:
        copy.wait()


def results(sums, last_land, out, grads):
    _, count, tall, fold = sums.shape
    tok, model = out.shape
    hbm = pl.BlockSpec(memory_space=pl.ANY)
    row = jax.ShapeDtypeStruct((tok, model), BF16)
    rows = pltpu.VMEM((tok, model), BF16)
    return pl.pallas_call(
        result_kernel,
        in_specs=[hbm] * 6,
        out_specs=[hbm] * 5,
        out_shape=[row, row] + [jax.ShapeDtypeStruct(g.shape, g.dtype) for g in grads],
        scratch_shapes=[pltpu.VMEM((3, count, tall, fold), F32), rows, rows]
        + [pltpu.VMEM(g.shape, g.dtype) for g in grads]
        + [pltpu.SemaphoreType.DMA((7,)), pltpu.SemaphoreType.DMA((5,))],
        compiler_params=pltpu.CompilerParams(vmem_limit_bytes=VMEM_LIMIT),
        name="results",
    )(sums, last_land, out, *grads)


def solution(mesh):
    ep_size, tp_size = mesh.shape["ep"], mesh.shape["tp"]
    row_spec = P(("dp", "ep", "tp"), None)
    col_spec = P("ep", None, "tp")
    down_spec = P("ep", "tp", None)
    grad_col = P(("dp", "ep"), None, "tp")
    grad_down = P(("dp", "ep"), "tp", None)

    def local_step(tokens, expert_ids, gate_vals, w_one, w_three, w_two, d_out):
        cap = slot_count(expert_ids.shape[1], tokens.shape[0], w_one.shape[0] * ep_size)
        sums, last_land, out, grads = layer(tokens, d_out, expert_ids.T, gate_vals.T, w_one, w_three, w_two, ep_size, tp_size, cap)
        return tuple(results(sums, last_land, out, grads))

    return jax.shard_map(local_step, mesh=mesh,
                         in_specs=(row_spec, row_spec, row_spec, col_spec, col_spec, down_spec, row_spec),
                         out_specs=(row_spec, row_spec, grad_col, grad_col, grad_down), check_vma=False)
```

```python
import functools

import jax
import jax.numpy as jnp
from jax import lax
from jax.experimental import pallas as pl
from jax.experimental.pallas import tpu as pltpu
from jax.sharding import PartitionSpec as P

BF16 = jnp.bfloat16
F32 = jnp.float32
MESH = pl.DeviceIdType.MESH
VMEM_LIMIT = 67_043_328
PARTS = 3


def slot_count(num_top, tok_dev, experts):
    return 8 * ((5 * num_top * tok_dev + 32 * experts - 1) // (32 * experts))


def dot(a, b):
    return jnp.dot(a, b, preferred_element_type=F32)


def dot_tb(a, b):
    return lax.dot_general(a, b, (((1,), (1,)), ((), ())), preferred_element_type=F32)


def dot_ta(a, b):
    return lax.dot_general(a, b, (((0,), (0,)), ((), ())), preferred_element_type=F32)


def earlier_rows(tok):
    row = lax.broadcasted_iota(jnp.int32, (tok, tok), 0)
    col = lax.broadcasted_iota(jnp.int32, (tok, tok), 1)
    return jnp.where(row < col, 1.0, 0.0).astype(BF16)


def expert_rows(routes, first, own, earlier):
    top = routes.shape[0] // 2
    ids, gates = routes[:top], routes[top:]
    hits = [ids == (first + e).astype(F32) for e in range(own)]
    routed = jnp.concatenate([jnp.sum(jnp.where(m, 1.0, 0.0), axis=0, keepdims=True) for m in hits], axis=0)
    gate = jnp.concatenate([jnp.sum(jnp.where(m, gates, 0.0), axis=0, keepdims=True) for m in hits], axis=0)
    return jnp.where(routed > 0.0, dot(routed.astype(BF16), earlier), -1.0), gate


def hit_masks(pos, cap):
    slot = lax.broadcasted_iota(jnp.int32, (cap, pos.shape[1]), 0).astype(F32)
    return [pos[e : e + 1, :] == slot for e in range(pos.shape[0])]


def one_hot(masks):
    return jnp.concatenate([jnp.where(m, 1.0, 0.0) for m in masks], axis=0).astype(BF16)


def slot_gates(masks, gate):
    return jnp.concatenate([jnp.where(m, gate[e : e + 1, :], 0.0) for e, m in enumerate(masks)], axis=0)


def three_parts(x):
    hi = x.astype(BF16)
    rest = x - hi.astype(F32)
    mid = rest.astype(BF16)
    return hi, mid, (rest - mid.astype(F32)).astype(BF16)


class Links:
    def __init__(self, send_sem, recv_sem):
        self.send_sem, self.recv_sem, self.sent, self.finished = send_sem, recv_sem, [], set()
        self.send_of, self.recv_of = {}, {}

    def copy(self, s, r, src, dst, to):
        return pltpu.make_async_remote_copy(src_ref=src, dst_ref=dst, send_sem=self.send_sem.at[s],
                                            recv_sem=self.recv_sem.at[r], device_id=to, device_id_type=MESH)

    def send(self, src, dst, to, together=None, landing=None):
        k = len(self.sent)
        s = self.send_of.setdefault(k if together is None else together, len(self.send_of))
        r = self.recv_of.setdefault(k if landing is None else landing, len(self.recv_of))
        copy = self.copy(s, r, src, dst, to)
        copy.start()
        self.sent.append((s, r, copy))
        if together is not None:
            self.finished.add(k)
        return k

    def arrive(self, k, dst, to):
        s, r, _ = self.sent[k]
        self.copy(s, r, dst, dst, to).wait_recv()

    def arrive_all(self, landing, ref, to):
        self.copy(0, self.recv_of[landing], ref, ref, to).wait_recv()

    def finish(self, k):
        self.finished.add(k)
        self.sent[k][2].wait_send()

    def finish_all(self, together, ref, to):
        self.copy(self.send_of[together], 0, ref, ref, to).wait_send()

    def drain(self):
        for k in range(len(self.sent)):
            if k not in self.finished:
                self.finish(k)


def copy_counts(own):
    sums = 2 * PARTS * 8
    return 3 * 5 + 2 + sums, 6 + 3 * 3 * 4 + 24 + 4 * own + 4 * (PARTS + 1) + sums


def layer_kernel(own, cap, width, tokens, d_out, ids, gate_vals, w1, w3, w2, x_all, dy_all, r_all, w13_all, w2_all, xs_all,
                 us_all, ab_all, sums, far_land, last_land, out, g1, g3, g2, r_own, i_own, w13, w2s, xb,
                 dyb, rb, routes, earlier, xs, us, acc13, acc2, wide_buf, w2v, ab_buf, d_all, y_buf, give, keep_sum, mate_sum,
                 far_sum, send_sem, recv_sem, row_sem, load_sem, w_sem, slot_sem, in_sem, ab_sem, sum_sem, own_sem, g_sem, free_sem):
    ep, tp = lax.axis_index("ep"), lax.axis_index("tp")
    eps, tps = x_all.shape[0], x_all.shape[1]
    model = x_all.shape[3]
    part = model // PARTS
    half = eps // 2
    x_own, dy_own = xs.at[0], xs.at[1]
    step = lambda n: lax.rem(ep + (n + eps), eps)
    turn = lambda n: lax.rem(tp + (n + tps), tps)
    right, left, far = step(2), step(-2), step(4)
    mate = ep + 1 - 2 * lax.rem(ep, 2)
    mate_step = lambda n: lax.rem(mate + (n + eps), eps)
    up, down, over = turn(1), turn(-1), turn(2)
    to_right, to_left, to_mate = {"ep": right}, {"ep": left}, {"ep": mate}
    to_up, to_down = {"tp": up}, {"tp": down}
    links = Links(send_sem, recv_sem)

    barrier = pltpu.get_barrier_semaphore()
    for to in (to_right, to_left, to_mate, to_up, to_down):
        pl.semaphore_signal(barrier, inc=1, device_id=to, device_id_type=MESH)
    top = ids.shape[0]
    firsts = [pltpu.make_async_copy(ids, i_own, row_sem.at[0]), pltpu.make_async_copy(gate_vals, r_own.at[pl.ds(top, top)], row_sem.at[1]),
              pltpu.make_async_copy(tokens, x_own, row_sem.at[2]), pltpu.make_async_copy(d_out, dy_own, row_sem.at[3])]
    loads = [pltpu.make_async_copy(src.at[:, pl.ds(m * part, part)], w13.at[:, m, :, pl.ds(k * width, width)], w_sem.at[PARTS * k + m])
             for k, src in ((0, w1), (1, w3)) for m in range(PARTS)]
    loads.append(pltpu.make_async_copy(w2, w2s, w_sem.at[2 * PARTS]))
    for copy in firsts + loads:
        copy.start()
    firsts[0].wait()
    r_own[0:top] = i_own[...].astype(F32)
    for copy in firsts[1:]:
        copy.wait()
    with jax.named_scope("barrier"):
        pl.semaphore_wait(barrier, 5)

    own_refs, all_refs = (x_own, dy_own, r_own), (x_all, dy_all, r_all)
    upward = (True, False, True)
    kinds = (0, 1, 2)

    def spread(g, srcs):
        out, t = {}, groups[g]
        set_of = lambda kind: ("rows", kind, g) if g else ("first", kind)
        for kind in kinds:
            to = to_right if upward[kind] else to_left
            out[kind, upward[kind]] = links.send(srcs[kind], all_refs[kind].at[ep, t], to, set_of(kind))
        for kind in kinds:
            to = to_left if upward[kind] else to_right
            out[kind, not upward[kind]] = links.send(srcs[kind], all_refs[kind].at[ep, t], to, set_of(kind))
        for kind in kinds:
            links.send(srcs[kind], all_refs[kind].at[ep, t], to_mate, set_of(kind), ("mate", kind, g))
        return out

    def pass_on(g):
        state, t = states[g], groups[g]
        for kind in kinds:
            got, to = (left, to_right) if upward[kind] else (right, to_left)
            block = all_refs[kind].at[got, t]
            links.arrive(state[kind, upward[kind]], block, to)
            state[kind, "far"] = links.send(block, block, to, ("rows", kind, g))
            links.send(block, block, to_mate, ("rows", kind, g), ("mate", kind, g))

    def share(g):
        state, t = states[g], groups[g]
        for kind in kinds:
            got, to = (right, to_left) if upward[kind] else (left, to_right)
            block = all_refs[kind].at[got, t]
            links.arrive(state[kind, not upward[kind]], block, to)
            links.send(block, block, to_mate, ("rows", kind, g), ("mate", kind, g))

    def last(g):
        state, t = states[g], groups[g]
        for kind in kinds:
            block = all_refs[kind].at[far, t]
            links.arrive(state[kind, "far"], block, to_right if upward[kind] else to_left)
            links.send(block, block, to_mate, ("rows", kind, g), ("mate", kind, g))

    def from_mate(g):
        for kind in kinds:
            links.arrive_all(("mate", kind, g), all_refs[kind].at[pl.ds(0, half), groups[g]], to_mate)

    core = lax.rem(ep, 2)

    def send_over():
        return [{kind: links.send(all_refs[kind].at[core + 2 * m, down if upward[kind] else up],
                                  all_refs[kind].at[core + 2 * m, down if upward[kind] else up],
                                  to_up if upward[kind] else to_down, ("over", kind)) for kind in kinds} for m in range(half)]

    def share_over(m):
        for kind in kinds:
            block = all_refs[kind].at[core + 2 * m, over]
            links.arrive(over_state[m][kind], block, to_up if upward[kind] else to_down)
            over_state[m][kind, "mate"] = links.send(block, block, to_mate, ("over", kind))

    def have_over(m):
        for kind in kinds:
            links.arrive(over_state[m][kind, "mate"], all_refs[kind].at[1 - core + 2 * m, over], to_mate)

    def both_ways(src, dst, which):
        return {True: links.send(src, dst, to_up, which), False: links.send(src, dst, to_down, which)}

    def pass_halves(state, below, above, split, which):
        links.arrive(state[True], below, to_up)
        state["first"] = links.send(split(below, 0), split(below, 0), to_up, which)
        links.arrive(state[False], above, to_down)
        state["second"] = links.send(split(above, 1), split(above, 1), to_down, which)

    def have_halves(state, block, split):
        links.arrive(state["first"], split(block, 0), to_up)
        links.arrive(state["second"], split(block, 1), to_down)

    w13_state, w2_state = [None] * own, [None] * (PARTS + 1)
    split13 = lambda ref, k: ref.at[:, pl.ds(k * (part // 2), part // 2)]
    split2 = lambda ref, k: ref.at[:, pl.ds(k * (width // 2), width // 2)]

    def send13(e):
        w13_state[e] = both_ways(w13.at[e], w13_all.at[tp, e], "w13")

    def pass13(e):
        pass_halves(w13_state[e], w13_all.at[down, e], w13_all.at[up, e], split13, "w13")

    def have13(e):
        have_halves(w13_state[e], w13_all.at[over, e], split13)

    pieces = [(q, pl.ds(0, own)) for q in range(PARTS - 1)] + [(PARTS - 1, pl.ds(0, 2)), (PARTS - 1, pl.ds(2, own - 2))]

    def piece(j, p):
        q, experts = pieces[p]
        return w2_all.at[j, q, experts]

    def send2(p):
        q, experts = pieces[p]
        w2_state[p] = both_ways(w2s.at[experts, :, pl.ds(q * part, part)], piece(tp, p), "w2")

    def pass2(p):
        pass_halves(w2_state[p], piece(down, p), piece(up, p), split2, "w2")

    def have2(p):
        have_halves(w2_state[p], piece(over, p), split2)

    def grad_stores(e, slot):
        rows = pl.ds(0, PARTS)
        return [pltpu.make_async_copy(wide_buf.at[slot, rows, :, pl.ds(0, width)], g1.at[e], g_sem.at[slot, 0]),
                pltpu.make_async_copy(wide_buf.at[slot, rows, :, pl.ds(width, width)], g3.at[e], g_sem.at[slot, 1]),
                pltpu.make_async_copy(xs.at[slot, pl.ds(0, width)], g2.at[e], g_sem.at[slot, 2])]

    def write_grads(e):
        slot = lax.rem(e, 2)

        @pl.when(e >= 2)
        def _():
            for copy in grad_stores(e - 2, slot):
                copy.wait()

        for m in range(PARTS):
            wide_buf[slot, m] = acc13[e, :, m * part : (m + 1) * part].T.astype(BF16)
        xs[slot, pl.ds(0, width), :] = acc2[e].astype(BF16)
        for copy in grad_stores(e, slot):
            copy.start()

    def pair_loads(t, h, p):
        at = pl.ds(h * half + p * (half // 2), half // 2)
        return [pltpu.make_async_copy(src.at[at, t], dst.at[p], load_sem.at[k, p])
                for k, (src, dst) in enumerate(((x_all, xb), (dy_all, dyb), (r_all, rb)))]

    def half_group(t, h, keep, ahead, pairs=(0, 2), grads=True, write=False):
        def gather(p, b):
            pos, gate = expert_rows(rb[p, b], ep * own, own, earlier[...])
            masks = hit_masks(pos, cap)
            pick = one_hot(masks)
            gates = jnp.sum(slot_gates(masks, gate), axis=1, keepdims=True)
            rows = pl.ds(pl.multiple_of((p * (half // 2) + b) * cap, cap), cap)
            picked = dot(pick, xb[p, b]).astype(BF16)
            for e in range(own):
                xs[e, rows, :] = picked[e * cap : (e + 1) * cap]
            scaled = (gates * dot(pick, dyb[p, b])).astype(BF16)
            for e in range(own):
                us[e, rows, :] = scaled[e * cap : (e + 1) * cap]

        def pair(p, carry):
            for copy in pair_loads(t, h, p):
                copy.wait()
            for b in range(half // 2):
                gather(p, b)

            @pl.when(ahead)
            def _():
                for copy in pair_loads(t, 1, p):
                    copy.start()

            return carry

        if pairs[0] < pairs[1]:
            lax.fori_loop(pairs[0], pairs[1], pair, 0)
        if not grads:
            return

        stores = []
        if keep:
            stores = [pltpu.make_async_copy(xs, xs_all.at[:, h], slot_sem.at[0]),
                      pltpu.make_async_copy(us, us_all.at[:, h], slot_sem.at[1])]
        for copy in stores:
            copy.start()

        def expert(e, carry):
            ab = dot(xs[e], w13[e].reshape(model, 2 * width))
            a, b = ab[:, :width], ab[:, width:]
            dh = dot_tb(us[e], w2s[e])
            sig = jax.nn.sigmoid(a)
            silu = a * sig
            hid = (silu * b).astype(BF16)
            da = (dh * b * sig * (1.0 + a * (1.0 - sig))).astype(BF16)
            db = (dh * silu).astype(BF16)
            acc13[e] += dot_ta(jnp.concatenate([da, db], axis=1), xs[e])
            acc2[e] += dot_ta(hid, us[e])
            if write:
                write_grads(e)
            return carry

        lax.fori_loop(0, own, expert, 0)
        for copy in stores:
            copy.wait()

    def start_loads(t, h, pairs=(0, 1)):
        for p in pairs:
            for copy in pair_loads(t, h, p):
                copy.start()

    def compute(t, keep):
        start_loads(t, 0)

        def one_half(h, carry):
            half_group(t, h, keep, h == 0)
            return carry

        lax.fori_loop(0, 2, one_half, 0)

    slots = eps * cap
    pending = []

    def settle():
        while pending:
            pending.pop().wait()

    def hidden(e):
        rows = pltpu.make_async_copy(xs_all.at[e], xs.at[pl.ds(0, 2)], in_sem.at[tps])
        rows.start()
        for j in range(tps):
            pltpu.make_async_copy(w13_all.at[j, e], wide_buf.at[pl.ds(0, PARTS), j], in_sem.at[j]).start()
        settle()
        rows.wait()

        def shard(j, carry):
            pltpu.make_async_copy(w13_all.at[j, e], wide_buf.at[pl.ds(0, PARTS), j], in_sem.at[j]).wait()
            ab = dot(xs[0:2].reshape(slots, model), wide_buf[0:PARTS, j].reshape(model, 2 * width))
            ab_buf[j] = ab
            a, b = ab[:, :width], ab[:, width:]
            at = pl.ds(pl.multiple_of(lax.rem(j, 2) * width, width), width)
            d_all[e, j // 2, :, at] = (a * jax.nn.sigmoid(a) * b).astype(BF16)
            return carry

        lax.fori_loop(0, tps, shard, 0)
        pending.append(pltpu.make_async_copy(ab_buf, ab_all.at[e], ab_sem.at[0]))
        pending[-1].start()

    def put_rows(e, value):
        for k in range(eps):
            y_buf[k, e] = value[k * cap : (k + 1) * cap]

    def down_load(q, j):
        return pltpu.make_async_copy(w2_all.at[j, q], w2v.at[q, j], in_sem.at[j])

    def load_down(q):
        for j in (tp, up, down):
            down_load(q, j).start()

    def y_part(q):
        down_load(q, over).start()
        for j in range(tps):
            down_load(q, j).wait()

        def one(e, carry):
            y = dot(d_all[e, 0], w2v[q, 0:2, e].reshape(2 * width, part)) + dot(d_all[e, 1], w2v[q, 2:4, e].reshape(2 * width, part))
            put_rows(e, y.astype(BF16))
            return carry

        lax.fori_loop(0, own, one, 0)

    def ab_load(e, j):
        return pltpu.make_async_copy(ab_all.at[e, j], ab_buf.at[j], ab_sem.at[j])

    def u_load(e, slot):
        return pltpu.make_async_copy(us_all.at[e], us.at[pl.ds(2 * slot, 2)], slot_sem.at[slot])

    def hidden_grads():
        settle()
        u_load(0, 0).start()
        for j in range(tps):
            ab_load(0, j).start()

        def one(e, carry):
            slot = lax.rem(e, 2)
            u_load(e, slot).wait()

            @pl.when(e + 1 < own)
            def _():
                u_load(e + 1, 1 - slot).start()

            def two(k, carry):
                dh = None
                for q in range(PARTS):
                    at = pl.ds(q * part, part)
                    u = us[pl.ds(2 * slot, 2), :, at].reshape(slots, part)
                    term = dot_tb(u, w2v[q, pl.ds(2 * k, 2), e].reshape(2 * width, part))
                    dh = term if dh is None else dh + term
                for i in range(2):
                    j = 2 * k + i
                    ab_load(e, j).wait()
                    a, b, d = ab_buf[j, :, :width], ab_buf[j, :, width:], dh[:, i * width : (i + 1) * width]
                    sig = jax.nn.sigmoid(a)
                    d_all[e, j, :, :width] = (d * b * sig * (1.0 + a * (1.0 - sig))).astype(BF16)
                    d_all[e, j, :, width:] = (d * (a * sig)).astype(BF16)

                    @pl.when(e + 1 < own)
                    def _():
                        ab_load(e + 1, j).start()
                return carry

            lax.fori_loop(0, tps // 2, two, 0)
            return carry

        lax.fori_loop(0, own, one, 0)

    def v_load(q):
        return pltpu.make_async_copy(w13_all.at[:, :, q], wide_buf, in_sem.at[tps])

    def v_part(q):
        v_load(q).wait()

        def one(e, carry):
            v = dot_tb(d_all[e, 0], wide_buf[0, e])
            for j in range(1, tps):
                v = v + dot_tb(d_all[e, j], wide_buf[j, e])
            put_rows(e, v.astype(BF16))
            return carry

        lax.fori_loop(0, own, one, 0)
        if q + 1 < PARTS:
            v_load(q + 1).start()

    gifts, writes, stages = {}, {}, {}

    def combine(kind, block):
        masks = hit_masks(routes[block, 0:own], cap)
        rows = y_buf[block].reshape(own * cap, part)
        if kind == 1:
            return dot_ta(one_hot(masks), rows)
        hi, mid, low = three_parts(slot_gates(masks, routes[block, top : top + own]))
        return dot_ta(hi, rows) + (dot_ta(mid, rows) + dot_ta(low, rows))

    numbers, ready = {}, {}
    tok = far_sum.shape[0] // 2
    fold = part // 2
    buffers = [keep_sum.at[0], keep_sum.at[1], keep_sum.at[0], ab_buf, keep_sum.at[1], keep_sum.at[0]]
    earlier_user = {2: 0, 4: 1, 5: 2}
    assert ab_buf.shape == give.shape and len(buffers) == 2 * PARTS
    halves = (pl.ds(0, tok), pl.ds(tok, tok))

    def put_tile(ref, i, value):
        ref[i, 0:tok] = value[:, :fold]
        ref[i, tok : 2 * tok] = value[:, fold:]

    def sum_begin(kind, q):
        n = numbers[kind, q] = len(numbers)
        tiles = buffers[n]
        for k in gifts.get(n - 1, ()):
            links.finish(k)
        if n in earlier_user:
            for k in ready[earlier_user[n]]:
                links.finish(k)
            writes.pop(earlier_user[n]).wait()

        def to_other(i, carry):
            for k in range(2):
                put_tile(give, 2 * i + k, combine(kind, lax.rem(mate + 4 - 2 * (2 * i + k) + eps, eps)))
            return carry

        def to_own(i, carry):
            put_tile(tiles, i, combine(kind, lax.rem(ep + 4 - 2 * i + eps, eps)))
            return carry

        for i in range(2):
            to_other(i, 0)
            if n and not i:
                pl.semaphore_wait(free_sem, 1)
            pair = pl.ds(2 * i, 2)
            gifts.setdefault(n, []).append(links.send(give.at[pair], mate_sum.at[pair], to_mate))
        lax.fori_loop(0, 2, to_own, 0)
        second[n] = to_own

    second = {}

    def take_pair(n, i):
        pair = pl.ds(2 * i, 2)
        links.arrive(gifts[n][i], mate_sum.at[pair], to_mate)
        buffers[n][pair] += mate_sum[pair]

    def sum_far(kind, q):
        n = numbers[kind, q]
        tiles = buffers[n]
        take_pair(n, 0)
        stages[n] = [links.send(tiles.at[0, halves[h]], far_land.at[kind, q, halves[h]], to) for h, to in ((0, to_right), (1, to_left))]
        stages[n].append(links.send(tiles.at[1, halves[1]], last_land.at[kind, 0, q, halves[1]], to_right))
        lax.fori_loop(2, 4, second[n], 0)

    def free_mate():
        pl.semaphore_signal(free_sem, inc=1, device_id=to_mate, device_id_type=MESH)

    def sum_near(kind, q):
        n = numbers[kind, q]
        tiles = buffers[n]
        take_pair(n, 1)
        if n + 1 < 2 * PARTS:
            free_mate()
        stages[n].append(links.send(tiles.at[3, halves[0]], last_land.at[kind, 1, q, halves[0]], to_left))
        writes[n] = pltpu.make_async_copy(tiles.at[2], sums.at[kind, q], own_sem.at[n])
        writes[n].start()

    def sum_end(kind, q):
        sum_far(kind, q)
        sum_near(kind, q)

    def sum_turn(kind, q):
        n = numbers[kind, q]
        tiles = buffers[n]
        for h, to in ((0, to_right), (1, to_left)):
            links.arrive(stages[n][h], far_land.at[kind, q, halves[h]], to)
        load = pltpu.make_async_copy(far_land.at[kind, q], far_sum, sum_sem.at[2])
        load.start()
        load.wait()
        for i, h, side, to in ((1, 0, 0, to_right), (3, 1, 1, to_left)):
            tiles[i, halves[h]] += far_sum[halves[h]]
            stages[n].append(links.send(tiles.at[i, halves[h]], last_land.at[kind, side, q, halves[h]], to))
        ready[n] = tuple(stages[n])

    def sums_here(kind):
        for q in range(PARTS):
            sent = stages[numbers[kind, q]]
            for k, h, side, to in ((2, 1, 0, to_right), (3, 0, 1, to_left), (4, 0, 0, to_right), (5, 1, 1, to_left)):
                links.arrive(sent[k], last_land.at[kind, side, q, halves[h]], to)

    three = pl.ds(0, PARTS)
    out_loads = [pltpu.make_async_copy(sums.at[0], give.at[three], sum_sem.at[0]),
                 pltpu.make_async_copy(last_land.at[0, 0], mate_sum.at[three], sum_sem.at[1]),
                 pltpu.make_async_copy(last_land.at[0, 1], mate_sum.at[three], sum_sem.at[1])]
    out_store = pltpu.make_async_copy(xb.at[0, 0], out, sum_sem.at[0])

    def out_start():
        sums_here(0)
        for k in gifts[2 * PARTS - 1]:
            links.finish(k)
        out_loads[0].start()
        out_loads[1].start()

    def out_middle():
        out_loads[0].wait()
        out_loads[1].wait()
        give[three] += mate_sum[three]
        out_loads[2].start()

    def out_finish():
        out_loads[2].wait()
        for q in range(PARTS):
            for h in range(2):
                at = q * part + h * fold
                xb[0, 0, :, at : at + fold] = (give[q, halves[h]] + mate_sum[q, halves[h]]).astype(BF16)
        out_store.start()

    y_state = {}
    for way in (True, False):
        for kind in kinds:
            go_up = upward[kind] == way
            y_state[kind, go_up] = links.send(own_refs[kind], all_refs[kind].at[ep, tp], to_up if go_up else to_down, ("first", kind))
    groups = (tp, down, up)
    states = [spread(0, own_refs)]
    hold = [pltpu.make_async_copy(own_refs[kind], all_refs[kind].at[ep, tp], row_sem.at[kind]) for kind in range(3)]
    for copy in hold:
        copy.start()
    for copy in loads:
        copy.wait()
    stow = [pltpu.make_async_copy(w13, w13_all.at[tp], w_sem.at[0])]
    stow += [pltpu.make_async_copy(w2s.at[:, :, pl.ds(q * part, part)], w2_all.at[tp, q], w_sem.at[1 + q]) for q in range(PARTS)]
    for copy in stow:
        copy.start()
    with jax.named_scope("send13_0"):
        send13(0)
    with jax.named_scope("send13_1"):
        send13(1)
    with jax.named_scope("send13_2"):
        send13(2)
    earlier[...] = earlier_rows(earlier.shape[0])
    with jax.named_scope("zeros"):
        acc13[...] = jnp.zeros_like(acc13)
        acc2[...] = jnp.zeros_like(acc2)

    def y_arrive(kind, way):
        block = all_refs[kind].at[ep, down if way else up]
        links.arrive(y_state[kind, way], block, to_up if way else to_down)
        return block

    with jax.named_scope("pass_on_0"):
        pass_on(0)
    with jax.named_scope("y_arrive"):
        for way in (True, False):
            for kind in kinds:
                y_arrive(kind, way)
    states.append(spread(1, [ref.at[ep, down] for ref in all_refs]))
    with jax.named_scope("share_0"):
        share(0)
    with jax.named_scope("last_0"):
        last(0)
    for copy in hold + stow:
        copy.wait()
    with jax.named_scope("from_mate_0"):
        from_mate(0)
    route_copy = pltpu.make_async_copy(r_all.at[:, tp], routes, row_sem.at[0])
    route_copy.start()
    route_copy.wait()

    def tabulate(b, carry):
        pos, gate = expert_rows(routes[b], ep * own, own, earlier[...])
        routes[b, 0:own] = pos
        routes[b, top : top + own] = gate
        return carry

    lax.fori_loop(0, eps, tabulate, 0)
    for kind in kinds:
        links.finish_all(("first", kind), all_refs[kind].at[pl.ds(0, 5), tp], to_mate)
    with jax.named_scope("compute_tp_True"):
        compute(tp, True)
    with jax.named_scope("pass13_0"):
        pass13(0)
    with jax.named_scope("send13_3"):
        send13(3)
    with jax.named_scope("pass_on_1"):
        pass_on(1)
    states.append(spread(2, [ref.at[ep, up] for ref in all_refs]))
    with jax.named_scope("share_1"):
        share(1)
    with jax.named_scope("pass13_1"):
        pass13(1)
    with jax.named_scope("send13_4"):
        send13(4)
    with jax.named_scope("have13_0"):
        have13(0)
    with jax.named_scope("hidden_0"):
        hidden(0)
    with jax.named_scope("pass13_2"):
        pass13(2)
    with jax.named_scope("last_1"):
        last(1)
    with jax.named_scope("from_mate_1"):
        from_mate(1)
    with jax.named_scope("compute_down_False"):
        compute(down, False)
    with jax.named_scope("pass13_3"):
        pass13(3)
    with jax.named_scope("send2_0"):
        send2(0)
    with jax.named_scope("pass_on_2"):
        pass_on(2)
    with jax.named_scope("have13_1"):
        have13(1)
    with jax.named_scope("hidden_1"):
        hidden(1)
    with jax.named_scope("share_2"):
        share(2)
    with jax.named_scope("pass13_4"):
        pass13(4)
    with jax.named_scope("have13_2"):
        have13(2)
    with jax.named_scope("hidden_2"):
        hidden(2)
    with jax.named_scope("last_2"):
        last(2)
    with jax.named_scope("from_mate_2"):
        from_mate(2)
    with jax.named_scope("have13_3"):
        have13(3)
    with jax.named_scope("hidden_3"):
        hidden(3)
    with jax.named_scope("start_loads_up_0"):
        start_loads(up, 0)
    with jax.named_scope("gather_up_0"):
        half_group(up, 0, False, True, grads=False)
    with jax.named_scope("pass2_0"):
        pass2(0)
    with jax.named_scope("send2_1"):
        send2(1)
        send2(2)
    with jax.named_scope("grads_up_0"):
        half_group(up, 0, False, False, pairs=(2, 2))
    with jax.named_scope("half_group_up_1_False_False"):
        half_group(up, 1, False, False)
    with jax.named_scope("have13_4"):
        have13(4)
    with jax.named_scope("hidden_4"):
        hidden(4)

    with jax.named_scope("have2_0"):
        have2(0)
    load_down(0)
    with jax.named_scope("y_part_0"):
        y_part(0)
    with jax.named_scope("sum_begin_0_0"):
        sum_begin(0, 0)
    with jax.named_scope("sum_end_0_0"):
        sum_end(0, 0)
    v_load(0).start()
    with jax.named_scope("pass2_1"):
        pass2(1)
    with jax.named_scope("send2_3"):
        send2(3)
    with jax.named_scope("pass2_2"):
        pass2(2)
    with jax.named_scope("sum_turn_0_0"):
        sum_turn(0, 0)
    load_down(1)
    with jax.named_scope("have2_1"):
        have2(1)
    with jax.named_scope("y_part_1"):
        y_part(1)
    with jax.named_scope("sum_begin_0_1"):
        sum_begin(0, 1)
    with jax.named_scope("pass2_3"):
        pass2(3)
    over_state = send_over()
    with jax.named_scope("sum_end_0_1"):
        sum_end(0, 1)
    load_down(2)
    with jax.named_scope("have2_2"):
        have2(2)
        have2(3)
    with jax.named_scope("y_part_2"):
        y_part(2)
    with jax.named_scope("sum_turn_0_1"):
        sum_turn(0, 1)
    with jax.named_scope("sum_begin_0_2"):
        sum_begin(0, 2)
    with jax.named_scope("sum_end_0_2"):
        sum_end(0, 2)
    with jax.named_scope("hidden_grads"):
        hidden_grads()
    with jax.named_scope("sum_turn_0_2"):
        sum_turn(0, 2)
    with jax.named_scope("share_over_0"):
        share_over(0)
    with jax.named_scope("v_part_0"):
        v_part(0)
    with jax.named_scope("sum_begin_1_0"):
        sum_begin(1, 0)
    with jax.named_scope("sum_far_1_0"):
        sum_far(1, 0)
    with jax.named_scope("v_part_1"):
        v_part(1)
    with jax.named_scope("sum_near_1_0"):
        sum_near(1, 0)
    with jax.named_scope("sum_begin_1_1"):
        sum_begin(1, 1)
    with jax.named_scope("sum_far_1_1"):
        sum_far(1, 1)
    with jax.named_scope("share_over_1"):
        share_over(1)
    with jax.named_scope("v_part_2"):
        v_part(2)
    with jax.named_scope("sum_near_1_1"):
        sum_near(1, 1)
    with jax.named_scope("sum_begin_1_2"):
        sum_begin(1, 2)
    with jax.named_scope("sum_far_1_2"):
        sum_far(1, 2)
    with jax.named_scope("sum_turn_1_0"):
        sum_turn(1, 0)
    with jax.named_scope("have_over_0"):
        have_over(0)
    with jax.named_scope("have_over_1"):
        have_over(1)
    with jax.named_scope("start_loads_over_0"):
        start_loads(over, 0)
    with jax.named_scope("sum_near_1_2"):
        sum_near(1, 2)
    with jax.named_scope("out_start"):
        out_start()
    with jax.named_scope("half_group_over_0_False_False"):
        half_group(over, 0, False, False)
    with jax.named_scope("share_over_2"):
        share_over(2)
    with jax.named_scope("sum_turn_1_1"):
        sum_turn(1, 1)
    with jax.named_scope("out_middle"):
        out_middle()
    with jax.named_scope("sum_turn_1_2"):
        sum_turn(1, 2)
    with jax.named_scope("have_over_2"):
        have_over(2)
    with jax.named_scope("start_loads_over_1_0"):
        start_loads(over, 1, (0,))
    with jax.named_scope("half_group_over_1_False_False_0_1_False"):
        half_group(over, 1, False, False, (0, 1), False)
    with jax.named_scope("share_over_3"):
        share_over(3)
    with jax.named_scope("have_over_3"):
        have_over(3)
    with jax.named_scope("start_loads_over_1_1"):
        start_loads(over, 1, (1,))
    with jax.named_scope("half_group_over_1_False_False_1_2"):
        half_group(over, 1, False, False, (1, 2), write=True)

    with jax.named_scope("out_finish"):
        out_finish()
    with jax.named_scope("sums_here_1"):
        sums_here(1)
    out_store.wait()
    for e in range(max(own - 2, 0), own):
        for copy in grad_stores(e, e % 2):
            copy.wait()
    for n in sorted(writes):
        writes[n].wait()
    for kind in kinds:
        for g, count in ((0, half), (1, 3 + half), (2, 3 + half)):
            links.finish_all(("rows", kind, g), all_refs[kind].at[pl.ds(0, count), tp], to_mate)
        links.finish_all(("over", kind), all_refs[kind].at[pl.ds(0, 2 * half), tp], to_mate)
    links.finish_all("w13", w13_all.at[pl.ds(0, 3)], to_up)
    links.finish_all("w2", w2_all.at[pl.ds(0, 3)], to_up)
    with jax.named_scope("drain"):
        links.drain()


def layer(tokens, d_out, ids, gate_vals, w_one, w_three, w_two, ep_size, tp_size, cap):
    tok, model = tokens.shape
    own, width, _ = w_two.shape
    half = ep_size // 2
    rows = half * cap
    part = model // PARTS
    hbm = pl.BlockSpec(memory_space=pl.ANY)
    shape = jax.ShapeDtypeStruct
    routes = (2 * ids.shape[0], tok)
    sends, receives = copy_counts(own)
    slot_rows = ep_size * tp_size * cap * own
    vector = pltpu.VMEM
    dma = pltpu.SemaphoreType.DMA
    outs = pl.pallas_call(
        functools.partial(layer_kernel, own, cap, width),
        in_specs=[hbm] * 7,
        out_specs=[hbm] * 15,
        out_shape=[
            shape((ep_size, tp_size, tok, model), BF16),
            shape((ep_size, tp_size, tok, model), BF16),
            shape((ep_size, tp_size) + routes, F32),
            shape((tp_size, own, PARTS, part, 2 * width), BF16),
            shape((tp_size, PARTS, own, width, part), BF16),
            shape((own, 2, rows, model), BF16),
            shape((own, 2, rows, model), BF16),
            shape((own, tp_size, 2 * rows, 2 * width), F32),
            shape((2, PARTS, 2 * tok, part // 2), F32),
            shape((2, PARTS, 2 * tok, part // 2), F32),
            shape((2, 2, PARTS, 2 * tok, part // 2), F32),
            shape((tok, model), BF16),
            shape((own, PARTS, part, width), BF16),
            shape((own, PARTS, part, width), BF16),
            shape((own, width, model), BF16),
        ],
        scratch_shapes=[
            vector(routes, F32),
            vector(ids.shape, jnp.int32),
            vector((own, PARTS, part, 2 * width), BF16),
            vector((own, width, model), BF16),
            vector((2, half // 2, tok, model), BF16),
            vector((2, half // 2, tok, model), BF16),
            vector((2, half // 2) + routes, F32),
            vector((ep_size,) + routes, F32),
            vector((tok, tok), BF16),
            vector((own, rows, model), BF16),
            vector((own, rows, model), BF16),
            vector((own, 2 * width, model), F32),
            vector((own, width, model), F32),
            vector((tp_size, own, part, 2 * width), BF16),
            vector((PARTS, tp_size, own, width, part), BF16),
            vector((tp_size, 2 * rows, 2 * width), F32),
            vector((own, tp_size, 2 * rows, 2 * width), BF16),
            vector((ep_size, own, cap, part), BF16),
            vector((4, 2 * tok, part // 2), F32),
            vector((2, 4, 2 * tok, part // 2), F32),
            vector((4, 2 * tok, part // 2), F32),
            vector((2 * tok, part // 2), F32),
            dma((sends,)),
            dma((receives,)),
            dma((4,)),
            dma((3, 2)),
            dma((2 * PARTS + 1,)),
            dma((2,)),
            dma((1 + tp_size,)),
            dma((tp_size,)),
            dma((3,)),
            dma((2 * PARTS,)),
            dma((2, 3)),
            pltpu.SemaphoreType.REGULAR,
        ],
        compiler_params=pltpu.CompilerParams(vmem_limit_bytes=VMEM_LIMIT, collective_id=0, has_side_effects=True),
        cost_estimate=pl.CostEstimate(
            flops=2 * slot_rows * model * (2 * tok + 12 * width),
            bytes_accessed=4 * ep_size * tp_size * tok * model,
            transcendentals=0,
        ),
        name="layer",
    )(tokens, d_out, ids, gate_vals, w_one, w_three, w_two)
    g1, g3, g2 = outs[12:]
    return outs[8], outs[10], outs[11], (g1.reshape(own, model, width), g3.reshape(own, model, width), g2)


def result_kernel(sums, last_land, rows_in, g1, g3, g2, out, dx, o1, o3, o2, parts, rows, row_buf, b1, b3, b2, in_sem, out_sem):
    moves = ((g1, b1, o1), (g3, b3, o3), (g2, b2, o2), (rows_in, row_buf, out))
    takes = [pltpu.make_async_copy(src, buf, in_sem.at[k]) for k, (src, buf, _) in enumerate(moves)]
    terms = [pltpu.make_async_copy(src, parts.at[k], in_sem.at[4 + k])
             for k, src in enumerate((sums.at[1], last_land.at[1, 0], last_land.at[1, 1]))]
    for copy in terms + takes:
        copy.start()
    for copy in terms:
        copy.wait()
    tok, fold = rows.shape[0], parts.shape[3]
    for q in range(parts.shape[1]):
        for h in range(2):
            at, half = (2 * q + h) * fold, pl.ds(h * tok, tok)
            rows[:, at : at + fold] = (parts[0, q, half] + (parts[1, q, half] + parts[2, q, half])).astype(BF16)
    puts = [pltpu.make_async_copy(rows, dx, out_sem.at[4])]
    puts[0].start()
    for k, (take, (_, buf, to)) in enumerate(zip(takes, moves)):
        take.wait()
        puts.append(pltpu.make_async_copy(buf, to, out_sem.at[k]))
        puts[-1].start()
    for copy in puts:
        copy.wait()


def results(sums, last_land, out, grads):
    _, count, tall, fold = sums.shape
    tok, model = out.shape
    hbm = pl.BlockSpec(memory_space=pl.ANY)
    row = jax.ShapeDtypeStruct((tok, model), BF16)
    rows = pltpu.VMEM((tok, model), BF16)
    return pl.pallas_call(
        result_kernel,
        in_specs=[hbm] * 6,
        out_specs=[hbm] * 5,
        out_shape=[row, row] + [jax.ShapeDtypeStruct(g.shape, g.dtype) for g in grads],
        scratch_shapes=[pltpu.VMEM((3, count, tall, fold), F32), rows, rows]
        + [pltpu.VMEM(g.shape, g.dtype) for g in grads]
        + [pltpu.SemaphoreType.DMA((7,)), pltpu.SemaphoreType.DMA((5,))],
        compiler_params=pltpu.CompilerParams(vmem_limit_bytes=VMEM_LIMIT),
        name="results",
    )(sums, last_land, out, *grads)


def solution(mesh):
    ep_size, tp_size = mesh.shape["ep"], mesh.shape["tp"]
    row_spec = P(("dp", "ep", "tp"), None)
    col_spec = P("ep", None, "tp")
    down_spec = P("ep", "tp", None)
    grad_col = P(("dp", "ep"), None, "tp")
    grad_down = P(("dp", "ep"), "tp", None)

    def local_step(tokens, expert_ids, gate_vals, w_one, w_three, w_two, d_out):
        cap = slot_count(expert_ids.shape[1], tokens.shape[0], w_one.shape[0] * ep_size)
        sums, last_land, out, grads = layer(tokens, d_out, expert_ids.T, gate_vals.T, w_one, w_three, w_two, ep_size, tp_size, cap)
        return tuple(results(sums, last_land, out, grads))

    return jax.shard_map(local_step, mesh=mesh,
                         in_specs=(row_spec, row_spec, row_spec, col_spec, col_spec, down_spec, row_spec),
                         out_specs=(row_spec, row_spec, grad_col, grad_col, grad_down), check_vma=False)
```

```python
import functools

import jax
import jax.numpy as jnp
from jax import lax
from jax.experimental import pallas as pl
from jax.experimental.pallas import tpu as pltpu
from jax.sharding import PartitionSpec as P

BF16 = jnp.bfloat16
F32 = jnp.float32
MESH = pl.DeviceIdType.MESH
VMEM_LIMIT = 67_043_328
PARTS = 3


def slot_count(num_top, tok_dev, experts):
    return 8 * ((5 * num_top * tok_dev + 32 * experts - 1) // (32 * experts))


def dot(a, b):
    return jnp.dot(a, b, preferred_element_type=F32)


def dot_tb(a, b):
    return lax.dot_general(a, b, (((1,), (1,)), ((), ())), preferred_element_type=F32)


def dot_ta(a, b):
    return lax.dot_general(a, b, (((0,), (0,)), ((), ())), preferred_element_type=F32)


def earlier_rows(tok):
    row = lax.broadcasted_iota(jnp.int32, (tok, tok), 0)
    col = lax.broadcasted_iota(jnp.int32, (tok, tok), 1)
    return jnp.where(row < col, 1.0, 0.0).astype(BF16)


def expert_rows(routes, first, own, earlier):
    top = routes.shape[0] // 2
    ids, gates = routes[:top], routes[top:]
    hits = [ids == (first + e).astype(F32) for e in range(own)]
    routed = jnp.concatenate([jnp.sum(jnp.where(m, 1.0, 0.0), axis=0, keepdims=True) for m in hits], axis=0)
    gate = jnp.concatenate([jnp.sum(jnp.where(m, gates, 0.0), axis=0, keepdims=True) for m in hits], axis=0)
    return jnp.where(routed > 0.0, dot(routed.astype(BF16), earlier), -1.0), gate


def hit_masks(pos, cap):
    slot = lax.broadcasted_iota(jnp.int32, (cap, pos.shape[1]), 0).astype(F32)
    return [pos[e : e + 1, :] == slot for e in range(pos.shape[0])]


def one_hot(masks):
    return jnp.concatenate([jnp.where(m, 1.0, 0.0) for m in masks], axis=0).astype(BF16)


def slot_gates(masks, gate):
    return jnp.concatenate([jnp.where(m, gate[e : e + 1, :], 0.0) for e, m in enumerate(masks)], axis=0)


def three_parts(x):
    hi = x.astype(BF16)
    rest = x - hi.astype(F32)
    mid = rest.astype(BF16)
    return hi, mid, (rest - mid.astype(F32)).astype(BF16)


class Links:
    def __init__(self, send_sem, recv_sem):
        self.send_sem, self.recv_sem, self.sent, self.finished = send_sem, recv_sem, [], set()
        self.send_of, self.recv_of = {}, {}

    def copy(self, s, r, src, dst, to):
        return pltpu.make_async_remote_copy(src_ref=src, dst_ref=dst, send_sem=self.send_sem.at[s],
                                            recv_sem=self.recv_sem.at[r], device_id=to, device_id_type=MESH)

    def send(self, src, dst, to, together=None, landing=None):
        k = len(self.sent)
        s = self.send_of.setdefault(k if together is None else together, len(self.send_of))
        r = self.recv_of.setdefault(k if landing is None else landing, len(self.recv_of))
        copy = self.copy(s, r, src, dst, to)
        copy.start()
        self.sent.append((s, r, copy))
        if together is not None:
            self.finished.add(k)
        return k

    def arrive(self, k, dst, to):
        s, r, _ = self.sent[k]
        self.copy(s, r, dst, dst, to).wait_recv()

    def arrive_all(self, landing, ref, to):
        self.copy(0, self.recv_of[landing], ref, ref, to).wait_recv()

    def finish(self, k):
        self.finished.add(k)
        self.sent[k][2].wait_send()

    def finish_all(self, together, ref, to):
        self.copy(self.send_of[together], 0, ref, ref, to).wait_send()

    def drain(self):
        for k in range(len(self.sent)):
            if k not in self.finished:
                self.finish(k)


def copy_counts(own):
    sums = 2 * PARTS * 8
    return 3 * 5 + 2 + sums, 6 + 3 * 3 * 4 + 24 + 4 * own + 4 * (PARTS + 1) + sums


def layer_kernel(own, cap, width, tokens, d_out, ids, gate_vals, w1, w3, w2, x_all, dy_all, r_all, w13_all, w2_all, xs_all,
                 us_all, ab_all, sums, far_land, last_land, out, g1, g3, g2, r_own, i_own, w13, w2s, xb,
                 dyb, rb, routes, earlier, xs, us, acc13, acc2, wide_buf, w2v, ab_buf, d_all, y_buf, give, keep_sum, mate_sum,
                 far_sum, send_sem, recv_sem, row_sem, load_sem, w_sem, slot_sem, in_sem, ab_sem, sum_sem, own_sem, g_sem, free_sem):
    ep, tp = lax.axis_index("ep"), lax.axis_index("tp")
    eps, tps = x_all.shape[0], x_all.shape[1]
    model = x_all.shape[3]
    part = model // PARTS
    half = eps // 2
    x_own, dy_own = xs.at[0], xs.at[1]
    step = lambda n: lax.rem(ep + (n + eps), eps)
    turn = lambda n: lax.rem(tp + (n + tps), tps)
    right, left, far = step(2), step(-2), step(4)
    mate = ep + 1 - 2 * lax.rem(ep, 2)
    mate_step = lambda n: lax.rem(mate + (n + eps), eps)
    up, down, over = turn(1), turn(-1), turn(2)
    to_right, to_left, to_mate = {"ep": right}, {"ep": left}, {"ep": mate}
    to_up, to_down = {"tp": up}, {"tp": down}
    links = Links(send_sem, recv_sem)

    barrier = pltpu.get_barrier_semaphore()
    for to in (to_right, to_left, to_mate, to_up, to_down):
        pl.semaphore_signal(barrier, inc=1, device_id=to, device_id_type=MESH)
    top = ids.shape[0]
    firsts = [pltpu.make_async_copy(ids, i_own, row_sem.at[0]), pltpu.make_async_copy(gate_vals, r_own.at[pl.ds(top, top)], row_sem.at[1]),
              pltpu.make_async_copy(tokens, x_own, row_sem.at[2]), pltpu.make_async_copy(d_out, dy_own, row_sem.at[3])]
    loads = [pltpu.make_async_copy(src.at[:, pl.ds(m * part, part)], w13.at[:, m, :, pl.ds(k * width, width)], w_sem.at[PARTS * k + m])
             for k, src in ((0, w1), (1, w3)) for m in range(PARTS)]
    loads.append(pltpu.make_async_copy(w2, w2s, w_sem.at[2 * PARTS]))
    for copy in firsts + loads:
        copy.start()
    firsts[0].wait()
    r_own[0:top] = i_own[...].astype(F32)
    for copy in firsts[1:]:
        copy.wait()
    with jax.named_scope("barrier"):
        pl.semaphore_wait(barrier, 5)

    own_refs, all_refs = (x_own, dy_own, r_own), (x_all, dy_all, r_all)
    upward = (True, False, True)
    kinds = (0, 1, 2)

    def spread(g, srcs):
        out, t = {}, groups[g]
        set_of = lambda kind: ("rows", kind, g) if g else ("first", kind)
        for kind in kinds:
            to = to_right if upward[kind] else to_left
            out[kind, upward[kind]] = links.send(srcs[kind], all_refs[kind].at[ep, t], to, set_of(kind))
        for kind in kinds:
            to = to_left if upward[kind] else to_right
            out[kind, not upward[kind]] = links.send(srcs[kind], all_refs[kind].at[ep, t], to, set_of(kind))
        for kind in kinds:
            links.send(srcs[kind], all_refs[kind].at[ep, t], to_mate, set_of(kind), ("mate", kind, g))
        return out

    def pass_on(g):
        state, t = states[g], groups[g]
        for kind in kinds:
            got, to = (left, to_right) if upward[kind] else (right, to_left)
            block = all_refs[kind].at[got, t]
            links.arrive(state[kind, upward[kind]], block, to)
            state[kind, "far"] = links.send(block, block, to, ("rows", kind, g))
            links.send(block, block, to_mate, ("rows", kind, g), ("mate", kind, g))

    def share(g):
        state, t = states[g], groups[g]
        for kind in kinds:
            got, to = (right, to_left) if upward[kind] else (left, to_right)
            block = all_refs[kind].at[got, t]
            links.arrive(state[kind, not upward[kind]], block, to)
            links.send(block, block, to_mate, ("rows", kind, g), ("mate", kind, g))

    def last(g):
        state, t = states[g], groups[g]
        for kind in kinds:
            block = all_refs[kind].at[far, t]
            links.arrive(state[kind, "far"], block, to_right if upward[kind] else to_left)
            links.send(block, block, to_mate, ("rows", kind, g), ("mate", kind, g))

    def from_mate(g):
        for kind in kinds:
            links.arrive_all(("mate", kind, g), all_refs[kind].at[pl.ds(0, half), groups[g]], to_mate)

    core = lax.rem(ep, 2)

    def send_over():
        return [{kind: links.send(all_refs[kind].at[core + 2 * m, down if upward[kind] else up],
                                  all_refs[kind].at[core + 2 * m, down if upward[kind] else up],
                                  to_up if upward[kind] else to_down, ("over", kind)) for kind in kinds} for m in range(half)]

    def share_over(m):
        for kind in kinds:
            block = all_refs[kind].at[core + 2 * m, over]
            links.arrive(over_state[m][kind], block, to_up if upward[kind] else to_down)
            over_state[m][kind, "mate"] = links.send(block, block, to_mate, ("over", kind))

    def have_over(m):
        for kind in kinds:
            links.arrive(over_state[m][kind, "mate"], all_refs[kind].at[1 - core + 2 * m, over], to_mate)

    def both_ways(src, dst, which):
        return {True: links.send(src, dst, to_up, which), False: links.send(src, dst, to_down, which)}

    def pass_halves(state, below, above, split, which):
        links.arrive(state[True], below, to_up)
        state["first"] = links.send(split(below, 0), split(below, 0), to_up, which)
        links.arrive(state[False], above, to_down)
        state["second"] = links.send(split(above, 1), split(above, 1), to_down, which)

    def have_halves(state, block, split):
        links.arrive(state["first"], split(block, 0), to_up)
        links.arrive(state["second"], split(block, 1), to_down)

    w13_state, w2_state = [None] * own, [None] * (PARTS + 1)
    split13 = lambda ref, k: ref.at[:, pl.ds(k * (part // 2), part // 2)]
    split2 = lambda ref, k: ref.at[:, pl.ds(k * (width // 2), width // 2)]

    def send13(e):
        w13_state[e] = both_ways(w13.at[e], w13_all.at[tp, e], "w13")

    def pass13(e):
        pass_halves(w13_state[e], w13_all.at[down, e], w13_all.at[up, e], split13, "w13")

    def have13(e):
        have_halves(w13_state[e], w13_all.at[over, e], split13)

    pieces = [(q, pl.ds(0, own)) for q in range(PARTS - 1)] + [(PARTS - 1, pl.ds(0, 2)), (PARTS - 1, pl.ds(2, own - 2))]

    def piece(j, p):
        q, experts = pieces[p]
        return w2_all.at[j, q, experts]

    def send2(p):
        q, experts = pieces[p]
        w2_state[p] = both_ways(w2s.at[experts, :, pl.ds(q * part, part)], piece(tp, p), "w2")

    def pass2(p):
        pass_halves(w2_state[p], piece(down, p), piece(up, p), split2, "w2")

    def have2(p):
        have_halves(w2_state[p], piece(over, p), split2)

    def grad_stores(e, slot):
        rows = pl.ds(0, PARTS)
        return [pltpu.make_async_copy(wide_buf.at[slot, rows, :, pl.ds(0, width)], g1.at[e], g_sem.at[slot, 0]),
                pltpu.make_async_copy(wide_buf.at[slot, rows, :, pl.ds(width, width)], g3.at[e], g_sem.at[slot, 1]),
                pltpu.make_async_copy(xs.at[slot, pl.ds(0, width)], g2.at[e], g_sem.at[slot, 2])]

    def write_grads(e):
        slot = lax.rem(e, 2)

        @pl.when(e >= 2)
        def _():
            for copy in grad_stores(e - 2, slot):
                copy.wait()

        for m in range(PARTS):
            wide_buf[slot, m] = acc13[e, :, m * part : (m + 1) * part].T.astype(BF16)
        xs[slot, pl.ds(0, width), :] = acc2[e].astype(BF16)
        for copy in grad_stores(e, slot):
            copy.start()

    def pair_loads(t, h, p):
        at = pl.ds(h * half + p * (half // 2), half // 2)
        return [pltpu.make_async_copy(src.at[at, t], dst.at[p], load_sem.at[k, p])
                for k, (src, dst) in enumerate(((x_all, xb), (dy_all, dyb), (r_all, rb)))]

    def half_group(t, h, keep, ahead, pairs=(0, 2), grads=True, write=False):
        def gather(p, b):
            pos, gate = expert_rows(rb[p, b], ep * own, own, earlier[...])
            masks = hit_masks(pos, cap)
            pick = one_hot(masks)
            gates = jnp.sum(slot_gates(masks, gate), axis=1, keepdims=True)
            rows = pl.ds(pl.multiple_of((p * (half // 2) + b) * cap, cap), cap)
            picked = dot(pick, xb[p, b]).astype(BF16)
            for e in range(own):
                xs[e, rows, :] = picked[e * cap : (e + 1) * cap]
            scaled = (gates * dot(pick, dyb[p, b])).astype(BF16)
            for e in range(own):
                us[e, rows, :] = scaled[e * cap : (e + 1) * cap]

        def pair(p, carry):
            for copy in pair_loads(t, h, p):
                copy.wait()
            for b in range(half // 2):
                gather(p, b)

            @pl.when(ahead)
            def _():
                for copy in pair_loads(t, 1, p):
                    copy.start()

            return carry

        if pairs[0] < pairs[1]:
            lax.fori_loop(pairs[0], pairs[1], pair, 0)
        if not grads:
            return

        stores = []
        if keep:
            stores = [pltpu.make_async_copy(xs, xs_all.at[:, h], slot_sem.at[0]),
                      pltpu.make_async_copy(us, us_all.at[:, h], slot_sem.at[1])]
        for copy in stores:
            copy.start()

        def expert(e, carry):
            ab = dot(xs[e], w13[e].reshape(model, 2 * width))
            a, b = ab[:, :width], ab[:, width:]
            dh = dot_tb(us[e], w2s[e])
            sig = jax.nn.sigmoid(a)
            silu = a * sig
            hid = (silu * b).astype(BF16)
            da = (dh * b * sig * (1.0 + a * (1.0 - sig))).astype(BF16)
            db = (dh * silu).astype(BF16)
            acc13[e] += dot_ta(jnp.concatenate([da, db], axis=1), xs[e])
            acc2[e] += dot_ta(hid, us[e])
            if write:
                write_grads(e)
            return carry

        lax.fori_loop(0, own, expert, 0)
        for copy in stores:
            copy.wait()

    def start_loads(t, h, pairs=(0, 1)):
        for p in pairs:
            for copy in pair_loads(t, h, p):
                copy.start()

    def compute(t, keep):
        start_loads(t, 0)

        def one_half(h, carry):
            half_group(t, h, keep, h == 0)
            return carry

        lax.fori_loop(0, 2, one_half, 0)

    slots = eps * cap
    pending = []

    def settle():
        while pending:
            pending.pop().wait()

    def hidden(e):
        rows = pltpu.make_async_copy(xs_all.at[e], xs.at[pl.ds(0, 2)], in_sem.at[tps])
        rows.start()
        for j in range(tps):
            pltpu.make_async_copy(w13_all.at[j, e], wide_buf.at[pl.ds(0, PARTS), j], in_sem.at[j]).start()
        settle()
        rows.wait()

        def shard(j, carry):
            pltpu.make_async_copy(w13_all.at[j, e], wide_buf.at[pl.ds(0, PARTS), j], in_sem.at[j]).wait()
            ab = dot(xs[0:2].reshape(slots, model), wide_buf[0:PARTS, j].reshape(model, 2 * width))
            ab_buf[j] = ab
            a, b = ab[:, :width], ab[:, width:]
            at = pl.ds(pl.multiple_of(lax.rem(j, 2) * width, width), width)
            d_all[e, j // 2, :, at] = (a * jax.nn.sigmoid(a) * b).astype(BF16)
            return carry

        lax.fori_loop(0, tps, shard, 0)
        pending.append(pltpu.make_async_copy(ab_buf, ab_all.at[e], ab_sem.at[0]))
        pending[-1].start()

    def put_rows(e, value):
        for k in range(eps):
            y_buf[k, e] = value[k * cap : (k + 1) * cap]

    def down_load(q, j):
        return pltpu.make_async_copy(w2_all.at[j, q], w2v.at[q, j], in_sem.at[j])

    def load_down(q):
        for j in (tp, up, down):
            down_load(q, j).start()

    def y_part(q):
        down_load(q, over).start()
        for j in range(tps):
            down_load(q, j).wait()

        def one(e, carry):
            y = dot(d_all[e, 0], w2v[q, 0:2, e].reshape(2 * width, part)) + dot(d_all[e, 1], w2v[q, 2:4, e].reshape(2 * width, part))
            put_rows(e, y.astype(BF16))
            return carry

        lax.fori_loop(0, own, one, 0)

    def ab_load(e, j):
        return pltpu.make_async_copy(ab_all.at[e, j], ab_buf.at[j], ab_sem.at[j])

    def u_load(e, slot):
        return pltpu.make_async_copy(us_all.at[e], us.at[pl.ds(2 * slot, 2)], slot_sem.at[slot])

    def hidden_grads():
        settle()
        u_load(0, 0).start()
        for j in range(tps):
            ab_load(0, j).start()

        def one(e, carry):
            slot = lax.rem(e, 2)
            u_load(e, slot).wait()

            @pl.when(e + 1 < own)
            def _():
                u_load(e + 1, 1 - slot).start()

            def two(k, carry):
                dh = None
                for q in range(PARTS):
                    at = pl.ds(q * part, part)
                    u = us[pl.ds(2 * slot, 2), :, at].reshape(slots, part)
                    term = dot_tb(u, w2v[q, pl.ds(2 * k, 2), e].reshape(2 * width, part))
                    dh = term if dh is None else dh + term
                for i in range(2):
                    j = 2 * k + i
                    ab_load(e, j).wait()
                    a, b, d = ab_buf[j, :, :width], ab_buf[j, :, width:], dh[:, i * width : (i + 1) * width]
                    sig = jax.nn.sigmoid(a)
                    d_all[e, j, :, :width] = (d * b * sig * (1.0 + a * (1.0 - sig))).astype(BF16)
                    d_all[e, j, :, width:] = (d * (a * sig)).astype(BF16)

                    @pl.when(e + 1 < own)
                    def _():
                        ab_load(e + 1, j).start()
                return carry

            lax.fori_loop(0, tps // 2, two, 0)
            return carry

        lax.fori_loop(0, own, one, 0)

    def v_load(q):
        return pltpu.make_async_copy(w13_all.at[:, :, q], wide_buf, in_sem.at[tps])

    def v_part(q):
        v_load(q).wait()

        def one(e, carry):
            v = dot_tb(d_all[e, 0], wide_buf[0, e])
            for j in range(1, tps):
                v = v + dot_tb(d_all[e, j], wide_buf[j, e])
            put_rows(e, v.astype(BF16))
            return carry

        lax.fori_loop(0, own, one, 0)
        if q + 1 < PARTS:
            v_load(q + 1).start()

    gifts, writes, stages = {}, {}, {}

    def combine(kind, block):
        masks = hit_masks(routes[block, 0:own], cap)
        rows = y_buf[block].reshape(own * cap, part)
        if kind == 1:
            return dot_ta(one_hot(masks), rows)
        hi, mid, low = three_parts(slot_gates(masks, routes[block, top : top + own]))
        return dot_ta(hi, rows) + (dot_ta(mid, rows) + dot_ta(low, rows))

    numbers, ready = {}, {}
    tok = far_sum.shape[0] // 2
    fold = part // 2
    buffers = [keep_sum.at[0], keep_sum.at[1], keep_sum.at[0], ab_buf, keep_sum.at[1], keep_sum.at[0]]
    earlier_user = {2: 0, 4: 1, 5: 2}
    assert ab_buf.shape == give.shape and len(buffers) == 2 * PARTS
    halves = (pl.ds(0, tok), pl.ds(tok, tok))

    def put_tile(ref, i, value):
        ref[i, 0:tok] = value[:, :fold]
        ref[i, tok : 2 * tok] = value[:, fold:]

    def sum_begin(kind, q):
        n = numbers[kind, q] = len(numbers)
        tiles = buffers[n]
        for k in gifts.get(n - 1, ()):
            links.finish(k)
        if n in earlier_user:
            for k in ready[earlier_user[n]]:
                links.finish(k)
            writes.pop(earlier_user[n]).wait()

        def to_other(i, carry):
            for k in range(2):
                put_tile(give, 2 * i + k, combine(kind, lax.rem(mate + 4 - 2 * (2 * i + k) + eps, eps)))
            return carry

        def to_own(i, carry):
            put_tile(tiles, i, combine(kind, lax.rem(ep + 4 - 2 * i + eps, eps)))
            return carry

        for i in range(2):
            to_other(i, 0)
            if n and not i:
                pl.semaphore_wait(free_sem, 1)
            pair = pl.ds(2 * i, 2)
            gifts.setdefault(n, []).append(links.send(give.at[pair], mate_sum.at[pair], to_mate))
        lax.fori_loop(0, 2, to_own, 0)
        second[n] = to_own

    second = {}

    def take_pair(n, i):
        pair = pl.ds(2 * i, 2)
        links.arrive(gifts[n][i], mate_sum.at[pair], to_mate)
        buffers[n][pair] += mate_sum[pair]

    def sum_far(kind, q):
        n = numbers[kind, q]
        tiles = buffers[n]
        take_pair(n, 0)
        stages[n] = [links.send(tiles.at[0, halves[h]], far_land.at[kind, q, halves[h]], to) for h, to in ((0, to_right), (1, to_left))]
        stages[n].append(links.send(tiles.at[1, halves[1]], last_land.at[kind, 0, q, halves[1]], to_right))
        lax.fori_loop(2, 4, second[n], 0)

    def free_mate():
        pl.semaphore_signal(free_sem, inc=1, device_id=to_mate, device_id_type=MESH)

    def sum_near(kind, q):
        n = numbers[kind, q]
        tiles = buffers[n]
        take_pair(n, 1)
        if n + 1 < 2 * PARTS:
            free_mate()
        stages[n].append(links.send(tiles.at[3, halves[0]], last_land.at[kind, 1, q, halves[0]], to_left))
        writes[n] = pltpu.make_async_copy(tiles.at[2], sums.at[kind, q], own_sem.at[n])
        writes[n].start()

    def sum_end(kind, q):
        sum_far(kind, q)
        sum_near(kind, q)

    def sum_turn(kind, q):
        n = numbers[kind, q]
        tiles = buffers[n]
        for h, to in ((0, to_right), (1, to_left)):
            links.arrive(stages[n][h], far_land.at[kind, q, halves[h]], to)
        load = pltpu.make_async_copy(far_land.at[kind, q], far_sum, sum_sem.at[2])
        load.start()
        load.wait()
        for i, h, side, to in ((1, 0, 0, to_right), (3, 1, 1, to_left)):
            tiles[i, halves[h]] += far_sum[halves[h]]
            stages[n].append(links.send(tiles.at[i, halves[h]], last_land.at[kind, side, q, halves[h]], to))
        ready[n] = tuple(stages[n])

    def sums_here(kind):
        for q in range(PARTS):
            sent = stages[numbers[kind, q]]
            for k, h, side, to in ((2, 1, 0, to_right), (3, 0, 1, to_left), (4, 0, 0, to_right), (5, 1, 1, to_left)):
                links.arrive(sent[k], last_land.at[kind, side, q, halves[h]], to)

    three = pl.ds(0, PARTS)
    out_loads = [pltpu.make_async_copy(sums.at[0], give.at[three], sum_sem.at[0]),
                 pltpu.make_async_copy(last_land.at[0, 0], mate_sum.at[three], sum_sem.at[1]),
                 pltpu.make_async_copy(last_land.at[0, 1], mate_sum.at[three], sum_sem.at[1])]
    out_store = pltpu.make_async_copy(xb.at[0, 0], out, sum_sem.at[0])

    def out_start():
        sums_here(0)
        for k in gifts[2 * PARTS - 1]:
            links.finish(k)
        out_loads[0].start()
        out_loads[1].start()

    def out_middle():
        out_loads[0].wait()
        out_loads[1].wait()
        give[three] += mate_sum[three]
        out_loads[2].start()

    def out_finish():
        out_loads[2].wait()
        for q in range(PARTS):
            for h in range(2):
                at = q * part + h * fold
                xb[0, 0, :, at : at + fold] = (give[q, halves[h]] + mate_sum[q, halves[h]]).astype(BF16)
        out_store.start()

    y_state = {}
    for way in (True, False):
        for kind in kinds:
            go_up = upward[kind] == way
            y_state[kind, go_up] = links.send(own_refs[kind], all_refs[kind].at[ep, tp], to_up if go_up else to_down, ("first", kind))
    groups = (tp, down, up)
    states = [spread(0, own_refs)]
    hold = [pltpu.make_async_copy(own_refs[kind], all_refs[kind].at[ep, tp], row_sem.at[kind]) for kind in range(3)]
    for copy in hold:
        copy.start()
    for copy in loads:
        copy.wait()
    stow = [pltpu.make_async_copy(w13, w13_all.at[tp], w_sem.at[0])]
    stow += [pltpu.make_async_copy(w2s.at[:, :, pl.ds(q * part, part)], w2_all.at[tp, q], w_sem.at[1 + q]) for q in range(PARTS)]
    for copy in stow:
        copy.start()
    with jax.named_scope("send13_0"):
        send13(0)
    with jax.named_scope("send13_1"):
        send13(1)
    with jax.named_scope("send13_2"):
        send13(2)
    earlier[...] = earlier_rows(earlier.shape[0])
    with jax.named_scope("zeros"):
        acc13[...] = jnp.zeros_like(acc13)
        acc2[...] = jnp.zeros_like(acc2)

    def y_arrive(kind, way):
        block = all_refs[kind].at[ep, down if way else up]
        links.arrive(y_state[kind, way], block, to_up if way else to_down)
        return block

    with jax.named_scope("pass_on_0"):
        pass_on(0)
    with jax.named_scope("y_arrive"):
        for way in (True, False):
            for kind in kinds:
                y_arrive(kind, way)
    states.append(spread(1, [ref.at[ep, down] for ref in all_refs]))
    with jax.named_scope("share_0"):
        share(0)
    with jax.named_scope("last_0"):
        last(0)
    for copy in hold + stow:
        copy.wait()
    with jax.named_scope("from_mate_0"):
        from_mate(0)
    route_copy = pltpu.make_async_copy(r_all.at[:, tp], routes, row_sem.at[0])
    route_copy.start()
    route_copy.wait()

    def tabulate(b, carry):
        pos, gate = expert_rows(routes[b], ep * own, own, earlier[...])
        routes[b, 0:own] = pos
        routes[b, top : top + own] = gate
        return carry

    lax.fori_loop(0, eps, tabulate, 0)
    for kind in kinds:
        links.finish_all(("first", kind), all_refs[kind].at[pl.ds(0, 5), tp], to_mate)
    with jax.named_scope("compute_tp_True"):
        compute(tp, True)
    with jax.named_scope("pass13_0"):
        pass13(0)
    with jax.named_scope("send13_3"):
        send13(3)
    with jax.named_scope("pass_on_1"):
        pass_on(1)
    states.append(spread(2, [ref.at[ep, up] for ref in all_refs]))
    with jax.named_scope("share_1"):
        share(1)
    with jax.named_scope("pass13_1"):
        pass13(1)
    with jax.named_scope("send13_4"):
        send13(4)
    with jax.named_scope("have13_0"):
        have13(0)
    with jax.named_scope("hidden_0"):
        hidden(0)
    with jax.named_scope("pass13_2"):
        pass13(2)
    with jax.named_scope("last_1"):
        last(1)
    with jax.named_scope("from_mate_1"):
        from_mate(1)
    with jax.named_scope("compute_down_False"):
        compute(down, False)
    with jax.named_scope("pass13_3"):
        pass13(3)
    with jax.named_scope("send2_0"):
        send2(0)
    with jax.named_scope("pass_on_2"):
        pass_on(2)
    with jax.named_scope("have13_1"):
        have13(1)
    with jax.named_scope("hidden_1"):
        hidden(1)
    with jax.named_scope("share_2"):
        share(2)
    with jax.named_scope("pass13_4"):
        pass13(4)
    with jax.named_scope("have13_2"):
        have13(2)
    with jax.named_scope("hidden_2"):
        hidden(2)
    with jax.named_scope("last_2"):
        last(2)
    with jax.named_scope("from_mate_2"):
        from_mate(2)
    with jax.named_scope("have13_3"):
        have13(3)
    with jax.named_scope("hidden_3"):
        hidden(3)
    with jax.named_scope("start_loads_up_0"):
        start_loads(up, 0)
    with jax.named_scope("gather_up_0"):
        half_group(up, 0, False, True, grads=False)
    with jax.named_scope("pass2_0"):
        pass2(0)
    with jax.named_scope("send2_1"):
        send2(1)
        send2(2)
    with jax.named_scope("grads_up_0"):
        half_group(up, 0, False, False, pairs=(2, 2))
    with jax.named_scope("half_group_up_1_False_False"):
        half_group(up, 1, False, False)
    with jax.named_scope("have13_4"):
        have13(4)
    with jax.named_scope("hidden_4"):
        hidden(4)

    with jax.named_scope("have2_0"):
        have2(0)
    load_down(0)
    v_load(0).start()
    with jax.named_scope("y_part_0"):
        y_part(0)
    with jax.named_scope("sum_begin_0_0"):
        sum_begin(0, 0)
    with jax.named_scope("sum_end_0_0"):
        sum_end(0, 0)
    with jax.named_scope("pass2_1"):
        pass2(1)
    with jax.named_scope("send2_3"):
        send2(3)
    with jax.named_scope("pass2_2"):
        pass2(2)
    with jax.named_scope("sum_turn_0_0"):
        sum_turn(0, 0)
    load_down(1)
    with jax.named_scope("have2_1"):
        have2(1)
    with jax.named_scope("y_part_1"):
        y_part(1)
    with jax.named_scope("sum_begin_0_1"):
        sum_begin(0, 1)
    with jax.named_scope("pass2_3"):
        pass2(3)
    over_state = send_over()
    with jax.named_scope("sum_end_0_1"):
        sum_end(0, 1)
    load_down(2)
    with jax.named_scope("have2_2"):
        have2(2)
        have2(3)
    with jax.named_scope("y_part_2"):
        y_part(2)
    with jax.named_scope("sum_turn_0_1"):
        sum_turn(0, 1)
    with jax.named_scope("sum_begin_0_2"):
        sum_begin(0, 2)
    with jax.named_scope("sum_end_0_2"):
        sum_end(0, 2)
    with jax.named_scope("hidden_grads"):
        hidden_grads()
    with jax.named_scope("sum_turn_0_2"):
        sum_turn(0, 2)
    with jax.named_scope("share_over_0"):
        share_over(0)
    with jax.named_scope("v_part_0"):
        v_part(0)
    with jax.named_scope("sum_begin_1_0"):
        sum_begin(1, 0)
    with jax.named_scope("sum_far_1_0"):
        sum_far(1, 0)
    with jax.named_scope("v_part_1"):
        v_part(1)
    with jax.named_scope("sum_near_1_0"):
        sum_near(1, 0)
    with jax.named_scope("sum_begin_1_1"):
        sum_begin(1, 1)
    with jax.named_scope("sum_far_1_1"):
        sum_far(1, 1)
    with jax.named_scope("share_over_1"):
        share_over(1)
    with jax.named_scope("v_part_2"):
        v_part(2)
    with jax.named_scope("sum_near_1_1"):
        sum_near(1, 1)
    with jax.named_scope("sum_begin_1_2"):
        sum_begin(1, 2)
    with jax.named_scope("sum_far_1_2"):
        sum_far(1, 2)
    with jax.named_scope("sum_turn_1_0"):
        sum_turn(1, 0)
    with jax.named_scope("have_over_0"):
        have_over(0)
    with jax.named_scope("have_over_1"):
        have_over(1)
    with jax.named_scope("start_loads_over_0"):
        start_loads(over, 0)
    with jax.named_scope("sum_near_1_2"):
        sum_near(1, 2)
    with jax.named_scope("out_start"):
        out_start()
    with jax.named_scope("half_group_over_0_False_False"):
        half_group(over, 0, False, False)
    with jax.named_scope("share_over_2"):
        share_over(2)
    with jax.named_scope("sum_turn_1_1"):
        sum_turn(1, 1)
    with jax.named_scope("out_middle"):
        out_middle()
    with jax.named_scope("sum_turn_1_2"):
        sum_turn(1, 2)
    with jax.named_scope("have_over_2"):
        have_over(2)
    with jax.named_scope("start_loads_over_1_0"):
        start_loads(over, 1, (0,))
    with jax.named_scope("half_group_over_1_False_False_0_1_False"):
        half_group(over, 1, False, False, (0, 1), False)
    with jax.named_scope("share_over_3"):
        share_over(3)
    with jax.named_scope("have_over_3"):
        have_over(3)
    with jax.named_scope("start_loads_over_1_1"):
        start_loads(over, 1, (1,))
    with jax.named_scope("half_group_over_1_False_False_1_2"):
        half_group(over, 1, False, False, (1, 2), write=True)

    with jax.named_scope("out_finish"):
        out_finish()
    with jax.named_scope("sums_here_1"):
        sums_here(1)
    out_store.wait()
    for e in range(max(own - 2, 0), own):
        for copy in grad_stores(e, e % 2):
            copy.wait()
    for n in sorted(writes):
        writes[n].wait()
    for kind in kinds:
        for g, count in ((0, half), (1, 3 + half), (2, 3 + half)):
            links.finish_all(("rows", kind, g), all_refs[kind].at[pl.ds(0, count), tp], to_mate)
        links.finish_all(("over", kind), all_refs[kind].at[pl.ds(0, 2 * half), tp], to_mate)
    links.finish_all("w13", w13_all.at[pl.ds(0, 3)], to_up)
    links.finish_all("w2", w2_all.at[pl.ds(0, 3)], to_up)
    with jax.named_scope("drain"):
        links.drain()


def layer(tokens, d_out, ids, gate_vals, w_one, w_three, w_two, ep_size, tp_size, cap):
    tok, model = tokens.shape
    own, width, _ = w_two.shape
    half = ep_size // 2
    rows = half * cap
    part = model // PARTS
    hbm = pl.BlockSpec(memory_space=pl.ANY)
    shape = jax.ShapeDtypeStruct
    routes = (2 * ids.shape[0], tok)
    sends, receives = copy_counts(own)
    slot_rows = ep_size * tp_size * cap * own
    vector = pltpu.VMEM
    dma = pltpu.SemaphoreType.DMA
    outs = pl.pallas_call(
        functools.partial(layer_kernel, own, cap, width),
        in_specs=[hbm] * 7,
        out_specs=[hbm] * 15,
        out_shape=[
            shape((ep_size, tp_size, tok, model), BF16),
            shape((ep_size, tp_size, tok, model), BF16),
            shape((ep_size, tp_size) + routes, F32),
            shape((tp_size, own, PARTS, part, 2 * width), BF16),
            shape((tp_size, PARTS, own, width, part), BF16),
            shape((own, 2, rows, model), BF16),
            shape((own, 2, rows, model), BF16),
            shape((own, tp_size, 2 * rows, 2 * width), F32),
            shape((2, PARTS, 2 * tok, part // 2), F32),
            shape((2, PARTS, 2 * tok, part // 2), F32),
            shape((2, 2, PARTS, 2 * tok, part // 2), F32),
            shape((tok, model), BF16),
            shape((own, PARTS, part, width), BF16),
            shape((own, PARTS, part, width), BF16),
            shape((own, width, model), BF16),
        ],
        scratch_shapes=[
            vector(routes, F32),
            vector(ids.shape, jnp.int32),
            vector((own, PARTS, part, 2 * width), BF16),
            vector((own, width, model), BF16),
            vector((2, half // 2, tok, model), BF16),
            vector((2, half // 2, tok, model), BF16),
            vector((2, half // 2) + routes, F32),
            vector((ep_size,) + routes, F32),
            vector((tok, tok), BF16),
            vector((own, rows, model), BF16),
            vector((own, rows, model), BF16),
            vector((own, 2 * width, model), F32),
            vector((own, width, model), F32),
            vector((tp_size, own, part, 2 * width), BF16),
            vector((PARTS, tp_size, own, width, part), BF16),
            vector((tp_size, 2 * rows, 2 * width), F32),
            vector((own, tp_size, 2 * rows, 2 * width), BF16),
            vector((ep_size, own, cap, part), BF16),
            vector((4, 2 * tok, part // 2), F32),
            vector((2, 4, 2 * tok, part // 2), F32),
            vector((4, 2 * tok, part // 2), F32),
            vector((2 * tok, part // 2), F32),
            dma((sends,)),
            dma((receives,)),
            dma((4,)),
            dma((3, 2)),
            dma((2 * PARTS + 1,)),
            dma((2,)),
            dma((1 + tp_size,)),
            dma((tp_size,)),
            dma((3,)),
            dma((2 * PARTS,)),
            dma((2, 3)),
            pltpu.SemaphoreType.REGULAR,
        ],
        compiler_params=pltpu.CompilerParams(vmem_limit_bytes=VMEM_LIMIT, collective_id=0, has_side_effects=True),
        cost_estimate=pl.CostEstimate(
            flops=2 * slot_rows * model * (2 * tok + 12 * width),
            bytes_accessed=4 * ep_size * tp_size * tok * model,
            transcendentals=0,
        ),
        name="layer",
    )(tokens, d_out, ids, gate_vals, w_one, w_three, w_two)
    g1, g3, g2 = outs[12:]
    return outs[8], outs[10], outs[11], (g1.reshape(own, model, width), g3.reshape(own, model, width), g2)


def result_kernel(sums, last_land, rows_in, g1, g3, g2, out, dx, o1, o3, o2, parts, rows, row_buf, b1, b3, b2, in_sem, out_sem):
    moves = ((g1, b1, o1), (g3, b3, o3), (g2, b2, o2), (rows_in, row_buf, out))
    takes = [pltpu.make_async_copy(src, buf, in_sem.at[k]) for k, (src, buf, _) in enumerate(moves)]
    terms = [pltpu.make_async_copy(src, parts.at[k], in_sem.at[4 + k])
             for k, src in enumerate((sums.at[1], last_land.at[1, 0], last_land.at[1, 1]))]
    for copy in terms + takes:
        copy.start()
    for copy in terms:
        copy.wait()
    tok, fold = rows.shape[0], parts.shape[3]
    for q in range(parts.shape[1]):
        for h in range(2):
            at, half = (2 * q + h) * fold, pl.ds(h * tok, tok)
            rows[:, at : at + fold] = (parts[0, q, half] + (parts[1, q, half] + parts[2, q, half])).astype(BF16)
    puts = [pltpu.make_async_copy(rows, dx, out_sem.at[4])]
    puts[0].start()
    for k, (take, (_, buf, to)) in enumerate(zip(takes, moves)):
        take.wait()
        puts.append(pltpu.make_async_copy(buf, to, out_sem.at[k]))
        puts[-1].start()
    for copy in puts:
        copy.wait()


def results(sums, last_land, out, grads):
    _, count, tall, fold = sums.shape
    tok, model = out.shape
    hbm = pl.BlockSpec(memory_space=pl.ANY)
    row = jax.ShapeDtypeStruct((tok, model), BF16)
    rows = pltpu.VMEM((tok, model), BF16)
    return pl.pallas_call(
        result_kernel,
        in_specs=[hbm] * 6,
        out_specs=[hbm] * 5,
        out_shape=[row, row] + [jax.ShapeDtypeStruct(g.shape, g.dtype) for g in grads],
        scratch_shapes=[pltpu.VMEM((3, count, tall, fold), F32), rows, rows]
        + [pltpu.VMEM(g.shape, g.dtype) for g in grads]
        + [pltpu.SemaphoreType.DMA((7,)), pltpu.SemaphoreType.DMA((5,))],
        compiler_params=pltpu.CompilerParams(vmem_limit_bytes=VMEM_LIMIT),
        name="results",
    )(sums, last_land, out, *grads)


def solution(mesh):
    ep_size, tp_size = mesh.shape["ep"], mesh.shape["tp"]
    row_spec = P(("dp", "ep", "tp"), None)
    col_spec = P("ep", None, "tp")
    down_spec = P("ep", "tp", None)
    grad_col = P(("dp", "ep"), None, "tp")
    grad_down = P(("dp", "ep"), "tp", None)

    def local_step(tokens, expert_ids, gate_vals, w_one, w_three, w_two, d_out):
        cap = slot_count(expert_ids.shape[1], tokens.shape[0], w_one.shape[0] * ep_size)
        sums, last_land, out, grads = layer(tokens, d_out, expert_ids.T, gate_vals.T, w_one, w_three, w_two, ep_size, tp_size, cap)
        return tuple(results(sums, last_land, out, grads))

    return jax.shard_map(local_step, mesh=mesh,
                         in_specs=(row_spec, row_spec, row_spec, col_spec, col_spec, down_spec, row_spec),
                         out_specs=(row_spec, row_spec, grad_col, grad_col, grad_down), check_vma=False)
```
